32 devices in a mesh: dp: 8 (over z, y), tensor: 4 (over x, core).
Axes of the slice: x: 2, y: 2, z: 4, core: 2. Of those that a mesh axis runs over, the one named last changes fastest.
Arguments:
- block_input: float32 [2, 4096, 2048], P(None, ('dp', 'tensor')), may hold values from -6 to 6
- cotangent: float32 [2, 4096, 2048], P(None, ('dp', 'tensor')), may hold values from -6 to 6
- first_gain: bfloat16 [2048], P('dp'), may hold values from 0.5 to 1.5
- second_gain: bfloat16 [2048], P('dp'), may hold values from 0.5 to 1.5
- query_weight: bfloat16 [2048, 2048], P('dp', 'tensor'), may hold values from -0.125 to 0.125
- key_weight: bfloat16 [2048, 2048], P('dp', 'tensor'), may hold values from -0.125 to 0.125
- value_weight: bfloat16 [2048, 3456], P('dp', 'tensor'), may hold values from -0.125 to 0.125
- swish_weight: bfloat16 [2048, 3456], P('dp', 'tensor'), may hold values from -0.125 to 0.125
- output_weight: bfloat16 [3456, 2048], P('tensor', 'dp'), may hold values from -0.109375 to 0.109375
- up_projection_matrix: bfloat16 [2048, 3456], P('dp', 'tensor'), may hold values from -0.125 to 0.125
- gelu_weight: bfloat16 [2048, 3456], P('dp', 'tensor'), may hold values from -0.125 to 0.125
- down_weight: bfloat16 [3456, 2048], P('tensor', 'dp'), may hold values from -0.109375 to 0.109375
Outputs:
- block_output: float32 [2, 4096, 2048], P(None, ('dp', 'tensor'))
- grad_input: float32 [2, 4096, 2048], P(None, ('dp', 'tensor'))
- grad_first: float32 [2048], P('dp')
- grad_second: float32 [2048], P('dp')
- grad_query: float32 [2048, 2048], P('dp', 'tensor')
- grad_key: float32 [2048, 2048], P('dp', 'tensor')
- grad_value: float32 [2048, 3456], P('dp', 'tensor')
- grad_swish: float32 [2048, 3456], P('dp', 'tensor')
- grad_out: float32 [3456, 2048], P('tensor', 'dp')
- grad_up: float32 [2048, 3456], P('dp', 'tensor')
- grad_gelu: float32 [2048, 3456], P('dp', 'tensor')
- grad_down: float32 [3456, 2048], P('tensor', 'dp')
The draws below stay inside these ranges and needn't reach their ends.
All inputs are finite; a program needn't handle non-finite values.
Results may differ from the reference program's by a relative error of at most 0.014.
Values may be sent and summed in bfloat16 or wider, within the bound.
A program may use at most 256 MiB of HBM per device.

```python
import math
import jax
import jax.numpy as jnp
from jax import lax

D = 2048
HEADS = 8
HK = 256
HV = 432
FF = 3456
LEN = 512
MICRO = 2
ROWS_MB = 4096


def strengthened(array, key, source, target, parts, factor):
    def block_of(dim):
        return (jnp.arange(array.shape[dim]) // (array.shape[dim] // parts)).reshape((-1,) + (1,) * (array.ndim - 1 - dim))

    one_side = jax.random.permutation(key, parts)[block_of(target)]
    far = (block_of(target) + parts // 2) % parts
    return jnp.where((block_of(source) == one_side) | (block_of(source) == far), factor * array, array)


def steps_of(key, shape, cuts, smallest, largest):
    loudness = 1.0
    for axis_at, parts in cuts:
        draws = jax.random.uniform(jax.random.fold_in(jax.random.fold_in(key, 6), axis_at), (parts,), jnp.float32, smallest / len(cuts), largest / len(cuts))
        loudness = loudness * jnp.repeat(jnp.exp(draws), shape[axis_at] // parts).reshape((-1,) + (1,) * (len(shape) - 1 - axis_at))
    return loudness


def gaussian(key, shape, spread, bound, shards=(), kind=jnp.bfloat16):
    entries = spread * jax.random.normal(key, shape, jnp.float32)
    if shards:
        entries = entries * steps_of(key, shape, shards, -0.22, 0.18)
    return jnp.clip(entries, -bound, bound).astype(kind)


def noise_with(rng, extent, deviation, reach, shards, heavy, held_as=jnp.bfloat16):
    result = deviation * jax.random.normal(rng, extent, jnp.float32)
    if shards:
        result = result * steps_of(rng, extent, shards, -0.22, 0.18)
    return jnp.clip(strengthened(result, jax.random.fold_in(rng, 3), *heavy), -reach, reach).astype(held_as)


def setup_inputs(seed: int = 0) -> dict:
    key_list = jax.random.split(jax.random.key(seed), 13)
    return {
        "block_input": noise_with(key_list[0], (MICRO, ROWS_MB, D), 1.0, 6.0, ((1, 32),), (1, 2, 32, 2.75), jnp.float32),
        "cotangent": noise_with(key_list[1], (MICRO, ROWS_MB, D), 1.0, 6.0, ((1, 32),), (1, 2, 32, 2.75), jnp.float32),
        "first_gain": jnp.clip(1.0 + 0.1 * jax.random.normal(key_list[2], (D,), jnp.float32), 0.5, 1.5).astype(jnp.bfloat16),
        "second_gain": jnp.clip(1.0 + 0.1 * jax.random.normal(key_list[3], (D,), jnp.float32), 0.5, 1.5).astype(jnp.bfloat16),
        "query_weight": gaussian(key_list[4], (D, HEADS * HK), D ** -0.5, 0.125, ((0, 8), (1, 4))),
        "key_weight": gaussian(key_list[5], (D, HEADS * HK), D ** -0.5, 0.125, ((0, 8), (1, 4))),
        "value_weight": gaussian(key_list[6], (D, HEADS * HV), D ** -0.5, 0.125, ((0, 8), (1, 4))),
        "swish_weight": gaussian(key_list[7], (D, HEADS * HV), D ** -0.5, 0.125, ((0, 8), (1, 4))),
        "output_weight": gaussian(key_list[8], (HEADS * HV, D), (HEADS * HV) ** -0.5, 0.109375, ((0, 4), (1, 8))),
        "up_projection_matrix": gaussian(key_list[9], (D, FF), D ** -0.5, 0.125, ((0, 8), (1, 4))),
        "gelu_weight": gaussian(key_list[10], (D, FF), D ** -0.5, 0.125, ((0, 8), (1, 4))),
        "down_weight": gaussian(key_list[11], (FF, D), FF ** -0.5, 0.109375, ((0, 4), (1, 8))),
    }


EPS = 1e-05
GROUP_EPS = 1.0

def normalize(row_block, gain_vec):
    row_scale = lax.rsqrt(lax.optimization_barrier(jnp.mean(row_block * row_block, axis=-1, keepdims=True)) + EPS)
    return (row_block * row_scale * gain_vec.astype(jnp.float32), row_scale)

def norm_back(grad_rows, row_block, row_scale, gain_vec):
    scaled_grad = grad_rows * gain_vec.astype(jnp.float32)
    back_rows = row_scale * (scaled_grad - row_block * row_scale * row_scale * lax.optimization_barrier(jnp.mean(scaled_grad * row_block, axis=-1, keepdims=True)))
    return (back_rows, lax.optimization_barrier(jnp.sum(grad_rows * row_block * row_scale, axis=0)))

def angles(length, feature_width):
    half_width = feature_width // 2
    frequency = jnp.exp(-math.log(10000.0) * jnp.arange(half_width, dtype=jnp.float32) / half_width)
    turns = jnp.arange(length, dtype=jnp.float32)[:, None] * frequency[None, :]
    return (jnp.cos(turns)[:, None, :], jnp.sin(turns)[:, None, :])

def decays(length, head_ids):
    places = jnp.arange(length, dtype=jnp.float32)
    spacing = places[:, None] - places[None, :]
    log_rate = jnp.log(1.0 - jnp.exp2(-5.0 - head_ids))
    return jnp.where(spacing[None] >= 0.0, jnp.exp(jnp.maximum(spacing, 0.0)[None] * log_rate[:, None, None]), 0.0)

def rotate(value_vectors, cosine_table, sine_table):
    half_width = value_vectors.shape[-1] // 2
    lower = value_vectors[..., :half_width]
    upper = value_vectors[..., half_width:]
    return jnp.concatenate([lower * cosine_table - upper * sine_table, upper * cosine_table + lower * sine_table], axis=-1)

def unrotate(value_vectors, cosine_table, sine_table):
    half_width = value_vectors.shape[-1] // 2
    lower = value_vectors[..., :half_width]
    upper = value_vectors[..., half_width:]
    return jnp.concatenate([lower * cosine_table + upper * sine_table, upper * cosine_table - lower * sine_table], axis=-1)

def gelu_parts(pre_act):
    normal_cdf = 0.5 * (1.0 + lax.erf(pre_act * (1.0 / math.sqrt(2.0))))
    density = jnp.exp(-0.5 * pre_act * pre_act) * (1.0 / math.sqrt(2.0 * math.pi))
    return (pre_act * normal_cdf, normal_cdf + pre_act * density)

def inner_rows(left_rows, right_rows):
    return lax.dot_general(left_rows, right_rows, (((0,), (0,)), ((), ())), preferred_element_type=jnp.float32)

def times_t(left_rows, right_rows):
    return lax.dot_general(left_rows, right_rows, (((1,), (1,)), ((), ())), preferred_element_type=jnp.float32)

def one_sequence(weights, rows_in, cot_in, cosine_table, sine_table, decay_mask):
    first_gain, second_gain, query_weight, key_weight, value_weight, swish_weight, output_weight, up_projection_matrix, gelu_weight, down_weight = weights
    length = rows_in.shape[0]
    scale_qk = 1.0 / math.sqrt(HK)
    normed, first_scale = normalize(rows_in, first_gain)
    normed_bf = normed.astype(jnp.bfloat16)
    query_turned_rows = rotate(jnp.dot(normed_bf, query_weight, preferred_element_type=jnp.float32).reshape(length, HEADS, HK), cosine_table, sine_table).astype(jnp.bfloat16)
    key_turned_rows = rotate(jnp.dot(normed_bf, key_weight, preferred_element_type=jnp.float32).reshape(length, HEADS, HK), cosine_table, sine_table).astype(jnp.bfloat16)
    value_rows = jnp.dot(normed_bf, value_weight, preferred_element_type=jnp.float32).astype(jnp.bfloat16).reshape(length, HEADS, HV)
    gate_pre = jnp.dot(normed_bf, swish_weight, preferred_element_type=jnp.float32)
    unscaled_logits = jnp.einsum('koy,roy->okr', query_turned_rows.astype(jnp.float32), key_turned_rows.astype(jnp.float32))
    weight_bf = (unscaled_logits * (decay_mask * scale_qk)).astype(jnp.bfloat16)
    retained = jnp.einsum('hnm,mhe->nhe', weight_bf.astype(jnp.float32), value_rows.astype(jnp.float32))
    group_scale = lax.rsqrt(lax.optimization_barrier(jnp.mean(retained * retained, axis=-1, keepdims=True)) + GROUP_EPS)
    grouped = (retained * group_scale).reshape(length, HEADS * HV)
    sigmoid_gate = jax.nn.sigmoid(gate_pre)
    swish_val = gate_pre * sigmoid_gate
    gated_rows = (swish_val * grouped).astype(jnp.bfloat16)
    middle = rows_in + jnp.dot(gated_rows, output_weight, preferred_element_type=jnp.float32)
    second, second_scale = normalize(middle, second_gain)
    second_bf = second.astype(jnp.bfloat16)
    up_pre = jnp.dot(second_bf, up_projection_matrix, preferred_element_type=jnp.float32)
    gelu_pre = jnp.dot(second_bf, gelu_weight, preferred_element_type=jnp.float32)
    gelu_val, gelu_slope = gelu_parts(gelu_pre)
    hidden = (gelu_val * up_pre).astype(jnp.bfloat16)
    block_rows = middle + jnp.dot(hidden, down_weight, preferred_element_type=jnp.float32)
    cot_bf = cot_in.astype(jnp.bfloat16)
    grad_hidden = times_t(cot_bf, down_weight)
    grad_down = inner_rows(hidden, cot_bf)
    grad_uppre = (grad_hidden * gelu_val).astype(jnp.bfloat16)
    grad_gelupre = (grad_hidden * up_pre * gelu_slope).astype(jnp.bfloat16)
    grad_up = inner_rows(second_bf, grad_uppre)
    grad_gelu = inner_rows(second_bf, grad_gelupre)
    second_back = times_t(grad_uppre, up_projection_matrix) + times_t(grad_gelupre, gelu_weight)
    middle_back, grad_gain_two = norm_back(second_back, middle, second_scale, second_gain)
    grad_middle = cot_in + middle_back
    middle_cot = grad_middle.astype(jnp.bfloat16)
    grad_gated = times_t(middle_cot, output_weight)
    grad_out = inner_rows(gated_rows, middle_cot)
    grad_swishpre = (grad_gated * grouped * (sigmoid_gate * (1.0 + gate_pre * (1.0 - sigmoid_gate)))).astype(jnp.bfloat16)
    grad_grouped = (grad_gated * swish_val).reshape(length, HEADS, HV)
    grad_retained = (group_scale * (grad_grouped - retained * group_scale * group_scale * lax.optimization_barrier(jnp.mean(grad_grouped * retained, axis=-1, keepdims=True)))).astype(jnp.bfloat16)
    grad_valrows = jnp.einsum('hnm,nhe->mhe', weight_bf.astype(jnp.float32), grad_retained.astype(jnp.float32)).astype(jnp.bfloat16)
    grad_weight = jnp.einsum('nhe,mhe->hnm', grad_retained.astype(jnp.float32), value_rows.astype(jnp.float32))
    grad_retention_logits = (grad_weight * (decay_mask * scale_qk)).astype(jnp.bfloat16)
    grad_query_rotated_rows = jnp.einsum('uyq,quv->yuv', grad_retention_logits.astype(jnp.float32), key_turned_rows.astype(jnp.float32))
    grad_key_rotated_rows = jnp.einsum('zlt,lzi->tzi', grad_retention_logits.astype(jnp.float32), query_turned_rows.astype(jnp.float32))
    grad_qpre = unrotate(grad_query_rotated_rows, cosine_table, sine_table).astype(jnp.bfloat16).reshape(length, HEADS * HK)
    grad_kpre = unrotate(grad_key_rotated_rows, cosine_table, sine_table).astype(jnp.bfloat16).reshape(length, HEADS * HK)
    grad_vflat = grad_valrows.reshape(length, HEADS * HV)
    first_back = times_t(grad_qpre, query_weight) + times_t(grad_kpre, key_weight) + times_t(grad_vflat, value_weight) + times_t(grad_swishpre, swish_weight)
    grad_query = inner_rows(normed_bf, grad_qpre)
    grad_key = inner_rows(normed_bf, grad_kpre)
    grad_value = inner_rows(normed_bf, grad_vflat)
    grad_swish = inner_rows(normed_bf, grad_swishpre)
    input_back, grad_gain_one = norm_back(first_back, rows_in, first_scale, first_gain)
    grad_rows = grad_middle + input_back
    pieces = (grad_gain_one, grad_gain_two, grad_query, grad_key, grad_value, grad_swish, grad_out, grad_up, grad_gelu, grad_down)
    return (block_rows, grad_rows, pieces)

def reference(block_input, cotangent, first_gain, second_gain, query_weight, key_weight, value_weight, swish_weight, output_weight, up_projection_matrix, gelu_weight, down_weight):
    weights = (first_gain, second_gain, query_weight, key_weight, value_weight, swish_weight, output_weight, up_projection_matrix, gelu_weight, down_weight)
    sequences = block_input.shape[0] * block_input.shape[1] // LEN
    input_seqs = block_input.reshape(sequences, LEN, D)
    cot_seqs = cotangent.reshape(sequences, LEN, D)
    cosine_table, sine_table = angles(LEN, HK)
    decay_mask = decays(LEN, jnp.arange(HEADS, dtype=jnp.float32))
    initial = tuple((jnp.zeros(weight_arr.shape, jnp.float32) for weight_arr in weights))

    def advance(totals, both_rows):
        block_rows, grad_rows, pieces = one_sequence(weights, both_rows[0], both_rows[1], cosine_table, sine_table, decay_mask)
        return (tuple((total + piece for total, piece in zip(totals, pieces))), (block_rows, grad_rows))
    totals, (output_seqs, grad_seqs) = lax.scan(advance, initial, (input_seqs, cot_seqs))
    return (output_seqs.reshape(block_input.shape), grad_seqs.reshape(block_input.shape), totals[0], totals[1], totals[2], totals[3], totals[4], totals[5], totals[6], totals[7], totals[8], totals[9])
```

```python
import math

import jax
import jax.numpy as jnp
from jax import lax
from jax.sharding import PartitionSpec as P

HK = 256
HV = 432
LEN = 512
EPS = 1e-05
GROUP_EPS = 1.0
BF = jnp.bfloat16
F32 = jnp.float32


def ring_order(count):
    return list(range(0, count, 2)) + list(range(1, count, 2))[::-1]


def gelu_parts(pre_act):
    normal_cdf = 0.5 * (1.0 + lax.erf(pre_act * (1.0 / math.sqrt(2.0))))
    density = jnp.exp(-0.5 * pre_act * pre_act) * (1.0 / math.sqrt(2.0 * math.pi))
    return (pre_act * normal_cdf, normal_cdf + pre_act * density)


def row_scale_of(rows):
    return lax.rsqrt(jnp.mean(rows * rows, axis=-1, keepdims=True) + EPS)


def norm_back(grad_rows, rows, row_scale, gain):
    scaled = grad_rows * gain
    return row_scale * (
        scaled
        - rows * row_scale * row_scale * jnp.mean(scaled * rows, axis=-1, keepdims=True)
    )


def nt(left, right):
    return lax.dot_general(left, right, (((1,), (1,)), ((), ())), preferred_element_type=F32)


def nn(left, right):
    return lax.dot_general(left, right, (((1,), (0,)), ((), ())), preferred_element_type=F32)


def tn(left, right):
    return lax.dot_general(left, right, (((0,), (0,)), ((), ())), preferred_element_type=F32)


def rotate(pairs, cosine, sine):
    half = pairs.shape[-1] // 2
    lower, upper = pairs[..., :half], pairs[..., half:]
    return jnp.concatenate(
        [lower * cosine - upper * sine, upper * cosine + lower * sine], axis=-1
    )


def after(value, *tokens):
    return lax.optimization_barrier((value,) + tokens)[0]


class Rings:
    def __init__(self, n_dp, n_tp):
        self.n, self.t = n_dp, n_tp
        ring = ring_order(n_dp)
        self.ring = ring
        self.cw = [(ring[i], ring[(i + 1) % n_dp]) for i in range(n_dp)]
        self.ccw = [(b, a) for a, b in self.cw]

    def half_blocks(self):
        position = jnp.array([self.ring.index(i) for i in range(self.n)], jnp.int32)[
            lax.axis_index("dp")
        ]
        steps = jnp.arange(self.n, dtype=jnp.int32)
        order = jnp.array(self.ring, jnp.int32)
        down = order[(position - steps + self.n) % self.n] * 2
        up = order[(position + steps) % self.n] * 2 + 1
        return jnp.concatenate([down, up])

    def gather(self, own, start_after=()):
        width = own.shape[1] // 2
        first, second = own[:, :width], own[:, width:]
        if start_after:
            first, second = after(first, *start_after), after(second, *start_after)
        downs, ups = [first], [second]
        for _ in range(self.n - 1):
            downs.append(lax.ppermute(downs[-1], "dp", self.cw))
            ups.append(lax.ppermute(ups[-1], "dp", self.ccw))
        return downs, ups

    def scatter(self, grads):
        n = self.n
        width = grads.shape[1] // (2 * n)

        def part(side, index):
            at = (side * n + index) * width
            return grads[:, at : at + width]

        sums = []
        for side, perm in ((0, self.cw), (1, self.ccw)):
            total = part(side, 1 % n)
            for step in range(n - 1):
                moved = lax.ppermute(total, "dp", perm).astype(F32)
                total = moved + part(side, (step + 2) % n).astype(F32)
                if step < n - 2:
                    total = total.astype(BF)
            sums.append(total.astype(F32))
        return jnp.concatenate(sums, axis=1)

    def swap(self, array, bit):
        return lax.ppermute(array, "tensor", [(i, i ^ bit) for i in range(self.t)])

    def bits(self):
        return [1 << i for i in range(self.t.bit_length() - 1)]

    def share(self, own):
        chunks = {0: own}
        for bit in self.bits()[::-1]:
            for key in sorted(chunks):
                chunks[key ^ bit] = self.swap(chunks[key], bit)
        return jnp.concatenate([chunks[j] for j in range(self.t)], axis=1)

    def collect(self, partial):
        rows = partial.shape[1] // self.t
        chunks = {j: partial[:, j * rows : (j + 1) * rows] for j in range(self.t)}
        for bit in self.bits():
            for key in sorted(chunks):
                if key & bit:
                    moved = self.swap(chunks[key], bit)
                    total = chunks[key ^ bit].astype(F32) + moved.astype(F32)
                    chunks[key ^ bit] = total
                    del chunks[key]
            chunks = {k: (v.astype(BF) if len(chunks) > 1 else v) for k, v in chunks.items()}
        return chunks[0].astype(F32)

    def sum_tensor(self, value):
        for bit in self.bits():
            value = value + self.swap(value, bit)
        return value


def body(
    n_dp,
    n_tp,
    block_input,
    cotangent,
    first_gain,
    second_gain,
    query_weight,
    key_weight,
    value_weight,
    swish_weight,
    output_weight,
    up_projection_matrix,
    gelu_weight,
    down_weight,
):
    rings = Rings(n_dp, n_tp)
    micro, rows, width = block_input.shape
    local_heads = query_weight.shape[1] // HK
    window = n_tp * rows
    total = micro * window
    scale_qk = 1.0 / math.sqrt(HK)

    me = lax.axis_index("tensor")
    head_ids = (me * local_heads + jnp.arange(local_heads)).astype(F32)
    chunk_of = jnp.arange(n_tp) ^ me
    natural = (chunk_of[:, None] * rows + jnp.arange(rows)[None, :]).reshape(window)
    sequence = natural // LEN
    place = (natural % LEN).astype(F32)
    half_key = HK // 2
    frequency = jnp.exp(-math.log(10000.0) * jnp.arange(half_key, dtype=F32) / half_key)
    turns = place[:, None] * frequency[None, :]
    cosine, sine = jnp.cos(turns)[:, None, :], jnp.sin(turns)[:, None, :]
    spacing = place[:, None] - place[None, :]
    log_rate = jnp.log(1.0 - jnp.exp2(-5.0 - head_ids))
    allowed = (spacing >= 0.0) & (sequence[:, None] == sequence[None, :])
    decay = jnp.where(
        allowed[None],
        jnp.exp(jnp.maximum(spacing, 0.0)[None] * log_rate[:, None, None]),
        0.0,
    ) * scale_qk

    in_proj = jnp.concatenate(
        [query_weight.T, key_weight.T, value_weight.T, swish_weight.T], axis=0
    )
    up_gelu = jnp.concatenate([up_projection_matrix.T, gelu_weight.T], axis=0)
    in_down, in_up = rings.gather(in_proj)
    mark = max(0, n_dp - 2)
    out_down, out_up = rings.gather(output_weight, (in_down[mark], in_up[mark]))
    ug_down, ug_up = rings.gather(up_gelu, (out_down[mark], out_up[mark]))
    dn_down, dn_up = rings.gather(down_weight, (ug_down[mark], ug_up[mark]))

    half_blocks = rings.half_blocks()
    piece = width // (2 * n_dp)

    def to_ring(array):
        split = array.reshape(array.shape[:-1] + (2 * n_dp, piece))
        return jnp.take(split, half_blocks, axis=-2).reshape(array.shape)

    def from_ring(array):
        split = array.reshape(array.shape[:-1] + (2 * n_dp, piece))
        back = jnp.zeros((2 * n_dp,), jnp.int32).at[half_blocks].set(
            jnp.arange(2 * n_dp, dtype=jnp.int32)
        )
        return jnp.take(split, back, axis=-2).reshape(array.shape)

    gains = lax.all_gather(jnp.stack([first_gain, second_gain]), "dp", axis=1, tiled=True)
    gains = to_ring(gains).astype(F32)
    gain_one, gain_two = gains[0], gains[1]
    rows_in = to_ring(block_input)
    cot_in = to_ring(cotangent)

    first_scale = row_scale_of(rows_in)
    normed = rings.share((rows_in * first_scale * gain_one).astype(BF)).reshape(total, width)
    cot_all = rings.share(cot_in.astype(BF)).reshape(total, width)

    w_in = jnp.concatenate(in_down + in_up, axis=1)
    hk, hv = local_heads * HK, local_heads * HV
    w_q, w_k = w_in[:hk], w_in[hk : 2 * hk]
    w_v, w_g = w_in[2 * hk : 2 * hk + hv], w_in[2 * hk + hv :]

    def heads(flat, size):
        return flat.reshape(micro, window, local_heads, size)

    query = rotate(heads(nt(normed, w_q), HK), cosine, sine).astype(BF)
    key = rotate(heads(nt(normed, w_k), HK), cosine, sine).astype(BF)
    value = heads(nt(normed, w_v).astype(BF), HV)
    gate_pre = nt(normed, w_g)
    logits = jnp.einsum("snhd,smhd->shnm", query, key, preferred_element_type=F32)
    weight_bf = (logits * decay).astype(BF)
    retained = jnp.einsum("shnm,smhe->snhe", weight_bf, value, preferred_element_type=F32)
    group_scale = lax.rsqrt(jnp.mean(retained * retained, axis=-1, keepdims=True) + GROUP_EPS)
    grouped = (retained * group_scale).reshape(total, hv)
    sigmoid = jax.nn.sigmoid(gate_pre)
    swish = gate_pre * sigmoid
    gated = (swish * grouped).astype(BF)

    w_o = jnp.concatenate(out_down + out_up, axis=1)
    attention = rings.collect(nn(gated, w_o).astype(BF).reshape(micro, window, width))
    middle = rows_in + attention
    second_scale = row_scale_of(middle)
    second = rings.share((middle * second_scale * gain_two).astype(BF)).reshape(total, width)

    w_ug = jnp.concatenate(ug_down + ug_up, axis=1)
    units = up_projection_matrix.shape[1]
    w_u, w_l = w_ug[:units], w_ug[units:]
    up_pre = nt(second, w_u)
    gelu_pre = nt(second, w_l)
    gelu_val, gelu_slope = gelu_parts(gelu_pre)
    hidden = (gelu_val * up_pre).astype(BF)
    w_d = jnp.concatenate(dn_down + dn_up, axis=1)
    block_rows = middle + rings.collect(nn(hidden, w_d).astype(BF).reshape(micro, window, width))

    grad_down = rings.scatter(tn(hidden, cot_all).astype(BF))
    grad_hidden = nt(cot_all, w_d)
    grad_up_pre = (grad_hidden * gelu_val).astype(BF)
    grad_gelu_pre = (grad_hidden * up_pre * gelu_slope).astype(BF)
    second_back = rings.collect(
        (nn(grad_up_pre, w_u) + nn(grad_gelu_pre, w_l)).astype(BF).reshape(micro, window, width)
    )
    grad_up = rings.scatter(tn(grad_up_pre, second).astype(BF))
    grad_gelu = rings.scatter(tn(grad_gelu_pre, second).astype(BF))
    grad_middle = cot_in + norm_back(second_back, middle, second_scale, gain_two)
    middle_all = rings.share(grad_middle.astype(BF)).reshape(total, width)
    grad_gated = nt(middle_all, w_o)
    grad_out = rings.scatter(tn(gated, middle_all).astype(BF))
    grad_swish_pre = (grad_gated * grouped * (sigmoid * (1.0 + gate_pre * (1.0 - sigmoid)))).astype(
        BF
    )
    grad_grouped = heads(grad_gated * swish, HV)
    grad_retained = (
        group_scale
        * (
            grad_grouped
            - retained
            * group_scale
            * group_scale
            * jnp.mean(grad_grouped * retained, axis=-1, keepdims=True)
        )
    ).astype(BF)
    grad_swish = rings.scatter(tn(grad_swish_pre, normed).astype(BF))
    grad_value_rows = jnp.einsum(
        "shnm,snhe->smhe", weight_bf, grad_retained, preferred_element_type=F32
    ).astype(BF).reshape(total, hv)
    grad_value = rings.scatter(tn(grad_value_rows, normed).astype(BF))
    grad_logits = (
        jnp.einsum("snhe,smhe->shnm", grad_retained, value, preferred_element_type=F32) * decay
    ).astype(BF)
    grad_query_rot = jnp.einsum("shnm,smhd->snhd", grad_logits, key, preferred_element_type=F32)
    grad_key_rot = jnp.einsum("shnm,snhd->smhd", grad_logits, query, preferred_element_type=F32)
    grad_q_pre = rotate(grad_query_rot, cosine, -sine).astype(BF).reshape(total, hk)
    grad_k_pre = rotate(grad_key_rot, cosine, -sine).astype(BF).reshape(total, hk)
    grad_query = rings.scatter(tn(grad_q_pre, normed).astype(BF))
    grad_key = rings.scatter(tn(grad_k_pre, normed).astype(BF))
    first_back = rings.collect(
        (
            nn(grad_q_pre, w_q)
            + nn(grad_k_pre, w_k)
            + nn(grad_value_rows, w_v)
            + nn(grad_swish_pre, w_g)
        )
        .astype(BF)
        .reshape(micro, window, width)
    )
    grad_rows = grad_middle + norm_back(first_back, rows_in, first_scale, gain_one)

    def gain_sum(*pairs):
        return sum(jnp.sum(w.astype(F32).T * g, axis=0) for w, g in pairs)

    sum_one = gain_sum(
        (query_weight, grad_query),
        (key_weight, grad_key),
        (value_weight, grad_value),
        (swish_weight, grad_swish),
    )
    sum_two = gain_sum((up_projection_matrix, grad_up), (gelu_weight, grad_gelu))
    gain_grads = rings.sum_tensor(jnp.stack([sum_one, sum_two])) / jnp.stack(
        [first_gain, second_gain]
    ).astype(F32)
    return (
        from_ring(block_rows),
        from_ring(grad_rows),
        gain_grads[0],
        gain_grads[1],
        grad_query.T,
        grad_key.T,
        grad_value.T,
        grad_swish.T,
        grad_out,
        grad_up.T,
        grad_gelu.T,
        grad_down,
    )


def solution(mesh):
    rows = P(None, ("dp", "tensor"), None)
    wide, tall, gain = P("dp", "tensor"), P("tensor", "dp"), P("dp")
    n_dp, n_tp = mesh.shape["dp"], mesh.shape["tensor"]

    def run(*arrays):
        return body(n_dp, n_tp, *arrays)

    return jax.shard_map(
        run,
        mesh=mesh,
        in_specs=(rows, rows, gain, gain) + (wide,) * 4 + (tall, wide, wide, tall),
        out_specs=(rows, rows, gain, gain) + (wide,) * 4 + (tall, wide, wide, tall),
        check_vma=False,
    )
```

```python
import functools
import math

import jax
import jax.numpy as jnp
from jax import lax
from jax.experimental import pallas as pl
from jax.experimental.pallas import tpu as pltpu
from jax.sharding import PartitionSpec as P

HK = 256
HV = 432
LEN = 512
EPS = 1e-05
GROUP_EPS = 1.0
BF = jnp.bfloat16
F32 = jnp.float32
MESH = pl.DeviceIdType.MESH
LANE = 128
BLOCK = 2 * LANE
SLOTS = 4


def ring_position(index, count):
    low = index // 2
    return low + (index % 2) * (count - 1 - 2 * low)


def ring_index(position, count):
    high = position // (count // 2)
    return (1 - high) * (2 * position) + high * (2 * (count - 1 - position) + 1)


def bits_of(count):
    return [1 << i for i in range(count.bit_length() - 1)]


def anyspec():
    return pl.BlockSpec(memory_space=pl.ANY)


def vmem():
    return pl.BlockSpec(memory_space=pltpu.VMEM)


def in_kernel(
    n,
    n_tp,
    x_ref,
    cot_ref,
    gains_ref,
    cos_ref,
    sin_ref,
    wq_ref,
    wk_ref,
    wv_ref,
    wg_ref,
    q_out,
    k_out,
    v_out,
    g_out,
    xr_out,
    cr_out,
    gain_out,
    nall_out,
    call_out,
    wq_out,
    wk_out,
    wv_out,
    wg_out,
    x_v,
    rel_v,
    own_v,
    nall_v,
    gain_v,
    q_acc,
    k_acc,
    v_acc,
    g_acc,
    wq_s,
    wk_s,
    wv_s,
    wg_s,
    ring_send,
    ring_recv,
    gain_send,
    gain_recv,
    share_send,
    share_recv,
    load_sem,
    local_sem,
):
    micro, rows, width = x_ref.shape
    window = n_tp * rows
    mine = micro * rows
    dp, tp = lax.axis_index("dp"), lax.axis_index("tensor")
    pos = ring_position(dp, n)
    cw = ring_index((pos + 1) % n, n)
    ccw = ring_index((pos + n - 1) % n, n)
    bits = bits_of(n_tp)

    def flip(bit):
        return tp + bit - 2 * bit * ((tp // bit) % 2)

    barrier = pltpu.get_barrier_semaphore()
    for k in range(1, n):
        pl.semaphore_signal(
            barrier, inc=1, device_id=(ring_index((pos + k) % n, n), tp), device_id_type=MESH
        )
    for bit in bits:
        pl.semaphore_signal(barrier, inc=1, device_id=(dp, flip(bit)), device_id_type=MESH)
    pl.semaphore_wait(barrier, n - 1 + len(bits))

    shards = (wq_ref, wk_ref, wv_ref, wg_ref)
    wholes = (wq_out, wk_out, wv_out, wg_out)
    slots = (wq_s, wk_s, wv_s, wg_s)
    accs = (q_acc, k_acc, v_acc, g_acc)

    def hop(i, a, side):
        here = pl.ds(i * BLOCK + side * LANE, LANE)
        there = pl.ds((i + 1) * BLOCK + side * LANE, LANE)
        source = shards[a].at[pl.ds(side * LANE, LANE)] if i == 0 else wholes[a].at[here]
        return pltpu.make_async_remote_copy(
            src_ref=source,
            dst_ref=wholes[a].at[there],
            send_sem=ring_send.at[i, a, side],
            recv_sem=ring_recv.at[i, a, side],
            device_id=((cw, ccw)[side], tp),
            device_id_type=MESH,
        )

    def load(i, a):
        source = shards[a] if i == 0 else wholes[a].at[pl.ds(i * BLOCK, BLOCK)]
        return pltpu.make_async_copy(source, slots[a].at[i % SLOTS], load_sem.at[i % SLOTS, a])

    for a in range(4):
        for side in range(2):
            hop(0, a, side).start()
    x_copy = pltpu.make_async_copy(x_ref, x_v, local_sem.at[0])
    x_copy.start()
    for a in range(4):
        load(0, a).start()

    def gain_copy(k):
        return pltpu.make_async_remote_copy(
            src_ref=gains_ref,
            dst_ref=gain_v.at[k],
            send_sem=gain_send.at[k],
            recv_sem=gain_recv.at[k],
            device_id=(ring_index((pos + k) % n, n), tp),
            device_id_type=MESH,
        )

    own_gain = pltpu.make_async_copy(gains_ref, gain_v.at[0], local_sem.at[1])
    own_gain.start()
    for k in range(1, n):
        gain_copy(k).start()
    own_gain.wait()
    for k in range(1, n):
        gain_copy(k).wait()
    for i in range(n):
        gain_out[:, pl.ds(i * BLOCK, LANE)] = gain_v[i, :, pl.ds(0, LANE)]
        gain_out[:, pl.ds(i * BLOCK + LANE, LANE)] = gain_v[(n - i) % n, :, pl.ds(LANE, LANE)]

    def natural(i, side):
        at = ring_index((pos + (n - i if side == 0 else i)) % n, n) * BLOCK + side * LANE
        return pl.ds(pl.multiple_of(at, LANE), LANE)

    def share_copy(source, target, slot, m, key, bit):
        start = m * window + key * rows
        arrive = m * window + (key ^ bit) * rows
        return pltpu.make_async_remote_copy(
            src_ref=source.at[pl.ds(start, rows)] if source.shape[0] != mine
            else source.at[pl.ds(m * rows, rows)],
            dst_ref=target.at[pl.ds(arrive, rows)],
            send_sem=share_send.at[slot, m, key ^ bit],
            recv_sem=share_recv.at[slot, m, key ^ bit],
            device_id=(dp, flip(bit)),
            device_id_type=MESH,
        )

    x_copy.wait()
    step_rows = min(rows, 32)

    @pl.loop(0, mine // step_rows)
    def _(r):
        at = pl.multiple_of(r * step_rows, step_rows)
        m, inner = at // rows, at % rows
        chunk = x_v[m, pl.ds(pl.multiple_of(inner, step_rows), step_rows), :]
        scale = lax.rsqrt(jnp.mean(chunk * chunk, axis=-1, keepdims=True) + EPS)
        there = pl.ds(pl.multiple_of(m * window + inner, step_rows), step_rows)
        for i in range(n):
            for side in range(2):
                lanes = pl.ds(i * BLOCK + side * LANE, LANE)
                part = x_v[
                    m, pl.ds(pl.multiple_of(inner, step_rows), step_rows), natural(i, side)
                ]
                rel_v[0, pl.ds(at, step_rows), lanes] = part
                nall_v[there, lanes] = (part * scale * gain_out[0:1, lanes]).astype(BF)

    for bit in bits[::-1]:
        for m in range(micro):
            share_copy(nall_v, nall_v, 0, m, 0, bit).start()
    rel_copy = pltpu.make_async_copy(rel_v.at[0], xr_out, local_sem.at[2])
    rel_copy.start()
    c_copy = pltpu.make_async_copy(cot_ref, x_v, local_sem.at[0])
    c_copy.start()
    c_copy.wait()

    @pl.loop(0, mine // step_rows)
    def _(r):
        at = pl.multiple_of(r * step_rows, step_rows)
        m, inner = at // rows, at % rows
        for i in range(n):
            for side in range(2):
                lanes = pl.ds(i * BLOCK + side * LANE, LANE)
                part = x_v[
                    m, pl.ds(pl.multiple_of(inner, step_rows), step_rows), natural(i, side)
                ]
                rel_v[1, pl.ds(at, step_rows), lanes] = part
                own_v[pl.ds(at, step_rows), lanes] = part.astype(BF)

    cot_rel = pltpu.make_async_copy(rel_v.at[1], cr_out, local_sem.at[1])
    cot_rel.start()
    own_copies = [
        pltpu.make_async_copy(
            own_v.at[pl.ds(m * rows, rows)],
            call_out.at[pl.ds(m * window, rows)],
            local_sem.at[3 + m],
        )
        for m in range(micro)
    ]
    for copy in own_copies:
        copy.start()

    def relay(target, slot):
        source0 = nall_v if slot == 0 else own_v
        for at, bit in enumerate(bits[::-1]):
            for key in range(0, n_tp, 2 * bit):
                for m in range(micro):
                    if key:
                        share_copy(target, target, slot, m, key, bit).start()
            for key in range(0, n_tp, 2 * bit):
                for m in range(micro):
                    share_copy(
                        source0 if key == 0 else target, target, slot, m, key, bit
                    ).wait_recv()

    tile = 256
    heads = wq_ref.shape[1] // HK
    half = HK // 2

    def product(j, a, last):
        load(j, a).wait()
        if j == 0:
            pltpu.make_async_copy(
                slots[a].at[0], wholes[a].at[pl.ds(0, BLOCK)], load_sem.at[SLOTS, a]
            ).start()

        @pl.loop(0, micro * window // tile)
        def _(r):
            at = pl.multiple_of(r * tile, tile)
            here = pl.ds(at, tile)
            part = jnp.dot(
                nall_v[here, pl.ds(j * BLOCK, BLOCK)],
                slots[a][j % SLOTS],
                preferred_element_type=F32,
            )
            if j > 0:
                part = accs[a][here, :] + part
            if not last:
                accs[a][here, :] = part
            elif a < 2:
                place = pl.ds(pl.multiple_of(at % window, tile), tile)
                cosine, sine = cos_ref[place, :], sin_ref[place, :]
                out = (q_out, k_out)[a]
                for h in range(heads):
                    low = part[:, h * HK : h * HK + half]
                    high = part[:, h * HK + half : (h + 1) * HK]
                    out[here, pl.ds(h * HK, half)] = (low * cosine - high * sine).astype(BF)
                    out[here, pl.ds(h * HK + half, half)] = (high * cosine + low * sine).astype(BF)
            elif a == 2:
                v_out[here, :] = part.astype(BF)
            else:
                g_out[here, :] = part

        if j == 0:
            pltpu.make_async_copy(
                slots[a].at[0], wholes[a].at[pl.ds(0, BLOCK)], load_sem.at[SLOTS, a]
            ).wait()

    nall_copy = pltpu.make_async_copy(nall_v, nall_out, local_sem.at[0])
    start_at = 3
    done = 0
    for i in range(n + 1):
        if i == start_at:
            relay(nall_v, 0)
            nall_copy.start()
            for bit in bits[::-1]:
                for m in range(micro):
                    share_copy(own_v, call_out, 1, m, 0, bit).start()
        if i == n - 1:
            relay(call_out, 1)
        todo = []
        if i >= start_at:
            goal = min(i - 1, done + 1) if i < n else n - 1
            todo = list(range(done, goal + 1))
            done = goal + 1
        for a in range(4):
            if 0 < i < n:
                hop(i - 1, a, 0).wait_recv()
                hop(i - 1, a, 1).wait_recv()
                if i < n - 1:
                    hop(i, a, 0).start()
                    hop(i, a, 1).start()
                load(i, a).start()
            for j in todo:
                product(j, a, j == n - 1)

    for i in range(n - 1):
        for a in range(4):
            hop(i, a, 0).wait_send()
            hop(i, a, 1).wait_send()
    for slot, source0, target in ((0, nall_v, nall_v), (1, own_v, call_out)):
        for bit in bits[::-1]:
            for key in range(0, n_tp, 2 * bit):
                for m in range(micro):
                    share_copy(
                        source0 if key == 0 else target, target, slot, m, key, bit
                    ).wait_send()
    for copy in own_copies + [rel_copy, cot_rel, nall_copy]:
        copy.wait()


def project_in(n, n_tp, x, cot, gains, cosine, sine, weights):
    micro, rows, width = x.shape
    total = micro * n_tp * rows
    mine = micro * rows
    sizes = [w.shape[1] for w in weights]
    shape = jax.ShapeDtypeStruct
    flops = 2 * total * width * sum(sizes)
    return pl.pallas_call(
        functools.partial(in_kernel, n, n_tp),
        out_shape=(
            shape((total, sizes[0]), BF),
            shape((total, sizes[1]), BF),
            shape((total, sizes[2]), BF),
            shape((total, sizes[3]), F32),
            shape((mine, width), F32),
            shape((mine, width), F32),
            shape((2, width), F32),
            shape((total, width), BF),
            shape((total, width), BF),
        )
        + tuple(shape((width, s), BF) for s in sizes),
        in_specs=[anyspec(), anyspec(), anyspec(), vmem(), vmem()] + [anyspec()] * 4,
        out_specs=(vmem(),) * 4 + (anyspec(),) * 2 + (vmem(),) + (anyspec(),) * 6,
        scratch_shapes=[
            pltpu.VMEM(x.shape, F32),
            pltpu.VMEM((2, mine, width), F32),
            pltpu.VMEM((mine, width), BF),
            pltpu.VMEM((total, width), BF),
            pltpu.VMEM((n, 2, BLOCK), F32),
        ]
        + [pltpu.VMEM((total, s), F32) for s in sizes]
        + [pltpu.VMEM((SLOTS, BLOCK, s), BF) for s in sizes]
        + [
            pltpu.SemaphoreType.DMA((n, 4, 2)),
            pltpu.SemaphoreType.DMA((n, 4, 2)),
            pltpu.SemaphoreType.DMA((n,)),
            pltpu.SemaphoreType.DMA((n,)),
            pltpu.SemaphoreType.DMA((2, micro, n_tp)),
            pltpu.SemaphoreType.DMA((2, micro, n_tp)),
            pltpu.SemaphoreType.DMA((SLOTS + 1, 4)),
            pltpu.SemaphoreType.DMA((3 + micro,)),
        ],
        compiler_params=pltpu.CompilerParams(
            collective_id=1, has_side_effects=True, vmem_limit_bytes=64_000_000
        ),
        cost_estimate=pl.CostEstimate(
            flops=flops, bytes_accessed=60_000_000, transcendentals=0
        ),
        name="in_kernel",
    )(x, cot, gains, cosine, sine, *weights)


def out_kernel(
    n,
    n_tp,
    gq_ref,
    gk_ref,
    gv_ref,
    gs_ref,
    nall_ref,
    mid_ref,
    x_ref,
    gain_ref,
    wq_ref,
    wk_ref,
    wv_ref,
    wg_ref,
    dq_out,
    dk_out,
    dv_out,
    ds_out,
    rows_out,
    dq_s,
    dk_s,
    dv_s,
    ds_s,
    sq_s,
    sk_s,
    sv_s,
    ss_s,
    rq_s,
    rk_s,
    rv_s,
    rs_s,
    wq_s,
    wk_s,
    wv_s,
    wg_s,
    back_v,
    own_v,
    got_v,
    ring_send,
    ring_recv,
    part_send,
    part_recv,
    load_sem,
):
    micro, rows, width = rows_out.shape
    window = n_tp * rows
    total = micro * window
    mine = micro * rows
    dp, tp = lax.axis_index("dp"), lax.axis_index("tensor")
    pos = ring_position(dp, n)
    cw = ring_index((pos + 1) % n, n)
    ccw = ring_index((pos + n - 1) % n, n)
    bits = bits_of(n_tp)

    def flip(bit):
        return tp + bit - 2 * bit * ((tp // bit) % 2)

    barrier = pltpu.get_barrier_semaphore()
    for d in (cw, ccw):
        pl.semaphore_signal(barrier, inc=1, device_id=(d, tp), device_id_type=MESH)
    for bit in bits:
        pl.semaphore_signal(barrier, inc=1, device_id=(dp, flip(bit)), device_id_type=MESH)
    pl.semaphore_wait(barrier, 2 + len(bits))

    grads = (gq_ref, gk_ref, gv_ref, gs_ref)
    outs = (dq_out, dk_out, dv_out, ds_out)
    parts = (dq_s, dk_s, dv_s, ds_s)
    sends = (sq_s, sk_s, sv_s, ss_s)
    recvs = (rq_s, rk_s, rv_s, rs_s)
    wholes = (wq_ref, wk_ref, wv_ref, wg_ref)
    slots = (wq_s, wk_s, wv_s, wg_s)

    def hop(s, a, side):
        return pltpu.make_async_remote_copy(
            src_ref=sends[a].at[s % 2, pl.ds(side * LANE, LANE)],
            dst_ref=recvs[a].at[s, pl.ds(side * LANE, LANE)],
            send_sem=ring_send.at[s, a, side],
            recv_sem=ring_recv.at[s, a, side],
            device_id=((cw, ccw)[side], tp),
            device_id_type=MESH,
        )

    def load(i, a):
        return pltpu.make_async_copy(
            wholes[a].at[pl.ds(i * BLOCK, BLOCK)], slots[a].at[i % 2], load_sem.at[i % 2, a]
        )

    def gradient(i, a):
        parts[a][...] = lax.dot_general(
            nall_ref[:, pl.ds(i * BLOCK, BLOCK)],
            grads[a][...],
            (((0,), (0,)), ((), ())),
            preferred_element_type=F32,
        )

    tile = 256

    def backward(i):
        for a in range(4):
            load(i, a).wait()
            if i + 1 < n:
                load(i + 1, a).start()

        @pl.loop(0, total // tile)
        def _(r):
            here = pl.ds(pl.multiple_of(r * tile, tile), tile)
            block = None
            for a in range(4):
                term = lax.dot_general(
                    grads[a][here, :],
                    slots[a][i % 2],
                    (((1,), (1,)), ((), ())),
                    preferred_element_type=F32,
                )
                block = term if block is None else block + term
            back_v[here, pl.ds(i * BLOCK, BLOCK)] = block.astype(BF)

    def part_copy(bit, key, m):
        return pltpu.make_async_remote_copy(
            src_ref=back_v.at[pl.ds(m * window + key * rows, rows)],
            dst_ref=got_v.at[key, pl.ds(m * rows, rows)],
            send_sem=part_send.at[key, m],
            recv_sem=part_recv.at[key, m],
            device_id=(dp, flip(bit)),
            device_id_type=MESH,
        )

    def keys_of(bit):
        return [key for key in range(0, n_tp, bit) if key & bit]

    def send_parts(bit):
        for key in keys_of(bit):
            for m in range(micro):
                part_copy(bit, key, m).start()

    step_rows = 32

    def add_parts(bit):
        for key in keys_of(bit):
            for m in range(micro):
                part_copy(bit, key, m).wait_recv()
        for key in keys_of(bit):
            target = key ^ bit

            @pl.loop(0, mine // step_rows)
            def _(r):
                at = pl.multiple_of(r * step_rows, step_rows)
                m, inner = at // rows, at % rows
                here = pl.ds(at, step_rows)
                there = pl.ds(
                    pl.multiple_of(m * window + target * rows + inner, step_rows), step_rows
                )
                got = got_v[key, here, :].astype(F32)
                if target == 0:
                    held = back_v[there, :].astype(F32) if bit == 1 else own_v[here, :]
                    own_v[here, :] = held + got
                else:
                    back_v[there, :] = (back_v[there, :].astype(F32) + got).astype(BF)

    def natural(i, side):
        at = ring_index((pos + (n - i if side == 0 else i)) % n, n) * BLOCK + side * LANE
        return pl.ds(pl.multiple_of(at, LANE), LANE)

    def finish_rows():
        @pl.loop(0, mine // step_rows)
        def _(r):
            at = pl.multiple_of(r * step_rows, step_rows)
            m, inner = at // rows, pl.multiple_of(at % rows, step_rows)
            here = pl.ds(at, step_rows)
            x = x_ref[here, :]
            scale = lax.rsqrt(jnp.mean(x * x, axis=-1, keepdims=True) + EPS)
            inside = jnp.mean(own_v[here, :] * gain_ref[...] * x, axis=-1, keepdims=True)
            slope = scale * scale * inside
            for i in range(n):
                for side in range(2):
                    lanes = pl.ds(i * BLOCK + side * LANE, LANE)
                    scaled = own_v[here, lanes] * gain_ref[:, lanes]
                    rows_out[m, pl.ds(inner, step_rows), natural(i, side)] = mid_ref[
                        here, lanes
                    ] + scale * (scaled - x_ref[here, lanes] * slope)

    for a in range(4):
        load(0, a).start()
    for a in range(4):
        gradient(1 % n, a)
        sends[a][0] = parts[a][...].astype(BF)
        hop(0, a, 0).start()
        hop(0, a, 1).start()
    blocks = [i for i in range(n)]
    per_step = -(-n // max(1, (n - 1) // 2))
    stage = list(bits)
    for s in range(1, n):
        i = (s + 1) % n
        for a in range(4):
            gradient(i, a)
        for _ in range(per_step):
            if blocks:
                backward(blocks.pop(0))
                if not blocks:
                    send_parts(stage[0])
        if not blocks and stage and s > (n - 1) // 2 + 1:
            add_parts(stage.pop(0))
            if stage:
                send_parts(stage[0])
            else:
                finish_rows()
        for a in range(4):
            hop(s - 1, a, 0).wait_recv()
            hop(s - 1, a, 1).wait_recv()
            if s < n - 1:
                if s >= 2:
                    hop(s - 2, a, 0).wait_send()
                    hop(s - 2, a, 1).wait_send()
                sends[a][s % 2] = (parts[a][...] + recvs[a][s - 1].astype(F32)).astype(BF)
                hop(s, a, 0).start()
                hop(s, a, 1).start()
            else:
                outs[a][...] = parts[a][...] + recvs[a][s - 1].astype(F32)
    while stage:
        add_parts(stage.pop(0))
        if stage:
            send_parts(stage[0])
        else:
            finish_rows()
    for s in range(max(0, n - 3), n - 1):
        for a in range(4):
            hop(s, a, 0).wait_send()
            hop(s, a, 1).wait_send()
    for bit in bits:
        for key in keys_of(bit):
            for m in range(micro):
                part_copy(bit, key, m).wait_send()


def project_back(n, n_tp, rows, grads, normed, grad_middle, x_rel, gain, weights):
    total, width = normed.shape
    mine = x_rel.shape[0]
    sizes = [g.shape[1] for g in grads]
    shape = jax.ShapeDtypeStruct
    return pl.pallas_call(
        functools.partial(out_kernel, n, n_tp),
        out_shape=tuple(shape((BLOCK, s), F32) for s in sizes)
        + (shape((mine // rows, rows, width), F32),),
        in_specs=[vmem()] * 8 + [anyspec()] * 4,
        out_specs=(vmem(),) * 5,
        scratch_shapes=[pltpu.VMEM((BLOCK, s), F32) for s in sizes]
        + [pltpu.VMEM((2, BLOCK, s), BF) for s in sizes]
        + [pltpu.VMEM((n - 1, BLOCK, s), BF) for s in sizes]
        + [pltpu.VMEM((2, BLOCK, s), BF) for s in sizes]
        + [
            pltpu.VMEM((total, width), BF),
            pltpu.VMEM((mine, width), F32),
            pltpu.VMEM((n_tp, mine, width), BF),
            pltpu.SemaphoreType.DMA((n - 1, 4, 2)),
            pltpu.SemaphoreType.DMA((n - 1, 4, 2)),
            pltpu.SemaphoreType.DMA((n_tp, mine // rows)),
            pltpu.SemaphoreType.DMA((n_tp, mine // rows)),
            pltpu.SemaphoreType.DMA((2, 4)),
        ],
        compiler_params=pltpu.CompilerParams(
            collective_id=2, has_side_effects=True, vmem_limit_bytes=64_000_000
        ),
        cost_estimate=pl.CostEstimate(
            flops=4 * total * width * sum(sizes), bytes_accessed=60_000_000, transcendentals=0
        ),
        name="out_kernel",
    )(*grads, normed, grad_middle, x_rel, gain, *weights)


def normalize(row_block, gain_vec):
    row_scale = lax.rsqrt(jnp.mean(row_block * row_block, axis=-1, keepdims=True) + EPS)
    return (row_block * row_scale * gain_vec.astype(jnp.float32), row_scale)


def norm_back(grad_rows, row_block, row_scale, gain_vec):
    scaled_grad = grad_rows * gain_vec.astype(jnp.float32)
    back_rows = row_scale * (
        scaled_grad
        - row_block
        * row_scale
        * row_scale
        * jnp.mean(scaled_grad * row_block, axis=-1, keepdims=True)
    )
    return (back_rows, jnp.sum(grad_rows * row_block * row_scale, axis=0))


def angles(length, feature_width):
    half_width = feature_width // 2
    frequency = jnp.exp(-math.log(10000.0) * jnp.arange(half_width, dtype=jnp.float32) / half_width)
    turns = jnp.arange(length, dtype=jnp.float32)[:, None] * frequency[None, :]
    return (jnp.cos(turns)[:, None, :], jnp.sin(turns)[:, None, :])


def decays(length, head_ids):
    places = jnp.arange(length, dtype=jnp.float32)
    spacing = places[:, None] - places[None, :]
    log_rate = jnp.log(1.0 - jnp.exp2(-5.0 - head_ids))
    return jnp.where(
        spacing[None] >= 0.0,
        jnp.exp(jnp.maximum(spacing, 0.0)[None] * log_rate[:, None, None]),
        0.0,
    )


def rotate(value_vectors, cosine_table, sine_table):
    half_width = value_vectors.shape[-1] // 2
    lower = value_vectors[..., :half_width]
    upper = value_vectors[..., half_width:]
    return jnp.concatenate(
        [lower * cosine_table - upper * sine_table, upper * cosine_table + lower * sine_table],
        axis=-1,
    )


def unrotate(value_vectors, cosine_table, sine_table):
    half_width = value_vectors.shape[-1] // 2
    lower = value_vectors[..., :half_width]
    upper = value_vectors[..., half_width:]
    return jnp.concatenate(
        [lower * cosine_table + upper * sine_table, upper * cosine_table - lower * sine_table],
        axis=-1,
    )


def gelu_parts(pre_act):
    normal_cdf = 0.5 * (1.0 + lax.erf(pre_act * (1.0 / math.sqrt(2.0))))
    density = jnp.exp(-0.5 * pre_act * pre_act) * (1.0 / math.sqrt(2.0 * math.pi))
    return (pre_act * normal_cdf, normal_cdf + pre_act * density)


def inner_rows(left_rows, right_rows):
    return lax.dot_general(
        left_rows, right_rows, (((0,), (0,)), ((), ())), preferred_element_type=jnp.float32
    )


def times_t(left_rows, right_rows):
    return lax.dot_general(
        left_rows, right_rows, (((1,), (1,)), ((), ())), preferred_element_type=jnp.float32
    )


def forward_pass(rows_in, gathered, cosine_table, sine_table, decay_mask):
    (
        first_gain,
        second_gain,
        query_weight,
        key_weight,
        value_weight,
        swish_weight,
        output_weight,
        up_projection_matrix,
        gelu_weight,
        down_weight,
    ) = gathered
    local_heads = decay_mask.shape[0]
    scale_qk = 1.0 / math.sqrt(HK)
    normed, first_scale = normalize(rows_in, first_gain)
    normed_all = lax.all_gather(normed.astype(jnp.bfloat16), "tensor", axis=0, tiled=True)
    total_rows = normed_all.shape[0]
    sequences = total_rows // LEN
    query_turned_rows = rotate(
        jnp.dot(normed_all, query_weight, preferred_element_type=jnp.float32).reshape(
            sequences, LEN, local_heads, HK
        ),
        cosine_table,
        sine_table,
    ).astype(jnp.bfloat16)
    key_turned_rows = rotate(
        jnp.dot(normed_all, key_weight, preferred_element_type=jnp.float32).reshape(
            sequences, LEN, local_heads, HK
        ),
        cosine_table,
        sine_table,
    ).astype(jnp.bfloat16)
    value_rows = (
        jnp.dot(normed_all, value_weight, preferred_element_type=jnp.float32)
        .astype(jnp.bfloat16)
        .reshape(sequences, LEN, local_heads, HV)
    )
    gate_pre = jnp.dot(normed_all, swish_weight, preferred_element_type=jnp.float32)
    unscaled_logits = jnp.einsum(
        "snhd,smhd->shnm", query_turned_rows, key_turned_rows, preferred_element_type=jnp.float32
    )
    weight_bf = (unscaled_logits * (decay_mask * scale_qk)).astype(jnp.bfloat16)
    retained = jnp.einsum(
        "shnm,smhe->snhe", weight_bf, value_rows, preferred_element_type=jnp.float32
    )
    group_scale = lax.rsqrt(jnp.mean(retained * retained, axis=-1, keepdims=True) + GROUP_EPS)
    grouped = (retained * group_scale).reshape(total_rows, local_heads * HV)
    sigmoid_gate = jax.nn.sigmoid(gate_pre)
    swish_val = gate_pre * sigmoid_gate
    gated_rows = (swish_val * grouped).astype(jnp.bfloat16)
    attention = lax.psum_scatter(
        jnp.dot(gated_rows, output_weight, preferred_element_type=jnp.float32),
        "tensor",
        scatter_dimension=0,
        tiled=True,
    )
    middle = rows_in + attention
    second, second_scale = normalize(middle, second_gain)
    second_all = lax.all_gather(second.astype(jnp.bfloat16), "tensor", axis=0, tiled=True)
    up_pre = jnp.dot(second_all, up_projection_matrix, preferred_element_type=jnp.float32)
    gelu_pre = jnp.dot(second_all, gelu_weight, preferred_element_type=jnp.float32)
    gelu_val, gelu_slope = gelu_parts(gelu_pre)
    hidden = (gelu_val * up_pre).astype(jnp.bfloat16)
    block_rows = middle + lax.psum_scatter(
        jnp.dot(hidden, down_weight, preferred_element_type=jnp.float32).astype(jnp.bfloat16),
        "tensor",
        scatter_dimension=0,
        tiled=True,
    ).astype(jnp.float32)
    kept_state = (
        rows_in,
        first_scale,
        normed_all,
        query_turned_rows,
        key_turned_rows,
        value_rows,
        gate_pre,
        weight_bf,
        retained,
        group_scale,
        grouped,
        gated_rows,
        middle,
        second_scale,
        second_all,
        up_pre,
        gelu_val,
        gelu_slope,
        hidden,
    )
    return (block_rows, kept_state)


def backward_pass(kept_state, cot_in, gathered, cosine_table, sine_table, decay_mask):
    (
        first_gain,
        second_gain,
        query_weight,
        key_weight,
        value_weight,
        swish_weight,
        output_weight,
        up_projection_matrix,
        gelu_weight,
        down_weight,
    ) = gathered
    (
        rows_in,
        first_scale,
        normed_all,
        query_turned_rows,
        key_turned_rows,
        value_rows,
        gate_pre,
        weight_bf,
        retained,
        group_scale,
        grouped,
        gated_rows,
        middle,
        second_scale,
        second_all,
        up_pre,
        gelu_val,
        gelu_slope,
        hidden,
    ) = kept_state
    local_heads = decay_mask.shape[0]
    total_rows = normed_all.shape[0]
    scale_qk = 1.0 / math.sqrt(HK)
    cot_all = lax.all_gather(cot_in.astype(jnp.bfloat16), "tensor", axis=0, tiled=True)
    grad_hidden = times_t(cot_all, down_weight)
    grad_down = inner_rows(hidden, cot_all)
    grad_uppre = (grad_hidden * gelu_val).astype(jnp.bfloat16)
    grad_gelupre = (grad_hidden * up_pre * gelu_slope).astype(jnp.bfloat16)
    grad_up = inner_rows(second_all, grad_uppre)
    grad_gelu = inner_rows(second_all, grad_gelupre)
    second_back = lax.psum_scatter(
        times_t(grad_uppre, up_projection_matrix) + times_t(grad_gelupre, gelu_weight),
        "tensor",
        scatter_dimension=0,
        tiled=True,
    )
    middle_back, grad_gain_two = norm_back(second_back, middle, second_scale, second_gain)
    grad_middle = cot_in + middle_back
    middle_all = lax.all_gather(grad_middle.astype(jnp.bfloat16), "tensor", axis=0, tiled=True)
    grad_gated = times_t(middle_all, output_weight)
    grad_out = inner_rows(gated_rows, middle_all)
    sigmoid_gate = jax.nn.sigmoid(gate_pre)
    swish_val = gate_pre * sigmoid_gate
    grad_swishpre = (
        grad_gated * grouped * (sigmoid_gate * (1.0 + gate_pre * (1.0 - sigmoid_gate)))
    ).astype(jnp.bfloat16)
    grad_grouped = (grad_gated * swish_val).reshape(retained.shape)
    grad_retained = (
        group_scale
        * (
            grad_grouped
            - retained
            * group_scale
            * group_scale
            * jnp.mean(grad_grouped * retained, axis=-1, keepdims=True)
        )
    ).astype(jnp.bfloat16)
    grad_valrows = jnp.einsum(
        "shnm,snhe->smhe", weight_bf, grad_retained, preferred_element_type=jnp.float32
    ).astype(jnp.bfloat16)
    grad_weight = jnp.einsum(
        "snhe,smhe->shnm", grad_retained, value_rows, preferred_element_type=jnp.float32
    )
    grad_retention_logits = (grad_weight * (decay_mask * scale_qk)).astype(jnp.bfloat16)
    grad_query_rotated_rows = jnp.einsum(
        "shnm,smhd->snhd",
        grad_retention_logits,
        key_turned_rows,
        preferred_element_type=jnp.float32,
    )
    grad_key_rotated_rows = jnp.einsum(
        "shnm,snhd->smhd",
        grad_retention_logits,
        query_turned_rows,
        preferred_element_type=jnp.float32,
    )
    grad_qpre = (
        unrotate(grad_query_rotated_rows, cosine_table, sine_table)
        .astype(jnp.bfloat16)
        .reshape(total_rows, local_heads * HK)
    )
    grad_kpre = (
        unrotate(grad_key_rotated_rows, cosine_table, sine_table)
        .astype(jnp.bfloat16)
        .reshape(total_rows, local_heads * HK)
    )
    grad_vflat = grad_valrows.reshape(total_rows, local_heads * HV)
    first_back = lax.psum_scatter(
        times_t(grad_qpre, query_weight)
        + times_t(grad_kpre, key_weight)
        + times_t(grad_vflat, value_weight)
        + times_t(grad_swishpre, swish_weight),
        "tensor",
        scatter_dimension=0,
        tiled=True,
    )
    grad_query = inner_rows(normed_all, grad_qpre)
    grad_key = inner_rows(normed_all, grad_kpre)
    grad_value = inner_rows(normed_all, grad_vflat)
    grad_swish = inner_rows(normed_all, grad_swishpre)
    input_back, grad_gain_one = norm_back(first_back, rows_in, first_scale, first_gain)
    grad_rows = grad_middle + input_back
    pieces = (
        grad_gain_one,
        grad_gain_two,
        grad_query,
        grad_key,
        grad_value,
        grad_swish,
        grad_out,
        grad_up,
        grad_gelu,
        grad_down,
    )
    return (grad_rows, pieces)


def plain_body(
    block_input,
    cotangent,
    first_gain,
    second_gain,
    query_weight,
    key_weight,
    value_weight,
    swish_weight,
    output_weight,
    up_projection_matrix,
    gelu_weight,
    down_weight,
):
    local_heads = query_weight.shape[1] // HK
    head_ids = (lax.axis_index("tensor") * local_heads + jnp.arange(local_heads)).astype(
        jnp.float32
    )
    cosine_table, sine_table = angles(LEN, HK)
    decay_mask = decays(LEN, head_ids)
    output_list = []
    grad_list = []
    totals = ()
    for micro_idx in range(block_input.shape[0]):
        forward_set = (
            lax.all_gather(first_gain, "dp", axis=0, tiled=True),
            lax.all_gather(second_gain, "dp", axis=0, tiled=True),
            lax.all_gather(query_weight, "dp", axis=0, tiled=True),
            lax.all_gather(key_weight, "dp", axis=0, tiled=True),
            lax.all_gather(value_weight, "dp", axis=0, tiled=True),
            lax.all_gather(swish_weight, "dp", axis=0, tiled=True),
            lax.all_gather(output_weight, "dp", axis=1, tiled=True),
            lax.all_gather(up_projection_matrix, "dp", axis=0, tiled=True),
            lax.all_gather(gelu_weight, "dp", axis=0, tiled=True),
            lax.all_gather(down_weight, "dp", axis=1, tiled=True),
        )
        block_rows, kept_state = forward_pass(
            block_input[micro_idx], forward_set, cosine_table, sine_table, decay_mask
        )
        held = lax.optimization_barrier(
            (
                (
                    first_gain,
                    second_gain,
                    query_weight,
                    key_weight,
                    value_weight,
                    swish_weight,
                    output_weight,
                    up_projection_matrix,
                    gelu_weight,
                    down_weight,
                ),
                block_rows,
            )
        )[0]
        backward_set = (
            lax.all_gather(held[0], "dp", axis=0, tiled=True),
            lax.all_gather(held[1], "dp", axis=0, tiled=True),
            lax.all_gather(held[2], "dp", axis=0, tiled=True),
            lax.all_gather(held[3], "dp", axis=0, tiled=True),
            lax.all_gather(held[4], "dp", axis=0, tiled=True),
            lax.all_gather(held[5], "dp", axis=0, tiled=True),
            lax.all_gather(held[6], "dp", axis=1, tiled=True),
            lax.all_gather(held[7], "dp", axis=0, tiled=True),
            lax.all_gather(held[8], "dp", axis=0, tiled=True),
            lax.all_gather(held[9], "dp", axis=1, tiled=True),
        )
        grad_rows, pieces = backward_pass(
            kept_state, cotangent[micro_idx], backward_set, cosine_table, sine_table, decay_mask
        )
        output_list.append(block_rows)
        grad_list.append(grad_rows)
        if micro_idx == 0:
            totals = tuple(pieces)
        else:
            totals = tuple((total + piece for total, piece in zip(totals, pieces)))
    totals = (
        lax.psum_scatter(totals[0], "dp", scatter_dimension=0, tiled=True),
        lax.psum_scatter(totals[1], "dp", scatter_dimension=0, tiled=True),
        lax.psum_scatter(totals[2], "dp", scatter_dimension=0, tiled=True),
        lax.psum_scatter(totals[3], "dp", scatter_dimension=0, tiled=True),
        lax.psum_scatter(totals[4], "dp", scatter_dimension=0, tiled=True),
        lax.psum_scatter(totals[5], "dp", scatter_dimension=0, tiled=True),
        lax.psum_scatter(totals[6], "dp", scatter_dimension=1, tiled=True),
        lax.psum_scatter(totals[7], "dp", scatter_dimension=0, tiled=True),
        lax.psum_scatter(totals[8], "dp", scatter_dimension=0, tiled=True),
        lax.psum_scatter(totals[9], "dp", scatter_dimension=1, tiled=True),
    )
    gain_first, gain_second = lax.psum((totals[0], totals[1]), "tensor")
    return (
        jnp.stack(output_list, axis=0),
        jnp.stack(grad_list, axis=0),
        gain_first,
        gain_second,
        totals[2],
        totals[3],
        totals[4],
        totals[5],
        totals[6],
        totals[7],
        totals[8],
        totals[9],
    )


def gelu_parts(pre_act):
    normal_cdf = 0.5 * (1.0 + lax.erf(pre_act * (1.0 / math.sqrt(2.0))))
    density = jnp.exp(-0.5 * pre_act * pre_act) * (1.0 / math.sqrt(2.0 * math.pi))
    return (pre_act * normal_cdf, normal_cdf + pre_act * density)


def row_scale_of(rows):
    return lax.rsqrt(jnp.mean(rows * rows, axis=-1, keepdims=True) + EPS)


def back_of_norm(grad_rows, rows, row_scale, gain):
    scaled = grad_rows * gain
    return row_scale * (
        scaled
        - rows * row_scale * row_scale * jnp.mean(scaled * rows, axis=-1, keepdims=True)
    )


def nt(left, right):
    return lax.dot_general(left, right, (((1,), (1,)), ((), ())), preferred_element_type=F32)


def nn(left, right):
    return lax.dot_general(left, right, (((1,), (0,)), ((), ())), preferred_element_type=F32)


def tn(left, right):
    return lax.dot_general(left, right, (((0,), (0,)), ((), ())), preferred_element_type=F32)


def turned(pairs, cosine, sine):
    half = pairs.shape[-1] // 2
    lower, upper = pairs[..., :half], pairs[..., half:]
    return jnp.concatenate(
        [lower * cosine - upper * sine, upper * cosine + lower * sine], axis=-1
    )


def after(value, *tokens):
    return lax.optimization_barrier((value,) + tokens)[0]


class Rings:
    def __init__(self, n_dp, n_tp):
        self.n, self.t = n_dp, n_tp
        ring = [ring_index(p, n_dp) for p in range(n_dp)]
        self.cw = [(ring[i], ring[(i + 1) % n_dp]) for i in range(n_dp)]
        self.ccw = [(b, a) for a, b in self.cw]

    def gather(self, own, axis):
        pair = jnp.split(own, 2, axis=axis)
        pieces = list(pair)
        for _ in range(self.n - 1):
            pair = [lax.ppermute(pair[0], "dp", self.cw), lax.ppermute(pair[1], "dp", self.ccw)]
            pieces += pair
        return pieces

    def scatter(self, grads, axis):
        n = self.n
        pieces = jnp.split(grads, 2 * n, axis=axis)
        sums = []
        for side, perm in ((0, self.cw), (1, self.ccw)):
            total = pieces[2 * (1 % n) + side]
            for step in range(n - 1):
                moved = lax.ppermute(total, "dp", perm).astype(F32)
                total = moved + pieces[2 * ((step + 2) % n) + side].astype(F32)
                if step < n - 2:
                    total = total.astype(BF)
            sums.append(total.astype(F32))
        return jnp.concatenate(sums, axis=axis)

    def swap(self, array, bit):
        return lax.ppermute(array, "tensor", [(i, i ^ bit) for i in range(self.t)])

    def share(self, own):
        chunks = {0: own}
        for bit in bits_of(self.t)[::-1]:
            for key in sorted(chunks):
                chunks[key ^ bit] = self.swap(chunks[key], bit)
        return jnp.concatenate([chunks[j] for j in range(self.t)], axis=1)

    def collect(self, partial):
        rows = partial.shape[1] // self.t
        chunks = {j: partial[:, j * rows : (j + 1) * rows] for j in range(self.t)}
        for bit in bits_of(self.t):
            for key in sorted(chunks):
                if key & bit:
                    moved = self.swap(chunks[key], bit)
                    chunks[key ^ bit] = chunks[key ^ bit].astype(F32) + moved.astype(F32)
                    del chunks[key]
            chunks = {k: (v.astype(BF) if len(chunks) > 1 else v) for k, v in chunks.items()}
        return chunks[0].astype(F32)

    def sum_tensor(self, value):
        for bit in bits_of(self.t):
            value = value + self.swap(value, bit)
        return value


def ring_body(
    n_dp,
    n_tp,
    block_input,
    cotangent,
    first_gain,
    second_gain,
    query_weight,
    key_weight,
    value_weight,
    swish_weight,
    output_weight,
    up_projection_matrix,
    gelu_weight,
    down_weight,
):
    rings = Rings(n_dp, n_tp)
    micro, rows, width = block_input.shape
    local_heads = query_weight.shape[1] // HK
    window = n_tp * rows
    total = micro * window
    hk, hv = local_heads * HK, local_heads * HV
    scale_qk = 1.0 / math.sqrt(HK)

    me = lax.axis_index("tensor")
    head_ids = (me * local_heads + jnp.arange(local_heads)).astype(F32)
    chunk_of = jnp.arange(n_tp) ^ me
    natural = (chunk_of[:, None] * rows + jnp.arange(rows)[None, :]).reshape(window)
    sequence = natural // LEN
    place = (natural % LEN).astype(F32)
    half_key = HK // 2
    frequency = jnp.exp(-math.log(10000.0) * jnp.arange(half_key, dtype=F32) / half_key)
    turns = place[:, None] * frequency[None, :]
    cos_table, sin_table = jnp.cos(turns), jnp.sin(turns)
    cosine, sine = cos_table[:, None, :], sin_table[:, None, :]
    spacing = place[:, None] - place[None, :]
    log_rate = jnp.log(1.0 - jnp.exp2(-5.0 - head_ids))
    allowed = (spacing >= 0.0) & (sequence[:, None] == sequence[None, :])
    decay = scale_qk * jnp.where(
        allowed[None],
        jnp.exp(jnp.maximum(spacing, 0.0)[None] * log_rate[:, None, None]),
        0.0,
    )

    gains_own = jnp.stack([first_gain, second_gain]).astype(F32)
    query, key, value, gate_pre, rows_in, cot_in, gains, normed, cot_all, w_q, w_k, w_v, w_g = (
        project_in(
            n_dp,
            n_tp,
            block_input,
            cotangent,
            gains_own,
            cos_table,
            sin_table,
            (query_weight, key_weight, value_weight, swish_weight),
        )
    )
    gain_two = gains[1]
    rows_in = rows_in.reshape(micro, rows, width)
    cot_in = cot_in.reshape(micro, rows, width)

    out_pieces = rings.gather(after(output_weight, query), 1)
    up_pieces = rings.gather(
        after(up_projection_matrix, out_pieces[-4], out_pieces[-3]), 0
    )
    gelu_pieces = rings.gather(after(gelu_weight, up_pieces[-4], up_pieces[-3]), 0)
    down_pieces = rings.gather(after(down_weight, gelu_pieces[-4], gelu_pieces[-3]), 1)

    def heads(flat, size):
        return flat.reshape(micro, window, local_heads, size)

    query, key, value = heads(query, HK), heads(key, HK), heads(value, HV)
    logits = jnp.einsum("snhd,smhd->shnm", query, key, preferred_element_type=F32)
    weight_bf = (logits * decay).astype(BF)
    retained = jnp.einsum("shnm,smhe->snhe", weight_bf, value, preferred_element_type=F32)
    group_scale = lax.rsqrt(jnp.mean(retained * retained, axis=-1, keepdims=True) + GROUP_EPS)
    grouped = (retained * group_scale).reshape(total, hv)
    sigmoid = jax.nn.sigmoid(gate_pre)
    swish = gate_pre * sigmoid
    gated = (swish * grouped).astype(BF)

    w_o = jnp.concatenate(out_pieces, axis=1)
    attention = rings.collect(nn(gated, w_o).astype(BF).reshape(micro, window, width))
    middle = rows_in + attention
    second_scale = row_scale_of(middle)
    second = rings.share((middle * second_scale * gain_two).astype(BF)).reshape(total, width)

    w_u = jnp.concatenate(up_pieces, axis=0)
    up_pre = nn(second, w_u)
    w_l = jnp.concatenate(gelu_pieces, axis=0)
    gelu_pre = nn(second, w_l)
    gelu_val, gelu_slope = gelu_parts(gelu_pre)
    hidden = (gelu_val * up_pre).astype(BF)
    w_d = jnp.concatenate(down_pieces, axis=1)
    block_rows = middle + rings.collect(nn(hidden, w_d).astype(BF).reshape(micro, window, width))

    grad_down = rings.scatter(tn(hidden, cot_all).astype(BF), 1)
    grad_hidden = nt(cot_all, w_d)
    grad_up_pre = (grad_hidden * gelu_val).astype(BF)
    grad_gelu_pre = (grad_hidden * up_pre * gelu_slope).astype(BF)
    second_back = rings.collect(
        (nt(grad_up_pre, w_u) + nt(grad_gelu_pre, w_l)).astype(BF).reshape(micro, window, width)
    )
    grad_up = rings.scatter(tn(second, grad_up_pre).astype(BF), 0)
    grad_gelu = rings.scatter(tn(second, grad_gelu_pre).astype(BF), 0)
    grad_middle = cot_in + back_of_norm(second_back, middle, second_scale, gain_two)
    middle_all = rings.share(grad_middle.astype(BF)).reshape(total, width)
    grad_gated = nt(middle_all, w_o)
    grad_out = rings.scatter(tn(gated, middle_all).astype(BF), 1)
    grad_swish_pre = (grad_gated * grouped * (sigmoid * (1.0 + gate_pre * (1.0 - sigmoid)))).astype(
        BF
    )
    grad_grouped = heads(grad_gated * swish, HV)
    grad_retained = (
        group_scale
        * (
            grad_grouped
            - retained
            * group_scale
            * group_scale
            * jnp.mean(grad_grouped * retained, axis=-1, keepdims=True)
        )
    ).astype(BF)
    grad_value_rows = jnp.einsum(
        "shnm,snhe->smhe", weight_bf, grad_retained, preferred_element_type=F32
    ).astype(BF).reshape(total, hv)
    grad_logits = (
        jnp.einsum("snhe,smhe->shnm", grad_retained, value, preferred_element_type=F32) * decay
    ).astype(BF)
    grad_query_rot = jnp.einsum("shnm,smhd->snhd", grad_logits, key, preferred_element_type=F32)
    grad_key_rot = jnp.einsum("shnm,snhd->smhd", grad_logits, query, preferred_element_type=F32)
    grad_q_pre = turned(grad_query_rot, cosine, -sine).astype(BF).reshape(total, hk)
    grad_k_pre = turned(grad_key_rot, cosine, -sine).astype(BF).reshape(total, hk)
    grad_query, grad_key, grad_value, grad_swish, grad_rows = project_back(
        n_dp,
        n_tp,
        rows,
        (grad_q_pre, grad_k_pre, grad_value_rows, grad_swish_pre),
        normed,
        grad_middle.reshape(micro * rows, width),
        rows_in.reshape(micro * rows, width),
        gains[0:1],
        (w_q, w_k, w_v, w_g),
    )

    def gain_sum(*pairs):
        return sum(jnp.sum(w.astype(F32) * g, axis=1) for w, g in pairs)

    sum_one = gain_sum(
        (query_weight, grad_query),
        (key_weight, grad_key),
        (value_weight, grad_value),
        (swish_weight, grad_swish),
    )
    sum_two = gain_sum((up_projection_matrix, grad_up), (gelu_weight, grad_gelu))
    gain_grads = rings.sum_tensor(jnp.stack([sum_one, sum_two])) / gains_own

    dp = lax.axis_index("dp")
    position = ring_position(dp, n_dp)
    index = jnp.arange(n_dp)
    spot = ring_position(index, n_dp)
    low = 2 * ((position - spot + n_dp) % n_dp)
    high = 2 * ((spot - position + n_dp) % n_dp) + 1
    back = jnp.stack([low, high], axis=1).reshape(2 * n_dp)

    def from_ring(array):
        split = array.reshape(micro, rows, 2 * n_dp, LANE)
        return jnp.take(split, back, axis=2).reshape(micro, rows, width)

    return (
        from_ring(block_rows),
        grad_rows,
        gain_grads[0],
        gain_grads[1],
        grad_query,
        grad_key,
        grad_value,
        grad_swish,
        grad_out,
        grad_up,
        grad_gelu,
        grad_down,
    )


def solution(mesh):
    rows = P(None, ("dp", "tensor"), None)
    wide, tall, gain = P("dp", "tensor"), P("tensor", "dp"), P("dp")
    n_dp, n_tp = mesh.shape["dp"], mesh.shape["tensor"]

    def run(*arrays):
        blocks = arrays[2].shape[0] == BLOCK and n_dp % 2 == 0 and n_dp > 2
        pairs = n_tp > 1 and n_tp & (n_tp - 1) == 0
        aligned = (n_tp * arrays[0].shape[1]) % LEN == 0 and arrays[0].shape[1] % LANE == 0
        if blocks and pairs and aligned:
            return ring_body(n_dp, n_tp, *arrays)
        return plain_body(*arrays)

    return jax.shard_map(
        run,
        mesh=mesh,
        in_specs=(rows, rows, gain, gain) + (wide,) * 4 + (tall, wide, wide, tall),
        out_specs=(rows, rows, gain, gain) + (wide,) * 4 + (tall, wide, wide, tall),
        check_vma=False,
    )
```

```python
import functools
import math

import jax
import jax.numpy as jnp
from jax import lax
from jax.experimental import pallas as pl
from jax.experimental.pallas import tpu as pltpu
from jax.sharding import PartitionSpec as P

HK = 256
HV = 432
LEN = 512
EPS = 1e-05
GROUP_EPS = 1.0
BF = jnp.bfloat16
F32 = jnp.float32
MESH = pl.DeviceIdType.MESH
LANE = 128
BLOCK = 2 * LANE
SLOTS = 4
STEP = 32


def ring_position(index, count):
    low = index // 2
    return low + (index % 2) * (count - 1 - 2 * low)


def ring_index(position, count):
    high = position // (count // 2)
    return (1 - high) * (2 * position) + high * (2 * (count - 1 - position) + 1)


def bits_of(count):
    return [1 << i for i in range(count.bit_length() - 1)]


def anyspec():
    return pl.BlockSpec(memory_space=pl.ANY)


def vmem():
    return pl.BlockSpec(memory_space=pltpu.VMEM)


def in_kernel(
    n,
    n_tp,
    x_ref,
    cot_ref,
    gains_ref,
    cos_ref,
    sin_ref,
    wq_ref,
    wk_ref,
    wv_ref,
    wg_ref,
    wo_ref,
    q_out,
    k_out,
    v_out,
    g_out,
    xr_out,
    cr_out,
    gain_out,
    nall_out,
    call_out,
    wq_out,
    wk_out,
    wv_out,
    wg_out,
    wo_out,
    x_v,
    rel_v,
    own_v,
    nall_v,
    gain_v,
    q_acc,
    k_acc,
    v_acc,
    g_acc,
    wq_s,
    wk_s,
    wv_s,
    wg_s,
    wo_s,
    ring_send,
    ring_recv,
    gain_send,
    gain_recv,
    share_send,
    share_recv,
    load_sem,
    local_sem,
):
    micro, rows, width = x_ref.shape
    window = n_tp * rows
    mine = micro * rows
    dp, tp = lax.axis_index("dp"), lax.axis_index("tensor")
    pos = ring_position(dp, n)
    cw = ring_index((pos + 1) % n, n)
    ccw = ring_index((pos + n - 1) % n, n)
    bits = bits_of(n_tp)

    def flip(bit):
        return tp + bit - 2 * bit * ((tp // bit) % 2)

    barrier = pltpu.get_barrier_semaphore()
    for k in range(1, n):
        pl.semaphore_signal(
            barrier, inc=1, device_id=(ring_index((pos + k) % n, n), tp), device_id_type=MESH
        )
    for bit in bits:
        pl.semaphore_signal(barrier, inc=1, device_id=(dp, flip(bit)), device_id_type=MESH)
    pl.semaphore_wait(barrier, n - 1 + len(bits))

    shards = (wq_ref, wk_ref, wv_ref, wg_ref)
    wholes = (wq_out, wk_out, wv_out, wg_out)
    slots = (wq_s, wk_s, wv_s, wg_s)
    accs = (q_acc, k_acc, v_acc, g_acc)

    def hop(i, a, side):
        if a < 4:
            here = pl.ds(i * BLOCK + side * LANE, LANE)
            there = pl.ds((i + 1) * BLOCK + side * LANE, LANE)
            source = shards[a].at[pl.ds(side * LANE, LANE)] if i == 0 else wholes[a].at[here]
            target = wholes[a].at[there]
        else:
            lanes = pl.ds(side * LANE, LANE)
            source = wo_ref.at[:, lanes] if i == 0 else wo_out.at[i, :, lanes]
            target = wo_out.at[i + 1, :, lanes]
        return pltpu.make_async_remote_copy(
            src_ref=source,
            dst_ref=target,
            send_sem=ring_send.at[i, a, side],
            recv_sem=ring_recv.at[i, a, side],
            device_id=((cw, ccw)[side], tp),
            device_id_type=MESH,
        )

    def load(i, a):
        source = shards[a] if i == 0 else wholes[a].at[pl.ds(i * BLOCK, BLOCK)]
        return pltpu.make_async_copy(source, slots[a].at[i % SLOTS], load_sem.at[i % SLOTS, a])

    for a in range(5):
        for side in range(2):
            hop(0, a, side).start()
    wo_own = pltpu.make_async_copy(wo_ref, wo_s, local_sem.at[3 + micro])
    wo_own.start()
    x_copy = pltpu.make_async_copy(x_ref, x_v, local_sem.at[0])
    x_copy.start()
    for a in range(4):
        load(0, a).start()

    def gain_copy(k):
        return pltpu.make_async_remote_copy(
            src_ref=gains_ref,
            dst_ref=gain_v.at[k],
            send_sem=gain_send.at[k],
            recv_sem=gain_recv.at[k],
            device_id=(ring_index((pos + k) % n, n), tp),
            device_id_type=MESH,
        )

    own_gain = pltpu.make_async_copy(gains_ref, gain_v.at[0], local_sem.at[1])
    own_gain.start()
    for k in range(1, n):
        gain_copy(k).start()
    own_gain.wait()
    for k in range(1, n):
        gain_copy(k).wait()
    for i in range(n):
        gain_out[:, pl.ds(i * BLOCK, LANE)] = gain_v[i, :, pl.ds(0, LANE)]
        gain_out[:, pl.ds(i * BLOCK + LANE, LANE)] = gain_v[(n - i) % n, :, pl.ds(LANE, LANE)]

    def natural(i, side):
        at = ring_index((pos + (n - i if side == 0 else i)) % n, n) * BLOCK + side * LANE
        return pl.ds(pl.multiple_of(at, LANE), LANE)

    def share_copy(source, target, slot, m, key, bit):
        start = m * window + key * rows
        arrive = m * window + (key ^ bit) * rows
        return pltpu.make_async_remote_copy(
            src_ref=source.at[pl.ds(start, rows)] if source.shape[0] != mine
            else source.at[pl.ds(m * rows, rows)],
            dst_ref=target.at[pl.ds(arrive, rows)],
            send_sem=share_send.at[slot, m, key ^ bit],
            recv_sem=share_recv.at[slot, m, key ^ bit],
            device_id=(dp, flip(bit)),
            device_id_type=MESH,
        )

    x_copy.wait()
    step_rows = min(rows, 32)

    @pl.loop(0, mine // step_rows)
    def _(r):
        at = pl.multiple_of(r * step_rows, step_rows)
        m, inner = at // rows, at % rows
        chunk = x_v[m, pl.ds(pl.multiple_of(inner, step_rows), step_rows), :]
        scale = lax.rsqrt(jnp.mean(chunk * chunk, axis=-1, keepdims=True) + EPS)
        there = pl.ds(pl.multiple_of(m * window + inner, step_rows), step_rows)
        for i in range(n):
            for side in range(2):
                lanes = pl.ds(i * BLOCK + side * LANE, LANE)
                part = x_v[
                    m, pl.ds(pl.multiple_of(inner, step_rows), step_rows), natural(i, side)
                ]
                rel_v[0, pl.ds(at, step_rows), lanes] = part
                nall_v[there, lanes] = (part * scale * gain_out[0:1, lanes]).astype(BF)

    for bit in bits[::-1]:
        for m in range(micro):
            share_copy(nall_v, nall_v, 0, m, 0, bit).start()
    rel_copy = pltpu.make_async_copy(rel_v.at[0], xr_out, local_sem.at[2])
    rel_copy.start()
    c_copy = pltpu.make_async_copy(cot_ref, x_v, local_sem.at[0])
    c_copy.start()
    c_copy.wait()

    @pl.loop(0, mine // step_rows)
    def _(r):
        at = pl.multiple_of(r * step_rows, step_rows)
        m, inner = at // rows, at % rows
        for i in range(n):
            for side in range(2):
                lanes = pl.ds(i * BLOCK + side * LANE, LANE)
                part = x_v[
                    m, pl.ds(pl.multiple_of(inner, step_rows), step_rows), natural(i, side)
                ]
                rel_v[1, pl.ds(at, step_rows), lanes] = part
                own_v[pl.ds(at, step_rows), lanes] = part.astype(BF)

    cot_rel = pltpu.make_async_copy(rel_v.at[1], cr_out, local_sem.at[1])
    cot_rel.start()
    own_copies = [
        pltpu.make_async_copy(
            own_v.at[pl.ds(m * rows, rows)],
            call_out.at[pl.ds(m * window, rows)],
            local_sem.at[3 + m],
        )
        for m in range(micro)
    ]
    for copy in own_copies:
        copy.start()

    def relay(target, slot):
        source0 = nall_v if slot == 0 else own_v
        for at, bit in enumerate(bits[::-1]):
            for key in range(0, n_tp, 2 * bit):
                for m in range(micro):
                    if key:
                        share_copy(target, target, slot, m, key, bit).start()
            for key in range(0, n_tp, 2 * bit):
                for m in range(micro):
                    share_copy(
                        source0 if key == 0 else target, target, slot, m, key, bit
                    ).wait_recv()

    tile = 256
    heads = wq_ref.shape[1] // HK
    half = HK // 2

    def product(j, a, last):
        load(j, a).wait()
        if j == 0:
            pltpu.make_async_copy(
                slots[a].at[0], wholes[a].at[pl.ds(0, BLOCK)], load_sem.at[SLOTS, a]
            ).start()

        @pl.loop(0, micro * window // tile)
        def _(r):
            at = pl.multiple_of(r * tile, tile)
            here = pl.ds(at, tile)
            part = jnp.dot(
                nall_v[here, pl.ds(j * BLOCK, BLOCK)],
                slots[a][j % SLOTS],
                preferred_element_type=F32,
            )
            if j > 0:
                part = accs[a][here, :] + part
            if not last:
                accs[a][here, :] = part
            elif a < 2:
                place = pl.ds(pl.multiple_of(at % window, tile), tile)
                cosine, sine = cos_ref[place, :], sin_ref[place, :]
                out = (q_out, k_out)[a]
                for h in range(heads):
                    low = part[:, h * HK : h * HK + half]
                    high = part[:, h * HK + half : (h + 1) * HK]
                    out[here, pl.ds(h * HK, half)] = (low * cosine - high * sine).astype(BF)
                    out[here, pl.ds(h * HK + half, half)] = (high * cosine + low * sine).astype(BF)
            elif a == 2:
                v_out[here, :] = part.astype(BF)
            else:
                g_out[here, :] = part

        if j == 0:
            pltpu.make_async_copy(
                slots[a].at[0], wholes[a].at[pl.ds(0, BLOCK)], load_sem.at[SLOTS, a]
            ).wait()

    nall_copy = pltpu.make_async_copy(nall_v, nall_out, local_sem.at[0])
    start_at = 3
    done = 0
    for i in range(n + 1):
        if i == start_at:
            relay(nall_v, 0)
            nall_copy.start()
            for bit in bits[::-1]:
                for m in range(micro):
                    share_copy(own_v, call_out, 1, m, 0, bit).start()
        if i == n - 1:
            relay(call_out, 1)
        todo = []
        if i >= start_at:
            goal = min(i - 1, done + 1) if i < n else n - 1
            todo = list(range(done, goal + 1))
            done = goal + 1
        if i == 1:
            wo_own.wait()
            wo_own = pltpu.make_async_copy(wo_s, wo_out.at[0], local_sem.at[3 + micro])
            wo_own.start()
        for a in range(5):
            if 0 < i < n:
                hop(i - 1, a, 0).wait_recv()
                hop(i - 1, a, 1).wait_recv()
                if i < n - 1:
                    hop(i, a, 0).start()
                    hop(i, a, 1).start()
                if a < 4:
                    load(i, a).start()
            if a < 4:
                for j in todo:
                    product(j, a, j == n - 1)

    for i in range(n - 1):
        for a in range(5):
            hop(i, a, 0).wait_send()
            hop(i, a, 1).wait_send()
    for slot, source0, target in ((0, nall_v, nall_v), (1, own_v, call_out)):
        for bit in bits[::-1]:
            for key in range(0, n_tp, 2 * bit):
                for m in range(micro):
                    share_copy(
                        source0 if key == 0 else target, target, slot, m, key, bit
                    ).wait_send()
    for copy in own_copies + [rel_copy, cot_rel, nall_copy, wo_own]:
        copy.wait()


def project_in(n, n_tp, x, cot, gains, cosine, sine, weights, wo):
    micro, rows, width = x.shape
    total = micro * n_tp * rows
    mine = micro * rows
    sizes = [w.shape[1] for w in weights]
    shape = jax.ShapeDtypeStruct
    flops = 2 * total * width * sum(sizes)
    return pl.pallas_call(
        functools.partial(in_kernel, n, n_tp),
        out_shape=(
            shape((total, sizes[0]), BF),
            shape((total, sizes[1]), BF),
            shape((total, sizes[2]), BF),
            shape((total, sizes[3]), F32),
            shape((mine, width), F32),
            shape((mine, width), F32),
            shape((2, width), F32),
            shape((total, width), BF),
            shape((total, width), BF),
        )
        + tuple(shape((width, s), BF) for s in sizes)
        + (shape((n,) + wo.shape, BF),),
        in_specs=[anyspec(), anyspec(), anyspec(), vmem(), vmem()] + [anyspec()] * 5,
        out_specs=(vmem(),) * 4 + (anyspec(),) * 2 + (vmem(),) + (anyspec(),) * 7,
        scratch_shapes=[
            pltpu.VMEM(x.shape, F32),
            pltpu.VMEM((2, mine, width), F32),
            pltpu.VMEM((mine, width), BF),
            pltpu.VMEM((total, width), BF),
            pltpu.VMEM((n, 2, BLOCK), F32),
        ]
        + [pltpu.VMEM((total, s), F32) for s in sizes]
        + [pltpu.VMEM((SLOTS, BLOCK, s), BF) for s in sizes]
        + [
            pltpu.VMEM(wo.shape, BF),
            pltpu.SemaphoreType.DMA((n - 1, 5, 2)),
            pltpu.SemaphoreType.DMA((n - 1, 5, 2)),
            pltpu.SemaphoreType.DMA((n,)),
            pltpu.SemaphoreType.DMA((n,)),
            pltpu.SemaphoreType.DMA((2, micro, n_tp)),
            pltpu.SemaphoreType.DMA((2, micro, n_tp)),
            pltpu.SemaphoreType.DMA((SLOTS + 1, 4)),
            pltpu.SemaphoreType.DMA((4 + micro,)),
        ],
        compiler_params=pltpu.CompilerParams(
            collective_id=1, has_side_effects=True, vmem_limit_bytes=64_000_000
        ),
        cost_estimate=pl.CostEstimate(
            flops=flops, bytes_accessed=60_000_000, transcendentals=0
        ),
        name="in_kernel",
    )(x, cot, gains, cosine, sine, *weights, wo)


def partner(tp, bit):
    return tp + bit - 2 * bit * ((tp // bit) % 2)


def neighbours(n):
    dp, tp = lax.axis_index("dp"), lax.axis_index("tensor")
    pos = ring_position(dp, n)
    return dp, tp, ring_index((pos + 1) % n, n), ring_index((pos + n - 1) % n, n)


def greet(devices):
    barrier = pltpu.get_barrier_semaphore()
    for device in devices:
        pl.semaphore_signal(barrier, inc=1, device_id=device, device_id_type=MESH)
    pl.semaphore_wait(barrier, len(devices))


class Share:
    def __init__(self, dp, tp, n_tp, micro, rows, buf, send, recv):
        self.dp, self.tp, self.n_tp, self.micro, self.rows = dp, tp, n_tp, micro, rows
        self.buf, self.send, self.recv = buf, send, recv
        self.bits = bits_of(n_tp)[::-1]

    def copies(self, bit, keys=None):
        window = self.n_tp * self.rows
        for key in range(0, self.n_tp, 2 * bit):
            if keys is None or (key == 0) == keys:
                for m in range(self.micro):
                    yield pltpu.make_async_remote_copy(
                        src_ref=self.buf.at[pl.ds(m * window + key * self.rows, self.rows)],
                        dst_ref=self.buf.at[
                            pl.ds(m * window + (key ^ bit) * self.rows, self.rows)
                        ],
                        send_sem=self.send.at[m, key ^ bit],
                        recv_sem=self.recv.at[m, key ^ bit],
                        device_id=(self.dp, partner(self.tp, bit)),
                        device_id_type=MESH,
                    )

    def begin(self):
        for bit in self.bits:
            for copy in self.copies(bit, True):
                copy.start()

    def relay(self):
        for bit in self.bits:
            for copy in self.copies(bit, False):
                copy.start()
            for copy in self.copies(bit):
                copy.wait_recv()

    def finish(self):
        for bit in self.bits:
            for copy in self.copies(bit):
                copy.wait_send()


class Collect:
    def __init__(self, dp, tp, n_tp, micro, rows, back, got, own, send, recv):
        self.dp, self.tp, self.n_tp, self.micro, self.rows = dp, tp, n_tp, micro, rows
        self.back, self.got, self.own, self.send, self.recv = back, got, own, send, recv
        self.bits = bits_of(n_tp)

    def keys(self, bit):
        return [key for key in range(0, self.n_tp, bit) if key & bit]

    def copies(self, bit):
        window = self.n_tp * self.rows
        for key in self.keys(bit):
            for m in range(self.micro):
                yield pltpu.make_async_remote_copy(
                    src_ref=self.back.at[pl.ds(m * window + key * self.rows, self.rows)],
                    dst_ref=self.got.at[key - 1, pl.ds(m * self.rows, self.rows)],
                    send_sem=self.send.at[key - 1, m],
                    recv_sem=self.recv.at[key - 1, m],
                    device_id=(self.dp, partner(self.tp, bit)),
                    device_id_type=MESH,
                )

    def start(self, bit):
        for copy in self.copies(bit):
            copy.start()

    def add(self, bit):
        window = self.n_tp * self.rows
        for copy in self.copies(bit):
            copy.wait_recv()
        for key in self.keys(bit):
            target = key ^ bit

            @pl.loop(0, self.micro * self.rows // STEP)
            def _(r):
                at = pl.multiple_of(r * STEP, STEP)
                m, inner = at // self.rows, at % self.rows
                here = pl.ds(at, STEP)
                there = pl.ds(pl.multiple_of(m * window + target * self.rows + inner, STEP), STEP)
                got = self.got[key - 1, here, :].astype(F32)
                if target == 0:
                    held = self.back[there, :].astype(F32) if bit == 1 else self.own[here, :]
                    self.own[here, :] = held + got
                else:
                    self.back[there, :] = (self.back[there, :].astype(F32) + got).astype(BF)

    def finish(self):
        for bit in self.bits:
            for copy in self.copies(bit):
                copy.wait_send()


def half_of(ref, side, axis):
    lead = (slice(None),) * (axis if axis == 1 else 0)
    return ref.at[lead + (pl.ds(side * LANE, LANE),)]


class SumRing:
    def __init__(self, n, tp, cw, ccw, arrays, gradient, send, recv, free):
        self.n, self.tp, self.ways, self.arrays = n, tp, (cw, ccw), arrays
        self.gradient, self.send, self.recv, self.free = gradient, send, recv, free
        self.slots = arrays[0][3].shape[0]
        self.ready = self.done = 0

    def hop(self, s, a, side):
        axis, _, send, recv, _ = self.arrays[a]
        return pltpu.make_async_remote_copy(
            src_ref=half_of(send.at[s % 2], side, axis),
            dst_ref=half_of(recv.at[s % self.slots], side, axis),
            send_sem=self.send.at[s, a, side],
            recv_sem=self.recv.at[s, a, side],
            device_id=(self.ways[side], self.tp),
            device_id_type=MESH,
        )

    def first(self, a):
        _, part, send, _, _ = self.arrays[a]
        self.gradient(1 % self.n, a)
        send[0] = part[...].astype(BF)
        self.hop(0, a, 0).start()
        self.hop(0, a, 1).start()

    def prepare(self):
        if self.ready == self.done and self.done < self.n - 1:
            self.ready += 1
            for a in range(len(self.arrays)):
                self.gradient((self.ready + 1) % self.n, a)

    def advance(self):
        n = self.n
        if self.done == n - 1:
            return
        self.prepare()
        self.done += 1
        s = self.done
        for a, (axis, part, send, recv, out) in enumerate(self.arrays):
            self.hop(s - 1, a, 0).wait_recv()
            self.hop(s - 1, a, 1).wait_recv()
            total = part[...] + recv[(s - 1) % self.slots].astype(F32)
            if s == n - 1:
                out[...] = total
                continue
            if s >= 2:
                self.hop(s - 2, a, 0).wait_send()
                self.hop(s - 2, a, 1).wait_send()
            send[s % 2] = total.astype(BF)
            for side in range(2):
                if self.slots < n - 1:
                    if s - 1 < n - 1 - self.slots:
                        pl.semaphore_signal(
                            self.free.at[a, side],
                            inc=1,
                            device_id=(self.ways[1 - side], self.tp),
                            device_id_type=MESH,
                        )
                    if s >= self.slots:
                        pl.semaphore_wait(self.free.at[a, side], 1)
                self.hop(s, a, side).start()

    def finish(self):
        for s in range(max(0, self.n - 3), self.n - 1):
            for a in range(len(self.arrays)):
                self.hop(s, a, 0).wait_send()
                self.hop(s, a, 1).wait_send()


def nt(left, right):
    return lax.dot_general(left, right, (((1,), (1,)), ((), ())), preferred_element_type=F32)


def nn(left, right):
    return lax.dot_general(left, right, (((1,), (0,)), ((), ())), preferred_element_type=F32)


def tn(left, right):
    return lax.dot_general(left, right, (((0,), (0,)), ((), ())), preferred_element_type=F32)


def fill_decay(decay_v, col_ref, row_ref, rate_ref):
    heads, window, _ = decay_v.shape
    scale_qk = 1.0 / math.sqrt(HK)
    for h in range(heads):

        @pl.loop(0, window // LANE)
        def _(r):
            here = pl.ds(pl.multiple_of(r * LANE, LANE), LANE)
            col, row = col_ref[here, :], row_ref[...]
            spacing = col - row
            same = jnp.floor(col * (1.0 / LEN)) == jnp.floor(row * (1.0 / LEN))
            kept = jnp.exp(jnp.maximum(spacing, 0.0) * rate_ref[h : h + 1, :]) * scale_qk
            decay_v[h, here, :] = jnp.where((spacing >= 0.0) & same, kept, 0.0)


def gelu_parts(pre_act):
    normal_cdf = 0.5 * (1.0 + lax.erf(pre_act * (1.0 / math.sqrt(2.0))))
    density = jnp.exp(-0.5 * pre_act * pre_act) * (1.0 / math.sqrt(2.0 * math.pi))
    return (pre_act * normal_cdf, normal_cdf + pre_act * density)


def forward_kernel(
    n,
    n_tp,
    q_ref,
    k_ref,
    v_ref,
    g_ref,
    x_ref,
    gain_ref,
    col_ref,
    row_ref,
    rate_ref,
    wo_ref,
    wu_ref,
    wl_ref,
    wd_ref,
    gated_out,
    middle_out,
    hidden_out,
    value_out,
    slope_out,
    second_out,
    wu_out,
    wl_out,
    wd_out,
    decay_v,
    wo_v,
    back_v,
    own_v,
    got_v,
    second_v,
    wu_v,
    wl_v,
    wd_v,
    up_v,
    gelu_v,
    ring_send,
    ring_recv,
    part_send,
    part_recv,
    share_send,
    share_recv,
    local_sem,
):
    total, width = second_v.shape
    mine = x_ref.shape[0]
    window = col_ref.shape[0]
    micro = total // window
    rows = mine // micro
    dp, tp, cw, ccw = neighbours(n)
    bits = bits_of(n_tp)
    greet([(cw, tp), (ccw, tp)] + [(dp, partner(tp, bit)) for bit in bits])

    tall = (wu_v, wl_v)
    shards = (wu_ref, wl_ref, wd_ref)

    def hop(i, a, side):
        if a < 2:
            source = (
                shards[a].at[pl.ds(side * LANE, LANE)]
                if i == 0
                else tall[a].at[pl.ds(i * BLOCK + side * LANE, LANE)]
            )
            target = tall[a].at[pl.ds((i + 1) * BLOCK + side * LANE, LANE)]
        else:
            lanes = pl.ds(side * LANE, LANE)
            source = wd_ref.at[:, lanes] if i == 0 else wd_out.at[i, :, lanes]
            target = wd_out.at[i + 1, :, lanes]
        return pltpu.make_async_remote_copy(
            src_ref=source,
            dst_ref=target,
            send_sem=ring_send.at[i, a, side],
            recv_sem=ring_recv.at[i, a, side],
            device_id=((cw, ccw)[side], tp),
            device_id_type=MESH,
        )

    def ring_step(s):
        for a in range(3):
            for side in range(2):
                hop(s - 1, a, side).wait_recv()
                if s < n - 1:
                    hop(s, a, side).start()

    for a in range(3):
        for side in range(2):
            hop(0, a, side).start()
    local = [
        pltpu.make_async_copy(wo_ref, wo_v, local_sem.at[0]),
        pltpu.make_async_copy(wu_ref, wu_v.at[pl.ds(0, BLOCK)], local_sem.at[1]),
        pltpu.make_async_copy(wl_ref, wl_v.at[pl.ds(0, BLOCK)], local_sem.at[2]),
        pltpu.make_async_copy(wd_ref, wd_v, local_sem.at[3]),
    ]
    for copy in local:
        copy.start()
    fill_decay(decay_v, col_ref, row_ref, rate_ref)
    heads = decay_v.shape[0]
    tile = 256
    for m in range(micro):
        for h in range(heads):
            keys = pl.ds(h * HK, HK)
            values = pl.ds(h * HV, HV)
            inside = pl.ds(m * window, window)

            @pl.loop(0, window // tile)
            def _(r):
                at = pl.multiple_of(r * tile, tile)
                here = pl.ds(pl.multiple_of(m * window + at, tile), tile)
                scores = nt(q_ref[here, keys], k_ref[inside, keys])
                weight = (scores * decay_v[h, pl.ds(at, tile), :]).astype(BF)
                kept = nn(weight, v_ref[inside, values])
                group = lax.rsqrt(jnp.mean(kept * kept, axis=-1, keepdims=True) + GROUP_EPS)
                gate = g_ref[here, values]
                gated_out[here, values] = (gate * jax.nn.sigmoid(gate) * (kept * group)).astype(BF)

    ring_step(1)
    local[0].wait()
    for i in range(n):

        @pl.loop(0, total // tile)
        def _(r):
            here = pl.ds(pl.multiple_of(r * tile, tile), tile)
            back_v[here, pl.ds(i * BLOCK, BLOCK)] = nn(gated_out[here, :], wo_v[i]).astype(BF)

    collect = Collect(dp, tp, n_tp, micro, rows, back_v, got_v, own_v, part_send, part_recv)
    share = Share(dp, tp, n_tp, micro, rows, second_v, share_send, share_recv)
    collect.start(bits[0])
    for copy in local[1:]:
        copy.wait()
    wd_own = pltpu.make_async_copy(wd_v, wd_out.at[0], local_sem.at[3])
    wd_own.start()
    done = 1
    for at, bit in enumerate(bits):
        collect.add(bit)
        if at + 1 < len(bits):
            collect.start(bits[at + 1])
            done += 1
            ring_step(done)

    @pl.loop(0, mine // STEP)
    def _(r):
        at = pl.multiple_of(r * STEP, STEP)
        m, inner = at // rows, at % rows
        here = pl.ds(at, STEP)
        there = pl.ds(pl.multiple_of(m * window + inner, STEP), STEP)
        middle = x_ref[here, :] + own_v[here, :]
        middle_out[here, :] = middle
        scale = lax.rsqrt(jnp.mean(middle * middle, axis=-1, keepdims=True) + EPS)
        second_v[there, :] = (middle * scale * gain_ref[...]).astype(BF)

    share.begin()
    for s in range(done + 1, n // 2 + 1):
        ring_step(s)
    share.relay()
    second_copy = pltpu.make_async_copy(second_v, second_out, local_sem.at[0])
    second_copy.start()
    depth = (n // 2) * BLOCK

    @pl.loop(0, total // tile)
    def _(r):
        here = pl.ds(pl.multiple_of(r * tile, tile), tile)
        left = second_v[here, pl.ds(0, depth)]
        up_v[here, :] = nn(left, wu_v[pl.ds(0, depth), :])
        gelu_v[here, :] = nn(left, wl_v[pl.ds(0, depth), :])

    for s in range(n // 2 + 1, n):
        ring_step(s)
    tall_copies = [
        pltpu.make_async_copy(wu_v, wu_out, local_sem.at[1]),
        pltpu.make_async_copy(wl_v, wl_out, local_sem.at[2]),
    ]
    for copy in tall_copies:
        copy.start()

    @pl.loop(0, total // tile)
    def _(r):
        here = pl.ds(pl.multiple_of(r * tile, tile), tile)
        left = second_v[here, pl.ds(depth, width - depth)]
        up = up_v[here, :] + nn(left, wu_v[pl.ds(depth, width - depth), :])
        gelu_val, gelu_slope = gelu_parts(
            gelu_v[here, :] + nn(left, wl_v[pl.ds(depth, width - depth), :])
        )
        hidden_out[here, :] = (gelu_val * up).astype(BF)
        value_out[here, :] = gelu_val.astype(BF)
        slope_out[here, :] = (up * gelu_slope).astype(BF)

    for i in range(n - 1):
        for a in range(3):
            hop(i, a, 0).wait_send()
            hop(i, a, 1).wait_send()
    collect.finish()
    share.finish()
    for copy in tall_copies + [second_copy, wd_own]:
        copy.wait()


def mid_forward(n, n_tp, q, k, v, g, x_rel, gain, tables, wo, wu, wl, wd):
    total, hv = v.shape
    mine, width = x_rel.shape
    units = wu.shape[1]
    heads = tables[2].shape[0]
    window = tables[0].shape[0]
    shape = jax.ShapeDtypeStruct
    dma = pltpu.SemaphoreType.DMA
    rows_parts = total // window
    return pl.pallas_call(
        functools.partial(forward_kernel, n, n_tp),
        out_shape=(
            shape((total, hv), BF),
            shape((mine, width), F32),
            shape((total, units), BF),
            shape((total, units), BF),
            shape((total, units), BF),
            shape((total, width), BF),
            shape((width, units), BF),
            shape((width, units), BF),
            shape((n, units, BLOCK), BF),
        ),
        in_specs=[vmem()] * 9 + [anyspec()] * 4,
        out_specs=(vmem(),) * 5 + (anyspec(),) * 4,
        scratch_shapes=[
            pltpu.VMEM((heads, window, window), F32),
            pltpu.VMEM(wo.shape, BF),
            pltpu.VMEM((total, width), BF),
            pltpu.VMEM((mine, width), F32),
            pltpu.VMEM((n_tp - 1, mine, width), BF),
            pltpu.VMEM((total, width), BF),
            pltpu.VMEM((width, units), BF),
            pltpu.VMEM((width, units), BF),
            pltpu.VMEM((units, BLOCK), BF),
            pltpu.VMEM((total, units), F32),
            pltpu.VMEM((total, units), F32),
            dma((n - 1, 3, 2)),
            dma((n - 1, 3, 2)),
            dma((n_tp - 1, rows_parts)),
            dma((n_tp - 1, rows_parts)),
            dma((rows_parts, n_tp)),
            dma((rows_parts, n_tp)),
            dma((4,)),
        ],
        compiler_params=pltpu.CompilerParams(
            collective_id=3, has_side_effects=True, vmem_limit_bytes=66_000_000
        ),
        cost_estimate=pl.CostEstimate(
            flops=6 * total * width * units, bytes_accessed=60_000_000, transcendentals=0
        ),
        name="forward_kernel",
    )(q, k, v, g, x_rel, gain, *tables, wo, wu, wl, wd)


def backward_kernel(
    n,
    n_tp,
    gain_ref,
    col_ref,
    row_ref,
    rate_ref,
    cos_ref,
    sin_ref,
    cot_ref,
    wd_ref,
    value_ref,
    slope_ref,
    hidden_ref,
    second_ref,
    wu_ref,
    wl_ref,
    middle_ref,
    cotf_ref,
    wo_ref,
    q_ref,
    k_ref,
    v_ref,
    g_ref,
    dd_out,
    du_out,
    dl_out,
    grad_out,
    mall_out,
    gq_out,
    gk_out,
    gv_out,
    gs_out,
    cot_v,
    w_v,
    gu_v,
    gl_v,
    hidden_v,
    second_v,
    wu_s,
    wl_s,
    middle_v,
    cotf_v,
    q_v,
    k_v,
    v_v,
    g_v,
    gs_v,
    gated_v,
    decay_v,
    gk_acc,
    gv_acc,
    back_v,
    own_v,
    got_v,
    mall_v,
    dd_p,
    du_p,
    dl_p,
    dd_s,
    du_s,
    dl_s,
    dd_r,
    du_r,
    dl_r,
    ring_send,
    ring_recv,
    ring_free,
    part_send,
    part_recv,
    share_send,
    share_recv,
    load_sem,
    local_sem,
):
    total, width = cot_v.shape
    mine = own_v.shape[0]
    window = col_ref.shape[0]
    micro = total // window
    rows = mine // micro
    heads = decay_v.shape[0]
    dp, tp, cw, ccw = neighbours(n)
    bits = bits_of(n_tp)
    greet([(cw, tp), (ccw, tp)] + [(dp, partner(tp, bit)) for bit in bits])

    pairs = (
        (hidden_ref, hidden_v),
        (cot_ref, cot_v),
        (wd_ref, w_v),
        (value_ref, gu_v),
        (slope_ref, gl_v),
        (second_ref, second_v),
        (middle_ref, middle_v),
        (cotf_ref, cotf_v),
        (q_ref, q_v),
        (k_ref, k_v),
        (v_ref, v_v),
        (g_ref, g_v),
    )
    loads = [
        pltpu.make_async_copy(source, target, local_sem.at[at])
        for at, (source, target) in enumerate(pairs)
    ]
    for copy in loads:
        copy.start()

    def block_load(i, a):
        source, target = ((wu_ref, wu_s), (wl_ref, wl_s))[a]
        return pltpu.make_async_copy(
            source.at[pl.ds(i * BLOCK, BLOCK)], target.at[i % 2], load_sem.at[i % 2, a]
        )

    block_load(0, 0).start()
    block_load(0, 1).start()

    def gradient(i, a):
        block = pl.ds(i * BLOCK, BLOCK)
        if a == 0:
            dd_p[...] = tn(hidden_v[...], cot_v[:, block])
        else:
            (du_p, dl_p)[a - 1][...] = tn(second_v[:, block], (gu_v, gl_v)[a - 1][...])

    ring = SumRing(
        n,
        tp,
        cw,
        ccw,
        (
            (1, dd_p, dd_s, dd_r, dd_out),
            (0, du_p, du_s, du_r, du_out),
            (0, dl_p, dl_s, dl_r, dl_out),
        ),
        gradient,
        ring_send,
        ring_recv,
        ring_free,
    )
    loads[0].wait()
    loads[1].wait()
    ring.first(0)
    for copy in loads[2:5]:
        copy.wait()
    tile = 256

    @pl.loop(0, total // tile)
    def _(r):
        here = pl.ds(pl.multiple_of(r * tile, tile), tile)
        grad = None
        for i in range(n):
            term = nt(cot_v[here, pl.ds(i * BLOCK, BLOCK)], w_v[i])
            grad = term if grad is None else grad + term
        gu_v[here, :] = (grad * gu_v[here, :].astype(F32)).astype(BF)
        gl_v[here, :] = (grad * gl_v[here, :].astype(F32)).astype(BF)

    wo_load = pltpu.make_async_copy(wo_ref, w_v, local_sem.at[2])
    wo_load.start()
    loads[5].wait()
    ring.first(1)
    ring.first(2)
    ring.prepare()
    for i in range(n):
        for a in range(2):
            block_load(i, a).wait()
            if i + 1 < n:
                block_load(i + 1, a).start()

        @pl.loop(0, total // tile)
        def _(r):
            here = pl.ds(pl.multiple_of(r * tile, tile), tile)
            back_v[here, pl.ds(i * BLOCK, BLOCK)] = (
                nt(gu_v[here, :], wu_s[i % 2]) + nt(gl_v[here, :], wl_s[i % 2])
            ).astype(BF)

    collect = Collect(dp, tp, n_tp, micro, rows, back_v, got_v, own_v, part_send, part_recv)
    share = Share(dp, tp, n_tp, micro, rows, mall_v, share_send, share_recv)
    collect.start(bits[0])
    ring.advance()
    for at, bit in enumerate(bits):
        collect.add(bit)
        if at + 1 < len(bits):
            collect.start(bits[at + 1])
            ring.advance()
            ring.prepare()
    fill_decay(decay_v, col_ref, row_ref, rate_ref)
    loads[6].wait()
    loads[7].wait()

    @pl.loop(0, mine // STEP)
    def _(r):
        at = pl.multiple_of(r * STEP, STEP)
        m, inner = at // rows, at % rows
        here = pl.ds(at, STEP)
        there = pl.ds(pl.multiple_of(m * window + inner, STEP), STEP)
        middle = middle_v[here, :]
        scale = lax.rsqrt(jnp.mean(middle * middle, axis=-1, keepdims=True) + EPS)
        scaled = own_v[here, :] * gain_ref[...]
        inside = jnp.mean(scaled * middle, axis=-1, keepdims=True)
        grad = cotf_v[here, :] + scale * (scaled - middle * (scale * scale * inside))
        cotf_v[here, :] = grad
        mall_v[there, :] = grad.astype(BF)

    share.begin()
    grad_copy = pltpu.make_async_copy(cotf_v, grad_out, local_sem.at[7])
    grad_copy.start()
    ring.advance()
    ring.prepare()
    for copy in loads[8:]:
        copy.wait()
    wo_load.wait()
    share.relay()
    mall_copy = pltpu.make_async_copy(mall_v, mall_out, local_sem.at[6])
    mall_copy.start()
    half = HK // 2
    for m in range(micro):
        ring.advance()

        @pl.loop(0, window // tile)
        def _(r):
            at = pl.multiple_of(r * tile, tile)
            here = pl.ds(pl.multiple_of(m * window + at, tile), tile)
            grad = None
            for i in range(n):
                term = nt(mall_v[here, pl.ds(i * BLOCK, BLOCK)], w_v[i])
                grad = term if grad is None else grad + term
            gated_v[pl.ds(at, tile), :] = grad

        ring.prepare()
        for h in range(heads):
            keys = pl.ds(h * HK, HK)
            values = pl.ds(h * HV, HV)
            inside = pl.ds(m * window, window)
            gk_acc[...] = jnp.zeros_like(gk_acc)
            gv_acc[...] = jnp.zeros_like(gv_acc)

            @pl.loop(0, window // tile)
            def _(r):
                at = pl.multiple_of(r * tile, tile)
                local = pl.ds(at, tile)
                here = pl.ds(pl.multiple_of(m * window + at, tile), tile)
                decay = decay_v[h, local, :]
                query = q_v[here, keys]
                weight = (nt(query, k_v[inside, keys]) * decay).astype(BF)
                kept = nn(weight, v_v[inside, values])
                group = lax.rsqrt(jnp.mean(kept * kept, axis=-1, keepdims=True) + GROUP_EPS)
                gate = g_v[here, values]
                sigmoid = jax.nn.sigmoid(gate)
                grad = gated_v[local, values]
                gs_v[here, values] = (
                    grad * (kept * group) * (sigmoid * (1.0 + gate * (1.0 - sigmoid)))
                ).astype(BF)
                lifted = grad * (gate * sigmoid)
                mean = jnp.mean(lifted * kept, axis=-1, keepdims=True)
                grad_kept = (group * (lifted - kept * (group * group * mean))).astype(BF)
                gv_acc[...] += tn(weight, grad_kept)
                score = (nt(grad_kept, v_v[inside, values]) * decay).astype(BF)
                gk_acc[...] += tn(score, query)
                turned = nn(score, k_v[inside, keys])
                low, high = turned[:, :half], turned[:, half:]
                cosine, sine = cos_ref[local, :], sin_ref[local, :]
                q_v[here, pl.ds(h * HK, half)] = (low * cosine + high * sine).astype(BF)
                q_v[here, pl.ds(h * HK + half, half)] = (high * cosine - low * sine).astype(BF)

            low, high = gk_acc[:, :half], gk_acc[:, half:]
            cosine, sine = cos_ref[...], sin_ref[...]
            k_v[inside, pl.ds(h * HK, half)] = (low * cosine + high * sine).astype(BF)
            k_v[inside, pl.ds(h * HK + half, half)] = (high * cosine - low * sine).astype(BF)
            v_v[inside, values] = gv_acc[...].astype(BF)
            if h == 0:
                ring.advance()
                ring.prepare()
    stores = [
        pltpu.make_async_copy(source, target, local_sem.at[8 + at])
        for at, (source, target) in enumerate(
            ((q_v, gq_out), (k_v, gk_out), (v_v, gv_out), (gs_v, gs_out))
        )
    ]
    for copy in stores:
        copy.start()
    for _ in range(n):
        ring.advance()
    ring.finish()
    collect.finish()
    share.finish()
    for copy in stores + [grad_copy, mall_copy]:
        copy.wait()


def mid_backward(n, n_tp, gain, tables, cosine, sine, cot, wd, value, slope, hidden, second,
                 wu, wl, middle, cot_rel, wo, q, k, v, g):
    total, width = cot.shape
    mine = middle.shape[0]
    units, hv, hk = wu.shape[1], v.shape[1], q.shape[1]
    heads = tables[2].shape[0]
    window = tables[0].shape[0]
    micro = total // window
    shape = jax.ShapeDtypeStruct
    dma = pltpu.SemaphoreType.DMA
    block_shapes = ((units, BLOCK), (BLOCK, units), (BLOCK, units))
    return pl.pallas_call(
        functools.partial(backward_kernel, n, n_tp),
        out_shape=tuple(shape(s, F32) for s in block_shapes)
        + (
            shape((mine, width), F32),
            shape((total, width), BF),
            shape((total, hk), BF),
            shape((total, hk), BF),
            shape((total, hv), BF),
            shape((total, hv), BF),
        ),
        in_specs=[vmem()] * 6 + [anyspec()] * 15,
        out_specs=(vmem(),) * 3 + (anyspec(),) * 6,
        scratch_shapes=[
            pltpu.VMEM((total, width), BF),
            pltpu.VMEM(wd.shape, BF),
            pltpu.VMEM((total, units), BF),
            pltpu.VMEM((total, units), BF),
            pltpu.VMEM((total, units), BF),
            pltpu.VMEM((total, width), BF),
            pltpu.VMEM((2, BLOCK, units), BF),
            pltpu.VMEM((2, BLOCK, units), BF),
            pltpu.VMEM((mine, width), F32),
            pltpu.VMEM((mine, width), F32),
            pltpu.VMEM((total, hk), BF),
            pltpu.VMEM((total, hk), BF),
            pltpu.VMEM((total, hv), BF),
            pltpu.VMEM((total, hv), F32),
            pltpu.VMEM((total, hv), BF),
            pltpu.VMEM((window, hv), F32),
            pltpu.VMEM((heads, window, window), F32),
            pltpu.VMEM((window, HK), F32),
            pltpu.VMEM((window, HV), F32),
            pltpu.VMEM((total, width), BF),
            pltpu.VMEM((mine, width), F32),
            pltpu.VMEM((n_tp - 1, mine, width), BF),
            pltpu.VMEM((total, width), BF),
        ]
        + [pltpu.VMEM(s, F32) for s in block_shapes]
        + [pltpu.VMEM((2,) + s, BF) for s in block_shapes]
        + [pltpu.VMEM((2,) + s, BF) for s in block_shapes]
        + [
            dma((n - 1, 3, 2)),
            dma((n - 1, 3, 2)),
            pltpu.SemaphoreType.REGULAR((3, 2)),
            dma((n_tp - 1, micro)),
            dma((n_tp - 1, micro)),
            dma((micro, n_tp)),
            dma((micro, n_tp)),
            dma((2, 2)),
            dma((12,)),
        ],
        compiler_params=pltpu.CompilerParams(
            collective_id=4, has_side_effects=True, vmem_limit_bytes=67_000_000
        ),
        cost_estimate=pl.CostEstimate(
            flops=16 * total * width * units, bytes_accessed=80_000_000, transcendentals=0
        ),
        name="backward_kernel",
    )(gain, *tables, cosine, sine, cot, wd, value, slope, hidden, second, wu, wl, middle,
      cot_rel, wo, q, k, v, g)


def out_kernel(
    n,
    n_tp,
    gq_ref,
    gk_ref,
    gv_ref,
    gs_ref,
    gain_ref,
    nall_ref,
    gated_ref,
    mall_ref,
    mid_ref,
    x_ref,
    wq_ref,
    wk_ref,
    wv_ref,
    wg_ref,
    dq_out,
    dk_out,
    dv_out,
    ds_out,
    do_out,
    rows_out,
    nall_v,
    gated_v,
    mall_v,
    mid_v,
    x_v,
    dq_p,
    dk_p,
    dv_p,
    ds_p,
    do_p,
    dq_s,
    dk_s,
    dv_s,
    ds_s,
    do_s,
    dq_r,
    dk_r,
    dv_r,
    ds_r,
    do_r,
    wq_s,
    wk_s,
    wv_s,
    wg_s,
    back_v,
    own_v,
    got_v,
    ring_send,
    ring_recv,
    ring_free,
    part_send,
    part_recv,
    load_sem,
    local_sem,
):
    micro, rows, width = rows_out.shape
    total = nall_v.shape[0]
    mine = micro * rows
    dp, tp, cw, ccw = neighbours(n)
    pos = ring_position(dp, n)
    bits = bits_of(n_tp)
    greet([(cw, tp), (ccw, tp)] + [(dp, partner(tp, bit)) for bit in bits])

    grads = (gq_ref, gk_ref, gv_ref, gs_ref)
    products = (dq_p, dk_p, dv_p, ds_p)
    wholes = (wq_ref, wk_ref, wv_ref, wg_ref)
    slots = (wq_s, wk_s, wv_s, wg_s)
    loads = [
        pltpu.make_async_copy(source, target, local_sem.at[at])
        for at, (source, target) in enumerate(
            (
                (nall_ref, nall_v),
                (gated_ref, gated_v),
                (mall_ref, mall_v),
                (mid_ref, mid_v),
                (x_ref, x_v),
            )
        )
    ]
    for copy in loads:
        copy.start()

    def load(i, a):
        return pltpu.make_async_copy(
            wholes[a].at[pl.ds(i * BLOCK, BLOCK)], slots[a].at[i % 2], load_sem.at[i % 2, a]
        )

    for a in range(4):
        load(0, a).start()

    def gradient(i, a):
        block = pl.ds(i * BLOCK, BLOCK)
        if a < 4:
            products[a][...] = tn(nall_v[:, block], grads[a][...])
        else:
            do_p[...] = tn(gated_v[...], mall_v[:, block])

    ring = SumRing(
        n,
        tp,
        cw,
        ccw,
        (
            (0, dq_p, dq_s, dq_r, dq_out),
            (0, dk_p, dk_s, dk_r, dk_out),
            (0, dv_p, dv_s, dv_r, dv_out),
            (0, ds_p, ds_s, ds_r, ds_out),
            (1, do_p, do_s, do_r, do_out),
        ),
        gradient,
        ring_send,
        ring_recv,
        ring_free,
    )
    tile = 256

    def backward(i):
        for a in range(4):
            load(i, a).wait()
            if i + 1 < n:
                load(i + 1, a).start()

        @pl.loop(0, total // tile)
        def _(r):
            here = pl.ds(pl.multiple_of(r * tile, tile), tile)
            block = None
            for a in range(4):
                term = nt(grads[a][here, :], slots[a][i % 2])
                block = term if block is None else block + term
            back_v[here, pl.ds(i * BLOCK, BLOCK)] = block.astype(BF)

    def natural(i, side):
        at = ring_index((pos + (n - i if side == 0 else i)) % n, n) * BLOCK + side * LANE
        return pl.ds(pl.multiple_of(at, LANE), LANE)

    def finish_rows():
        @pl.loop(0, mine // STEP)
        def _(r):
            at = pl.multiple_of(r * STEP, STEP)
            m, inner = at // rows, pl.multiple_of(at % rows, STEP)
            here = pl.ds(at, STEP)
            x = x_v[here, :]
            scale = lax.rsqrt(jnp.mean(x * x, axis=-1, keepdims=True) + EPS)
            inside = jnp.mean(own_v[here, :] * gain_ref[...] * x, axis=-1, keepdims=True)
            slope = scale * scale * inside
            for i in range(n):
                for side in range(2):
                    lanes = pl.ds(i * BLOCK + side * LANE, LANE)
                    scaled = own_v[here, lanes] * gain_ref[:, lanes]
                    rows_out[m, pl.ds(inner, STEP), natural(i, side)] = mid_v[
                        here, lanes
                    ] + scale * (scaled - x_v[here, lanes] * slope)

    collect = Collect(dp, tp, n_tp, micro, rows, back_v, got_v, own_v, part_send, part_recv)
    loads[0].wait()
    for a in range(4):
        ring.first(a)
    loads[1].wait()
    loads[2].wait()
    ring.first(4)
    ring.prepare()
    for i in range(n):
        backward(i)
        if i % 3 == 2:
            ring.advance()
            ring.prepare()
    collect.start(bits[0])
    ring.advance()
    ring.prepare()
    for at, bit in enumerate(bits):
        collect.add(bit)
        if at + 1 < len(bits):
            collect.start(bits[at + 1])
            ring.advance()
            ring.prepare()
            ring.advance()
            ring.prepare()
    loads[3].wait()
    loads[4].wait()
    finish_rows()
    for _ in range(n):
        ring.advance()
    ring.finish()
    collect.finish()


def project_back(n, n_tp, rows, grads, gain, normed, gated, middle_all, grad_middle, x_rel, weights):
    total, width = normed.shape
    mine = x_rel.shape[0]
    micro = mine // rows
    blocks = [(BLOCK, g.shape[1]) for g in grads] + [(gated.shape[1], BLOCK)]
    shape = jax.ShapeDtypeStruct
    dma = pltpu.SemaphoreType.DMA
    return pl.pallas_call(
        functools.partial(out_kernel, n, n_tp),
        out_shape=tuple(shape(s, F32) for s in blocks) + (shape((micro, rows, width), F32),),
        in_specs=[vmem()] * 5 + [anyspec()] * 9,
        out_specs=(vmem(),) * 6,
        scratch_shapes=[
            pltpu.VMEM((total, width), BF),
            pltpu.VMEM(gated.shape, BF),
            pltpu.VMEM((total, width), BF),
            pltpu.VMEM((mine, width), F32),
            pltpu.VMEM((mine, width), F32),
        ]
        + [pltpu.VMEM(s, F32) for s in blocks]
        + [pltpu.VMEM((2,) + s, BF) for s in blocks]
        + [pltpu.VMEM((2,) + s, BF) for s in blocks]
        + [pltpu.VMEM((2,) + s, BF) for s in blocks[:4]]
        + [
            pltpu.VMEM((total, width), BF),
            pltpu.VMEM((mine, width), F32),
            pltpu.VMEM((n_tp - 1, mine, width), BF),
            dma((n - 1, 5, 2)),
            dma((n - 1, 5, 2)),
            pltpu.SemaphoreType.REGULAR((5, 2)),
            dma((n_tp - 1, micro)),
            dma((n_tp - 1, micro)),
            dma((2, 4)),
            dma((5,)),
        ],
        compiler_params=pltpu.CompilerParams(
            collective_id=2, has_side_effects=True, vmem_limit_bytes=66_000_000
        ),
        cost_estimate=pl.CostEstimate(
            flops=4 * total * width * sum(s[1] for s in blocks),
            bytes_accessed=60_000_000,
            transcendentals=0,
        ),
        name="out_kernel",
    )(*grads, gain, normed, gated, middle_all, grad_middle, x_rel, *weights)


def normalize(row_block, gain_vec):
    row_scale = lax.rsqrt(jnp.mean(row_block * row_block, axis=-1, keepdims=True) + EPS)
    return (row_block * row_scale * gain_vec.astype(jnp.float32), row_scale)


def norm_back(grad_rows, row_block, row_scale, gain_vec):
    scaled_grad = grad_rows * gain_vec.astype(jnp.float32)
    back_rows = row_scale * (
        scaled_grad
        - row_block
        * row_scale
        * row_scale
        * jnp.mean(scaled_grad * row_block, axis=-1, keepdims=True)
    )
    return (back_rows, jnp.sum(grad_rows * row_block * row_scale, axis=0))


def angles(length, feature_width):
    half_width = feature_width // 2
    frequency = jnp.exp(-math.log(10000.0) * jnp.arange(half_width, dtype=jnp.float32) / half_width)
    turns = jnp.arange(length, dtype=jnp.float32)[:, None] * frequency[None, :]
    return (jnp.cos(turns)[:, None, :], jnp.sin(turns)[:, None, :])


def decays(length, head_ids):
    places = jnp.arange(length, dtype=jnp.float32)
    spacing = places[:, None] - places[None, :]
    log_rate = jnp.log(1.0 - jnp.exp2(-5.0 - head_ids))
    return jnp.where(
        spacing[None] >= 0.0,
        jnp.exp(jnp.maximum(spacing, 0.0)[None] * log_rate[:, None, None]),
        0.0,
    )


def rotate(value_vectors, cosine_table, sine_table):
    half_width = value_vectors.shape[-1] // 2
    lower = value_vectors[..., :half_width]
    upper = value_vectors[..., half_width:]
    return jnp.concatenate(
        [lower * cosine_table - upper * sine_table, upper * cosine_table + lower * sine_table],
        axis=-1,
    )


def unrotate(value_vectors, cosine_table, sine_table):
    half_width = value_vectors.shape[-1] // 2
    lower = value_vectors[..., :half_width]
    upper = value_vectors[..., half_width:]
    return jnp.concatenate(
        [lower * cosine_table + upper * sine_table, upper * cosine_table - lower * sine_table],
        axis=-1,
    )


def plain_gelu_parts(pre_act):
    normal_cdf = 0.5 * (1.0 + lax.erf(pre_act * (1.0 / math.sqrt(2.0))))
    density = jnp.exp(-0.5 * pre_act * pre_act) * (1.0 / math.sqrt(2.0 * math.pi))
    return (pre_act * normal_cdf, normal_cdf + pre_act * density)


def inner_rows(left_rows, right_rows):
    return lax.dot_general(
        left_rows, right_rows, (((0,), (0,)), ((), ())), preferred_element_type=jnp.float32
    )


def times_t(left_rows, right_rows):
    return lax.dot_general(
        left_rows, right_rows, (((1,), (1,)), ((), ())), preferred_element_type=jnp.float32
    )


def forward_pass(rows_in, gathered, cosine_table, sine_table, decay_mask):
    (
        first_gain,
        second_gain,
        query_weight,
        key_weight,
        value_weight,
        swish_weight,
        output_weight,
        up_projection_matrix,
        gelu_weight,
        down_weight,
    ) = gathered
    local_heads = decay_mask.shape[0]
    scale_qk = 1.0 / math.sqrt(HK)
    normed, first_scale = normalize(rows_in, first_gain)
    normed_all = lax.all_gather(normed.astype(jnp.bfloat16), "tensor", axis=0, tiled=True)
    total_rows = normed_all.shape[0]
    sequences = total_rows // LEN
    query_turned_rows = rotate(
        jnp.dot(normed_all, query_weight, preferred_element_type=jnp.float32).reshape(
            sequences, LEN, local_heads, HK
        ),
        cosine_table,
        sine_table,
    ).astype(jnp.bfloat16)
    key_turned_rows = rotate(
        jnp.dot(normed_all, key_weight, preferred_element_type=jnp.float32).reshape(
            sequences, LEN, local_heads, HK
        ),
        cosine_table,
        sine_table,
    ).astype(jnp.bfloat16)
    value_rows = (
        jnp.dot(normed_all, value_weight, preferred_element_type=jnp.float32)
        .astype(jnp.bfloat16)
        .reshape(sequences, LEN, local_heads, HV)
    )
    gate_pre = jnp.dot(normed_all, swish_weight, preferred_element_type=jnp.float32)
    unscaled_logits = jnp.einsum(
        "snhd,smhd->shnm", query_turned_rows, key_turned_rows, preferred_element_type=jnp.float32
    )
    weight_bf = (unscaled_logits * (decay_mask * scale_qk)).astype(jnp.bfloat16)
    retained = jnp.einsum(
        "shnm,smhe->snhe", weight_bf, value_rows, preferred_element_type=jnp.float32
    )
    group_scale = lax.rsqrt(jnp.mean(retained * retained, axis=-1, keepdims=True) + GROUP_EPS)
    grouped = (retained * group_scale).reshape(total_rows, local_heads * HV)
    sigmoid_gate = jax.nn.sigmoid(gate_pre)
    swish_val = gate_pre * sigmoid_gate
    gated_rows = (swish_val * grouped).astype(jnp.bfloat16)
    attention = lax.psum_scatter(
        jnp.dot(gated_rows, output_weight, preferred_element_type=jnp.float32),
        "tensor",
        scatter_dimension=0,
        tiled=True,
    )
    middle = rows_in + attention
    second, second_scale = normalize(middle, second_gain)
    second_all = lax.all_gather(second.astype(jnp.bfloat16), "tensor", axis=0, tiled=True)
    up_pre = jnp.dot(second_all, up_projection_matrix, preferred_element_type=jnp.float32)
    gelu_pre = jnp.dot(second_all, gelu_weight, preferred_element_type=jnp.float32)
    gelu_val, gelu_slope = plain_gelu_parts(gelu_pre)
    hidden = (gelu_val * up_pre).astype(jnp.bfloat16)
    block_rows = middle + lax.psum_scatter(
        jnp.dot(hidden, down_weight, preferred_element_type=jnp.float32).astype(jnp.bfloat16),
        "tensor",
        scatter_dimension=0,
        tiled=True,
    ).astype(jnp.float32)
    kept_state = (
        rows_in,
        first_scale,
        normed_all,
        query_turned_rows,
        key_turned_rows,
        value_rows,
        gate_pre,
        weight_bf,
        retained,
        group_scale,
        grouped,
        gated_rows,
        middle,
        second_scale,
        second_all,
        up_pre,
        gelu_val,
        gelu_slope,
        hidden,
    )
    return (block_rows, kept_state)


def backward_pass(kept_state, cot_in, gathered, cosine_table, sine_table, decay_mask):
    (
        first_gain,
        second_gain,
        query_weight,
        key_weight,
        value_weight,
        swish_weight,
        output_weight,
        up_projection_matrix,
        gelu_weight,
        down_weight,
    ) = gathered
    (
        rows_in,
        first_scale,
        normed_all,
        query_turned_rows,
        key_turned_rows,
        value_rows,
        gate_pre,
        weight_bf,
        retained,
        group_scale,
        grouped,
        gated_rows,
        middle,
        second_scale,
        second_all,
        up_pre,
        gelu_val,
        gelu_slope,
        hidden,
    ) = kept_state
    local_heads = decay_mask.shape[0]
    total_rows = normed_all.shape[0]
    scale_qk = 1.0 / math.sqrt(HK)
    cot_all = lax.all_gather(cot_in.astype(jnp.bfloat16), "tensor", axis=0, tiled=True)
    grad_hidden = times_t(cot_all, down_weight)
    grad_down = inner_rows(hidden, cot_all)
    grad_uppre = (grad_hidden * gelu_val).astype(jnp.bfloat16)
    grad_gelupre = (grad_hidden * up_pre * gelu_slope).astype(jnp.bfloat16)
    grad_up = inner_rows(second_all, grad_uppre)
    grad_gelu = inner_rows(second_all, grad_gelupre)
    second_back = lax.psum_scatter(
        times_t(grad_uppre, up_projection_matrix) + times_t(grad_gelupre, gelu_weight),
        "tensor",
        scatter_dimension=0,
        tiled=True,
    )
    middle_back, grad_gain_two = norm_back(second_back, middle, second_scale, second_gain)
    grad_middle = cot_in + middle_back
    middle_all = lax.all_gather(grad_middle.astype(jnp.bfloat16), "tensor", axis=0, tiled=True)
    grad_gated = times_t(middle_all, output_weight)
    grad_out = inner_rows(gated_rows, middle_all)
    sigmoid_gate = jax.nn.sigmoid(gate_pre)
    swish_val = gate_pre * sigmoid_gate
    grad_swishpre = (
        grad_gated * grouped * (sigmoid_gate * (1.0 + gate_pre * (1.0 - sigmoid_gate)))
    ).astype(jnp.bfloat16)
    grad_grouped = (grad_gated * swish_val).reshape(retained.shape)
    grad_retained = (
        group_scale
        * (
            grad_grouped
            - retained
            * group_scale
            * group_scale
            * jnp.mean(grad_grouped * retained, axis=-1, keepdims=True)
        )
    ).astype(jnp.bfloat16)
    grad_valrows = jnp.einsum(
        "shnm,snhe->smhe", weight_bf, grad_retained, preferred_element_type=jnp.float32
    ).astype(jnp.bfloat16)
    grad_weight = jnp.einsum(
        "snhe,smhe->shnm", grad_retained, value_rows, preferred_element_type=jnp.float32
    )
    grad_retention_logits = (grad_weight * (decay_mask * scale_qk)).astype(jnp.bfloat16)
    grad_query_rotated_rows = jnp.einsum(
        "shnm,smhd->snhd",
        grad_retention_logits,
        key_turned_rows,
        preferred_element_type=jnp.float32,
    )
    grad_key_rotated_rows = jnp.einsum(
        "shnm,snhd->smhd",
        grad_retention_logits,
        query_turned_rows,
        preferred_element_type=jnp.float32,
    )
    grad_qpre = (
        unrotate(grad_query_rotated_rows, cosine_table, sine_table)
        .astype(jnp.bfloat16)
        .reshape(total_rows, local_heads * HK)
    )
    grad_kpre = (
        unrotate(grad_key_rotated_rows, cosine_table, sine_table)
        .astype(jnp.bfloat16)
        .reshape(total_rows, local_heads * HK)
    )
    grad_vflat = grad_valrows.reshape(total_rows, local_heads * HV)
    first_back = lax.psum_scatter(
        times_t(grad_qpre, query_weight)
        + times_t(grad_kpre, key_weight)
        + times_t(grad_vflat, value_weight)
        + times_t(grad_swishpre, swish_weight),
        "tensor",
        scatter_dimension=0,
        tiled=True,
    )
    grad_query = inner_rows(normed_all, grad_qpre)
    grad_key = inner_rows(normed_all, grad_kpre)
    grad_value = inner_rows(normed_all, grad_vflat)
    grad_swish = inner_rows(normed_all, grad_swishpre)
    input_back, grad_gain_one = norm_back(first_back, rows_in, first_scale, first_gain)
    grad_rows = grad_middle + input_back
    pieces = (
        grad_gain_one,
        grad_gain_two,
        grad_query,
        grad_key,
        grad_value,
        grad_swish,
        grad_out,
        grad_up,
        grad_gelu,
        grad_down,
    )
    return (grad_rows, pieces)


def plain_body(
    block_input,
    cotangent,
    first_gain,
    second_gain,
    query_weight,
    key_weight,
    value_weight,
    swish_weight,
    output_weight,
    up_projection_matrix,
    gelu_weight,
    down_weight,
):
    local_heads = query_weight.shape[1] // HK
    head_ids = (lax.axis_index("tensor") * local_heads + jnp.arange(local_heads)).astype(
        jnp.float32
    )
    cosine_table, sine_table = angles(LEN, HK)
    decay_mask = decays(LEN, head_ids)
    output_list = []
    grad_list = []
    totals = ()
    for micro_idx in range(block_input.shape[0]):
        forward_set = (
            lax.all_gather(first_gain, "dp", axis=0, tiled=True),
            lax.all_gather(second_gain, "dp", axis=0, tiled=True),
            lax.all_gather(query_weight, "dp", axis=0, tiled=True),
            lax.all_gather(key_weight, "dp", axis=0, tiled=True),
            lax.all_gather(value_weight, "dp", axis=0, tiled=True),
            lax.all_gather(swish_weight, "dp", axis=0, tiled=True),
            lax.all_gather(output_weight, "dp", axis=1, tiled=True),
            lax.all_gather(up_projection_matrix, "dp", axis=0, tiled=True),
            lax.all_gather(gelu_weight, "dp", axis=0, tiled=True),
            lax.all_gather(down_weight, "dp", axis=1, tiled=True),
        )
        block_rows, kept_state = forward_pass(
            block_input[micro_idx], forward_set, cosine_table, sine_table, decay_mask
        )
        held = lax.optimization_barrier(
            (
                (
                    first_gain,
                    second_gain,
                    query_weight,
                    key_weight,
                    value_weight,
                    swish_weight,
                    output_weight,
                    up_projection_matrix,
                    gelu_weight,
                    down_weight,
                ),
                block_rows,
            )
        )[0]
        backward_set = (
            lax.all_gather(held[0], "dp", axis=0, tiled=True),
            lax.all_gather(held[1], "dp", axis=0, tiled=True),
            lax.all_gather(held[2], "dp", axis=0, tiled=True),
            lax.all_gather(held[3], "dp", axis=0, tiled=True),
            lax.all_gather(held[4], "dp", axis=0, tiled=True),
            lax.all_gather(held[5], "dp", axis=0, tiled=True),
            lax.all_gather(held[6], "dp", axis=1, tiled=True),
            lax.all_gather(held[7], "dp", axis=0, tiled=True),
            lax.all_gather(held[8], "dp", axis=0, tiled=True),
            lax.all_gather(held[9], "dp", axis=1, tiled=True),
        )
        grad_rows, pieces = backward_pass(
            kept_state, cotangent[micro_idx], backward_set, cosine_table, sine_table, decay_mask
        )
        output_list.append(block_rows)
        grad_list.append(grad_rows)
        if micro_idx == 0:
            totals = tuple(pieces)
        else:
            totals = tuple((total + piece for total, piece in zip(totals, pieces)))
    totals = (
        lax.psum_scatter(totals[0], "dp", scatter_dimension=0, tiled=True),
        lax.psum_scatter(totals[1], "dp", scatter_dimension=0, tiled=True),
        lax.psum_scatter(totals[2], "dp", scatter_dimension=0, tiled=True),
        lax.psum_scatter(totals[3], "dp", scatter_dimension=0, tiled=True),
        lax.psum_scatter(totals[4], "dp", scatter_dimension=0, tiled=True),
        lax.psum_scatter(totals[5], "dp", scatter_dimension=0, tiled=True),
        lax.psum_scatter(totals[6], "dp", scatter_dimension=1, tiled=True),
        lax.psum_scatter(totals[7], "dp", scatter_dimension=0, tiled=True),
        lax.psum_scatter(totals[8], "dp", scatter_dimension=0, tiled=True),
        lax.psum_scatter(totals[9], "dp", scatter_dimension=1, tiled=True),
    )
    gain_first, gain_second = lax.psum((totals[0], totals[1]), "tensor")
    return (
        jnp.stack(output_list, axis=0),
        jnp.stack(grad_list, axis=0),
        gain_first,
        gain_second,
        totals[2],
        totals[3],
        totals[4],
        totals[5],
        totals[6],
        totals[7],
        totals[8],
        totals[9],
    )


def ring_body(
    n_dp,
    n_tp,
    block_input,
    cotangent,
    first_gain,
    second_gain,
    query_weight,
    key_weight,
    value_weight,
    swish_weight,
    output_weight,
    up_projection_matrix,
    gelu_weight,
    down_weight,
):
    micro, rows, width = block_input.shape
    local_heads = query_weight.shape[1] // HK
    window = n_tp * rows

    me = lax.axis_index("tensor")
    head_ids = (me * local_heads + jnp.arange(local_heads)).astype(F32)
    chunk_of = jnp.arange(n_tp) ^ me
    natural = (chunk_of[:, None] * rows + jnp.arange(rows)[None, :]).reshape(window)
    place = (natural % LEN).astype(F32)
    half_key = HK // 2
    frequency = jnp.exp(-math.log(10000.0) * jnp.arange(half_key, dtype=F32) / half_key)
    turns = place[:, None] * frequency[None, :]
    cosine, sine = jnp.cos(turns), jnp.sin(turns)
    log_rate = jnp.log(1.0 - jnp.exp2(-5.0 - head_ids))
    spots = natural.astype(F32)
    tables = (
        spots[:, None],
        spots[None, :],
        jnp.broadcast_to(log_rate[:, None], (local_heads, window)),
    )

    gains_own = jnp.stack([first_gain, second_gain]).astype(F32)
    query, key, value, gate, x_rel, cot_rel, gains, normed, cot_all, *w_in, w_o = project_in(
        n_dp,
        n_tp,
        block_input,
        cotangent,
        gains_own,
        cosine,
        sine,
        (query_weight, key_weight, value_weight, swish_weight),
        output_weight,
    )
    gated, middle, hidden, gelu_val, up_slope, second, w_u, w_l, w_d = mid_forward(
        n_dp,
        n_tp,
        query,
        key,
        value,
        gate,
        x_rel,
        gains[1:2],
        tables,
        w_o,
        up_projection_matrix,
        gelu_weight,
        down_weight,
    )

    def swap(array, bit):
        return lax.ppermute(array, "tensor", [(i, i ^ bit) for i in range(n_tp)])

    partial = jnp.einsum("rc,ncb->rnb", hidden, w_d, preferred_element_type=F32)
    partial = partial.astype(BF).reshape(micro, n_tp, rows, width)
    chunks = {j: partial[:, j] for j in range(n_tp)}
    for bit in bits_of(n_tp):
        odd = [j for j in sorted(chunks) if j & bit]
        moved = swap(jnp.stack([chunks[j] for j in odd]), bit)
        for at, j in enumerate(odd):
            chunks[j ^ bit] = chunks[j ^ bit].astype(F32) + moved[at].astype(F32)
            del chunks[j]
        if len(chunks) > 1:
            chunks = {j: part.astype(BF) for j, part in chunks.items()}
    block_rows = middle.reshape(micro, rows, width) + chunks[0].astype(F32)

    grad_down, grad_up, grad_gelu, grad_middle, middle_all, grad_q, grad_k, grad_v, grad_s = (
        mid_backward(
            n_dp,
            n_tp,
            gains[1:2],
            tables,
            cosine,
            sine,
            cot_all,
            w_d,
            gelu_val,
            up_slope,
            hidden,
            second,
            w_u,
            w_l,
            middle,
            cot_rel,
            w_o,
            query,
            key,
            value,
            gate,
        )
    )
    grad_query, grad_key, grad_value, grad_swish, grad_out, grad_rows = project_back(
        n_dp,
        n_tp,
        rows,
        (grad_q, grad_k, grad_v, grad_s),
        gains[0:1],
        normed,
        gated,
        middle_all,
        grad_middle,
        x_rel,
        w_in,
    )

    def gain_sum(*pairs):
        return sum(jnp.sum(w.astype(F32) * g, axis=1) for w, g in pairs)

    sum_one = gain_sum(
        (query_weight, grad_query),
        (key_weight, grad_key),
        (value_weight, grad_value),
        (swish_weight, grad_swish),
    )
    sum_two = gain_sum((up_projection_matrix, grad_up), (gelu_weight, grad_gelu))
    gain_grads = jnp.stack([sum_one, sum_two])
    for bit in bits_of(n_tp):
        gain_grads = gain_grads + swap(gain_grads, bit)
    gain_grads = gain_grads / gains_own

    dp = lax.axis_index("dp")
    position = ring_position(dp, n_dp)
    spot = ring_position(jnp.arange(n_dp), n_dp)
    low = 2 * ((position - spot + n_dp) % n_dp)
    high = 2 * ((spot - position + n_dp) % n_dp) + 1
    back = jnp.stack([low, high], axis=1).reshape(2 * n_dp)
    split = block_rows.reshape(micro, rows, 2 * n_dp, LANE)
    block_rows = jnp.take(split, back, axis=2).reshape(micro, rows, width)

    return (
        block_rows,
        grad_rows,
        gain_grads[0],
        gain_grads[1],
        grad_query,
        grad_key,
        grad_value,
        grad_swish,
        grad_out,
        grad_up,
        grad_gelu,
        grad_down,
    )


def solution(mesh):
    rows = P(None, ("dp", "tensor"), None)
    wide, tall, gain = P("dp", "tensor"), P("tensor", "dp"), P("dp")
    n_dp, n_tp = mesh.shape["dp"], mesh.shape["tensor"]

    def run(*arrays):
        blocks = arrays[2].shape[0] == BLOCK and n_dp % 2 == 0 and n_dp > 2
        pairs = n_tp > 1 and n_tp & (n_tp - 1) == 0
        aligned = (n_tp * arrays[0].shape[1]) % LEN == 0 and arrays[0].shape[1] % LANE == 0
        if blocks and pairs and aligned:
            return ring_body(n_dp, n_tp, *arrays)
        return plain_body(*arrays)

    return jax.shard_map(
        run,
        mesh=mesh,
        in_specs=(rows, rows, gain, gain) + (wide,) * 4 + (tall, wide, wide, tall),
        out_specs=(rows, rows, gain, gain) + (wide,) * 4 + (tall, wide, wide, tall),
        check_vma=False,
    )
```

```python
import functools
import math

import jax
import jax.numpy as jnp
from jax import lax
from jax.experimental import pallas as pl
from jax.experimental.pallas import tpu as pltpu
from jax.sharding import PartitionSpec as P

HK = 256
HV = 432
LEN = 512
EPS = 1e-05
GROUP_EPS = 1.0
BF = jnp.bfloat16
F32 = jnp.float32
MESH = pl.DeviceIdType.MESH
LANE = 128
BLOCK = 2 * LANE
SLOTS = 4
STEP = 32


def ring_position(index, count):
    low = index // 2
    return low + (index % 2) * (count - 1 - 2 * low)


def ring_index(position, count):
    high = position // (count // 2)
    return (1 - high) * (2 * position) + high * (2 * (count - 1 - position) + 1)


def bits_of(count):
    return [1 << i for i in range(count.bit_length() - 1)]


def anyspec():
    return pl.BlockSpec(memory_space=pl.ANY)


def vmem():
    return pl.BlockSpec(memory_space=pltpu.VMEM)


def nt(left, right):
    return lax.dot_general(left, right, (((1,), (1,)), ((), ())), preferred_element_type=F32)


def nn(left, right):
    return lax.dot_general(left, right, (((1,), (0,)), ((), ())), preferred_element_type=F32)


def tn(left, right):
    return lax.dot_general(left, right, (((0,), (0,)), ((), ())), preferred_element_type=F32)


def in_kernel(
    n,
    n_tp,
    x_ref,
    cot_ref,
    gains_ref,
    cos_ref,
    sin_ref,
    wq_ref,
    wk_ref,
    wv_ref,
    wg_ref,
    wo_ref,
    q_out,
    k_out,
    v_out,
    g_out,
    xr_out,
    cr_out,
    gain_out,
    nall_out,
    call_out,
    wq_out,
    wk_out,
    wv_out,
    wg_out,
    wo_out,
    x_v,
    rel_v,
    own_v,
    nall_v,
    gain_v,
    q_acc,
    k_acc,
    v_acc,
    g_acc,
    wq_s,
    wk_s,
    wv_s,
    wg_s,
    wo_s,
    ring_send,
    ring_recv,
    gain_send,
    gain_recv,
    share_send,
    share_recv,
    load_sem,
    local_sem,
):
    micro, rows, width = x_ref.shape
    window = n_tp * rows
    mine = micro * rows
    dp, tp = lax.axis_index("dp"), lax.axis_index("tensor")
    pos = ring_position(dp, n)
    cw = ring_index((pos + 1) % n, n)
    ccw = ring_index((pos + n - 1) % n, n)
    bits = bits_of(n_tp)

    def flip(bit):
        return tp + bit - 2 * bit * ((tp // bit) % 2)

    barrier = pltpu.get_barrier_semaphore()
    for k in range(1, n):
        pl.semaphore_signal(
            barrier, inc=1, device_id=(ring_index((pos + k) % n, n), tp), device_id_type=MESH
        )
    for bit in bits:
        pl.semaphore_signal(barrier, inc=1, device_id=(dp, flip(bit)), device_id_type=MESH)
    pl.semaphore_wait(barrier, n - 1 + len(bits))

    shards = (wq_ref, wk_ref, wv_ref, wg_ref, wo_ref)
    wholes = (wq_out, wk_out, wv_out, wg_out, wo_out)
    slots = (wq_s, wk_s, wv_s, wg_s)
    accs = (q_acc, k_acc, v_acc, g_acc)

    def hop(i, a, side):
        lanes = pl.ds(side * LANE, LANE)
        source = shards[a].at[:, lanes] if i == 0 else wholes[a].at[i, :, lanes]
        target = wholes[a].at[i + 1, :, lanes]
        return pltpu.make_async_remote_copy(
            src_ref=source,
            dst_ref=target,
            send_sem=ring_send.at[i, a, side],
            recv_sem=ring_recv.at[i, a, side],
            device_id=((cw, ccw)[side], tp),
            device_id_type=MESH,
        )

    def load(i, a):
        source = shards[a] if i == 0 else wholes[a].at[i]
        return pltpu.make_async_copy(source, slots[a].at[i % SLOTS], load_sem.at[i % SLOTS, a])

    for a in range(5):
        for side in range(2):
            hop(0, a, side).start()
    wo_own = pltpu.make_async_copy(wo_ref, wo_s, local_sem.at[3 + micro])
    wo_own.start()
    x_copy = pltpu.make_async_copy(x_ref, x_v, local_sem.at[0])
    x_copy.start()
    for a in range(4):
        load(0, a).start()

    def gain_copy(k):
        return pltpu.make_async_remote_copy(
            src_ref=gains_ref,
            dst_ref=gain_v.at[k],
            send_sem=gain_send.at[k],
            recv_sem=gain_recv.at[k],
            device_id=(ring_index((pos + k) % n, n), tp),
            device_id_type=MESH,
        )

    own_gain = pltpu.make_async_copy(gains_ref, gain_v.at[0], local_sem.at[1])
    own_gain.start()
    for k in range(1, n):
        gain_copy(k).start()
    own_gain.wait()
    for k in range(1, n):
        gain_copy(k).wait()
    for i in range(n):
        gain_out[:, pl.ds(i * BLOCK, LANE)] = gain_v[i, :, pl.ds(0, LANE)]
        gain_out[:, pl.ds(i * BLOCK + LANE, LANE)] = gain_v[(n - i) % n, :, pl.ds(LANE, LANE)]

    def natural(i, side):
        at = ring_index((pos + (n - i if side == 0 else i)) % n, n) * BLOCK + side * LANE
        return pl.ds(pl.multiple_of(at, LANE), LANE)

    def share_copy(source, target, slot, m, key, bit):
        start = m * window + key * rows
        arrive = m * window + (key ^ bit) * rows
        return pltpu.make_async_remote_copy(
            src_ref=source.at[pl.ds(start, rows)] if source.shape[0] != mine
            else source.at[pl.ds(m * rows, rows)],
            dst_ref=target.at[pl.ds(arrive, rows)],
            send_sem=share_send.at[slot, m, key ^ bit],
            recv_sem=share_recv.at[slot, m, key ^ bit],
            device_id=(dp, flip(bit)),
            device_id_type=MESH,
        )

    x_copy.wait()
    step_rows = min(rows, 32)

    @pl.loop(0, mine // step_rows)
    def _(r):
        at = pl.multiple_of(r * step_rows, step_rows)
        m, inner = at // rows, at % rows
        chunk = x_v[m, pl.ds(pl.multiple_of(inner, step_rows), step_rows), :]
        scale = lax.rsqrt(jnp.mean(chunk * chunk, axis=-1, keepdims=True) + EPS)
        there = pl.ds(pl.multiple_of(m * window + inner, step_rows), step_rows)
        for i in range(n):
            for side in range(2):
                lanes = pl.ds(i * BLOCK + side * LANE, LANE)
                part = x_v[
                    m, pl.ds(pl.multiple_of(inner, step_rows), step_rows), natural(i, side)
                ]
                rel_v[0, pl.ds(at, step_rows), lanes] = part
                nall_v[there, lanes] = (part * scale * gain_out[0:1, lanes]).astype(BF)

    for bit in bits[::-1]:
        for m in range(micro):
            share_copy(nall_v, nall_v, 0, m, 0, bit).start()
    rel_copy = pltpu.make_async_copy(rel_v.at[0], xr_out, local_sem.at[2])
    rel_copy.start()
    c_copy = pltpu.make_async_copy(cot_ref, x_v, local_sem.at[0])
    c_copy.start()
    c_copy.wait()

    @pl.loop(0, mine // step_rows)
    def _(r):
        at = pl.multiple_of(r * step_rows, step_rows)
        m, inner = at // rows, at % rows
        for i in range(n):
            for side in range(2):
                lanes = pl.ds(i * BLOCK + side * LANE, LANE)
                part = x_v[
                    m, pl.ds(pl.multiple_of(inner, step_rows), step_rows), natural(i, side)
                ]
                rel_v[1, pl.ds(at, step_rows), lanes] = part
                own_v[pl.ds(at, step_rows), lanes] = part.astype(BF)

    cot_rel = pltpu.make_async_copy(rel_v.at[1], cr_out, local_sem.at[1])
    cot_rel.start()
    own_copies = [
        pltpu.make_async_copy(
            own_v.at[pl.ds(m * rows, rows)],
            call_out.at[pl.ds(m * window, rows)],
            local_sem.at[3 + m],
        )
        for m in range(micro)
    ]
    for copy in own_copies:
        copy.start()

    def relay(target, slot):
        source0 = nall_v if slot == 0 else own_v
        for at, bit in enumerate(bits[::-1]):
            for key in range(0, n_tp, 2 * bit):
                for m in range(micro):
                    if key:
                        share_copy(target, target, slot, m, key, bit).start()
            for key in range(0, n_tp, 2 * bit):
                for m in range(micro):
                    share_copy(
                        source0 if key == 0 else target, target, slot, m, key, bit
                    ).wait_recv()

    tile = 256
    heads = wq_ref.shape[0] // HK
    half = HK // 2

    def product(j, a, last):
        load(j, a).wait()
        if j == 0:
            pltpu.make_async_copy(
                slots[a].at[0], wholes[a].at[0], load_sem.at[SLOTS, a]
            ).start()

        @pl.loop(0, micro * window // tile)
        def _(r):
            at = pl.multiple_of(r * tile, tile)
            here = pl.ds(at, tile)
            part = nt(nall_v[here, pl.ds(j * BLOCK, BLOCK)], slots[a][j % SLOTS])
            if j > 0:
                part = accs[a][here, :] + part
            if not last:
                accs[a][here, :] = part
            elif a < 2:
                place = pl.ds(pl.multiple_of(at % window, tile), tile)
                cosine, sine = cos_ref[place, :], sin_ref[place, :]
                out = (q_out, k_out)[a]
                for h in range(heads):
                    low = part[:, h * HK : h * HK + half]
                    high = part[:, h * HK + half : (h + 1) * HK]
                    out[here, pl.ds(h * HK, half)] = (low * cosine - high * sine).astype(BF)
                    out[here, pl.ds(h * HK + half, half)] = (high * cosine + low * sine).astype(BF)
            elif a == 2:
                v_out[here, :] = part.astype(BF)
            else:
                g_out[here, :] = part

        if j == 0:
            pltpu.make_async_copy(
                slots[a].at[0], wholes[a].at[0], load_sem.at[SLOTS, a]
            ).wait()

    nall_copy = pltpu.make_async_copy(nall_v, nall_out, local_sem.at[0])
    start_at = 3
    done = 0
    for i in range(n + 1):
        if i == start_at:
            relay(nall_v, 0)
            nall_copy.start()
            for bit in bits[::-1]:
                for m in range(micro):
                    share_copy(own_v, call_out, 1, m, 0, bit).start()
        if i == n - 1:
            relay(call_out, 1)
        todo = []
        if i >= start_at:
            goal = min(i - 1, done + 1) if i < n else n - 1
            todo = list(range(done, goal + 1))
            done = goal + 1
        if i == 1:
            wo_own.wait()
            wo_own = pltpu.make_async_copy(wo_s, wo_out.at[0], local_sem.at[3 + micro])
            wo_own.start()
        for a in range(5):
            if 0 < i < n:
                hop(i - 1, a, 0).wait_recv()
                hop(i - 1, a, 1).wait_recv()
                if i < n - 1:
                    hop(i, a, 0).start()
                    hop(i, a, 1).start()
                if a < 4:
                    load(i, a).start()
            if a < 4:
                for j in todo:
                    product(j, a, j == n - 1)

    for i in range(n - 1):
        for a in range(5):
            hop(i, a, 0).wait_send()
            hop(i, a, 1).wait_send()
    for slot, source0, target in ((0, nall_v, nall_v), (1, own_v, call_out)):
        for bit in bits[::-1]:
            for key in range(0, n_tp, 2 * bit):
                for m in range(micro):
                    share_copy(
                        source0 if key == 0 else target, target, slot, m, key, bit
                    ).wait_send()
    for copy in own_copies + [rel_copy, cot_rel, nall_copy, wo_own]:
        copy.wait()


def project_in(n, n_tp, x, cot, gains, cosine, sine, weights, wo):
    micro, rows, width = x.shape
    total = micro * n_tp * rows
    mine = micro * rows
    sizes = [w.shape[0] for w in weights]
    shape = jax.ShapeDtypeStruct
    flops = 2 * total * width * sum(sizes)
    return pl.pallas_call(
        functools.partial(in_kernel, n, n_tp),
        out_shape=(
            shape((total, sizes[0]), BF),
            shape((total, sizes[1]), BF),
            shape((total, sizes[2]), BF),
            shape((total, sizes[3]), F32),
            shape((mine, width), F32),
            shape((mine, width), F32),
            shape((2, width), F32),
            shape((total, width), BF),
            shape((total, width), BF),
        )
        + tuple(shape((n, s, BLOCK), BF) for s in sizes)
        + (shape((n,) + wo.shape, BF),),
        in_specs=[anyspec(), anyspec(), anyspec(), vmem(), vmem()] + [anyspec()] * 5,
        out_specs=(vmem(),) * 4 + (anyspec(),) * 2 + (vmem(),) + (anyspec(),) * 7,
        scratch_shapes=[
            pltpu.VMEM(x.shape, F32),
            pltpu.VMEM((2, mine, width), F32),
            pltpu.VMEM((mine, width), BF),
            pltpu.VMEM((total, width), BF),
            pltpu.VMEM((n, 2, BLOCK), F32),
        ]
        + [pltpu.VMEM((total, s), F32) for s in sizes]
        + [pltpu.VMEM((SLOTS, s, BLOCK), BF) for s in sizes]
        + [
            pltpu.VMEM(wo.shape, BF),
            pltpu.SemaphoreType.DMA((n - 1, 5, 2)),
            pltpu.SemaphoreType.DMA((n - 1, 5, 2)),
            pltpu.SemaphoreType.DMA((n,)),
            pltpu.SemaphoreType.DMA((n,)),
            pltpu.SemaphoreType.DMA((2, micro, n_tp)),
            pltpu.SemaphoreType.DMA((2, micro, n_tp)),
            pltpu.SemaphoreType.DMA((SLOTS + 1, 4)),
            pltpu.SemaphoreType.DMA((4 + micro,)),
        ],
        compiler_params=pltpu.CompilerParams(
            collective_id=1, has_side_effects=True, vmem_limit_bytes=64_000_000
        ),
        cost_estimate=pl.CostEstimate(
            flops=flops, bytes_accessed=60_000_000, transcendentals=0
        ),
        name="in_kernel",
    )(x, cot, gains, cosine, sine, *weights, wo)


def partner(tp, bit):
    return tp + bit - 2 * bit * ((tp // bit) % 2)


def neighbours(n):
    dp, tp = lax.axis_index("dp"), lax.axis_index("tensor")
    pos = ring_position(dp, n)
    return dp, tp, ring_index((pos + 1) % n, n), ring_index((pos + n - 1) % n, n)


def greet(devices):
    barrier = pltpu.get_barrier_semaphore()
    for device in devices:
        pl.semaphore_signal(barrier, inc=1, device_id=device, device_id_type=MESH)
    pl.semaphore_wait(barrier, len(devices))


class Share:
    def __init__(self, dp, tp, n_tp, micro, rows, buf, send, recv):
        self.dp, self.tp, self.n_tp, self.micro, self.rows = dp, tp, n_tp, micro, rows
        self.buf, self.send, self.recv = buf, send, recv
        self.bits = bits_of(n_tp)[::-1]

    def copies(self, bit, keys=None):
        window = self.n_tp * self.rows
        for key in range(0, self.n_tp, 2 * bit):
            if keys is None or (key == 0) == keys:
                for m in range(self.micro):
                    yield pltpu.make_async_remote_copy(
                        src_ref=self.buf.at[pl.ds(m * window + key * self.rows, self.rows)],
                        dst_ref=self.buf.at[
                            pl.ds(m * window + (key ^ bit) * self.rows, self.rows)
                        ],
                        send_sem=self.send.at[m, key ^ bit],
                        recv_sem=self.recv.at[m, key ^ bit],
                        device_id=(self.dp, partner(self.tp, bit)),
                        device_id_type=MESH,
                    )

    def begin(self):
        for bit in self.bits:
            for copy in self.copies(bit, True):
                copy.start()

    def relay(self):
        for bit in self.bits:
            for copy in self.copies(bit, False):
                copy.start()
            for copy in self.copies(bit):
                copy.wait_recv()

    def finish(self):
        for bit in self.bits:
            for copy in self.copies(bit):
                copy.wait_send()


class Collect:
    def __init__(self, dp, tp, n_tp, micro, rows, back, got, own, send, recv):
        self.dp, self.tp, self.n_tp, self.micro, self.rows = dp, tp, n_tp, micro, rows
        self.back, self.got, self.own, self.send, self.recv = back, got, own, send, recv
        self.bits = bits_of(n_tp)

    def keys(self, bit):
        return [key for key in range(0, self.n_tp, bit) if key & bit]

    def copies(self, bit):
        window = self.n_tp * self.rows
        for key in self.keys(bit):
            for m in range(self.micro):
                yield pltpu.make_async_remote_copy(
                    src_ref=self.back.at[pl.ds(m * window + key * self.rows, self.rows)],
                    dst_ref=self.got.at[key - 1, pl.ds(m * self.rows, self.rows)],
                    send_sem=self.send.at[key - 1, m],
                    recv_sem=self.recv.at[key - 1, m],
                    device_id=(self.dp, partner(self.tp, bit)),
                    device_id_type=MESH,
                )

    def start(self, bit):
        for copy in self.copies(bit):
            copy.start()

    def add(self, bit):
        window = self.n_tp * self.rows
        for copy in self.copies(bit):
            copy.wait_recv()
        for key in self.keys(bit):
            target = key ^ bit

            @pl.loop(0, self.micro * self.rows // STEP)
            def _(r):
                at = pl.multiple_of(r * STEP, STEP)
                m, inner = at // self.rows, at % self.rows
                here = pl.ds(at, STEP)
                there = pl.ds(pl.multiple_of(m * window + target * self.rows + inner, STEP), STEP)
                got = self.got[key - 1, here, :].astype(F32)
                if target == 0:
                    held = self.back[there, :].astype(F32) if bit == 1 else self.own[here, :]
                    self.own[here, :] = held + got
                else:
                    self.back[there, :] = (self.back[there, :].astype(F32) + got).astype(BF)

    def finish(self, bits=None):
        for bit in self.bits if bits is None else bits:
            for copy in self.copies(bit):
                copy.wait_send()


class SumRing:
    def __init__(self, n, tp, cw, ccw, arrays, gradient, send, recv, free):
        self.n, self.tp, self.ways, self.arrays = n, tp, (cw, ccw), arrays
        self.gradient, self.send, self.recv, self.free = gradient, send, recv, free
        self.slots = arrays[0][2].shape[0]
        self.ready = self.done = 0

    def hop(self, s, a, side):
        _, send, recv, _ = self.arrays[a]
        lanes = pl.ds(side * LANE, LANE)
        return pltpu.make_async_remote_copy(
            src_ref=send.at[s % 2, :, lanes],
            dst_ref=recv.at[s % self.slots, :, lanes],
            send_sem=self.send.at[s, a, side],
            recv_sem=self.recv.at[s, a, side],
            device_id=(self.ways[side], self.tp),
            device_id_type=MESH,
        )

    def first(self, a):
        part, send, _, _ = self.arrays[a]
        self.gradient(1 % self.n, a)
        send[0] = part[...].astype(BF)
        self.hop(0, a, 0).start()
        self.hop(0, a, 1).start()

    def prepare(self):
        if self.ready == self.done and self.done < self.n - 1:
            self.ready += 1
            for a in range(len(self.arrays)):
                self.gradient((self.ready + 1) % self.n, a)

    def advance(self):
        n = self.n
        if self.done == n - 1:
            return
        self.prepare()
        self.done += 1
        s = self.done
        for a, (part, send, recv, out) in enumerate(self.arrays):
            self.hop(s - 1, a, 0).wait_recv()
            self.hop(s - 1, a, 1).wait_recv()
            total = part[...] + recv[(s - 1) % self.slots].astype(F32)
            if s == n - 1:
                out[...] = total
                continue
            if s >= 2:
                self.hop(s - 2, a, 0).wait_send()
                self.hop(s - 2, a, 1).wait_send()
            send[s % 2] = total.astype(BF)
            for side in range(2):
                if self.slots < n - 1:
                    if s - 1 < n - 1 - self.slots:
                        pl.semaphore_signal(
                            self.free.at[a, side],
                            inc=1,
                            device_id=(self.ways[1 - side], self.tp),
                            device_id_type=MESH,
                        )
                    if s >= self.slots:
                        pl.semaphore_wait(self.free.at[a, side], 1)
                self.hop(s, a, side).start()

    def finish(self):
        for s in range(max(0, self.n - 3), self.n - 1):
            for a in range(len(self.arrays)):
                self.hop(s, a, 0).wait_send()
                self.hop(s, a, 1).wait_send()


def fill_decay(decay_v, col_ref, row_ref, rate_ref):
    heads, window, _ = decay_v.shape
    scale_qk = 1.0 / math.sqrt(HK)
    for h in range(heads):

        @pl.loop(0, window // LANE)
        def _(r):
            here = pl.ds(pl.multiple_of(r * LANE, LANE), LANE)
            col, row = col_ref[here, 0:1], row_ref[...]
            spacing = col - row
            same = jnp.floor(col * (1.0 / LEN)) == jnp.floor(row * (1.0 / LEN))
            kept = jnp.exp(jnp.maximum(spacing, 0.0) * rate_ref[h : h + 1, :]) * scale_qk
            decay_v[h, here, :] = jnp.where((spacing >= 0.0) & same, kept, 0.0)


def gelu_parts(pre_act):
    normal_cdf = 0.5 * (1.0 + lax.erf(pre_act * (1.0 / math.sqrt(2.0))))
    density = jnp.exp(-0.5 * pre_act * pre_act) * (1.0 / math.sqrt(2.0 * math.pi))
    return (pre_act * normal_cdf, normal_cdf + pre_act * density)


def forward_kernel(
    n,
    n_tp,
    q_ref,
    k_ref,
    v_ref,
    g_ref,
    x_ref,
    gain_ref,
    col_ref,
    row_ref,
    rate_ref,
    wo_ref,
    wu_ref,
    wl_ref,
    wd_ref,
    gated_out,
    middle_out,
    hidden_out,
    value_out,
    slope_out,
    second_out,
    wu_out,
    wl_out,
    wd_out,
    near_out,
    far_out,
    decay_v,
    wo_v,
    back_v,
    own_v,
    got_v,
    second_v,
    wu_v,
    wl_v,
    wd_v,
    up_v,
    gelu_v,
    ring_send,
    ring_recv,
    part_send,
    part_recv,
    share_send,
    share_recv,
    last_send,
    last_recv,
    local_sem,
):
    total, width = second_v.shape
    mine = x_ref.shape[0]
    window = col_ref.shape[0]
    micro = total // window
    rows = mine // micro
    dp, tp, cw, ccw = neighbours(n)
    bits = bits_of(n_tp)
    greet([(cw, tp), (ccw, tp)] + [(dp, partner(tp, bit)) for bit in bits])

    wholes = (wu_v, wl_v, wd_v)
    shards = (wu_ref, wl_ref, wd_ref)

    def hop(i, a, side):
        lanes = pl.ds(side * LANE, LANE)
        return pltpu.make_async_remote_copy(
            src_ref=shards[a].at[:, lanes] if i == 0 else wholes[a].at[i, :, lanes],
            dst_ref=wholes[a].at[i + 1, :, lanes],
            send_sem=ring_send.at[i, a, side],
            recv_sem=ring_recv.at[i, a, side],
            device_id=((cw, ccw)[side], tp),
            device_id_type=MESH,
        )

    def ring_step(s):
        for a in range(3):
            for side in range(2):
                hop(s - 1, a, side).wait_recv()
                if s < n - 1:
                    hop(s, a, side).start()

    for a in range(3):
        for side in range(2):
            hop(0, a, side).start()
    local = [
        pltpu.make_async_copy(wo_ref, wo_v, local_sem.at[0]),
        pltpu.make_async_copy(wu_ref, wu_v.at[0], local_sem.at[1]),
        pltpu.make_async_copy(wl_ref, wl_v.at[0], local_sem.at[2]),
        pltpu.make_async_copy(wd_ref, wd_v.at[0], local_sem.at[3]),
    ]
    for copy in local:
        copy.start()
    fill_decay(decay_v, col_ref, row_ref, rate_ref)
    heads = decay_v.shape[0]
    tile = 256
    for m in range(micro):
        for h in range(heads):
            keys = pl.ds(h * HK, HK)
            values = pl.ds(h * HV, HV)
            inside = pl.ds(m * window, window)

            @pl.loop(0, window // tile)
            def _(r):
                at = pl.multiple_of(r * tile, tile)
                here = pl.ds(pl.multiple_of(m * window + at, tile), tile)
                scores = nt(q_ref[here, keys], k_ref[inside, keys])
                weight = (scores * decay_v[h, pl.ds(at, tile), :]).astype(BF)
                kept = nn(weight, v_ref[inside, values])
                group = lax.rsqrt(jnp.mean(kept * kept, axis=-1, keepdims=True) + GROUP_EPS)
                gate = g_ref[here, values]
                gated_out[here, values] = (gate * jax.nn.sigmoid(gate) * (kept * group)).astype(BF)

    ring_step(1)
    local[0].wait()
    for i in range(n):

        @pl.loop(0, total // tile)
        def _(r):
            here = pl.ds(pl.multiple_of(r * tile, tile), tile)
            back_v[here, pl.ds(i * BLOCK, BLOCK)] = nn(gated_out[here, :], wo_v[i]).astype(BF)

    collect = Collect(dp, tp, n_tp, micro, rows, back_v, got_v, own_v, part_send, part_recv)
    share = Share(dp, tp, n_tp, micro, rows, second_v, share_send, share_recv)
    collect.start(bits[0])
    for copy in local[1:]:
        copy.wait()
    done = 1
    for at, bit in enumerate(bits):
        collect.add(bit)
        if at + 1 < len(bits):
            collect.start(bits[at + 1])
            done += 1
            ring_step(done)

    @pl.loop(0, mine // STEP)
    def _(r):
        at = pl.multiple_of(r * STEP, STEP)
        m, inner = at // rows, at % rows
        here = pl.ds(at, STEP)
        there = pl.ds(pl.multiple_of(m * window + inner, STEP), STEP)
        middle = x_ref[here, :] + own_v[here, :]
        middle_out[here, :] = middle
        scale = lax.rsqrt(jnp.mean(middle * middle, axis=-1, keepdims=True) + EPS)
        second_v[there, :] = (middle * scale * gain_ref[1:2, :]).astype(BF)

    share.begin()
    for s in range(done + 1, n // 2 + 1):
        ring_step(s)
    share.relay()
    second_copy = pltpu.make_async_copy(second_v, second_out, local_sem.at[0])
    second_copy.start()

    def rows_by(weights, here, blocks):
        result = None
        for i in blocks:
            term = nt(second_v[here, pl.ds(i * BLOCK, BLOCK)], weights[i])
            result = term if result is None else result + term
        return result

    @pl.loop(0, total // tile)
    def _(r):
        here = pl.ds(pl.multiple_of(r * tile, tile), tile)
        up_v[here, :] = rows_by(wu_v, here, range(n // 2))
        gelu_v[here, :] = rows_by(wl_v, here, range(n // 2))

    for s in range(n // 2 + 1, n):
        ring_step(s)
    whole_copies = [
        pltpu.make_async_copy(source, target, local_sem.at[1 + at])
        for at, (source, target) in enumerate(((wu_v, wu_out), (wl_v, wl_out), (wd_v, wd_out)))
    ]
    for copy in whole_copies:
        copy.start()

    @pl.loop(0, total // tile)
    def _(r):
        here = pl.ds(pl.multiple_of(r * tile, tile), tile)
        up = up_v[here, :] + rows_by(wu_v, here, range(n // 2, n))
        gelu_val, gelu_slope = gelu_parts(gelu_v[here, :] + rows_by(wl_v, here, range(n // 2, n)))
        hidden_out[here, :] = (gelu_val * up).astype(BF)
        value_out[here, :] = gelu_val.astype(BF)
        slope_out[here, :] = (up * gelu_slope).astype(BF)

    collect.finish()
    for i in range(n):

        @pl.loop(0, total // tile)
        def _(r):
            here = pl.ds(pl.multiple_of(r * tile, tile), tile)
            back_v[here, pl.ds(i * BLOCK, BLOCK)] = nn(hidden_out[here, :], wd_v[i]).astype(BF)

    last = Collect(dp, tp, n_tp, micro, rows, back_v, got_v, own_v, last_send, last_recv)
    for bit in bits[:-1]:
        last.start(bit)
        last.add(bit)
    near_copy = pltpu.make_async_copy(own_v, near_out, local_sem.at[4])
    near_copy.start()
    far_copies = [
        pltpu.make_async_copy(
            back_v.at[pl.ds(m * window + bits[-1] * rows, rows)],
            far_out.at[pl.ds(m * rows, rows)],
            local_sem.at[5 + m],
        )
        for m in range(micro)
    ]
    for copy in far_copies:
        copy.start()
    last.finish(bits[:-1])

    for i in range(n - 1):
        for a in range(3):
            hop(i, a, 0).wait_send()
            hop(i, a, 1).wait_send()
    share.finish()
    for copy in whole_copies + [second_copy, near_copy] + far_copies:
        copy.wait()


def mid_forward(n, n_tp, q, k, v, g, x_rel, gain, tables, wo, wu, wl, wd):
    total, hv = v.shape
    mine, width = x_rel.shape
    units = wu.shape[0]
    heads = tables[2].shape[0]
    window = tables[0].shape[0]
    shape = jax.ShapeDtypeStruct
    dma = pltpu.SemaphoreType.DMA
    rows_parts = total // window
    return pl.pallas_call(
        functools.partial(forward_kernel, n, n_tp),
        out_shape=(
            shape((total, hv), BF),
            shape((mine, width), F32),
            shape((total, units), BF),
            shape((total, units), BF),
            shape((total, units), BF),
            shape((total, width), BF),
            shape((n, units, BLOCK), BF),
            shape((n, units, BLOCK), BF),
            shape((n, units, BLOCK), BF),
            shape((mine, width), F32),
            shape((mine, width), BF),
        ),
        in_specs=[vmem()] * 9 + [anyspec()] * 4,
        out_specs=(vmem(),) * 5 + (anyspec(),) * 6,
        scratch_shapes=[
            pltpu.VMEM((heads, window, window), F32),
            pltpu.VMEM(wo.shape, BF),
            pltpu.VMEM((total, width), BF),
            pltpu.VMEM((mine, width), F32),
            pltpu.VMEM((n_tp - 1, mine, width), BF),
            pltpu.VMEM((total, width), BF),
            pltpu.VMEM((n, units, BLOCK), BF),
            pltpu.VMEM((n, units, BLOCK), BF),
            pltpu.VMEM((n, units, BLOCK), BF),
            pltpu.VMEM((total, units), F32),
            pltpu.VMEM((total, units), F32),
            dma((n - 1, 3, 2)),
            dma((n - 1, 3, 2)),
            dma((n_tp - 1, rows_parts)),
            dma((n_tp - 1, rows_parts)),
            dma((rows_parts, n_tp)),
            dma((rows_parts, n_tp)),
            dma((n_tp - 1, rows_parts)),
            dma((n_tp - 1, rows_parts)),
            dma((5 + rows_parts,)),
        ],
        compiler_params=pltpu.CompilerParams(
            collective_id=3, has_side_effects=True, vmem_limit_bytes=66_000_000
        ),
        cost_estimate=pl.CostEstimate(
            flops=6 * total * width * units, bytes_accessed=60_000_000, transcendentals=0
        ),
        name="forward_kernel",
    )(q, k, v, g, x_rel, gain, *tables, wo, wu, wl, wd)


def backward_kernel(
    n,
    n_tp,
    gain_ref,
    col_ref,
    row_ref,
    rate_ref,
    cos_ref,
    sin_ref,
    cot_ref,
    wd_ref,
    value_ref,
    slope_ref,
    hidden_ref,
    second_ref,
    wu_ref,
    wl_ref,
    middle_ref,
    cotf_ref,
    wo_ref,
    q_ref,
    k_ref,
    v_ref,
    g_ref,
    dd_out,
    du_out,
    dl_out,
    sum_out,
    grad_out,
    mall_out,
    gq_out,
    gk_out,
    gv_out,
    gs_out,
    cot_v,
    w_v,
    gu_v,
    gl_v,
    hidden_v,
    second_v,
    wu_s,
    wl_s,
    middle_v,
    cotf_v,
    q_v,
    k_v,
    v_v,
    g_v,
    gs_v,
    gated_v,
    decay_v,
    gk_acc,
    gv_acc,
    back_v,
    own_v,
    got_v,
    mall_v,
    dd_p,
    du_p,
    dl_p,
    dd_s,
    du_s,
    dl_s,
    dd_r,
    du_r,
    dl_r,
    ring_send,
    ring_recv,
    ring_free,
    part_send,
    part_recv,
    share_send,
    share_recv,
    load_sem,
    local_sem,
):
    total, width = cot_v.shape
    mine = own_v.shape[0]
    window = col_ref.shape[0]
    micro = total // window
    rows = mine // micro
    heads = decay_v.shape[0]
    dp, tp, cw, ccw = neighbours(n)
    bits = bits_of(n_tp)
    greet([(cw, tp), (ccw, tp)] + [(dp, partner(tp, bit)) for bit in bits])

    pairs = (
        (hidden_ref, hidden_v),
        (cot_ref, cot_v),
        (wd_ref, w_v),
        (value_ref, gu_v),
        (slope_ref, gl_v),
        (second_ref, second_v),
        (middle_ref, middle_v),
        (cotf_ref, cotf_v),
        (q_ref, q_v),
        (k_ref, k_v),
        (v_ref, v_v),
        (g_ref, g_v),
    )
    loads = [
        pltpu.make_async_copy(source, target, local_sem.at[at])
        for at, (source, target) in enumerate(pairs)
    ]
    for copy in loads:
        copy.start()

    def block_load(i, a):
        source, target = ((wu_ref, wu_s), (wl_ref, wl_s))[a]
        return pltpu.make_async_copy(
            source.at[i], target.at[i % 2], load_sem.at[i % 2, a]
        )

    block_load(0, 0).start()
    block_load(0, 1).start()

    def gradient(i, a):
        block = pl.ds(i * BLOCK, BLOCK)
        if a == 0:
            dd_p[...] = tn(hidden_v[...], cot_v[:, block])
        else:
            (du_p, dl_p)[a - 1][...] = tn((gu_v, gl_v)[a - 1][...], second_v[:, block])

    ring = SumRing(
        n,
        tp,
        cw,
        ccw,
        (
            (dd_p, dd_s, dd_r, dd_out),
            (du_p, du_s, du_r, du_out),
            (dl_p, dl_s, dl_r, dl_out),
        ),
        gradient,
        ring_send,
        ring_recv,
        ring_free,
    )
    loads[0].wait()
    loads[1].wait()
    ring.first(0)
    for copy in loads[2:5]:
        copy.wait()
    tile = 256

    @pl.loop(0, total // tile)
    def _(r):
        here = pl.ds(pl.multiple_of(r * tile, tile), tile)
        grad = None
        for i in range(n):
            term = nt(cot_v[here, pl.ds(i * BLOCK, BLOCK)], w_v[i])
            grad = term if grad is None else grad + term
        gu_v[here, :] = (grad * gu_v[here, :].astype(F32)).astype(BF)
        gl_v[here, :] = (grad * gl_v[here, :].astype(F32)).astype(BF)

    wo_load = pltpu.make_async_copy(wo_ref, w_v, local_sem.at[2])
    wo_load.start()
    loads[5].wait()
    ring.first(1)
    ring.first(2)
    ring.prepare()
    for i in range(n):
        for a in range(2):
            block_load(i, a).wait()
            if i + 1 < n:
                block_load(i + 1, a).start()

        @pl.loop(0, total // tile)
        def _(r):
            here = pl.ds(pl.multiple_of(r * tile, tile), tile)
            back_v[here, pl.ds(i * BLOCK, BLOCK)] = (
                nn(gu_v[here, :], wu_s[i % 2]) + nn(gl_v[here, :], wl_s[i % 2])
            ).astype(BF)

    collect = Collect(dp, tp, n_tp, micro, rows, back_v, got_v, own_v, part_send, part_recv)
    share = Share(dp, tp, n_tp, micro, rows, mall_v, share_send, share_recv)
    collect.start(bits[0])
    ring.advance()
    for at, bit in enumerate(bits):
        collect.add(bit)
        if at + 1 < len(bits):
            collect.start(bits[at + 1])
            ring.advance()
            ring.prepare()
    fill_decay(decay_v, col_ref, row_ref, rate_ref)
    loads[6].wait()
    loads[7].wait()

    @pl.loop(0, mine // STEP)
    def _(r):
        at = pl.multiple_of(r * STEP, STEP)
        m, inner = at // rows, at % rows
        here = pl.ds(at, STEP)
        there = pl.ds(pl.multiple_of(m * window + inner, STEP), STEP)
        middle = middle_v[here, :]
        scale = lax.rsqrt(jnp.mean(middle * middle, axis=-1, keepdims=True) + EPS)
        scaled = own_v[here, :] * gain_ref[1:2, :]
        inside = jnp.mean(scaled * middle, axis=-1, keepdims=True)
        grad = cotf_v[here, :] + scale * (scaled - middle * (scale * scale * inside))
        cotf_v[here, :] = grad
        mall_v[there, :] = grad.astype(BF)

    share.begin()
    grad_copy = pltpu.make_async_copy(cotf_v, grad_out, local_sem.at[7])
    grad_copy.start()
    ring.advance()
    ring.prepare()
    for copy in loads[8:]:
        copy.wait()
    wo_load.wait()
    share.relay()
    mall_copy = pltpu.make_async_copy(mall_v, mall_out, local_sem.at[6])
    mall_copy.start()
    half = HK // 2
    for m in range(micro):
        ring.advance()

        @pl.loop(0, window // tile)
        def _(r):
            at = pl.multiple_of(r * tile, tile)
            here = pl.ds(pl.multiple_of(m * window + at, tile), tile)
            grad = None
            for i in range(n):
                term = nt(mall_v[here, pl.ds(i * BLOCK, BLOCK)], w_v[i])
                grad = term if grad is None else grad + term
            gated_v[pl.ds(at, tile), :] = grad

        ring.prepare()
        for h in range(heads):
            keys = pl.ds(h * HK, HK)
            values = pl.ds(h * HV, HV)
            inside = pl.ds(m * window, window)
            gk_acc[...] = jnp.zeros_like(gk_acc)
            gv_acc[...] = jnp.zeros_like(gv_acc)

            @pl.loop(0, window // tile)
            def _(r):
                at = pl.multiple_of(r * tile, tile)
                local = pl.ds(at, tile)
                here = pl.ds(pl.multiple_of(m * window + at, tile), tile)
                decay = decay_v[h, local, :]
                query = q_v[here, keys]
                weight = (nt(query, k_v[inside, keys]) * decay).astype(BF)
                kept = nn(weight, v_v[inside, values])
                group = lax.rsqrt(jnp.mean(kept * kept, axis=-1, keepdims=True) + GROUP_EPS)
                gate = g_v[here, values]
                sigmoid = jax.nn.sigmoid(gate)
                grad = gated_v[local, values]
                gs_v[here, values] = (
                    grad * (kept * group) * (sigmoid * (1.0 + gate * (1.0 - sigmoid)))
                ).astype(BF)
                lifted = grad * (gate * sigmoid)
                mean = jnp.mean(lifted * kept, axis=-1, keepdims=True)
                grad_kept = (group * (lifted - kept * (group * group * mean))).astype(BF)
                gv_acc[...] += tn(weight, grad_kept)
                score = (nt(grad_kept, v_v[inside, values]) * decay).astype(BF)
                gk_acc[...] += tn(score, query)
                turned = nn(score, k_v[inside, keys])
                low, high = turned[:, :half], turned[:, half:]
                cosine, sine = cos_ref[local, :], sin_ref[local, :]
                q_v[here, pl.ds(h * HK, half)] = (low * cosine + high * sine).astype(BF)
                q_v[here, pl.ds(h * HK + half, half)] = (high * cosine - low * sine).astype(BF)

            low, high = gk_acc[:, :half], gk_acc[:, half:]
            cosine, sine = cos_ref[...], sin_ref[...]
            k_v[inside, pl.ds(h * HK, half)] = (low * cosine + high * sine).astype(BF)
            k_v[inside, pl.ds(h * HK + half, half)] = (high * cosine - low * sine).astype(BF)
            v_v[inside, values] = gv_acc[...].astype(BF)
            if h == 0:
                ring.advance()
                ring.prepare()
    stores = [
        pltpu.make_async_copy(source, target, local_sem.at[8 + at])
        for at, (source, target) in enumerate(
            ((q_v, gq_out), (k_v, gk_out), (v_v, gv_out), (gs_v, gs_out))
        )
    ]
    for copy in stores:
        copy.start()
    for a in range(2):
        block_load(0, a).start()
    for _ in range(n):
        ring.advance()
    for a in range(2):
        block_load(0, a).wait()
    sums = jnp.sum(wu_s[0].astype(F32) * du_out[...], axis=0, keepdims=True)
    sums += jnp.sum(wl_s[0].astype(F32) * dl_out[...], axis=0, keepdims=True)
    sum_out[...] = jnp.broadcast_to(sums, sum_out.shape)
    ring.finish()
    collect.finish()
    share.finish()
    for copy in stores + [grad_copy, mall_copy]:
        copy.wait()


def mid_backward(n, n_tp, gain, tables, cosine, sine, cot, wd, value, slope, hidden, second,
                 wu, wl, middle, cot_rel, wo, q, k, v, g):
    total, width = cot.shape
    mine = middle.shape[0]
    units, hv, hk = wu.shape[1], v.shape[1], q.shape[1]
    heads = tables[2].shape[0]
    window = tables[0].shape[0]
    micro = total // window
    shape = jax.ShapeDtypeStruct
    dma = pltpu.SemaphoreType.DMA
    block_shapes = ((units, BLOCK),) * 3
    return pl.pallas_call(
        functools.partial(backward_kernel, n, n_tp),
        out_shape=tuple(shape(s, F32) for s in block_shapes)
        + (
            shape((8, BLOCK), F32),
            shape((mine, width), F32),
            shape((total, width), BF),
            shape((total, hk), BF),
            shape((total, hk), BF),
            shape((total, hv), BF),
            shape((total, hv), BF),
        ),
        in_specs=[vmem()] * 6 + [anyspec()] * 15,
        out_specs=(vmem(),) * 4 + (anyspec(),) * 6,
        scratch_shapes=[
            pltpu.VMEM((total, width), BF),
            pltpu.VMEM(wd.shape, BF),
            pltpu.VMEM((total, units), BF),
            pltpu.VMEM((total, units), BF),
            pltpu.VMEM((total, units), BF),
            pltpu.VMEM((total, width), BF),
            pltpu.VMEM((2, units, BLOCK), BF),
            pltpu.VMEM((2, units, BLOCK), BF),
            pltpu.VMEM((mine, width), F32),
            pltpu.VMEM((mine, width), F32),
            pltpu.VMEM((total, hk), BF),
            pltpu.VMEM((total, hk), BF),
            pltpu.VMEM((total, hv), BF),
            pltpu.VMEM((total, hv), F32),
            pltpu.VMEM((total, hv), BF),
            pltpu.VMEM((window, hv), F32),
            pltpu.VMEM((heads, window, window), F32),
            pltpu.VMEM((window, HK), F32),
            pltpu.VMEM((window, HV), F32),
            pltpu.VMEM((total, width), BF),
            pltpu.VMEM((mine, width), F32),
            pltpu.VMEM((n_tp - 1, mine, width), BF),
            pltpu.VMEM((total, width), BF),
        ]
        + [pltpu.VMEM(s, F32) for s in block_shapes]
        + [pltpu.VMEM((2,) + s, BF) for s in block_shapes]
        + [pltpu.VMEM((2,) + s, BF) for s in block_shapes]
        + [
            dma((n - 1, 3, 2)),
            dma((n - 1, 3, 2)),
            pltpu.SemaphoreType.REGULAR((3, 2)),
            dma((n_tp - 1, micro)),
            dma((n_tp - 1, micro)),
            dma((micro, n_tp)),
            dma((micro, n_tp)),
            dma((2, 2)),
            dma((12,)),
        ],
        compiler_params=pltpu.CompilerParams(
            collective_id=4, has_side_effects=True, vmem_limit_bytes=67_000_000
        ),
        cost_estimate=pl.CostEstimate(
            flops=16 * total * width * units, bytes_accessed=80_000_000, transcendentals=0
        ),
        name="backward_kernel",
    )(gain, *tables, cosine, sine, cot, wd, value, slope, hidden, second, wu, wl, middle,
      cot_rel, wo, q, k, v, g)


def out_kernel(
    n,
    n_tp,
    gq_ref,
    gk_ref,
    gv_ref,
    gs_ref,
    gain_ref,
    own_gain_ref,
    sum_ref,
    nall_ref,
    gated_ref,
    mall_ref,
    mid_ref,
    x_ref,
    wq_ref,
    wk_ref,
    wv_ref,
    wg_ref,
    dq_out,
    dk_out,
    dv_out,
    ds_out,
    do_out,
    gain_out,
    rows_out,
    nall_v,
    gated_v,
    mall_v,
    mid_v,
    x_v,
    dq_p,
    dk_p,
    dv_p,
    ds_p,
    do_p,
    dq_s,
    dk_s,
    dv_s,
    ds_s,
    do_s,
    dq_r,
    dk_r,
    dv_r,
    ds_r,
    do_r,
    wq_s,
    wk_s,
    wv_s,
    wg_s,
    back_v,
    own_v,
    got_v,
    ring_send,
    ring_recv,
    ring_free,
    part_send,
    part_recv,
    sum_v,
    sum_send,
    sum_recv,
    load_sem,
    local_sem,
):
    micro, rows, width = rows_out.shape
    total = nall_v.shape[0]
    mine = micro * rows
    dp, tp, cw, ccw = neighbours(n)
    pos = ring_position(dp, n)
    bits = bits_of(n_tp)
    greet([(cw, tp), (ccw, tp)] + [(dp, partner(tp, bit)) for bit in bits])

    grads = (gq_ref, gk_ref, gv_ref, gs_ref)
    outs = (dq_out, dk_out, dv_out, ds_out)
    products = (dq_p, dk_p, dv_p, ds_p)
    wholes = (wq_ref, wk_ref, wv_ref, wg_ref)
    slots = (wq_s, wk_s, wv_s, wg_s)
    loads = [
        pltpu.make_async_copy(source, target, local_sem.at[at])
        for at, (source, target) in enumerate(
            (
                (nall_ref, nall_v),
                (gated_ref, gated_v),
                (mall_ref, mall_v),
                (mid_ref, mid_v),
                (x_ref, x_v),
            )
        )
    ]
    for copy in loads:
        copy.start()

    def load(i, a):
        return pltpu.make_async_copy(
            wholes[a].at[i], slots[a].at[i % 2], load_sem.at[i % 2, a]
        )

    for a in range(4):
        load(0, a).start()

    def gradient(i, a):
        block = pl.ds(i * BLOCK, BLOCK)
        if a < 4:
            products[a][...] = tn(grads[a][...], nall_v[:, block])
        else:
            do_p[...] = tn(gated_v[...], mall_v[:, block])

    ring = SumRing(
        n,
        tp,
        cw,
        ccw,
        (
            (dq_p, dq_s, dq_r, dq_out),
            (dk_p, dk_s, dk_r, dk_out),
            (dv_p, dv_s, dv_r, dv_out),
            (ds_p, ds_s, ds_r, ds_out),
            (do_p, do_s, do_r, do_out),
        ),
        gradient,
        ring_send,
        ring_recv,
        ring_free,
    )
    tile = 256

    def backward(i):
        for a in range(4):
            load(i, a).wait()
            if i + 1 < n:
                load(i + 1, a).start()

        @pl.loop(0, total // tile)
        def _(r):
            here = pl.ds(pl.multiple_of(r * tile, tile), tile)
            block = None
            for a in range(4):
                term = nn(grads[a][here, :], slots[a][i % 2])
                block = term if block is None else block + term
            back_v[here, pl.ds(i * BLOCK, BLOCK)] = block.astype(BF)

    def natural(i, side):
        at = ring_index((pos + (n - i if side == 0 else i)) % n, n) * BLOCK + side * LANE
        return pl.ds(pl.multiple_of(at, LANE), LANE)

    def finish_rows():
        @pl.loop(0, mine // STEP)
        def _(r):
            at = pl.multiple_of(r * STEP, STEP)
            m, inner = at // rows, pl.multiple_of(at % rows, STEP)
            here = pl.ds(at, STEP)
            x = x_v[here, :]
            scale = lax.rsqrt(jnp.mean(x * x, axis=-1, keepdims=True) + EPS)
            inside = jnp.mean(own_v[here, :] * gain_ref[0:1, :] * x, axis=-1, keepdims=True)
            slope = scale * scale * inside
            for i in range(n):
                for side in range(2):
                    lanes = pl.ds(i * BLOCK + side * LANE, LANE)
                    scaled = own_v[here, lanes] * gain_ref[0:1, lanes]
                    rows_out[m, pl.ds(inner, STEP), natural(i, side)] = mid_v[
                        here, lanes
                    ] + scale * (scaled - x_v[here, lanes] * slope)

    collect = Collect(dp, tp, n_tp, micro, rows, back_v, got_v, own_v, part_send, part_recv)
    loads[0].wait()
    for a in range(4):
        ring.first(a)
    loads[1].wait()
    loads[2].wait()
    ring.first(4)
    ring.prepare()
    for i in range(n):
        backward(i)
        if i % 3 == 2:
            ring.advance()
            ring.prepare()
    collect.start(bits[0])
    ring.advance()
    ring.prepare()
    for at, bit in enumerate(bits):
        collect.add(bit)
        if at + 1 < len(bits):
            collect.start(bits[at + 1])
            ring.advance()
            ring.prepare()
            ring.advance()
            ring.prepare()
    loads[3].wait()
    loads[4].wait()
    finish_rows()
    for a in range(4):
        load(0, a).start()
    for _ in range(n):
        ring.advance()

    sums = None
    for a in range(4):
        load(0, a).wait()
        term = jnp.sum(slots[a][0].astype(F32) * outs[a][...], axis=0, keepdims=True)
        sums = term if sums is None else sums + term
    sum_v[0] = jnp.concatenate([sums, sum_ref[1:8, :]], axis=0)
    for at, bit in enumerate(bits):
        swap = pltpu.make_async_remote_copy(
            src_ref=sum_v.at[2 * at],
            dst_ref=sum_v.at[2 * at + 1],
            send_sem=sum_send.at[at],
            recv_sem=sum_recv.at[at],
            device_id=(dp, partner(tp, bit)),
            device_id_type=MESH,
        )
        swap.start()
        swap.wait()
        sum_v[2 * at + 2] = sum_v[2 * at] + sum_v[2 * at + 1]
    gain_out[...] = sum_v[2 * len(bits)] / own_gain_ref[...]
    ring.finish()
    collect.finish()


def project_back(n, n_tp, rows, grads, gain, own_gain, sums, normed, gated, middle_all, grad_middle, x_rel, weights):
    total, width = normed.shape
    mine = x_rel.shape[0]
    micro = mine // rows
    blocks = [(g.shape[1], BLOCK) for g in grads] + [(gated.shape[1], BLOCK)]
    shape = jax.ShapeDtypeStruct
    dma = pltpu.SemaphoreType.DMA
    return pl.pallas_call(
        functools.partial(out_kernel, n, n_tp),
        out_shape=tuple(shape(s, F32) for s in blocks)
        + (shape((8, BLOCK), F32), shape((micro, rows, width), F32)),
        in_specs=[vmem()] * 7 + [anyspec()] * 9,
        out_specs=(vmem(),) * 7,
        scratch_shapes=[
            pltpu.VMEM((total, width), BF),
            pltpu.VMEM(gated.shape, BF),
            pltpu.VMEM((total, width), BF),
            pltpu.VMEM((mine, width), F32),
            pltpu.VMEM((mine, width), F32),
        ]
        + [pltpu.VMEM(s, F32) for s in blocks]
        + [pltpu.VMEM((2,) + s, BF) for s in blocks]
        + [pltpu.VMEM((2,) + s, BF) for s in blocks]
        + [pltpu.VMEM((2,) + s, BF) for s in blocks[:4]]
        + [
            pltpu.VMEM((total, width), BF),
            pltpu.VMEM((mine, width), F32),
            pltpu.VMEM((n_tp - 1, mine, width), BF),
            dma((n - 1, 5, 2)),
            dma((n - 1, 5, 2)),
            pltpu.SemaphoreType.REGULAR((5, 2)),
            dma((n_tp - 1, micro)),
            dma((n_tp - 1, micro)),
            pltpu.VMEM((2 * len(bits_of(n_tp)) + 1, 8, BLOCK), F32),
            dma((len(bits_of(n_tp)),)),
            dma((len(bits_of(n_tp)),)),
            dma((2, 4)),
            dma((5,)),
        ],
        compiler_params=pltpu.CompilerParams(
            collective_id=2, has_side_effects=True, vmem_limit_bytes=66_000_000
        ),
        cost_estimate=pl.CostEstimate(
            flops=4 * total * width * sum(s[0] for s in blocks),
            bytes_accessed=60_000_000,
            transcendentals=0,
        ),
        name="out_kernel",
    )(*grads, gain, own_gain, sums, normed, gated, middle_all, grad_middle, x_rel, *weights)


def finish_kernel(
    n,
    n_tp,
    passed,
    turned,
    *refs,
):
    sources = refs[: passed + turned]
    middle_ref, near_ref, far_ref = refs[passed + turned : passed + turned + 3]
    targets = refs[passed + turned + 3 : 2 * (passed + turned) + 3]
    block_out = refs[2 * (passed + turned) + 3]
    scratch = refs[2 * (passed + turned) + 4 :]
    held, (middle_v, near_v, far_v, block_v), (sem_in, sem_out) = (
        scratch[: passed + 2 * turned],
        scratch[passed + 2 * turned : passed + 2 * turned + 4],
        scratch[passed + 2 * turned + 4 :],
    )
    micro, rows, width = block_v.shape
    pos = ring_position(lax.axis_index("dp"), n)
    count = passed + turned
    ins = [
        pltpu.make_async_copy(sources[i], held[i], sem_in.at[i]) for i in range(count)
    ] + [
        pltpu.make_async_copy(source, target, sem_in.at[count + i])
        for i, (source, target) in enumerate(
            ((middle_ref, middle_v), (near_ref, near_v), (far_ref, far_v))
        )
    ]
    for copy in ins[count:] + ins[:count]:
        copy.start()
    results = list(held[:passed]) + list(held[count:])
    outs = [pltpu.make_async_copy(results[i], targets[i], sem_out.at[i]) for i in range(count)]
    outs.append(pltpu.make_async_copy(block_v, block_out, sem_out.at[count]))
    for copy in ins[count:]:
        copy.wait()

    @pl.loop(0, micro * rows // STEP)
    def _(r):
        at = pl.multiple_of(r * STEP, STEP)
        m, inner = at // rows, pl.multiple_of(at % rows, STEP)
        here = pl.ds(at, STEP)
        for i in range(n):
            for side in range(2):
                lanes = pl.ds(i * BLOCK + side * LANE, LANE)
                spot = ring_index((pos + (n - i if side == 0 else i)) % n, n)
                there = pl.ds(pl.multiple_of(spot * BLOCK + side * LANE, LANE), LANE)
                block_v[m, pl.ds(inner, STEP), there] = middle_v[here, lanes] + (
                    near_v[here, lanes] + far_v[here, lanes].astype(F32)
                )

    outs[count].start()
    for i in range(passed):
        ins[i].wait()
        outs[i].start()
    for i in range(turned):
        ins[passed + i].wait()
        held[count + i][...] = held[passed + i][...].T
        outs[passed + i].start()
    for copy in outs:
        copy.wait()


def finish(n, n_tp, passed, turned, middle, near, far, block_shape):
    shape = jax.ShapeDtypeStruct
    results = tuple(shape(a.shape, a.dtype) for a in passed) + tuple(
        shape(a.shape[::-1], a.dtype) for a in turned
    )
    count = len(passed) + len(turned)
    return pl.pallas_call(
        functools.partial(finish_kernel, n, n_tp, len(passed), len(turned)),
        out_shape=results + (shape(block_shape, F32),),
        in_specs=[anyspec()] * (count + 3),
        out_specs=(anyspec(),) * (count + 1),
        scratch_shapes=[pltpu.VMEM(a.shape, a.dtype) for a in passed]
        + [pltpu.VMEM(a.shape, a.dtype) for a in turned]
        + [pltpu.VMEM(a.shape[::-1], a.dtype) for a in turned]
        + [
            pltpu.VMEM(middle.shape, F32),
            pltpu.VMEM(near.shape, F32),
            pltpu.VMEM(far.shape, BF),
            pltpu.VMEM(block_shape, F32),
            pltpu.SemaphoreType.DMA((count + 3,)),
            pltpu.SemaphoreType.DMA((count + 1,)),
        ],
        compiler_params=pltpu.CompilerParams(vmem_limit_bytes=48_000_000),
        name="finish_kernel",
    )(*passed, *turned, middle, near, far)


def normalize(row_block, gain_vec):
    row_scale = lax.rsqrt(jnp.mean(row_block * row_block, axis=-1, keepdims=True) + EPS)
    return (row_block * row_scale * gain_vec.astype(jnp.float32), row_scale)


def norm_back(grad_rows, row_block, row_scale, gain_vec):
    scaled_grad = grad_rows * gain_vec.astype(jnp.float32)
    back_rows = row_scale * (
        scaled_grad
        - row_block
        * row_scale
        * row_scale
        * jnp.mean(scaled_grad * row_block, axis=-1, keepdims=True)
    )
    return (back_rows, jnp.sum(grad_rows * row_block * row_scale, axis=0))


def angles(length, feature_width):
    half_width = feature_width // 2
    frequency = jnp.exp(-math.log(10000.0) * jnp.arange(half_width, dtype=jnp.float32) / half_width)
    turns = jnp.arange(length, dtype=jnp.float32)[:, None] * frequency[None, :]
    return (jnp.cos(turns)[:, None, :], jnp.sin(turns)[:, None, :])


def decays(length, head_ids):
    places = jnp.arange(length, dtype=jnp.float32)
    spacing = places[:, None] - places[None, :]
    log_rate = jnp.log(1.0 - jnp.exp2(-5.0 - head_ids))
    return jnp.where(
        spacing[None] >= 0.0,
        jnp.exp(jnp.maximum(spacing, 0.0)[None] * log_rate[:, None, None]),
        0.0,
    )


def rotate(value_vectors, cosine_table, sine_table):
    half_width = value_vectors.shape[-1] // 2
    lower = value_vectors[..., :half_width]
    upper = value_vectors[..., half_width:]
    return jnp.concatenate(
        [lower * cosine_table - upper * sine_table, upper * cosine_table + lower * sine_table],
        axis=-1,
    )


def unrotate(value_vectors, cosine_table, sine_table):
    half_width = value_vectors.shape[-1] // 2
    lower = value_vectors[..., :half_width]
    upper = value_vectors[..., half_width:]
    return jnp.concatenate(
        [lower * cosine_table + upper * sine_table, upper * cosine_table - lower * sine_table],
        axis=-1,
    )


def plain_gelu_parts(pre_act):
    normal_cdf = 0.5 * (1.0 + lax.erf(pre_act * (1.0 / math.sqrt(2.0))))
    density = jnp.exp(-0.5 * pre_act * pre_act) * (1.0 / math.sqrt(2.0 * math.pi))
    return (pre_act * normal_cdf, normal_cdf + pre_act * density)


def inner_rows(left_rows, right_rows):
    return lax.dot_general(
        left_rows, right_rows, (((0,), (0,)), ((), ())), preferred_element_type=jnp.float32
    )


def times_t(left_rows, right_rows):
    return lax.dot_general(
        left_rows, right_rows, (((1,), (1,)), ((), ())), preferred_element_type=jnp.float32
    )


def forward_pass(rows_in, gathered, cosine_table, sine_table, decay_mask):
    (
        first_gain,
        second_gain,
        query_weight,
        key_weight,
        value_weight,
        swish_weight,
        output_weight,
        up_projection_matrix,
        gelu_weight,
        down_weight,
    ) = gathered
    local_heads = decay_mask.shape[0]
    scale_qk = 1.0 / math.sqrt(HK)
    normed, first_scale = normalize(rows_in, first_gain)
    normed_all = lax.all_gather(normed.astype(jnp.bfloat16), "tensor", axis=0, tiled=True)
    total_rows = normed_all.shape[0]
    sequences = total_rows // LEN
    query_turned_rows = rotate(
        jnp.dot(normed_all, query_weight, preferred_element_type=jnp.float32).reshape(
            sequences, LEN, local_heads, HK
        ),
        cosine_table,
        sine_table,
    ).astype(jnp.bfloat16)
    key_turned_rows = rotate(
        jnp.dot(normed_all, key_weight, preferred_element_type=jnp.float32).reshape(
            sequences, LEN, local_heads, HK
        ),
        cosine_table,
        sine_table,
    ).astype(jnp.bfloat16)
    value_rows = (
        jnp.dot(normed_all, value_weight, preferred_element_type=jnp.float32)
        .astype(jnp.bfloat16)
        .reshape(sequences, LEN, local_heads, HV)
    )
    gate_pre = jnp.dot(normed_all, swish_weight, preferred_element_type=jnp.float32)
    unscaled_logits = jnp.einsum(
        "snhd,smhd->shnm", query_turned_rows, key_turned_rows, preferred_element_type=jnp.float32
    )
    weight_bf = (unscaled_logits * (decay_mask * scale_qk)).astype(jnp.bfloat16)
    retained = jnp.einsum(
        "shnm,smhe->snhe", weight_bf, value_rows, preferred_element_type=jnp.float32
    )
    group_scale = lax.rsqrt(jnp.mean(retained * retained, axis=-1, keepdims=True) + GROUP_EPS)
    grouped = (retained * group_scale).reshape(total_rows, local_heads * HV)
    sigmoid_gate = jax.nn.sigmoid(gate_pre)
    swish_val = gate_pre * sigmoid_gate
    gated_rows = (swish_val * grouped).astype(jnp.bfloat16)
    attention = lax.psum_scatter(
        jnp.dot(gated_rows, output_weight, preferred_element_type=jnp.float32),
        "tensor",
        scatter_dimension=0,
        tiled=True,
    )
    middle = rows_in + attention
    second, second_scale = normalize(middle, second_gain)
    second_all = lax.all_gather(second.astype(jnp.bfloat16), "tensor", axis=0, tiled=True)
    up_pre = jnp.dot(second_all, up_projection_matrix, preferred_element_type=jnp.float32)
    gelu_pre = jnp.dot(second_all, gelu_weight, preferred_element_type=jnp.float32)
    gelu_val, gelu_slope = plain_gelu_parts(gelu_pre)
    hidden = (gelu_val * up_pre).astype(jnp.bfloat16)
    block_rows = middle + lax.psum_scatter(
        jnp.dot(hidden, down_weight, preferred_element_type=jnp.float32).astype(jnp.bfloat16),
        "tensor",
        scatter_dimension=0,
        tiled=True,
    ).astype(jnp.float32)
    kept_state = (
        rows_in,
        first_scale,
        normed_all,
        query_turned_rows,
        key_turned_rows,
        value_rows,
        gate_pre,
        weight_bf,
        retained,
        group_scale,
        grouped,
        gated_rows,
        middle,
        second_scale,
        second_all,
        up_pre,
        gelu_val,
        gelu_slope,
        hidden,
    )
    return (block_rows, kept_state)


def backward_pass(kept_state, cot_in, gathered, cosine_table, sine_table, decay_mask):
    (
        first_gain,
        second_gain,
        query_weight,
        key_weight,
        value_weight,
        swish_weight,
        output_weight,
        up_projection_matrix,
        gelu_weight,
        down_weight,
    ) = gathered
    (
        rows_in,
        first_scale,
        normed_all,
        query_turned_rows,
        key_turned_rows,
        value_rows,
        gate_pre,
        weight_bf,
        retained,
        group_scale,
        grouped,
        gated_rows,
        middle,
        second_scale,
        second_all,
        up_pre,
        gelu_val,
        gelu_slope,
        hidden,
    ) = kept_state
    local_heads = decay_mask.shape[0]
    total_rows = normed_all.shape[0]
    scale_qk = 1.0 / math.sqrt(HK)
    cot_all = lax.all_gather(cot_in.astype(jnp.bfloat16), "tensor", axis=0, tiled=True)
    grad_hidden = times_t(cot_all, down_weight)
    grad_down = inner_rows(hidden, cot_all)
    grad_uppre = (grad_hidden * gelu_val).astype(jnp.bfloat16)
    grad_gelupre = (grad_hidden * up_pre * gelu_slope).astype(jnp.bfloat16)
    grad_up = inner_rows(second_all, grad_uppre)
    grad_gelu = inner_rows(second_all, grad_gelupre)
    second_back = lax.psum_scatter(
        times_t(grad_uppre, up_projection_matrix) + times_t(grad_gelupre, gelu_weight),
        "tensor",
        scatter_dimension=0,
        tiled=True,
    )
    middle_back, grad_gain_two = norm_back(second_back, middle, second_scale, second_gain)
    grad_middle = cot_in + middle_back
    middle_all = lax.all_gather(grad_middle.astype(jnp.bfloat16), "tensor", axis=0, tiled=True)
    grad_gated = times_t(middle_all, output_weight)
    grad_out = inner_rows(gated_rows, middle_all)
    sigmoid_gate = jax.nn.sigmoid(gate_pre)
    swish_val = gate_pre * sigmoid_gate
    grad_swishpre = (
        grad_gated * grouped * (sigmoid_gate * (1.0 + gate_pre * (1.0 - sigmoid_gate)))
    ).astype(jnp.bfloat16)
    grad_grouped = (grad_gated * swish_val).reshape(retained.shape)
    grad_retained = (
        group_scale
        * (
            grad_grouped
            - retained
            * group_scale
            * group_scale
            * jnp.mean(grad_grouped * retained, axis=-1, keepdims=True)
        )
    ).astype(jnp.bfloat16)
    grad_valrows = jnp.einsum(
        "shnm,snhe->smhe", weight_bf, grad_retained, preferred_element_type=jnp.float32
    ).astype(jnp.bfloat16)
    grad_weight = jnp.einsum(
        "snhe,smhe->shnm", grad_retained, value_rows, preferred_element_type=jnp.float32
    )
    grad_retention_logits = (grad_weight * (decay_mask * scale_qk)).astype(jnp.bfloat16)
    grad_query_rotated_rows = jnp.einsum(
        "shnm,smhd->snhd",
        grad_retention_logits,
        key_turned_rows,
        preferred_element_type=jnp.float32,
    )
    grad_key_rotated_rows = jnp.einsum(
        "shnm,snhd->smhd",
        grad_retention_logits,
        query_turned_rows,
        preferred_element_type=jnp.float32,
    )
    grad_qpre = (
        unrotate(grad_query_rotated_rows, cosine_table, sine_table)
        .astype(jnp.bfloat16)
        .reshape(total_rows, local_heads * HK)
    )
    grad_kpre = (
        unrotate(grad_key_rotated_rows, cosine_table, sine_table)
        .astype(jnp.bfloat16)
        .reshape(total_rows, local_heads * HK)
    )
    grad_vflat = grad_valrows.reshape(total_rows, local_heads * HV)
    first_back = lax.psum_scatter(
        times_t(grad_qpre, query_weight)
        + times_t(grad_kpre, key_weight)
        + times_t(grad_vflat, value_weight)
        + times_t(grad_swishpre, swish_weight),
        "tensor",
        scatter_dimension=0,
        tiled=True,
    )
    grad_query = inner_rows(normed_all, grad_qpre)
    grad_key = inner_rows(normed_all, grad_kpre)
    grad_value = inner_rows(normed_all, grad_vflat)
    grad_swish = inner_rows(normed_all, grad_swishpre)
    input_back, grad_gain_one = norm_back(first_back, rows_in, first_scale, first_gain)
    grad_rows = grad_middle + input_back
    pieces = (
        grad_gain_one,
        grad_gain_two,
        grad_query,
        grad_key,
        grad_value,
        grad_swish,
        grad_out,
        grad_up,
        grad_gelu,
        grad_down,
    )
    return (grad_rows, pieces)


def plain_body(
    block_input,
    cotangent,
    first_gain,
    second_gain,
    query_weight,
    key_weight,
    value_weight,
    swish_weight,
    output_weight,
    up_projection_matrix,
    gelu_weight,
    down_weight,
):
    local_heads = query_weight.shape[1] // HK
    head_ids = (lax.axis_index("tensor") * local_heads + jnp.arange(local_heads)).astype(
        jnp.float32
    )
    cosine_table, sine_table = angles(LEN, HK)
    decay_mask = decays(LEN, head_ids)
    output_list = []
    grad_list = []
    totals = ()
    for micro_idx in range(block_input.shape[0]):
        forward_set = (
            lax.all_gather(first_gain, "dp", axis=0, tiled=True),
            lax.all_gather(second_gain, "dp", axis=0, tiled=True),
            lax.all_gather(query_weight, "dp", axis=0, tiled=True),
            lax.all_gather(key_weight, "dp", axis=0, tiled=True),
            lax.all_gather(value_weight, "dp", axis=0, tiled=True),
            lax.all_gather(swish_weight, "dp", axis=0, tiled=True),
            lax.all_gather(output_weight, "dp", axis=1, tiled=True),
            lax.all_gather(up_projection_matrix, "dp", axis=0, tiled=True),
            lax.all_gather(gelu_weight, "dp", axis=0, tiled=True),
            lax.all_gather(down_weight, "dp", axis=1, tiled=True),
        )
        block_rows, kept_state = forward_pass(
            block_input[micro_idx], forward_set, cosine_table, sine_table, decay_mask
        )
        held = lax.optimization_barrier(
            (
                (
                    first_gain,
                    second_gain,
                    query_weight,
                    key_weight,
                    value_weight,
                    swish_weight,
                    output_weight,
                    up_projection_matrix,
                    gelu_weight,
                    down_weight,
                ),
                block_rows,
            )
        )[0]
        backward_set = (
            lax.all_gather(held[0], "dp", axis=0, tiled=True),
            lax.all_gather(held[1], "dp", axis=0, tiled=True),
            lax.all_gather(held[2], "dp", axis=0, tiled=True),
            lax.all_gather(held[3], "dp", axis=0, tiled=True),
            lax.all_gather(held[4], "dp", axis=0, tiled=True),
            lax.all_gather(held[5], "dp", axis=0, tiled=True),
            lax.all_gather(held[6], "dp", axis=1, tiled=True),
            lax.all_gather(held[7], "dp", axis=0, tiled=True),
            lax.all_gather(held[8], "dp", axis=0, tiled=True),
            lax.all_gather(held[9], "dp", axis=1, tiled=True),
        )
        grad_rows, pieces = backward_pass(
            kept_state, cotangent[micro_idx], backward_set, cosine_table, sine_table, decay_mask
        )
        output_list.append(block_rows)
        grad_list.append(grad_rows)
        if micro_idx == 0:
            totals = tuple(pieces)
        else:
            totals = tuple((total + piece for total, piece in zip(totals, pieces)))
    totals = (
        lax.psum_scatter(totals[0], "dp", scatter_dimension=0, tiled=True),
        lax.psum_scatter(totals[1], "dp", scatter_dimension=0, tiled=True),
        lax.psum_scatter(totals[2], "dp", scatter_dimension=0, tiled=True),
        lax.psum_scatter(totals[3], "dp", scatter_dimension=0, tiled=True),
        lax.psum_scatter(totals[4], "dp", scatter_dimension=0, tiled=True),
        lax.psum_scatter(totals[5], "dp", scatter_dimension=0, tiled=True),
        lax.psum_scatter(totals[6], "dp", scatter_dimension=1, tiled=True),
        lax.psum_scatter(totals[7], "dp", scatter_dimension=0, tiled=True),
        lax.psum_scatter(totals[8], "dp", scatter_dimension=0, tiled=True),
        lax.psum_scatter(totals[9], "dp", scatter_dimension=1, tiled=True),
    )
    gain_first, gain_second = lax.psum((totals[0], totals[1]), "tensor")
    return (
        jnp.stack(output_list, axis=0),
        jnp.stack(grad_list, axis=0),
        gain_first,
        gain_second,
        totals[2],
        totals[3],
        totals[4],
        totals[5],
        totals[6],
        totals[7],
        totals[8],
        totals[9],
    )


def ring_body(
    n_dp,
    n_tp,
    block_input,
    cotangent,
    first_gain,
    second_gain,
    query_weight,
    key_weight,
    value_weight,
    swish_weight,
    output_weight,
    up_projection_matrix,
    gelu_weight,
    down_weight,
):
    micro, rows, width = block_input.shape
    local_heads = query_weight.shape[1] // HK
    window = n_tp * rows

    me = lax.axis_index("tensor")
    head_ids = (me * local_heads + jnp.arange(local_heads)).astype(F32)
    chunk_of = jnp.arange(n_tp) ^ me
    natural = (chunk_of[:, None] * rows + jnp.arange(rows)[None, :]).reshape(window)
    place = (natural % LEN).astype(F32)
    half_key = HK // 2
    frequency = jnp.exp(-math.log(10000.0) * jnp.arange(half_key, dtype=F32) / half_key)
    turns = place[:, None] * frequency[None, :]
    cosine, sine = jnp.cos(turns), jnp.sin(turns)
    log_rate = jnp.log(1.0 - jnp.exp2(-5.0 - head_ids))
    spots = natural.astype(F32)
    tables = (
        jnp.broadcast_to(spots[:, None], (window, LANE)),
        spots[None, :],
        jnp.broadcast_to(log_rate[:, None], (local_heads, window)),
    )

    gains_own = jnp.stack([first_gain, second_gain]).astype(F32)
    query, key, value, gate, x_rel, cot_rel, gains, normed, cot_all, *w_in, w_o = project_in(
        n_dp,
        n_tp,
        block_input,
        cotangent,
        gains_own,
        cosine,
        sine,
        (query_weight.T, key_weight.T, value_weight.T, swish_weight.T),
        output_weight,
    )
    gated, middle, hidden, gelu_val, up_slope, second, w_u, w_l, w_d, near, far = mid_forward(
        n_dp,
        n_tp,
        query,
        key,
        value,
        gate,
        x_rel,
        gains,
        tables,
        w_o,
        up_projection_matrix.T,
        gelu_weight.T,
        down_weight,
    )

    far = lax.ppermute(far, "tensor", [(i, i ^ (n_tp // 2)) for i in range(n_tp)])

    grad_down, grad_up, grad_gelu, sums, grad_middle, middle_all, *grads = (
        mid_backward(
            n_dp,
            n_tp,
            gains,
            tables,
            cosine,
            sine,
            cot_all,
            w_d,
            gelu_val,
            up_slope,
            hidden,
            second,
            w_u,
            w_l,
            middle,
            cot_rel,
            w_o,
            query,
            key,
            value,
            gate,
        )
    )
    grad_query, grad_key, grad_value, grad_swish, grad_out, gain_grads, grad_rows = project_back(
        n_dp,
        n_tp,
        rows,
        grads,
        gains,
        jnp.pad(gains_own, ((0, 6), (0, 0)), constant_values=1.0),
        sums,
        normed,
        gated,
        middle_all,
        grad_middle,
        x_rel,
        w_in,
    )

    passed = (grad_value, grad_swish, grad_out, grad_up, grad_gelu, grad_down, grad_rows)
    *passed, grad_query, grad_key, block_rows = finish(
        n_dp, n_tp, passed, (grad_query, grad_key), middle, near, far, block_input.shape
    )
    grad_value, grad_swish, grad_out, grad_up, grad_gelu, grad_down, grad_rows = passed

    return (
        block_rows,
        grad_rows,
        gain_grads[0],
        gain_grads[1],
        grad_query,
        grad_key,
        grad_value.T,
        grad_swish.T,
        grad_out,
        grad_up.T,
        grad_gelu.T,
        grad_down,
    )


def solution(mesh):
    rows = P(None, ("dp", "tensor"), None)
    wide, tall, gain = P("dp", "tensor"), P("tensor", "dp"), P("dp")
    n_dp, n_tp = mesh.shape["dp"], mesh.shape["tensor"]

    def run(*arrays):
        blocks = arrays[2].shape[0] == BLOCK and n_dp % 2 == 0 and n_dp > 2
        pairs = n_tp > 1 and n_tp & (n_tp - 1) == 0
        aligned = (n_tp * arrays[0].shape[1]) % LEN == 0 and arrays[0].shape[1] % LANE == 0
        if blocks and pairs and aligned:
            return ring_body(n_dp, n_tp, *arrays)
        return plain_body(*arrays)

    return jax.shard_map(
        run,
        mesh=mesh,
        in_specs=(rows, rows, gain, gain) + (wide,) * 4 + (tall, wide, wide, tall),
        out_specs=(rows, rows, gain, gain) + (wide,) * 4 + (tall, wide, wide, tall),
        check_vma=False,
    )
```

```python
import functools
import math

import jax
import jax.numpy as jnp
from jax import lax
from jax.experimental import pallas as pl
from jax.experimental.pallas import tpu as pltpu
from jax.sharding import PartitionSpec as P

HK = 256
HV = 432
LEN = 512
EPS = 1e-05
GROUP_EPS = 1.0
BF = jnp.bfloat16
F32 = jnp.float32
MESH = pl.DeviceIdType.MESH
LANE = 128
BLOCK = 2 * LANE
SLOTS = 4
STEP = 32


def ring_position(index, count):
    low = index // 2
    return low + (index % 2) * (count - 1 - 2 * low)


def ring_index(position, count):
    high = position // (count // 2)
    return (1 - high) * (2 * position) + high * (2 * (count - 1 - position) + 1)


def bits_of(count):
    return [1 << i for i in range(count.bit_length() - 1)]


def anyspec():
    return pl.BlockSpec(memory_space=pl.ANY)


def vmem():
    return pl.BlockSpec(memory_space=pltpu.VMEM)


def nt(left, right):
    return lax.dot_general(left, right, (((1,), (1,)), ((), ())), preferred_element_type=F32)


def nn(left, right):
    return lax.dot_general(left, right, (((1,), (0,)), ((), ())), preferred_element_type=F32)


def tn(left, right):
    return lax.dot_general(left, right, (((0,), (0,)), ((), ())), preferred_element_type=F32)


def in_kernel(
    n,
    n_tp,
    x_ref,
    cot_ref,
    gains_ref,
    cos_ref,
    sin_ref,
    wq_ref,
    wk_ref,
    wv_ref,
    wg_ref,
    wo_ref,
    q_out,
    k_out,
    v_out,
    g_out,
    xr_out,
    cr_out,
    gain_out,
    nall_out,
    call_out,
    wq_out,
    wk_out,
    wv_out,
    wg_out,
    wo_out,
    x_v,
    rel_v,
    own_v,
    nall_v,
    gain_v,
    q_acc,
    k_acc,
    v_acc,
    g_acc,
    wq_s,
    wk_s,
    wv_s,
    wg_s,
    wo_s,
    ring_send,
    ring_recv,
    gain_send,
    gain_recv,
    share_send,
    share_recv,
    load_sem,
    local_sem,
):
    micro, rows, width = x_ref.shape
    window = n_tp * rows
    mine = micro * rows
    dp, tp = lax.axis_index("dp"), lax.axis_index("tensor")
    pos = ring_position(dp, n)
    cw = ring_index((pos + 1) % n, n)
    ccw = ring_index((pos + n - 1) % n, n)
    bits = bits_of(n_tp)

    def flip(bit):
        return tp + bit - 2 * bit * ((tp // bit) % 2)

    barrier = pltpu.get_barrier_semaphore()
    for k in range(1, n):
        pl.semaphore_signal(
            barrier, inc=1, device_id=(ring_index((pos + k) % n, n), tp), device_id_type=MESH
        )
    for bit in bits:
        pl.semaphore_signal(barrier, inc=1, device_id=(dp, flip(bit)), device_id_type=MESH)
    pl.semaphore_wait(barrier, n - 1 + len(bits))

    shards = (wq_ref, wk_ref, wv_ref, wg_ref, wo_ref)
    wholes = (wq_out, wk_out, wv_out, wg_out, wo_out)
    slots = (wq_s, wk_s, wv_s, wg_s)
    accs = (q_acc, k_acc, v_acc, g_acc)

    def hop(i, a, side):
        lanes = pl.ds(side * LANE, LANE)
        source = shards[a].at[:, lanes] if i == 0 else wholes[a].at[i, :, lanes]
        target = wholes[a].at[i + 1, :, lanes]
        return pltpu.make_async_remote_copy(
            src_ref=source,
            dst_ref=target,
            send_sem=ring_send.at[i, a, side],
            recv_sem=ring_recv.at[i, a, side],
            device_id=((cw, ccw)[side], tp),
            device_id_type=MESH,
        )

    def load(i, a):
        source = shards[a] if i == 0 else wholes[a].at[i]
        return pltpu.make_async_copy(source, slots[a].at[i % SLOTS], load_sem.at[i % SLOTS, a])

    for a in range(5):
        for side in range(2):
            hop(0, a, side).start()
    wo_own = pltpu.make_async_copy(wo_ref, wo_s, local_sem.at[3 + micro])
    wo_own.start()
    x_copy = pltpu.make_async_copy(x_ref, x_v, local_sem.at[0])
    x_copy.start()
    for a in range(4):
        load(0, a).start()

    def gain_copy(k):
        return pltpu.make_async_remote_copy(
            src_ref=gains_ref,
            dst_ref=gain_v.at[k],
            send_sem=gain_send.at[k],
            recv_sem=gain_recv.at[k],
            device_id=(ring_index((pos + k) % n, n), tp),
            device_id_type=MESH,
        )

    own_gain = pltpu.make_async_copy(gains_ref, gain_v.at[0], local_sem.at[1])
    own_gain.start()
    for k in range(1, n):
        gain_copy(k).start()
    own_gain.wait()
    for k in range(1, n):
        gain_copy(k).wait()
    for i in range(n):
        gain_out[:, pl.ds(i * BLOCK, LANE)] = gain_v[i, :, pl.ds(0, LANE)]
        gain_out[:, pl.ds(i * BLOCK + LANE, LANE)] = gain_v[(n - i) % n, :, pl.ds(LANE, LANE)]

    def natural(i, side):
        at = ring_index((pos + (n - i if side == 0 else i)) % n, n) * BLOCK + side * LANE
        return pl.ds(pl.multiple_of(at, LANE), LANE)

    def share_copy(source, target, slot, m, key, bit):
        start = m * window + key * rows
        arrive = m * window + (key ^ bit) * rows
        return pltpu.make_async_remote_copy(
            src_ref=source.at[pl.ds(start, rows)] if source.shape[0] != mine
            else source.at[pl.ds(m * rows, rows)],
            dst_ref=target.at[pl.ds(arrive, rows)],
            send_sem=share_send.at[slot, m, key ^ bit],
            recv_sem=share_recv.at[slot, m, key ^ bit],
            device_id=(dp, flip(bit)),
            device_id_type=MESH,
        )

    x_copy.wait()
    step_rows = min(rows, 32)

    @pl.loop(0, mine // step_rows)
    def _(r):
        at = pl.multiple_of(r * step_rows, step_rows)
        m, inner = at // rows, at % rows
        chunk = x_v[m, pl.ds(pl.multiple_of(inner, step_rows), step_rows), :]
        scale = lax.rsqrt(jnp.mean(chunk * chunk, axis=-1, keepdims=True) + EPS)
        there = pl.ds(pl.multiple_of(m * window + inner, step_rows), step_rows)
        for i in range(n):
            for side in range(2):
                lanes = pl.ds(i * BLOCK + side * LANE, LANE)
                part = x_v[
                    m, pl.ds(pl.multiple_of(inner, step_rows), step_rows), natural(i, side)
                ]
                rel_v[0, pl.ds(at, step_rows), lanes] = part
                nall_v[there, lanes] = (part * scale * gain_out[0:1, lanes]).astype(BF)

    for bit in bits[::-1]:
        for m in range(micro):
            share_copy(nall_v, nall_v, 0, m, 0, bit).start()
    rel_copy = pltpu.make_async_copy(rel_v.at[0], xr_out, local_sem.at[2])
    rel_copy.start()
    c_copy = pltpu.make_async_copy(cot_ref, x_v, local_sem.at[0])
    c_copy.start()
    c_copy.wait()

    @pl.loop(0, mine // step_rows)
    def _(r):
        at = pl.multiple_of(r * step_rows, step_rows)
        m, inner = at // rows, at % rows
        for i in range(n):
            for side in range(2):
                lanes = pl.ds(i * BLOCK + side * LANE, LANE)
                part = x_v[
                    m, pl.ds(pl.multiple_of(inner, step_rows), step_rows), natural(i, side)
                ]
                rel_v[1, pl.ds(at, step_rows), lanes] = part
                own_v[pl.ds(at, step_rows), lanes] = part.astype(BF)

    cot_rel = pltpu.make_async_copy(rel_v.at[1], cr_out, local_sem.at[1])
    cot_rel.start()
    own_copies = [
        pltpu.make_async_copy(
            own_v.at[pl.ds(m * rows, rows)],
            call_out.at[pl.ds(m * window, rows)],
            local_sem.at[3 + m],
        )
        for m in range(micro)
    ]
    for copy in own_copies:
        copy.start()

    def relay(target, slot):
        source0 = nall_v if slot == 0 else own_v
        for at, bit in enumerate(bits[::-1]):
            for key in range(0, n_tp, 2 * bit):
                for m in range(micro):
                    if key:
                        share_copy(target, target, slot, m, key, bit).start()
            for key in range(0, n_tp, 2 * bit):
                for m in range(micro):
                    share_copy(
                        source0 if key == 0 else target, target, slot, m, key, bit
                    ).wait_recv()

    tile = 256
    heads = wq_ref.shape[0] // HK
    half = HK // 2

    def product(j, a, last):
        load(j, a).wait()
        if j == 0:
            pltpu.make_async_copy(
                slots[a].at[0], wholes[a].at[0], load_sem.at[SLOTS, a]
            ).start()

        @pl.loop(0, micro * window // tile)
        def _(r):
            at = pl.multiple_of(r * tile, tile)
            here = pl.ds(at, tile)
            part = nt(nall_v[here, pl.ds(j * BLOCK, BLOCK)], slots[a][j % SLOTS])
            if j > 0:
                part = accs[a][here, :] + part
            if not last:
                accs[a][here, :] = part
            elif a < 2:
                place = pl.ds(pl.multiple_of(at % window, tile), tile)
                cosine, sine = cos_ref[place, :], sin_ref[place, :]
                out = (q_out, k_out)[a]
                for h in range(heads):
                    low = part[:, h * HK : h * HK + half]
                    high = part[:, h * HK + half : (h + 1) * HK]
                    out[here, pl.ds(h * HK, half)] = (low * cosine - high * sine).astype(BF)
                    out[here, pl.ds(h * HK + half, half)] = (high * cosine + low * sine).astype(BF)
            elif a == 2:
                v_out[here, :] = part.astype(BF)
            else:
                g_out[here, :] = part

        if j == 0:
            pltpu.make_async_copy(
                slots[a].at[0], wholes[a].at[0], load_sem.at[SLOTS, a]
            ).wait()

    nall_copy = pltpu.make_async_copy(nall_v, nall_out, local_sem.at[0])
    start_at = 3
    done = 0
    for i in range(n + 1):
        if i == start_at:
            relay(nall_v, 0)
            nall_copy.start()
            for bit in bits[::-1]:
                for m in range(micro):
                    share_copy(own_v, call_out, 1, m, 0, bit).start()
        if i == n - 1:
            relay(call_out, 1)
        todo = []
        if i >= start_at:
            goal = min(i - 1, done + 1) if i < n else n - 1
            todo = list(range(done, goal + 1))
            done = goal + 1
        if i == 1:
            wo_own.wait()
            wo_own = pltpu.make_async_copy(wo_s, wo_out.at[0], local_sem.at[3 + micro])
            wo_own.start()
        for a in range(5):
            if 0 < i < n:
                hop(i - 1, a, 0).wait_recv()
                hop(i - 1, a, 1).wait_recv()
                if i < n - 1:
                    hop(i, a, 0).start()
                    hop(i, a, 1).start()
                if a < 4:
                    load(i, a).start()
            if a < 4:
                for j in todo:
                    product(j, a, j == n - 1)

    for i in range(n - 1):
        for a in range(5):
            hop(i, a, 0).wait_send()
            hop(i, a, 1).wait_send()
    for slot, source0, target in ((0, nall_v, nall_v), (1, own_v, call_out)):
        for bit in bits[::-1]:
            for key in range(0, n_tp, 2 * bit):
                for m in range(micro):
                    share_copy(
                        source0 if key == 0 else target, target, slot, m, key, bit
                    ).wait_send()
    for copy in own_copies + [rel_copy, cot_rel, nall_copy, wo_own]:
        copy.wait()


def project_in(n, n_tp, x, cot, gains, cosine, sine, weights, wo):
    micro, rows, width = x.shape
    total = micro * n_tp * rows
    mine = micro * rows
    sizes = [w.shape[0] for w in weights]
    shape = jax.ShapeDtypeStruct
    flops = 2 * total * width * sum(sizes)
    return pl.pallas_call(
        functools.partial(in_kernel, n, n_tp),
        out_shape=(
            shape((total, sizes[0]), BF),
            shape((total, sizes[1]), BF),
            shape((total, sizes[2]), BF),
            shape((total, sizes[3]), F32),
            shape((mine, width), F32),
            shape((mine, width), F32),
            shape((2, width), F32),
            shape((total, width), BF),
            shape((total, width), BF),
        )
        + tuple(shape((n, s, BLOCK), BF) for s in sizes)
        + (shape((n,) + wo.shape, BF),),
        in_specs=[anyspec(), anyspec(), anyspec(), vmem(), vmem()] + [anyspec()] * 5,
        out_specs=(vmem(),) * 4 + (anyspec(),) * 2 + (vmem(),) + (anyspec(),) * 7,
        scratch_shapes=[
            pltpu.VMEM(x.shape, F32),
            pltpu.VMEM((2, mine, width), F32),
            pltpu.VMEM((mine, width), BF),
            pltpu.VMEM((total, width), BF),
            pltpu.VMEM((n, 2, BLOCK), F32),
        ]
        + [pltpu.VMEM((total, s), F32) for s in sizes]
        + [pltpu.VMEM((SLOTS, s, BLOCK), BF) for s in sizes]
        + [
            pltpu.VMEM(wo.shape, BF),
            pltpu.SemaphoreType.DMA((n - 1, 5, 2)),
            pltpu.SemaphoreType.DMA((n - 1, 5, 2)),
            pltpu.SemaphoreType.DMA((n,)),
            pltpu.SemaphoreType.DMA((n,)),
            pltpu.SemaphoreType.DMA((2, micro, n_tp)),
            pltpu.SemaphoreType.DMA((2, micro, n_tp)),
            pltpu.SemaphoreType.DMA((SLOTS + 1, 4)),
            pltpu.SemaphoreType.DMA((4 + micro,)),
        ],
        compiler_params=pltpu.CompilerParams(
            collective_id=1, has_side_effects=True, vmem_limit_bytes=64_000_000
        ),
        cost_estimate=pl.CostEstimate(
            flops=flops, bytes_accessed=60_000_000, transcendentals=0
        ),
        name="in_kernel",
    )(x, cot, gains, cosine, sine, *weights, wo)


def partner(tp, bit):
    return tp + bit - 2 * bit * ((tp // bit) % 2)


def neighbours(n):
    dp, tp = lax.axis_index("dp"), lax.axis_index("tensor")
    pos = ring_position(dp, n)
    return dp, tp, ring_index((pos + 1) % n, n), ring_index((pos + n - 1) % n, n)


def greet(devices):
    barrier = pltpu.get_barrier_semaphore()
    for device in devices:
        pl.semaphore_signal(barrier, inc=1, device_id=device, device_id_type=MESH)
    pl.semaphore_wait(barrier, len(devices))


class Share:
    def __init__(self, dp, tp, n_tp, micro, rows, buf, send, recv):
        self.dp, self.tp, self.n_tp, self.micro, self.rows = dp, tp, n_tp, micro, rows
        self.buf, self.send, self.recv = buf, send, recv
        self.bits = bits_of(n_tp)[::-1]

    def copies(self, bit, m, keys=None):
        window = self.n_tp * self.rows
        for key in range(0, self.n_tp, 2 * bit):
            if keys is None or (key == 0) == keys:
                yield pltpu.make_async_remote_copy(
                    src_ref=self.buf.at[pl.ds(m * window + key * self.rows, self.rows)],
                    dst_ref=self.buf.at[pl.ds(m * window + (key ^ bit) * self.rows, self.rows)],
                    send_sem=self.send.at[m, key ^ bit],
                    recv_sem=self.recv.at[m, key ^ bit],
                    device_id=(self.dp, partner(self.tp, bit)),
                    device_id_type=MESH,
                )

    def begin(self, m):
        for bit in self.bits:
            for copy in self.copies(bit, m, True):
                copy.start()

    def relay(self, m):
        for bit in self.bits:
            for copy in self.copies(bit, m, False):
                copy.start()
            for copy in self.copies(bit, m):
                copy.wait_recv()

    def finish(self):
        for m in range(self.micro):
            for bit in self.bits:
                for copy in self.copies(bit, m):
                    copy.wait_send()


class Collect:
    def __init__(self, dp, tp, n_tp, micro, rows, back, got, own, send, recv):
        self.dp, self.tp, self.n_tp, self.micro, self.rows = dp, tp, n_tp, micro, rows
        self.back, self.got, self.own, self.send, self.recv = back, got, own, send, recv
        self.bits = bits_of(n_tp)

    def keys(self, bit):
        return [key for key in range(0, self.n_tp, bit) if key & bit]

    def copies(self, bit, m):
        window = self.n_tp * self.rows
        for key in self.keys(bit):
            yield pltpu.make_async_remote_copy(
                src_ref=self.back.at[pl.ds(m * window + key * self.rows, self.rows)],
                dst_ref=self.got.at[key - 1, pl.ds(m * self.rows, self.rows)],
                send_sem=self.send.at[key - 1, m],
                recv_sem=self.recv.at[key - 1, m],
                device_id=(self.dp, partner(self.tp, bit)),
                device_id_type=MESH,
            )

    def start(self, bit, m):
        for copy in self.copies(bit, m):
            copy.start()

    def add(self, bit, m):
        window = self.n_tp * self.rows
        for copy in self.copies(bit, m):
            copy.wait_recv()
        for key in self.keys(bit):
            target = key ^ bit

            @pl.loop(0, self.rows // STEP)
            def _(r):
                inner = pl.multiple_of(r * STEP, STEP)
                here = pl.ds(pl.multiple_of(m * self.rows + inner, STEP), STEP)
                there = pl.ds(pl.multiple_of(m * window + target * self.rows + inner, STEP), STEP)
                got = self.got[key - 1, here, :].astype(F32)
                if target == 0:
                    held = self.back[there, :].astype(F32) if bit == 1 else self.own[here, :]
                    self.own[here, :] = held + got
                else:
                    self.back[there, :] = (self.back[there, :].astype(F32) + got).astype(BF)

    def finish(self, bits=None):
        for m in range(self.micro):
            for bit in self.bits if bits is None else bits:
                for copy in self.copies(bit, m):
                    copy.wait_send()


class SumRing:
    def __init__(self, n, tp, cw, ccw, arrays, gradient, send, recv, free):
        self.n, self.tp, self.ways, self.arrays = n, tp, (cw, ccw), arrays
        self.gradient, self.send, self.recv, self.free = gradient, send, recv, free
        self.slots = arrays[0][2].shape[0]
        self.ready = self.done = 0

    def hop(self, s, a, side):
        _, send, recv, _ = self.arrays[a]
        lanes = pl.ds(side * LANE, LANE)
        return pltpu.make_async_remote_copy(
            src_ref=send.at[s % 2, :, lanes],
            dst_ref=recv.at[s % self.slots, :, lanes],
            send_sem=self.send.at[s, a, side],
            recv_sem=self.recv.at[s, a, side],
            device_id=(self.ways[side], self.tp),
            device_id_type=MESH,
        )

    def first(self, a):
        part, send, _, _ = self.arrays[a]
        self.gradient(1 % self.n, a)
        send[0] = part[...].astype(BF)
        self.hop(0, a, 0).start()
        self.hop(0, a, 1).start()

    def prepare(self):
        if self.ready == self.done and self.done < self.n - 1:
            self.ready += 1
            for a in range(len(self.arrays)):
                self.gradient((self.ready + 1) % self.n, a)

    def advance(self):
        n = self.n
        if self.done == n - 1:
            return
        self.prepare()
        self.done += 1
        s = self.done
        for a, (part, send, recv, out) in enumerate(self.arrays):
            self.hop(s - 1, a, 0).wait_recv()
            self.hop(s - 1, a, 1).wait_recv()
            total = part[...] + recv[(s - 1) % self.slots].astype(F32)
            if s == n - 1:
                out[...] = total
                continue
            if s >= 2:
                self.hop(s - 2, a, 0).wait_send()
                self.hop(s - 2, a, 1).wait_send()
            send[s % 2] = total.astype(BF)
            for side in range(2):
                if self.slots < n - 1:
                    if s - 1 < n - 1 - self.slots:
                        pl.semaphore_signal(
                            self.free.at[a, side],
                            inc=1,
                            device_id=(self.ways[1 - side], self.tp),
                            device_id_type=MESH,
                        )
                    if s >= self.slots:
                        pl.semaphore_wait(self.free.at[a, side], 1)
                self.hop(s, a, side).start()

    def finish(self):
        for s in range(max(0, self.n - 3), self.n - 1):
            for a in range(len(self.arrays)):
                self.hop(s, a, 0).wait_send()
                self.hop(s, a, 1).wait_send()


def fill_decay(decay_v, col_ref, row_ref, rate_ref):
    heads, window, _ = decay_v.shape
    scale_qk = 1.0 / math.sqrt(HK)
    for h in range(heads):

        @pl.loop(0, window // LANE)
        def _(r):
            here = pl.ds(pl.multiple_of(r * LANE, LANE), LANE)
            col, row = col_ref[here, 0:1], row_ref[...]
            spacing = col - row
            same = jnp.floor(col * (1.0 / LEN)) == jnp.floor(row * (1.0 / LEN))
            kept = jnp.exp(jnp.maximum(spacing, 0.0) * rate_ref[h : h + 1, :]) * scale_qk
            decay_v[h, here, :] = jnp.where((spacing >= 0.0) & same, kept, 0.0)


def gelu_parts(pre_act):
    normal_cdf = 0.5 * (1.0 + lax.erf(pre_act * (1.0 / math.sqrt(2.0))))
    density = jnp.exp(-0.5 * pre_act * pre_act) * (1.0 / math.sqrt(2.0 * math.pi))
    return (pre_act * normal_cdf, normal_cdf + pre_act * density)


def forward_kernel(
    n,
    n_tp,
    q_ref,
    k_ref,
    v_ref,
    g_ref,
    x_ref,
    gain_ref,
    col_ref,
    row_ref,
    rate_ref,
    wo_ref,
    wu_ref,
    wl_ref,
    wd_ref,
    gated_out,
    middle_out,
    hidden_out,
    value_out,
    slope_out,
    second_out,
    wu_out,
    wl_out,
    wd_out,
    near_out,
    far_out,
    decay_v,
    wo_v,
    back_v,
    own_v,
    got_v,
    second_v,
    wu_v,
    wl_v,
    wd_v,
    up_v,
    ring_send,
    ring_recv,
    part_send,
    part_recv,
    share_send,
    share_recv,
    last_send,
    last_recv,
    local_sem,
):
    total, width = second_v.shape
    mine = x_ref.shape[0]
    window = col_ref.shape[0]
    micro = total // window
    rows = mine // micro
    dp, tp, cw, ccw = neighbours(n)
    bits = bits_of(n_tp)
    greet([(cw, tp), (ccw, tp)] + [(dp, partner(tp, bit)) for bit in bits])

    wholes = (wu_v, wl_v, wd_v)
    shards = (wu_ref, wl_ref, wd_ref)

    units = wd_ref.shape[0]
    split = units // 2 // 16 * 16
    pieces = (
        (0, 0, units),
        (1, 0, units),
        (2, 0, split),
        (2, split, units - split),
    )

    def hop(i, p, side):
        a, low, size = pieces[p]
        span, lanes = pl.ds(low, size), pl.ds(side * LANE, LANE)
        own = isinstance(i, int) and i == 0
        return pltpu.make_async_remote_copy(
            src_ref=shards[a].at[span, lanes] if own else wholes[a].at[i, span, lanes],
            dst_ref=wholes[a].at[i + 1, span, lanes],
            send_sem=ring_send.at[i, p, side],
            recv_sem=ring_recv.at[i, p, side],
            device_id=((cw, ccw)[side], tp),
            device_id_type=MESH,
        )

    def ring_start(i, group):
        for p in group:
            for side in range(2):
                hop(i, p, side).start()

    def ring_step(s, group):
        for p in group:
            for side in range(2):
                hop(s - 1, p, side).wait_recv()
                if isinstance(s, int):
                    if s < n - 1:
                        hop(s, p, side).start()
                else:

                    @pl.when(s < n - 1)
                    def _():
                        hop(s, p, side).start()

    first, second = (0, 1), (2, 3)
    passed = [0]

    def pairs_to(goal):
        while passed[0] < min(goal, n - 1):
            passed[0] += 1
            ring_step(passed[0], first)
            if passed[0] == n - 2:
                ring_start(0, second)

    ring_start(0, first)
    local = [
        pltpu.make_async_copy(wo_ref, wo_v, local_sem.at[0]),
        pltpu.make_async_copy(wu_ref, wu_v.at[0], local_sem.at[1]),
        pltpu.make_async_copy(wl_ref, wl_v.at[0], local_sem.at[2]),
        pltpu.make_async_copy(wd_ref, wd_v.at[0], local_sem.at[3]),
    ]
    for copy in local:
        copy.start()
    fill_decay(decay_v, col_ref, row_ref, rate_ref)
    heads = decay_v.shape[0]
    tile = 256
    collect = Collect(dp, tp, n_tp, micro, rows, back_v, got_v, own_v, part_send, part_recv)
    share = Share(dp, tp, n_tp, micro, rows, second_v, share_send, share_recv)
    for m in range(micro):
        for h in range(heads):
            keys = pl.ds(h * HK, HK)
            values = pl.ds(h * HV, HV)
            inside = pl.ds(m * window, window)

            @pl.loop(0, window // tile)
            def _(r):
                at = pl.multiple_of(r * tile, tile)
                here = pl.ds(pl.multiple_of(m * window + at, tile), tile)
                scores = nt(q_ref[here, keys], k_ref[inside, keys])
                weight = (scores * decay_v[h, pl.ds(at, tile), :]).astype(BF)
                kept = nn(weight, v_ref[inside, values])
                group = lax.rsqrt(jnp.mean(kept * kept, axis=-1, keepdims=True) + GROUP_EPS)
                gate = g_ref[here, values]
                gated_out[here, values] = (gate * jax.nn.sigmoid(gate) * (kept * group)).astype(BF)

        if m == 0:
            local[0].wait()
        for i in range(n):

            @pl.loop(0, window // tile)
            def _(r):
                here = pl.ds(pl.multiple_of(m * window + r * tile, tile), tile)
                back_v[here, pl.ds(i * BLOCK, BLOCK)] = nn(gated_out[here, :], wo_v[i]).astype(BF)

        collect.start(bits[0], m)
        pairs_to(m)

    for copy in local[1:]:
        copy.wait()
    for at, bit in enumerate(bits[:-1]):
        for m in range(micro):
            collect.add(bit, m)
            collect.start(bits[at + 1], m)
    pairs_to(2)
    for m in range(micro):
        collect.add(bits[-1], m)

        @pl.loop(0, rows // STEP)
        def _(r):
            inner = pl.multiple_of(r * STEP, STEP)
            here = pl.ds(pl.multiple_of(m * rows + inner, STEP), STEP)
            there = pl.ds(pl.multiple_of(m * window + inner, STEP), STEP)
            middle = x_ref[here, :] + own_v[here, :]
            middle_out[here, :] = middle
            scale = lax.rsqrt(jnp.mean(middle * middle, axis=-1, keepdims=True) + EPS)
            second_v[there, :] = (middle * scale * gain_ref[1:2, :]).astype(BF)

        share.begin(m)
        pairs_to(3 + m)
    for m in range(micro):
        pairs_to(5 + m)
        share.relay(m)
    pairs_to(n - 1)
    second_copy = pltpu.make_async_copy(second_v, second_out, local_sem.at[0])
    second_copy.start()
    whole_copies = [
        pltpu.make_async_copy(source, target, local_sem.at[1 + at])
        for at, (source, target) in enumerate(((wu_v, wu_out), (wl_v, wl_out), (wd_v, wd_out)))
    ]
    whole_copies[0].start()
    whole_copies[1].start()

    def rows_by(weights, here):
        result = None
        for i in range(n):
            term = nt(second_v[here, pl.ds(i * BLOCK, BLOCK)], weights[i])
            result = term if result is None else result + term
        return result

    tiles = total // tile
    inside_loop = min(tiles, n - 1)

    @pl.loop(0, tiles)
    def _(r):
        here = pl.ds(pl.multiple_of(r * tile, tile), tile)
        up_v[...] = rows_by(wu_v, here)
        gelu_val, gelu_slope = gelu_parts(rows_by(wl_v, here))
        up = up_v[...]
        hidden_out[here, :] = (gelu_val * up).astype(BF)
        value_out[here, :] = gelu_val.astype(BF)
        slope_out[here, :] = (up * gelu_slope).astype(BF)

        @pl.when(r < inside_loop)
        def _():
            ring_step(r + 1, second)

    for s in range(inside_loop + 1, n):
        ring_step(s, second)
    whole_copies[2].start()
    collect.finish()
    last = Collect(dp, tp, n_tp, micro, rows, back_v, got_v, own_v, last_send, last_recv)
    for m in range(micro):
        for i in range(n):

            @pl.loop(0, window // tile)
            def _(r):
                here = pl.ds(pl.multiple_of(m * window + r * tile, tile), tile)
                back_v[here, pl.ds(i * BLOCK, BLOCK)] = nn(hidden_out[here, :], wd_v[i]).astype(BF)

        last.start(bits[0], m)
    for at, bit in enumerate(bits[:-1]):
        for m in range(micro):
            last.add(bit, m)
            if at + 2 < len(bits):
                last.start(bits[at + 1], m)
    near_copy = pltpu.make_async_copy(own_v, near_out, local_sem.at[4])
    near_copy.start()
    far_copies = [
        pltpu.make_async_copy(
            back_v.at[pl.ds(m * window + bits[-1] * rows, rows)],
            far_out.at[pl.ds(m * rows, rows)],
            local_sem.at[5 + m],
        )
        for m in range(micro)
    ]
    for copy in far_copies:
        copy.start()
    last.finish(bits[:-1])
    for i in range(n - 1):
        for p in range(4):
            hop(i, p, 0).wait_send()
            hop(i, p, 1).wait_send()
    share.finish()
    for copy in whole_copies + [second_copy, near_copy] + far_copies:
        copy.wait()


def mid_forward(n, n_tp, q, k, v, g, x_rel, gain, tables, wo, wu, wl, wd):
    total, hv = v.shape
    mine, width = x_rel.shape
    units = wu.shape[0]
    heads = tables[2].shape[0]
    window = tables[0].shape[0]
    shape = jax.ShapeDtypeStruct
    dma = pltpu.SemaphoreType.DMA
    rows_parts = total // window
    return pl.pallas_call(
        functools.partial(forward_kernel, n, n_tp),
        out_shape=(
            shape((total, hv), BF),
            shape((mine, width), F32),
            shape((total, units), BF),
            shape((total, units), BF),
            shape((total, units), BF),
            shape((total, width), BF),
            shape((n, units, BLOCK), BF),
            shape((n, units, BLOCK), BF),
            shape((n, units, BLOCK), BF),
            shape((mine, width), F32),
            shape((mine, width), BF),
        ),
        in_specs=[vmem()] * 9 + [anyspec()] * 4,
        out_specs=(vmem(),) * 5 + (anyspec(),) * 6,
        scratch_shapes=[
            pltpu.VMEM((heads, window, window), F32),
            pltpu.VMEM(wo.shape, BF),
            pltpu.VMEM((total, width), BF),
            pltpu.VMEM((mine, width), F32),
            pltpu.VMEM((n_tp - 1, mine, width), BF),
            pltpu.VMEM((total, width), BF),
            pltpu.VMEM((n, units, BLOCK), BF),
            pltpu.VMEM((n, units, BLOCK), BF),
            pltpu.VMEM((n, units, BLOCK), BF),
            pltpu.VMEM((256, units), F32),
            dma((n - 1, 4, 2)),
            dma((n - 1, 4, 2)),
            dma((n_tp - 1, rows_parts)),
            dma((n_tp - 1, rows_parts)),
            dma((rows_parts, n_tp)),
            dma((rows_parts, n_tp)),
            dma((n_tp - 1, rows_parts)),
            dma((n_tp - 1, rows_parts)),
            dma((5 + rows_parts,)),
        ],
        compiler_params=pltpu.CompilerParams(
            collective_id=3, has_side_effects=True, vmem_limit_bytes=66_000_000
        ),
        cost_estimate=pl.CostEstimate(
            flops=6 * total * width * units, bytes_accessed=60_000_000, transcendentals=0
        ),
        name="forward_kernel",
    )(q, k, v, g, x_rel, gain, *tables, wo, wu, wl, wd)


def backward_kernel(
    n,
    n_tp,
    gain_ref,
    col_ref,
    row_ref,
    rate_ref,
    cos_ref,
    sin_ref,
    cot_ref,
    wd_ref,
    value_ref,
    slope_ref,
    hidden_ref,
    second_ref,
    wu_ref,
    wl_ref,
    middle_ref,
    cotf_ref,
    wo_ref,
    q_ref,
    k_ref,
    v_ref,
    g_ref,
    dd_out,
    du_out,
    dl_out,
    sum_out,
    grad_out,
    mall_out,
    gq_out,
    gk_out,
    gv_out,
    gs_out,
    cot_v,
    w_v,
    gu_v,
    gl_v,
    hidden_v,
    second_v,
    wu_s,
    wl_s,
    middle_v,
    cotf_v,
    q_v,
    k_v,
    v_v,
    g_v,
    gs_v,
    gated_v,
    decay_v,
    gk_acc,
    gv_acc,
    back_v,
    own_v,
    got_v,
    mall_v,
    dd_p,
    du_p,
    dl_p,
    dd_s,
    du_s,
    dl_s,
    dd_r,
    du_r,
    dl_r,
    ring_send,
    ring_recv,
    ring_free,
    part_send,
    part_recv,
    share_send,
    share_recv,
    load_sem,
    local_sem,
):
    total, width = cot_v.shape
    mine = own_v.shape[0]
    window = col_ref.shape[0]
    micro = total // window
    rows = mine // micro
    heads = decay_v.shape[0]
    dp, tp, cw, ccw = neighbours(n)
    bits = bits_of(n_tp)
    greet([(cw, tp), (ccw, tp)] + [(dp, partner(tp, bit)) for bit in bits])

    pairs = (
        (hidden_ref, hidden_v),
        (cot_ref, cot_v),
        (wd_ref, w_v),
        (value_ref, gu_v),
        (slope_ref, gl_v),
        (second_ref, second_v),
        (middle_ref, middle_v),
        (cotf_ref, cotf_v),
        (q_ref, q_v),
        (k_ref, k_v),
        (v_ref, v_v),
        (g_ref, g_v),
    )
    loads = [
        pltpu.make_async_copy(source, target, local_sem.at[at])
        for at, (source, target) in enumerate(pairs)
    ]
    for copy in loads:
        copy.start()

    def block_load(i, a):
        source, target = ((wu_ref, wu_s), (wl_ref, wl_s))[a]
        return pltpu.make_async_copy(
            source.at[i % n], target.at[i % 2], load_sem.at[i % 2, a]
        )

    block_load(0, 0).start()
    block_load(0, 1).start()

    def gradient(i, a):
        block = pl.ds(i * BLOCK, BLOCK)
        if a == 0:
            dd_p[...] = tn(hidden_v[...], cot_v[:, block])
        else:
            (du_p, dl_p)[a - 1][...] = tn((gu_v, gl_v)[a - 1][...], second_v[:, block])

    ring = SumRing(
        n,
        tp,
        cw,
        ccw,
        (
            (dd_p, dd_s, dd_r, dd_out),
            (du_p, du_s, du_r, du_out),
            (dl_p, dl_s, dl_r, dl_out),
        ),
        gradient,
        ring_send,
        ring_recv,
        ring_free,
    )
    loads[0].wait()
    loads[1].wait()
    ring.first(0)
    for copy in loads[2:5]:
        copy.wait()
    tile = 256

    @pl.loop(0, total // tile)
    def _(r):
        here = pl.ds(pl.multiple_of(r * tile, tile), tile)
        grad = None
        for i in range(n):
            term = nt(cot_v[here, pl.ds(i * BLOCK, BLOCK)], w_v[i])
            grad = term if grad is None else grad + term
        gu_v[here, :] = (grad * gu_v[here, :].astype(F32)).astype(BF)
        gl_v[here, :] = (grad * gl_v[here, :].astype(F32)).astype(BF)

    wo_load = pltpu.make_async_copy(wo_ref, w_v, local_sem.at[2])
    wo_load.start()
    loads[5].wait()
    ring.first(1)
    ring.first(2)
    ring.prepare()
    collect = Collect(dp, tp, n_tp, micro, rows, back_v, got_v, own_v, part_send, part_recv)
    share = Share(dp, tp, n_tp, micro, rows, mall_v, share_send, share_recv)
    for m in range(micro):
        for i in range(n):
            at = m * n + i
            for a in range(2):
                block_load(at, a).wait()
                if at + 1 < micro * n:
                    block_load(at + 1, a).start()

            @pl.loop(0, window // tile)
            def _(r):
                here = pl.ds(pl.multiple_of(m * window + r * tile, tile), tile)
                back_v[here, pl.ds(i * BLOCK, BLOCK)] = (
                    nn(gu_v[here, :], wu_s[at % 2]) + nn(gl_v[here, :], wl_s[at % 2])
                ).astype(BF)

        collect.start(bits[0], m)
    for at, bit in enumerate(bits[:-1]):
        for m in range(micro):
            collect.add(bit, m)
            collect.start(bits[at + 1], m)
    fill_decay(decay_v, col_ref, row_ref, rate_ref)
    ring.advance()
    ring.prepare()
    loads[6].wait()
    loads[7].wait()
    for m in range(micro):
        collect.add(bits[-1], m)

        @pl.loop(0, rows // STEP)
        def _(r):
            inner = pl.multiple_of(r * STEP, STEP)
            here = pl.ds(pl.multiple_of(m * rows + inner, STEP), STEP)
            there = pl.ds(pl.multiple_of(m * window + inner, STEP), STEP)
            middle = middle_v[here, :]
            scale = lax.rsqrt(jnp.mean(middle * middle, axis=-1, keepdims=True) + EPS)
            scaled = own_v[here, :] * gain_ref[1:2, :]
            inside = jnp.mean(scaled * middle, axis=-1, keepdims=True)
            grad = cotf_v[here, :] + scale * (scaled - middle * (scale * scale * inside))
            cotf_v[here, :] = grad
            mall_v[there, :] = grad.astype(BF)

        share.begin(m)
        ring.advance()
        ring.prepare()
    grad_copy = pltpu.make_async_copy(cotf_v, grad_out, local_sem.at[7])
    grad_copy.start()
    for copy in loads[8:]:
        copy.wait()
    wo_load.wait()
    half = HK // 2
    for m in range(micro):
        share.relay(m)

        @pl.loop(0, window // tile)
        def _(r):
            at = pl.multiple_of(r * tile, tile)
            here = pl.ds(pl.multiple_of(m * window + at, tile), tile)
            grad = None
            for i in range(n):
                term = nt(mall_v[here, pl.ds(i * BLOCK, BLOCK)], w_v[i])
                grad = term if grad is None else grad + term
            gated_v[pl.ds(at, tile), :] = grad

        for h in range(heads):
            ring.advance()
            ring.prepare()
            keys = pl.ds(h * HK, HK)
            values = pl.ds(h * HV, HV)
            inside = pl.ds(m * window, window)
            gk_acc[...] = jnp.zeros_like(gk_acc)
            gv_acc[...] = jnp.zeros_like(gv_acc)

            @pl.loop(0, window // tile)
            def _(r):
                at = pl.multiple_of(r * tile, tile)
                local = pl.ds(at, tile)
                here = pl.ds(pl.multiple_of(m * window + at, tile), tile)
                decay = decay_v[h, local, :]
                query = q_v[here, keys]
                weight = (nt(query, k_v[inside, keys]) * decay).astype(BF)
                kept = nn(weight, v_v[inside, values])
                group = lax.rsqrt(jnp.mean(kept * kept, axis=-1, keepdims=True) + GROUP_EPS)
                gate = g_v[here, values]
                sigmoid = jax.nn.sigmoid(gate)
                grad = gated_v[local, values]
                gs_v[here, values] = (
                    grad * (kept * group) * (sigmoid * (1.0 + gate * (1.0 - sigmoid)))
                ).astype(BF)
                lifted = grad * (gate * sigmoid)
                mean = jnp.mean(lifted * kept, axis=-1, keepdims=True)
                grad_kept = (group * (lifted - kept * (group * group * mean))).astype(BF)
                gv_acc[...] += tn(weight, grad_kept)
                score = (nt(grad_kept, v_v[inside, values]) * decay).astype(BF)
                gk_acc[...] += tn(score, query)
                turned = nn(score, k_v[inside, keys])
                low, high = turned[:, :half], turned[:, half:]
                cosine, sine = cos_ref[local, :], sin_ref[local, :]
                q_v[here, pl.ds(h * HK, half)] = (low * cosine + high * sine).astype(BF)
                q_v[here, pl.ds(h * HK + half, half)] = (high * cosine - low * sine).astype(BF)

            low, high = gk_acc[:, :half], gk_acc[:, half:]
            cosine, sine = cos_ref[...], sin_ref[...]
            k_v[inside, pl.ds(h * HK, half)] = (low * cosine + high * sine).astype(BF)
            k_v[inside, pl.ds(h * HK + half, half)] = (high * cosine - low * sine).astype(BF)
            v_v[inside, values] = gv_acc[...].astype(BF)
    mall_copy = pltpu.make_async_copy(mall_v, mall_out, local_sem.at[6])
    mall_copy.start()
    stores = [
        pltpu.make_async_copy(source, target, local_sem.at[8 + at])
        for at, (source, target) in enumerate(
            ((q_v, gq_out), (k_v, gk_out), (v_v, gv_out), (gs_v, gs_out))
        )
    ]
    for copy in stores:
        copy.start()
    for a in range(2):
        block_load(0, a).start()
    for _ in range(n):
        ring.advance()
    for a in range(2):
        block_load(0, a).wait()
    sums = jnp.sum(wu_s[0].astype(F32) * du_out[...], axis=0, keepdims=True)
    sums += jnp.sum(wl_s[0].astype(F32) * dl_out[...], axis=0, keepdims=True)
    sum_out[...] = jnp.broadcast_to(sums, sum_out.shape)
    ring.finish()
    collect.finish()
    share.finish()
    for copy in stores + [grad_copy, mall_copy]:
        copy.wait()


def mid_backward(n, n_tp, gain, tables, cosine, sine, cot, wd, value, slope, hidden, second,
                 wu, wl, middle, cot_rel, wo, q, k, v, g):
    total, width = cot.shape
    mine = middle.shape[0]
    units, hv, hk = wu.shape[1], v.shape[1], q.shape[1]
    heads = tables[2].shape[0]
    window = tables[0].shape[0]
    micro = total // window
    shape = jax.ShapeDtypeStruct
    dma = pltpu.SemaphoreType.DMA
    block_shapes = ((units, BLOCK),) * 3
    return pl.pallas_call(
        functools.partial(backward_kernel, n, n_tp),
        out_shape=tuple(shape(s, F32) for s in block_shapes)
        + (
            shape((8, BLOCK), F32),
            shape((mine, width), F32),
            shape((total, width), BF),
            shape((total, hk), BF),
            shape((total, hk), BF),
            shape((total, hv), BF),
            shape((total, hv), BF),
        ),
        in_specs=[vmem()] * 6 + [anyspec()] * 15,
        out_specs=(vmem(),) * 4 + (anyspec(),) * 6,
        scratch_shapes=[
            pltpu.VMEM((total, width), BF),
            pltpu.VMEM(wd.shape, BF),
            pltpu.VMEM((total, units), BF),
            pltpu.VMEM((total, units), BF),
            pltpu.VMEM((total, units), BF),
            pltpu.VMEM((total, width), BF),
            pltpu.VMEM((2, units, BLOCK), BF),
            pltpu.VMEM((2, units, BLOCK), BF),
            pltpu.VMEM((mine, width), F32),
            pltpu.VMEM((mine, width), F32),
            pltpu.VMEM((total, hk), BF),
            pltpu.VMEM((total, hk), BF),
            pltpu.VMEM((total, hv), BF),
            pltpu.VMEM((total, hv), F32),
            pltpu.VMEM((total, hv), BF),
            pltpu.VMEM((window, hv), F32),
            pltpu.VMEM((heads, window, window), F32),
            pltpu.VMEM((window, HK), F32),
            pltpu.VMEM((window, HV), F32),
            pltpu.VMEM((total, width), BF),
            pltpu.VMEM((mine, width), F32),
            pltpu.VMEM((n_tp - 1, mine, width), BF),
            pltpu.VMEM((total, width), BF),
        ]
        + [pltpu.VMEM(s, F32) for s in block_shapes]
        + [pltpu.VMEM((2,) + s, BF) for s in block_shapes]
        + [pltpu.VMEM((2,) + s, BF) for s in block_shapes]
        + [
            dma((n - 1, 3, 2)),
            dma((n - 1, 3, 2)),
            pltpu.SemaphoreType.REGULAR((3, 2)),
            dma((n_tp - 1, micro)),
            dma((n_tp - 1, micro)),
            dma((micro, n_tp)),
            dma((micro, n_tp)),
            dma((2, 2)),
            dma((12,)),
        ],
        compiler_params=pltpu.CompilerParams(
            collective_id=4, has_side_effects=True, vmem_limit_bytes=67_000_000
        ),
        cost_estimate=pl.CostEstimate(
            flops=16 * total * width * units, bytes_accessed=80_000_000, transcendentals=0
        ),
        name="backward_kernel",
    )(gain, *tables, cosine, sine, cot, wd, value, slope, hidden, second, wu, wl, middle,
      cot_rel, wo, q, k, v, g)


def out_kernel(
    n,
    n_tp,
    gq_ref,
    gk_ref,
    gv_ref,
    gs_ref,
    gain_ref,
    own_gain_ref,
    sum_ref,
    nall_ref,
    gated_ref,
    mall_ref,
    mid_ref,
    x_ref,
    wq_ref,
    wk_ref,
    wv_ref,
    wg_ref,
    dq_out,
    dk_out,
    dv_out,
    ds_out,
    do_out,
    gain_out,
    rows_out,
    nall_v,
    gated_v,
    mall_v,
    mid_v,
    x_v,
    dq_p,
    dk_p,
    dv_p,
    ds_p,
    do_p,
    dq_s,
    dk_s,
    dv_s,
    ds_s,
    do_s,
    dq_r,
    dk_r,
    dv_r,
    ds_r,
    do_r,
    wq_s,
    wk_s,
    wv_s,
    wg_s,
    back_v,
    own_v,
    got_v,
    ring_send,
    ring_recv,
    ring_free,
    part_send,
    part_recv,
    sum_v,
    sum_send,
    sum_recv,
    load_sem,
    local_sem,
):
    micro, rows, width = rows_out.shape
    total = nall_v.shape[0]
    mine = micro * rows
    dp, tp, cw, ccw = neighbours(n)
    pos = ring_position(dp, n)
    bits = bits_of(n_tp)
    greet([(cw, tp), (ccw, tp)] + [(dp, partner(tp, bit)) for bit in bits])

    grads = (gq_ref, gk_ref, gv_ref, gs_ref)
    outs = (dq_out, dk_out, dv_out, ds_out)
    products = (dq_p, dk_p, dv_p, ds_p)
    wholes = (wq_ref, wk_ref, wv_ref, wg_ref)
    slots = (wq_s, wk_s, wv_s, wg_s)
    loads = [
        pltpu.make_async_copy(source, target, local_sem.at[at])
        for at, (source, target) in enumerate(
            (
                (nall_ref, nall_v),
                (gated_ref, gated_v),
                (mall_ref, mall_v),
                (mid_ref, mid_v),
                (x_ref, x_v),
            )
        )
    ]
    for copy in loads:
        copy.start()

    def load(i, a):
        return pltpu.make_async_copy(
            wholes[a].at[i], slots[a].at[i % 2], load_sem.at[i % 2, a]
        )

    for a in range(4):
        load(0, a).start()

    def gradient(i, a):
        block = pl.ds(i * BLOCK, BLOCK)
        if a < 4:
            products[a][...] = tn(grads[a][...], nall_v[:, block])
        else:
            do_p[...] = tn(gated_v[...], mall_v[:, block])

    ring = SumRing(
        n,
        tp,
        cw,
        ccw,
        (
            (dq_p, dq_s, dq_r, dq_out),
            (dk_p, dk_s, dk_r, dk_out),
            (dv_p, dv_s, dv_r, dv_out),
            (ds_p, ds_s, ds_r, ds_out),
            (do_p, do_s, do_r, do_out),
        ),
        gradient,
        ring_send,
        ring_recv,
        ring_free,
    )
    tile = 256

    def backward(i):
        for a in range(4):
            load(i, a).wait()
            if i + 1 < n:
                load(i + 1, a).start()

        @pl.loop(0, total // tile)
        def _(r):
            here = pl.ds(pl.multiple_of(r * tile, tile), tile)
            block = None
            for a in range(4):
                term = nn(grads[a][here, :], slots[a][i % 2])
                block = term if block is None else block + term
            back_v[here, pl.ds(i * BLOCK, BLOCK)] = block.astype(BF)

    def natural(i, side):
        at = ring_index((pos + (n - i if side == 0 else i)) % n, n) * BLOCK + side * LANE
        return pl.ds(pl.multiple_of(at, LANE), LANE)

    def finish_rows():
        @pl.loop(0, mine // STEP)
        def _(r):
            at = pl.multiple_of(r * STEP, STEP)
            m, inner = at // rows, pl.multiple_of(at % rows, STEP)
            here = pl.ds(at, STEP)
            x = x_v[here, :]
            scale = lax.rsqrt(jnp.mean(x * x, axis=-1, keepdims=True) + EPS)
            inside = jnp.mean(own_v[here, :] * gain_ref[0:1, :] * x, axis=-1, keepdims=True)
            slope = scale * scale * inside
            for i in range(n):
                for side in range(2):
                    lanes = pl.ds(i * BLOCK + side * LANE, LANE)
                    scaled = own_v[here, lanes] * gain_ref[0:1, lanes]
                    rows_out[m, pl.ds(inner, STEP), natural(i, side)] = mid_v[
                        here, lanes
                    ] + scale * (scaled - x_v[here, lanes] * slope)

    collect = Collect(dp, tp, n_tp, micro, rows, back_v, got_v, own_v, part_send, part_recv)
    loads[0].wait()
    for a in range(4):
        ring.first(a)
    loads[1].wait()
    loads[2].wait()
    ring.first(4)
    ring.prepare()
    for i in range(n):
        backward(i)
        if i % 3 == 2:
            ring.advance()
            ring.prepare()
    for m in range(micro):
        collect.start(bits[0], m)
    ring.advance()
    ring.prepare()
    for at, bit in enumerate(bits):
        for m in range(micro):
            collect.add(bit, m)
            if at + 1 < len(bits):
                collect.start(bits[at + 1], m)
        if at + 1 < len(bits):
            ring.advance()
            ring.prepare()
            ring.advance()
            ring.prepare()
    loads[3].wait()
    loads[4].wait()
    finish_rows()
    for a in range(4):
        load(0, a).start()
    for _ in range(n):
        ring.advance()

    sums = None
    for a in range(4):
        load(0, a).wait()
        term = jnp.sum(slots[a][0].astype(F32) * outs[a][...], axis=0, keepdims=True)
        sums = term if sums is None else sums + term
    sum_v[0] = jnp.concatenate([sums, sum_ref[1:8, :]], axis=0)
    for at, bit in enumerate(bits):
        swap = pltpu.make_async_remote_copy(
            src_ref=sum_v.at[2 * at],
            dst_ref=sum_v.at[2 * at + 1],
            send_sem=sum_send.at[at],
            recv_sem=sum_recv.at[at],
            device_id=(dp, partner(tp, bit)),
            device_id_type=MESH,
        )
        swap.start()
        swap.wait()
        sum_v[2 * at + 2] = sum_v[2 * at] + sum_v[2 * at + 1]
    gain_out[...] = sum_v[2 * len(bits)] / own_gain_ref[...]
    ring.finish()
    collect.finish()


def project_back(n, n_tp, rows, grads, gain, own_gain, sums, normed, gated, middle_all, grad_middle, x_rel, weights):
    total, width = normed.shape
    mine = x_rel.shape[0]
    micro = mine // rows
    blocks = [(g.shape[1], BLOCK) for g in grads] + [(gated.shape[1], BLOCK)]
    shape = jax.ShapeDtypeStruct
    dma = pltpu.SemaphoreType.DMA
    return pl.pallas_call(
        functools.partial(out_kernel, n, n_tp),
        out_shape=tuple(shape(s, F32) for s in blocks)
        + (shape((8, BLOCK), F32), shape((micro, rows, width), F32)),
        in_specs=[vmem()] * 7 + [anyspec()] * 9,
        out_specs=(vmem(),) * 7,
        scratch_shapes=[
            pltpu.VMEM((total, width), BF),
            pltpu.VMEM(gated.shape, BF),
            pltpu.VMEM((total, width), BF),
            pltpu.VMEM((mine, width), F32),
            pltpu.VMEM((mine, width), F32),
        ]
        + [pltpu.VMEM(s, F32) for s in blocks]
        + [pltpu.VMEM((2,) + s, BF) for s in blocks]
        + [pltpu.VMEM((2,) + s, BF) for s in blocks]
        + [pltpu.VMEM((2,) + s, BF) for s in blocks[:4]]
        + [
            pltpu.VMEM((total, width), BF),
            pltpu.VMEM((mine, width), F32),
            pltpu.VMEM((n_tp - 1, mine, width), BF),
            dma((n - 1, 5, 2)),
            dma((n - 1, 5, 2)),
            pltpu.SemaphoreType.REGULAR((5, 2)),
            dma((n_tp - 1, micro)),
            dma((n_tp - 1, micro)),
            pltpu.VMEM((2 * len(bits_of(n_tp)) + 1, 8, BLOCK), F32),
            dma((len(bits_of(n_tp)),)),
            dma((len(bits_of(n_tp)),)),
            dma((2, 4)),
            dma((5,)),
        ],
        compiler_params=pltpu.CompilerParams(
            collective_id=2, has_side_effects=True, vmem_limit_bytes=66_000_000
        ),
        cost_estimate=pl.CostEstimate(
            flops=4 * total * width * sum(s[0] for s in blocks),
            bytes_accessed=60_000_000,
            transcendentals=0,
        ),
        name="out_kernel",
    )(*grads, gain, own_gain, sums, normed, gated, middle_all, grad_middle, x_rel, *weights)


def finish_kernel(
    n,
    n_tp,
    passed,
    turned,
    *refs,
):
    sources = refs[: passed + turned]
    middle_ref, near_ref, far_ref = refs[passed + turned : passed + turned + 3]
    targets = refs[passed + turned + 3 : 2 * (passed + turned) + 3]
    block_out = refs[2 * (passed + turned) + 3]
    scratch = refs[2 * (passed + turned) + 4 :]
    held, (middle_v, near_v, far_v, block_v), (sem_in, sem_out) = (
        scratch[: passed + 2 * turned],
        scratch[passed + 2 * turned : passed + 2 * turned + 4],
        scratch[passed + 2 * turned + 4 :],
    )
    micro, rows, width = block_v.shape
    pos = ring_position(lax.axis_index("dp"), n)
    count = passed + turned
    ins = [
        pltpu.make_async_copy(sources[i], held[i], sem_in.at[i]) for i in range(count)
    ] + [
        pltpu.make_async_copy(source, target, sem_in.at[count + i])
        for i, (source, target) in enumerate(
            ((middle_ref, middle_v), (near_ref, near_v), (far_ref, far_v))
        )
    ]
    for copy in ins[count:] + ins[:count]:
        copy.start()
    results = list(held[:passed]) + list(held[count:])
    outs = [pltpu.make_async_copy(results[i], targets[i], sem_out.at[i]) for i in range(count)]
    outs.append(pltpu.make_async_copy(block_v, block_out, sem_out.at[count]))
    for copy in ins[count:]:
        copy.wait()

    @pl.loop(0, micro * rows // STEP)
    def _(r):
        at = pl.multiple_of(r * STEP, STEP)
        m, inner = at // rows, pl.multiple_of(at % rows, STEP)
        here = pl.ds(at, STEP)
        for i in range(n):
            for side in range(2):
                lanes = pl.ds(i * BLOCK + side * LANE, LANE)
                spot = ring_index((pos + (n - i if side == 0 else i)) % n, n)
                there = pl.ds(pl.multiple_of(spot * BLOCK + side * LANE, LANE), LANE)
                block_v[m, pl.ds(inner, STEP), there] = middle_v[here, lanes] + (
                    near_v[here, lanes] + far_v[here, lanes].astype(F32)
                )

    outs[count].start()
    for i in range(passed):
        ins[i].wait()
        outs[i].start()
    for i in range(turned):
        ins[passed + i].wait()
        held[count + i][...] = held[passed + i][...].T
        outs[passed + i].start()
    for copy in outs:
        copy.wait()


def finish(n, n_tp, passed, turned, middle, near, far, block_shape):
    shape = jax.ShapeDtypeStruct
    results = tuple(shape(a.shape, a.dtype) for a in passed) + tuple(
        shape(a.shape[::-1], a.dtype) for a in turned
    )
    count = len(passed) + len(turned)
    return pl.pallas_call(
        functools.partial(finish_kernel, n, n_tp, len(passed), len(turned)),
        out_shape=results + (shape(block_shape, F32),),
        in_specs=[anyspec()] * (count + 3),
        out_specs=(anyspec(),) * (count + 1),
        scratch_shapes=[pltpu.VMEM(a.shape, a.dtype) for a in passed]
        + [pltpu.VMEM(a.shape, a.dtype) for a in turned]
        + [pltpu.VMEM(a.shape[::-1], a.dtype) for a in turned]
        + [
            pltpu.VMEM(middle.shape, F32),
            pltpu.VMEM(near.shape, F32),
            pltpu.VMEM(far.shape, BF),
            pltpu.VMEM(block_shape, F32),
            pltpu.SemaphoreType.DMA((count + 3,)),
            pltpu.SemaphoreType.DMA((count + 1,)),
        ],
        compiler_params=pltpu.CompilerParams(vmem_limit_bytes=66_000_000),
        name="finish_kernel",
    )(*passed, *turned, middle, near, far)


def normalize(row_block, gain_vec):
    row_scale = lax.rsqrt(jnp.mean(row_block * row_block, axis=-1, keepdims=True) + EPS)
    return (row_block * row_scale * gain_vec.astype(jnp.float32), row_scale)


def norm_back(grad_rows, row_block, row_scale, gain_vec):
    scaled_grad = grad_rows * gain_vec.astype(jnp.float32)
    back_rows = row_scale * (
        scaled_grad
        - row_block
        * row_scale
        * row_scale
        * jnp.mean(scaled_grad * row_block, axis=-1, keepdims=True)
    )
    return (back_rows, jnp.sum(grad_rows * row_block * row_scale, axis=0))


def angles(length, feature_width):
    half_width = feature_width // 2
    frequency = jnp.exp(-math.log(10000.0) * jnp.arange(half_width, dtype=jnp.float32) / half_width)
    turns = jnp.arange(length, dtype=jnp.float32)[:, None] * frequency[None, :]
    return (jnp.cos(turns)[:, None, :], jnp.sin(turns)[:, None, :])


def decays(length, head_ids):
    places = jnp.arange(length, dtype=jnp.float32)
    spacing = places[:, None] - places[None, :]
    log_rate = jnp.log(1.0 - jnp.exp2(-5.0 - head_ids))
    return jnp.where(
        spacing[None] >= 0.0,
        jnp.exp(jnp.maximum(spacing, 0.0)[None] * log_rate[:, None, None]),
        0.0,
    )


def rotate(value_vectors, cosine_table, sine_table):
    half_width = value_vectors.shape[-1] // 2
    lower = value_vectors[..., :half_width]
    upper = value_vectors[..., half_width:]
    return jnp.concatenate(
        [lower * cosine_table - upper * sine_table, upper * cosine_table + lower * sine_table],
        axis=-1,
    )


def unrotate(value_vectors, cosine_table, sine_table):
    half_width = value_vectors.shape[-1] // 2
    lower = value_vectors[..., :half_width]
    upper = value_vectors[..., half_width:]
    return jnp.concatenate(
        [lower * cosine_table + upper * sine_table, upper * cosine_table - lower * sine_table],
        axis=-1,
    )


def plain_gelu_parts(pre_act):
    normal_cdf = 0.5 * (1.0 + lax.erf(pre_act * (1.0 / math.sqrt(2.0))))
    density = jnp.exp(-0.5 * pre_act * pre_act) * (1.0 / math.sqrt(2.0 * math.pi))
    return (pre_act * normal_cdf, normal_cdf + pre_act * density)


def inner_rows(left_rows, right_rows):
    return lax.dot_general(
        left_rows, right_rows, (((0,), (0,)), ((), ())), preferred_element_type=jnp.float32
    )


def times_t(left_rows, right_rows):
    return lax.dot_general(
        left_rows, right_rows, (((1,), (1,)), ((), ())), preferred_element_type=jnp.float32
    )


def forward_pass(rows_in, gathered, cosine_table, sine_table, decay_mask):
    (
        first_gain,
        second_gain,
        query_weight,
        key_weight,
        value_weight,
        swish_weight,
        output_weight,
        up_projection_matrix,
        gelu_weight,
        down_weight,
    ) = gathered
    local_heads = decay_mask.shape[0]
    scale_qk = 1.0 / math.sqrt(HK)
    normed, first_scale = normalize(rows_in, first_gain)
    normed_all = lax.all_gather(normed.astype(jnp.bfloat16), "tensor", axis=0, tiled=True)
    total_rows = normed_all.shape[0]
    sequences = total_rows // LEN
    query_turned_rows = rotate(
        jnp.dot(normed_all, query_weight, preferred_element_type=jnp.float32).reshape(
            sequences, LEN, local_heads, HK
        ),
        cosine_table,
        sine_table,
    ).astype(jnp.bfloat16)
    key_turned_rows = rotate(
        jnp.dot(normed_all, key_weight, preferred_element_type=jnp.float32).reshape(
            sequences, LEN, local_heads, HK
        ),
        cosine_table,
        sine_table,
    ).astype(jnp.bfloat16)
    value_rows = (
        jnp.dot(normed_all, value_weight, preferred_element_type=jnp.float32)
        .astype(jnp.bfloat16)
        .reshape(sequences, LEN, local_heads, HV)
    )
    gate_pre = jnp.dot(normed_all, swish_weight, preferred_element_type=jnp.float32)
    unscaled_logits = jnp.einsum(
        "snhd,smhd->shnm", query_turned_rows, key_turned_rows, preferred_element_type=jnp.float32
    )
    weight_bf = (unscaled_logits * (decay_mask * scale_qk)).astype(jnp.bfloat16)
    retained = jnp.einsum(
        "shnm,smhe->snhe", weight_bf, value_rows, preferred_element_type=jnp.float32
    )
    group_scale = lax.rsqrt(jnp.mean(retained * retained, axis=-1, keepdims=True) + GROUP_EPS)
    grouped = (retained * group_scale).reshape(total_rows, local_heads * HV)
    sigmoid_gate = jax.nn.sigmoid(gate_pre)
    swish_val = gate_pre * sigmoid_gate
    gated_rows = (swish_val * grouped).astype(jnp.bfloat16)
    attention = lax.psum_scatter(
        jnp.dot(gated_rows, output_weight, preferred_element_type=jnp.float32),
        "tensor",
        scatter_dimension=0,
        tiled=True,
    )
    middle = rows_in + attention
    second, second_scale = normalize(middle, second_gain)
    second_all = lax.all_gather(second.astype(jnp.bfloat16), "tensor", axis=0, tiled=True)
    up_pre = jnp.dot(second_all, up_projection_matrix, preferred_element_type=jnp.float32)
    gelu_pre = jnp.dot(second_all, gelu_weight, preferred_element_type=jnp.float32)
    gelu_val, gelu_slope = plain_gelu_parts(gelu_pre)
    hidden = (gelu_val * up_pre).astype(jnp.bfloat16)
    block_rows = middle + lax.psum_scatter(
        jnp.dot(hidden, down_weight, preferred_element_type=jnp.float32).astype(jnp.bfloat16),
        "tensor",
        scatter_dimension=0,
        tiled=True,
    ).astype(jnp.float32)
    kept_state = (
        rows_in,
        first_scale,
        normed_all,
        query_turned_rows,
        key_turned_rows,
        value_rows,
        gate_pre,
        weight_bf,
        retained,
        group_scale,
        grouped,
        gated_rows,
        middle,
        second_scale,
        second_all,
        up_pre,
        gelu_val,
        gelu_slope,
        hidden,
    )
    return (block_rows, kept_state)


def backward_pass(kept_state, cot_in, gathered, cosine_table, sine_table, decay_mask):
    (
        first_gain,
        second_gain,
        query_weight,
        key_weight,
        value_weight,
        swish_weight,
        output_weight,
        up_projection_matrix,
        gelu_weight,
        down_weight,
    ) = gathered
    (
        rows_in,
        first_scale,
        normed_all,
        query_turned_rows,
        key_turned_rows,
        value_rows,
        gate_pre,
        weight_bf,
        retained,
        group_scale,
        grouped,
        gated_rows,
        middle,
        second_scale,
        second_all,
        up_pre,
        gelu_val,
        gelu_slope,
        hidden,
    ) = kept_state
    local_heads = decay_mask.shape[0]
    total_rows = normed_all.shape[0]
    scale_qk = 1.0 / math.sqrt(HK)
    cot_all = lax.all_gather(cot_in.astype(jnp.bfloat16), "tensor", axis=0, tiled=True)
    grad_hidden = times_t(cot_all, down_weight)
    grad_down = inner_rows(hidden, cot_all)
    grad_uppre = (grad_hidden * gelu_val).astype(jnp.bfloat16)
    grad_gelupre = (grad_hidden * up_pre * gelu_slope).astype(jnp.bfloat16)
    grad_up = inner_rows(second_all, grad_uppre)
    grad_gelu = inner_rows(second_all, grad_gelupre)
    second_back = lax.psum_scatter(
        times_t(grad_uppre, up_projection_matrix) + times_t(grad_gelupre, gelu_weight),
        "tensor",
        scatter_dimension=0,
        tiled=True,
    )
    middle_back, grad_gain_two = norm_back(second_back, middle, second_scale, second_gain)
    grad_middle = cot_in + middle_back
    middle_all = lax.all_gather(grad_middle.astype(jnp.bfloat16), "tensor", axis=0, tiled=True)
    grad_gated = times_t(middle_all, output_weight)
    grad_out = inner_rows(gated_rows, middle_all)
    sigmoid_gate = jax.nn.sigmoid(gate_pre)
    swish_val = gate_pre * sigmoid_gate
    grad_swishpre = (
        grad_gated * grouped * (sigmoid_gate * (1.0 + gate_pre * (1.0 - sigmoid_gate)))
    ).astype(jnp.bfloat16)
    grad_grouped = (grad_gated * swish_val).reshape(retained.shape)
    grad_retained = (
        group_scale
        * (
            grad_grouped
            - retained
            * group_scale
            * group_scale
            * jnp.mean(grad_grouped * retained, axis=-1, keepdims=True)
        )
    ).astype(jnp.bfloat16)
    grad_valrows = jnp.einsum(
        "shnm,snhe->smhe", weight_bf, grad_retained, preferred_element_type=jnp.float32
    ).astype(jnp.bfloat16)
    grad_weight = jnp.einsum(
        "snhe,smhe->shnm", grad_retained, value_rows, preferred_element_type=jnp.float32
    )
    grad_retention_logits = (grad_weight * (decay_mask * scale_qk)).astype(jnp.bfloat16)
    grad_query_rotated_rows = jnp.einsum(
        "shnm,smhd->snhd",
        grad_retention_logits,
        key_turned_rows,
        preferred_element_type=jnp.float32,
    )
    grad_key_rotated_rows = jnp.einsum(
        "shnm,snhd->smhd",
        grad_retention_logits,
        query_turned_rows,
        preferred_element_type=jnp.float32,
    )
    grad_qpre = (
        unrotate(grad_query_rotated_rows, cosine_table, sine_table)
        .astype(jnp.bfloat16)
        .reshape(total_rows, local_heads * HK)
    )
    grad_kpre = (
        unrotate(grad_key_rotated_rows, cosine_table, sine_table)
        .astype(jnp.bfloat16)
        .reshape(total_rows, local_heads * HK)
    )
    grad_vflat = grad_valrows.reshape(total_rows, local_heads * HV)
    first_back = lax.psum_scatter(
        times_t(grad_qpre, query_weight)
        + times_t(grad_kpre, key_weight)
        + times_t(grad_vflat, value_weight)
        + times_t(grad_swishpre, swish_weight),
        "tensor",
        scatter_dimension=0,
        tiled=True,
    )
    grad_query = inner_rows(normed_all, grad_qpre)
    grad_key = inner_rows(normed_all, grad_kpre)
    grad_value = inner_rows(normed_all, grad_vflat)
    grad_swish = inner_rows(normed_all, grad_swishpre)
    input_back, grad_gain_one = norm_back(first_back, rows_in, first_scale, first_gain)
    grad_rows = grad_middle + input_back
    pieces = (
        grad_gain_one,
        grad_gain_two,
        grad_query,
        grad_key,
        grad_value,
        grad_swish,
        grad_out,
        grad_up,
        grad_gelu,
        grad_down,
    )
    return (grad_rows, pieces)


def plain_body(
    block_input,
    cotangent,
    first_gain,
    second_gain,
    query_weight,
    key_weight,
    value_weight,
    swish_weight,
    output_weight,
    up_projection_matrix,
    gelu_weight,
    down_weight,
):
    local_heads = query_weight.shape[1] // HK
    head_ids = (lax.axis_index("tensor") * local_heads + jnp.arange(local_heads)).astype(
        jnp.float32
    )
    cosine_table, sine_table = angles(LEN, HK)
    decay_mask = decays(LEN, head_ids)
    output_list = []
    grad_list = []
    totals = ()
    for micro_idx in range(block_input.shape[0]):
        forward_set = (
            lax.all_gather(first_gain, "dp", axis=0, tiled=True),
            lax.all_gather(second_gain, "dp", axis=0, tiled=True),
            lax.all_gather(query_weight, "dp", axis=0, tiled=True),
            lax.all_gather(key_weight, "dp", axis=0, tiled=True),
            lax.all_gather(value_weight, "dp", axis=0, tiled=True),
            lax.all_gather(swish_weight, "dp", axis=0, tiled=True),
            lax.all_gather(output_weight, "dp", axis=1, tiled=True),
            lax.all_gather(up_projection_matrix, "dp", axis=0, tiled=True),
            lax.all_gather(gelu_weight, "dp", axis=0, tiled=True),
            lax.all_gather(down_weight, "dp", axis=1, tiled=True),
        )
        block_rows, kept_state = forward_pass(
            block_input[micro_idx], forward_set, cosine_table, sine_table, decay_mask
        )
        held = lax.optimization_barrier(
            (
                (
                    first_gain,
                    second_gain,
                    query_weight,
                    key_weight,
                    value_weight,
                    swish_weight,
                    output_weight,
                    up_projection_matrix,
                    gelu_weight,
                    down_weight,
                ),
                block_rows,
            )
        )[0]
        backward_set = (
            lax.all_gather(held[0], "dp", axis=0, tiled=True),
            lax.all_gather(held[1], "dp", axis=0, tiled=True),
            lax.all_gather(held[2], "dp", axis=0, tiled=True),
            lax.all_gather(held[3], "dp", axis=0, tiled=True),
            lax.all_gather(held[4], "dp", axis=0, tiled=True),
            lax.all_gather(held[5], "dp", axis=0, tiled=True),
            lax.all_gather(held[6], "dp", axis=1, tiled=True),
            lax.all_gather(held[7], "dp", axis=0, tiled=True),
            lax.all_gather(held[8], "dp", axis=0, tiled=True),
            lax.all_gather(held[9], "dp", axis=1, tiled=True),
        )
        grad_rows, pieces = backward_pass(
            kept_state, cotangent[micro_idx], backward_set, cosine_table, sine_table, decay_mask
        )
        output_list.append(block_rows)
        grad_list.append(grad_rows)
        if micro_idx == 0:
            totals = tuple(pieces)
        else:
            totals = tuple((total + piece for total, piece in zip(totals, pieces)))
    totals = (
        lax.psum_scatter(totals[0], "dp", scatter_dimension=0, tiled=True),
        lax.psum_scatter(totals[1], "dp", scatter_dimension=0, tiled=True),
        lax.psum_scatter(totals[2], "dp", scatter_dimension=0, tiled=True),
        lax.psum_scatter(totals[3], "dp", scatter_dimension=0, tiled=True),
        lax.psum_scatter(totals[4], "dp", scatter_dimension=0, tiled=True),
        lax.psum_scatter(totals[5], "dp", scatter_dimension=0, tiled=True),
        lax.psum_scatter(totals[6], "dp", scatter_dimension=1, tiled=True),
        lax.psum_scatter(totals[7], "dp", scatter_dimension=0, tiled=True),
        lax.psum_scatter(totals[8], "dp", scatter_dimension=0, tiled=True),
        lax.psum_scatter(totals[9], "dp", scatter_dimension=1, tiled=True),
    )
    gain_first, gain_second = lax.psum((totals[0], totals[1]), "tensor")
    return (
        jnp.stack(output_list, axis=0),
        jnp.stack(grad_list, axis=0),
        gain_first,
        gain_second,
        totals[2],
        totals[3],
        totals[4],
        totals[5],
        totals[6],
        totals[7],
        totals[8],
        totals[9],
    )


def ring_body(
    n_dp,
    n_tp,
    block_input,
    cotangent,
    first_gain,
    second_gain,
    query_weight,
    key_weight,
    value_weight,
    swish_weight,
    output_weight,
    up_projection_matrix,
    gelu_weight,
    down_weight,
):
    micro, rows, width = block_input.shape
    local_heads = query_weight.shape[1] // HK
    window = n_tp * rows

    me = lax.axis_index("tensor")
    head_ids = (me * local_heads + jnp.arange(local_heads)).astype(F32)
    chunk_of = jnp.arange(n_tp) ^ me
    natural = (chunk_of[:, None] * rows + jnp.arange(rows)[None, :]).reshape(window)
    place = (natural % LEN).astype(F32)
    half_key = HK // 2
    frequency = jnp.exp(-math.log(10000.0) * jnp.arange(half_key, dtype=F32) / half_key)
    turns = place[:, None] * frequency[None, :]
    cosine, sine = jnp.cos(turns), jnp.sin(turns)
    log_rate = jnp.log(1.0 - jnp.exp2(-5.0 - head_ids))
    spots = natural.astype(F32)
    tables = (
        jnp.broadcast_to(spots[:, None], (window, LANE)),
        spots[None, :],
        jnp.broadcast_to(log_rate[:, None], (local_heads, window)),
    )

    gains_own = jnp.stack([first_gain, second_gain]).astype(F32)
    query, key, value, gate, x_rel, cot_rel, gains, normed, cot_all, *w_in, w_o = project_in(
        n_dp,
        n_tp,
        block_input,
        cotangent,
        gains_own,
        cosine,
        sine,
        (query_weight.T, key_weight.T, value_weight.T, swish_weight.T),
        output_weight,
    )
    gated, middle, hidden, gelu_val, up_slope, second, w_u, w_l, w_d, near, far = mid_forward(
        n_dp,
        n_tp,
        query,
        key,
        value,
        gate,
        x_rel,
        gains,
        tables,
        w_o,
        up_projection_matrix.T,
        gelu_weight.T,
        down_weight,
    )

    far = lax.ppermute(far, "tensor", [(i, i ^ (n_tp // 2)) for i in range(n_tp)])

    grad_down, grad_up, grad_gelu, sums, grad_middle, middle_all, *grads = (
        mid_backward(
            n_dp,
            n_tp,
            gains,
            tables,
            cosine,
            sine,
            cot_all,
            w_d,
            gelu_val,
            up_slope,
            hidden,
            second,
            w_u,
            w_l,
            middle,
            cot_rel,
            w_o,
            query,
            key,
            value,
            gate,
        )
    )
    grad_query, grad_key, grad_value, grad_swish, grad_out, gain_grads, grad_rows = project_back(
        n_dp,
        n_tp,
        rows,
        grads,
        gains,
        jnp.pad(gains_own, ((0, 6), (0, 0)), constant_values=1.0),
        sums,
        normed,
        gated,
        middle_all,
        grad_middle,
        x_rel,
        w_in,
    )

    passed = (grad_value, grad_swish, grad_out, grad_up, grad_gelu, grad_down, grad_rows)
    *passed, grad_query, grad_key, block_rows = finish(
        n_dp, n_tp, passed, (grad_query, grad_key), middle, near, far, block_input.shape
    )
    grad_value, grad_swish, grad_out, grad_up, grad_gelu, grad_down, grad_rows = passed

    return (
        block_rows,
        grad_rows,
        gain_grads[0],
        gain_grads[1],
        grad_query,
        grad_key,
        grad_value.T,
        grad_swish.T,
        grad_out,
        grad_up.T,
        grad_gelu.T,
        grad_down,
    )


def solution(mesh):
    rows = P(None, ("dp", "tensor"), None)
    wide, tall, gain = P("dp", "tensor"), P("tensor", "dp"), P("dp")
    n_dp, n_tp = mesh.shape["dp"], mesh.shape["tensor"]

    def run(*arrays):
        blocks = arrays[2].shape[0] == BLOCK and n_dp % 2 == 0 and n_dp > 2
        pairs = n_tp > 1 and n_tp & (n_tp - 1) == 0
        aligned = (n_tp * arrays[0].shape[1]) % LEN == 0 and arrays[0].shape[1] % LANE == 0
        if blocks and pairs and aligned:
            return ring_body(n_dp, n_tp, *arrays)
        return plain_body(*arrays)

    return jax.shard_map(
        run,
        mesh=mesh,
        in_specs=(rows, rows, gain, gain) + (wide,) * 4 + (tall, wide, wide, tall),
        out_specs=(rows, rows, gain, gain) + (wide,) * 4 + (tall, wide, wide, tall),
        check_vma=False,
    )
```

```python
import functools
import math

import jax
import jax.numpy as jnp
from jax import lax
from jax.experimental import pallas as pl
from jax.experimental.pallas import tpu as pltpu
from jax.sharding import PartitionSpec as P

HK = 256
HV = 432
LEN = 512
EPS = 1e-05
GROUP_EPS = 1.0
BF = jnp.bfloat16
F32 = jnp.float32
MESH = pl.DeviceIdType.MESH
LANE = 128
BLOCK = 2 * LANE
SLOTS = 3
STEP = 32


def ring_position(index, count):
    low = index // 2
    return low + (index % 2) * (count - 1 - 2 * low)


def ring_index(position, count):
    high = position // (count // 2)
    return (1 - high) * (2 * position) + high * (2 * (count - 1 - position) + 1)


def bits_of(count):
    return [1 << i for i in range(count.bit_length() - 1)]


def anyspec():
    return pl.BlockSpec(memory_space=pl.ANY)


def vmem():
    return pl.BlockSpec(memory_space=pltpu.VMEM)


def nt(left, right):
    return lax.dot_general(left, right, (((1,), (1,)), ((), ())), preferred_element_type=F32)


def nn(left, right):
    return lax.dot_general(left, right, (((1,), (0,)), ((), ())), preferred_element_type=F32)


def tn(left, right):
    return lax.dot_general(left, right, (((0,), (0,)), ((), ())), preferred_element_type=F32)


def partner(tp, bit):
    return tp + bit - 2 * bit * ((tp // bit) % 2)


def neighbours(n):
    dp, tp = lax.axis_index("dp"), lax.axis_index("tensor")
    pos = ring_position(dp, n)
    return dp, tp, ring_index((pos + 1) % n, n), ring_index((pos + n - 1) % n, n)


def greet(devices):
    barrier = pltpu.get_barrier_semaphore()
    for device in devices:
        pl.semaphore_signal(barrier, inc=1, device_id=device, device_id_type=MESH)
    pl.semaphore_wait(barrier, len(devices))


class Share:
    def __init__(self, dp, tp, n_tp, micro, rows, buf, send, recv):
        self.dp, self.tp, self.n_tp, self.micro, self.rows = dp, tp, n_tp, micro, rows
        self.buf, self.send, self.recv = buf, send, recv
        self.bits = bits_of(n_tp)[::-1]

    def copies(self, bit, m, keys=None):
        window = self.n_tp * self.rows
        for key in range(0, self.n_tp, 2 * bit):
            if keys is None or (key == 0) == keys:
                yield pltpu.make_async_remote_copy(
                    src_ref=self.buf.at[pl.ds(m * window + key * self.rows, self.rows)],
                    dst_ref=self.buf.at[pl.ds(m * window + (key ^ bit) * self.rows, self.rows)],
                    send_sem=self.send.at[m, key ^ bit],
                    recv_sem=self.recv.at[m, key ^ bit],
                    device_id=(self.dp, partner(self.tp, bit)),
                    device_id_type=MESH,
                )

    def begin(self, m):
        for bit in self.bits:
            for copy in self.copies(bit, m, True):
                copy.start()

    def relay(self, m):
        for bit in self.bits:
            for copy in self.copies(bit, m, False):
                copy.start()
            for copy in self.copies(bit, m):
                copy.wait_recv()

    def finish(self):
        for m in range(self.micro):
            for bit in self.bits:
                for copy in self.copies(bit, m):
                    copy.wait_send()


class Collect:
    def __init__(self, dp, tp, n_tp, micro, rows, back, got, own, send, recv):
        self.dp, self.tp, self.n_tp, self.micro, self.rows = dp, tp, n_tp, micro, rows
        self.back, self.got, self.own, self.send, self.recv = back, got, own, send, recv
        self.bits = bits_of(n_tp)

    def keys(self, bit):
        return [key for key in range(0, self.n_tp, bit) if key & bit]

    def copies(self, bit, m):
        window = self.n_tp * self.rows
        for key in self.keys(bit):
            yield pltpu.make_async_remote_copy(
                src_ref=self.back.at[pl.ds(m * window + key * self.rows, self.rows)],
                dst_ref=self.got.at[key - 1, pl.ds(m * self.rows, self.rows)],
                send_sem=self.send.at[key - 1, m],
                recv_sem=self.recv.at[key - 1, m],
                device_id=(self.dp, partner(self.tp, bit)),
                device_id_type=MESH,
            )

    def start(self, bit, m):
        for copy in self.copies(bit, m):
            copy.start()

    def add(self, bit, m):
        window = self.n_tp * self.rows
        for copy in self.copies(bit, m):
            copy.wait_recv()
        for key in self.keys(bit):
            target = key ^ bit

            @pl.loop(0, self.rows // STEP)
            def _(r):
                inner = pl.multiple_of(r * STEP, STEP)
                here = pl.ds(pl.multiple_of(m * self.rows + inner, STEP), STEP)
                there = pl.ds(pl.multiple_of(m * window + target * self.rows + inner, STEP), STEP)
                got = self.got[key - 1, here, :].astype(F32)
                if target == 0:
                    held = self.back[there, :].astype(F32) if bit == 1 else self.own[here, :]
                    self.own[here, :] = held + got
                else:
                    self.back[there, :] = (self.back[there, :].astype(F32) + got).astype(BF)

    def finish(self, bits=None):
        for m in range(self.micro):
            for bit in self.bits if bits is None else bits:
                for copy in self.copies(bit, m):
                    copy.wait_send()


class SumRing:
    def __init__(self, n, tp, cw, ccw, arrays, gradient, send, recv, free):
        self.n, self.tp, self.ways, self.arrays = n, tp, (cw, ccw), arrays
        self.gradient, self.send, self.recv, self.free = gradient, send, recv, free
        self.slots = arrays[0][2].shape[0]
        self.ready = self.done = 0

    def hop(self, s, a, side):
        _, send, recv, _ = self.arrays[a]
        lanes = pl.ds(side * LANE, LANE)
        return pltpu.make_async_remote_copy(
            src_ref=send.at[s % 2, :, lanes],
            dst_ref=recv.at[s % self.slots, :, lanes],
            send_sem=self.send.at[s, a, side],
            recv_sem=self.recv.at[s, a, side],
            device_id=(self.ways[side], self.tp),
            device_id_type=MESH,
        )

    def first(self, a):
        part, send, _, _ = self.arrays[a]
        self.gradient(1 % self.n, a)
        send[0] = part[...].astype(BF)
        self.hop(0, a, 0).start()
        self.hop(0, a, 1).start()

    def prepare(self):
        if self.ready == self.done and self.done < self.n - 1:
            self.ready += 1
            for a in range(len(self.arrays)):
                self.gradient((self.ready + 1) % self.n, a)

    def advance(self):
        n = self.n
        if self.done == n - 1:
            return
        self.prepare()
        self.done += 1
        s = self.done
        for a, (part, send, recv, out) in enumerate(self.arrays):
            self.hop(s - 1, a, 0).wait_recv()
            self.hop(s - 1, a, 1).wait_recv()
            total = part[...] + recv[(s - 1) % self.slots].astype(F32)
            if s == n - 1:
                out[...] = total
                continue
            if s >= 2:
                self.hop(s - 2, a, 0).wait_send()
                self.hop(s - 2, a, 1).wait_send()
            send[s % 2] = total.astype(BF)
            for side in range(2):
                if self.slots < n - 1:
                    if s - 1 < n - 1 - self.slots:
                        pl.semaphore_signal(
                            self.free.at[a, side],
                            inc=1,
                            device_id=(self.ways[1 - side], self.tp),
                            device_id_type=MESH,
                        )
                    if s >= self.slots:
                        pl.semaphore_wait(self.free.at[a, side], 1)
                self.hop(s, a, side).start()

    def finish(self):
        for s in range(max(0, self.n - 3), self.n - 1):
            for a in range(len(self.arrays)):
                self.hop(s, a, 0).wait_send()
                self.hop(s, a, 1).wait_send()


def fill_decay(decay_v, col_ref, row_ref, rate_ref):
    heads, window, _ = decay_v.shape
    scale_qk = 1.0 / math.sqrt(HK)
    for h in range(heads):

        @pl.loop(0, window // LANE)
        def _(r):
            here = pl.ds(pl.multiple_of(r * LANE, LANE), LANE)
            col, row = col_ref[here, 0:1], row_ref[...]
            spacing = col - row
            same = jnp.floor(col * (1.0 / LEN)) == jnp.floor(row * (1.0 / LEN))
            kept = jnp.exp(jnp.maximum(spacing, 0.0) * rate_ref[h : h + 1, :]) * scale_qk
            decay_v[h, here, :] = jnp.where((spacing >= 0.0) & same, kept, 0.0)


def gelu_parts(pre_act):
    normal_cdf = 0.5 * (1.0 + lax.erf(pre_act * (1.0 / math.sqrt(2.0))))
    density = jnp.exp(-0.5 * pre_act * pre_act) * (1.0 / math.sqrt(2.0 * math.pi))
    return (pre_act * normal_cdf, normal_cdf + pre_act * density)


def forward_kernel(
    n,
    n_tp,
    x_ref,
    cot_ref,
    gains_ref,
    cos_ref,
    sin_ref,
    col_ref,
    row_ref,
    rate_ref,
    *refs,
):
    shards, refs = refs[:8], refs[8:]
    q_out, k_out, v_out, g_out, xr_out, cr_out, gain_out, nall_out, call_out = refs[:9]
    whole_outs, refs = refs[9:17], refs[17:]
    gated_out, middle_out, second_out, hidden_out, value_out, slope_out, near_out, far_out = refs[:8]
    nall_v, row_v, cot_v, gain_v, q_v, k_v, v_v, g_v, decay_v, got_v = refs[8:18]
    held, refs = refs[18:22], refs[22:]
    x_v, q_acc, k_acc, v_acc, wq_s, wk_s, wv_s, wg_s = refs[:8]
    back_v, own_v, gated_v, hidden_v, value_v, slope_v, up_v = refs[8:15]
    refs = refs[15:]
    ring_send, ring_recv, gain_send, gain_recv = refs[:4]
    first_send, first_recv, cot_send, cot_recv, share_send, share_recv = refs[4:10]
    part_send, part_recv, last_send, last_recv, load_sem, local_sem, out_sem = refs[10:]

    micro, rows, width = x_ref.shape
    window = n_tp * rows
    total, mine = micro * window, micro * rows
    dp, tp, cw, ccw = neighbours(n)
    pos = ring_position(dp, n)
    bits = bits_of(n_tp)
    heads = decay_v.shape[0]
    tile = 256
    half = HK // 2
    greet(
        [(ring_index((pos + k) % n, n), tp) for k in range(1, n)]
        + [(dp, partner(tp, bit)) for bit in bits]
    )

    wholes = tuple(whole_outs[:4]) + tuple(held)
    pieces = [(a, 0, shards[a].shape[0]) for a in range(4)]
    groups = [(0, 1, 2, 3)]
    for pair in ((4,), (5, 6), (7,)):
        group = []
        for a in pair:
            size = shards[a].shape[0]
            cut = size // 2 // 16 * 16 if len(pair) == 1 else size
            group.append(len(pieces))
            pieces.append((a, 0, cut))
            if cut < size:
                group.append(len(pieces))
                pieces.append((a, cut, size - cut))
        groups.append(tuple(group))
    ring_a, ring_b, ring_c, ring_d = groups

    def hop(i, p, side):
        a, low, size = pieces[p]
        span, lanes = pl.ds(low, size), pl.ds(side * LANE, LANE)
        own = isinstance(i, int) and i == 0
        return pltpu.make_async_remote_copy(
            src_ref=shards[a].at[span, lanes] if own else wholes[a].at[i, span, lanes],
            dst_ref=wholes[a].at[i + 1, span, lanes],
            send_sem=ring_send.at[i, p, side],
            recv_sem=ring_recv.at[i, p, side],
            device_id=((cw, ccw)[side], tp),
            device_id_type=MESH,
        )

    def ring_start(group):
        for p in group:
            for side in range(2):
                hop(0, p, side).start()

    def ring_pass(s, p):
        for side in range(2):
            hop(s - 1, p, side).wait_recv()
            if isinstance(s, int):
                if s < n - 1:
                    hop(s, p, side).start()
            else:

                @pl.when(s < n - 1)
                def _():
                    hop(s, p, side).start()

    def ring_step(s, group, following=()):
        for p in group:
            ring_pass(s, p)
        if isinstance(s, int) and s == n - 2:
            ring_start(following)

    def store(source, target):
        copy = pltpu.make_async_copy(source, target, out_sem.at[len(stores)])
        copy.start()
        stores.append(copy)

    stores = []
    ring_start(ring_a)
    own_blocks = [
        pltpu.make_async_copy(shards[4 + i], held[i].at[0], local_sem.at[4 + i]) for i in range(4)
    ]

    def natural(i, side):
        at = ring_index((pos + (n - i if side == 0 else i)) % n, n) * BLOCK + side * LANE
        return pl.ds(pl.multiple_of(at, LANE), LANE)

    first = Share(dp, tp, n_tp, micro, rows, nall_v, first_send, first_recv)
    share = Share(dp, tp, n_tp, micro, rows, nall_v, share_send, share_recv)

    def cot_copy(bit, m, key):
        source = cot_v.at[pl.ds(m * rows, rows)]
        if key:
            source = call_out.at[pl.ds(m * window + key * rows, rows)]
        return pltpu.make_async_remote_copy(
            src_ref=source,
            dst_ref=call_out.at[pl.ds(m * window + (key ^ bit) * rows, rows)],
            send_sem=cot_send.at[m, key ^ bit],
            recv_sem=cot_recv.at[m, key ^ bit],
            device_id=(dp, partner(tp, bit)),
            device_id_type=MESH,
        )

    def cot_copies(bit, keys=None):
        for m in range(micro):
            for key in range(0, n_tp, 2 * bit):
                if keys is None or (key == 0) == keys:
                    yield cot_copy(bit, m, key)

    def project():
        cot_rel_v = own_v
        slots = (wq_s, wk_s, wv_s, wg_s)
        accs = (q_acc, k_acc, v_acc, g_v)

        def load(i, a):
            source = shards[a] if i == 0 else wholes[a].at[i]
            return pltpu.make_async_copy(
                source, slots[a].at[i % SLOTS], load_sem.at[i % SLOTS, a]
            )

        x_copy = pltpu.make_async_copy(x_ref, x_v, local_sem.at[0])
        x_copy.start()
        for a in range(4):
            load(0, a).start()

        def gain_copy(k):
            return pltpu.make_async_remote_copy(
                src_ref=gains_ref,
                dst_ref=gain_v.at[k],
                send_sem=gain_send.at[k],
                recv_sem=gain_recv.at[k],
                device_id=(ring_index((pos + k) % n, n), tp),
                device_id_type=MESH,
            )

        own_gain = pltpu.make_async_copy(gains_ref, gain_v.at[0], local_sem.at[1])
        own_gain.start()
        for k in range(1, n):
            gain_copy(k).start()
        own_gain.wait()
        for k in range(1, n):
            gain_copy(k).wait()
        for i in range(n):
            gain_out[:, pl.ds(i * BLOCK, LANE)] = gain_v[i, :, pl.ds(0, LANE)]
            gain_out[:, pl.ds(i * BLOCK + LANE, LANE)] = gain_v[(n - i) % n, :, pl.ds(LANE, LANE)]
        x_copy.wait()

        def each_part(work):
            @pl.loop(0, mine // STEP)
            def _(r):
                at = pl.multiple_of(r * STEP, STEP)
                m, inner = at // rows, pl.multiple_of(at % rows, STEP)
                work(at, m, inner)

        def normalize_part(at, m, inner):
            chunk = x_v[m, pl.ds(inner, STEP), :]
            scale = lax.rsqrt(jnp.mean(chunk * chunk, axis=-1, keepdims=True) + EPS)
            there = pl.ds(pl.multiple_of(m * window + inner, STEP), STEP)
            for i in range(n):
                for side in range(2):
                    lanes = pl.ds(i * BLOCK + side * LANE, LANE)
                    part = x_v[m, pl.ds(inner, STEP), natural(i, side)]
                    row_v[pl.ds(at, STEP), lanes] = part
                    nall_v[there, lanes] = (part * scale * gain_out[0:1, lanes]).astype(BF)

        each_part(normalize_part)
        for m in range(micro):
            first.begin(m)
        store(row_v, xr_out)
        c_copy = pltpu.make_async_copy(cot_ref, x_v, local_sem.at[0])
        c_copy.start()
        c_copy.wait()

        def cot_part(at, m, inner):
            for i in range(n):
                for side in range(2):
                    lanes = pl.ds(i * BLOCK + side * LANE, LANE)
                    part = x_v[m, pl.ds(inner, STEP), natural(i, side)]
                    cot_rel_v[pl.ds(at, STEP), lanes] = part
                    cot_v[pl.ds(at, STEP), lanes] = part.astype(BF)

        each_part(cot_part)
        cot_rel = pltpu.make_async_copy(cot_rel_v, cr_out, local_sem.at[1])
        cot_rel.start()
        for m in range(micro):
            store(cot_v.at[pl.ds(m * rows, rows)], call_out.at[pl.ds(m * window, rows)])
        for copy in own_blocks:
            copy.start()

        def product(j, a, last):
            load(j, a).wait()
            if j == 0:
                pltpu.make_async_copy(
                    slots[a].at[0], wholes[a].at[0], load_sem.at[SLOTS, a]
                ).start()

            @pl.loop(0, total // tile)
            def _(r):
                at = pl.multiple_of(r * tile, tile)
                here = pl.ds(at, tile)
                part = nt(nall_v[here, pl.ds(j * BLOCK, BLOCK)], slots[a][j % SLOTS])
                if j > 0:
                    part = accs[a][here, :] + part
                if not last or a == 3:
                    accs[a][here, :] = part
                elif a == 2:
                    v_v[here, :] = part.astype(BF)
                else:
                    place = pl.ds(pl.multiple_of(at % window, tile), tile)
                    cosine, sine = cos_ref[place, :], sin_ref[place, :]
                    out = (q_v, k_v)[a]
                    for h in range(heads):
                        low = part[:, h * HK : h * HK + half]
                        high = part[:, h * HK + half : (h + 1) * HK]
                        out[here, pl.ds(h * HK, half)] = (low * cosine - high * sine).astype(BF)
                        out[here, pl.ds(h * HK + half, half)] = (
                            high * cosine + low * sine
                        ).astype(BF)

            if j == 0:
                pltpu.make_async_copy(
                    slots[a].at[0], wholes[a].at[0], load_sem.at[SLOTS, a]
                ).wait()

        start_at, done = 3, 0
        for i in range(n + 1):
            if i == 2:
                fill_decay(decay_v, col_ref, row_ref, rate_ref)
            if i == start_at:
                for m in range(micro):
                    first.relay(m)
                store(nall_v, nall_out)
                for bit in bits[::-1]:
                    for copy in cot_copies(bit, True):
                        copy.start()
            if i == n - 1:
                for bit in bits[::-1]:
                    for copy in cot_copies(bit, False):
                        copy.start()
                    for copy in cot_copies(bit):
                        copy.wait_recv()
            todo = []
            if i >= start_at:
                goal = min(i - 1, done + 1) if i < n else n - 1
                todo = list(range(done, goal + 1))
                done = goal + 1
            for a in range(4):
                if 0 < i < n:
                    ring_pass(i, a)
                if i == n - 2 and a == 3:
                    ring_start(ring_b)
                for j in todo:
                    product(j, a, j == n - 1)
                if 0 < i < n:
                    load(i, a).start()
                if i == n:
                    source, target = ((q_v, q_out), (k_v, k_out), (v_v, v_out), (g_v, g_out))[a]
                    store(source, target)
        cot_rel.wait()

    project()
    wo_v, wu_v, wl_v, wd_v = held
    units = shards[7].shape[0]

    def middle_part():
        for copy in own_blocks:
            copy.wait()

        def attend(m, h):
            keys = pl.ds(h * HK, HK)
            values = pl.ds(h * HV, HV)
            inside = pl.ds(m * window, window)

            @pl.loop(0, window // tile)
            def _(r):
                at = pl.multiple_of(r * tile, tile)
                here = pl.ds(pl.multiple_of(m * window + at, tile), tile)
                scores = nt(q_v[here, keys], k_v[inside, keys])
                weight = (scores * decay_v[h, pl.ds(at, tile), :]).astype(BF)
                kept = nn(weight, v_v[inside, values])
                group = lax.rsqrt(jnp.mean(kept * kept, axis=-1, keepdims=True) + GROUP_EPS)
                gate = g_v[here, values]
                gated_v[here, values] = (gate * jax.nn.sigmoid(gate) * (kept * group)).astype(BF)

        def times_block(left, weights, i):
            @pl.loop(0, total // tile)
            def _(r):
                here = pl.ds(pl.multiple_of(r * tile, tile), tile)
                back_v[here, pl.ds(i * BLOCK, BLOCK)] = nn(left[here, :], weights[i]).astype(BF)

        collect = Collect(dp, tp, n_tp, micro, rows, back_v, got_v, own_v, part_send, part_recv)
        jobs = [(m, h) for m in range(micro) for h in range(heads)]
        reached = 0
        while jobs:
            if reached < n - 1:
                reached += 1
                ring_step(reached, ring_b, ring_c)
            attend(*jobs.pop(0))
        store(gated_v, gated_out)
        ready = 0
        while ready < n:
            if reached < n - 1:
                reached += 1
                ring_step(reached, ring_b, ring_c)
            for _ in range(2 if reached < n - 1 else n):
                if ready < min(n, reached + 1):
                    times_block(gated_v, wo_v, ready)
                    ready += 1
        store(wo_v, whole_outs[4])
        first.finish()
        stores[0].wait()
        stores[micro + 1].wait()
        for m in range(micro):
            collect.start(bits[0], m)
        passed = [0]

        def pairs_to(goal):
            while passed[0] < min(goal, n - 1):
                passed[0] += 1
                ring_step(passed[0], ring_c, ring_d)

        for at, bit in enumerate(bits[:-1]):
            for m in range(micro):
                collect.add(bit, m)
                collect.start(bits[at + 1], m)
        pairs_to(1)
        for m in range(micro):
            pairs_to(2 + m)
            collect.add(bits[-1], m)

            @pl.loop(0, rows // STEP)
            def _(r):
                inner = pl.multiple_of(r * STEP, STEP)
                here = pl.ds(pl.multiple_of(m * rows + inner, STEP), STEP)
                there = pl.ds(pl.multiple_of(m * window + inner, STEP), STEP)
                middle = row_v[here, :] + own_v[here, :]
                row_v[here, :] = middle
                scale = lax.rsqrt(jnp.mean(middle * middle, axis=-1, keepdims=True) + EPS)
                nall_v[there, :] = (middle * scale * gain_out[1:2, :]).astype(BF)

            share.begin(m)
        store(row_v, middle_out)
        pairs_to(4)
        for m in range(micro):
            share.relay(m)
            pairs_to(5 + m)
        pairs_to(n - 1)
        store(nall_v, second_out)
        store(wu_v, whole_outs[5])
        store(wl_v, whole_outs[6])

        def rows_by(weights, here):
            result = None
            for i in range(n):
                term = nt(nall_v[here, pl.ds(i * BLOCK, BLOCK)], weights[i])
                result = term if result is None else result + term
            return result

        tiles = total // tile
        every = max(1, tiles // 2)
        inside_loop = min(tiles // every, n - 1)

        @pl.loop(0, tiles)
        def _(r):
            here = pl.ds(pl.multiple_of(r * tile, tile), tile)
            up_v[...] = rows_by(wu_v, here)
            gelu_val, gelu_slope = gelu_parts(rows_by(wl_v, here))
            up = up_v[...]
            hidden_v[here, :] = (gelu_val * up).astype(BF)
            value_v[here, :] = gelu_val.astype(BF)
            slope_v[here, :] = (up * gelu_slope).astype(BF)

            @pl.when((r % every == every - 1) & (r // every < inside_loop))
            def _():
                ring_step(r // every + 1, ring_d)

        store(hidden_v, hidden_out)
        store(value_v, value_out)
        store(slope_v, slope_out)
        collect.finish()
        ready = 0
        for s in range(inside_loop, n):
            if s > inside_loop:
                ring_step(s, ring_d)
            for _ in range(2 if s < n - 1 else n):
                if ready <= s and ready < n:
                    times_block(hidden_v, wd_v, ready)
                    ready += 1
        store(wd_v, whole_outs[7])
        last = Collect(dp, tp, n_tp, micro, rows, back_v, got_v, own_v, last_send, last_recv)
        for at, bit in enumerate(bits[:-1]):
            for m in range(micro):
                last.start(bit, m)
            for m in range(micro):
                last.add(bit, m)
        store(own_v, near_out)
        for m in range(micro):
            store(
                back_v.at[pl.ds(m * window + bits[-1] * rows, rows)],
                far_out.at[pl.ds(m * rows, rows)],
            )
        last.finish(bits[:-1])
        for i in range(n - 1):
            for p in range(len(pieces)):
                hop(i, p, 0).wait_send()
                hop(i, p, 1).wait_send()
        share.finish()
        for bit in bits:
            for copy in cot_copies(bit):
                copy.wait_send()
        for at, copy in enumerate(stores):
            if at not in waited:
                copy.wait()

    waited = (0, micro + 1)
    middle_part()


def forward(n, n_tp, x, cot, gains, cosine, sine, tables, weights):
    micro, rows, width = x.shape
    window = n_tp * rows
    total, mine = micro * window, micro * rows
    sizes = [w.shape[0] for w in weights]
    hv, units = sizes[2], sizes[7]
    shape = jax.ShapeDtypeStruct
    dma = pltpu.SemaphoreType.DMA
    count = 4 + 2 + 2 + 2
    return pl.pallas_call(
        functools.partial(forward_kernel, n, n_tp),
        out_shape=(
            shape((total, sizes[0]), BF),
            shape((total, sizes[1]), BF),
            shape((total, hv), BF),
            shape((total, sizes[3]), F32),
            shape((mine, width), F32),
            shape((mine, width), F32),
            shape((2, width), F32),
            shape((total, width), BF),
            shape((total, width), BF),
        )
        + tuple(shape((n, s, BLOCK), BF) for s in sizes)
        + (
            shape((total, hv), BF),
            shape((mine, width), F32),
            shape((total, width), BF),
            shape((total, units), BF),
            shape((total, units), BF),
            shape((total, units), BF),
            shape((mine, width), F32),
            shape((mine, width), BF),
        ),
        in_specs=[anyspec()] * 3 + [vmem()] * 5 + [anyspec()] * 8,
        out_specs=(anyspec(),) * 6 + (vmem(),) + (anyspec(),) * 18,
        scratch_shapes=[
            pltpu.VMEM((total, width), BF),
            pltpu.VMEM((mine, width), F32),
            pltpu.VMEM((mine, width), BF),
            pltpu.VMEM((n, 2, BLOCK), F32),
            pltpu.VMEM((total, sizes[0]), BF),
            pltpu.VMEM((total, sizes[1]), BF),
            pltpu.VMEM((total, hv), BF),
            pltpu.VMEM((total, sizes[3]), F32),
            pltpu.VMEM((tables[2].shape[0], window, window), F32),
            pltpu.VMEM((n_tp - 1, mine, width), BF),
        ]
        + [pltpu.VMEM((n, s, BLOCK), BF) for s in sizes[4:]]
        + [pltpu.VMEM((micro, rows, width), F32)]
        + [pltpu.VMEM((total, s), F32) for s in sizes[:3]]
        + [pltpu.VMEM((SLOTS, s, BLOCK), BF) for s in sizes[:4]]
        + [
            pltpu.VMEM((total, width), BF),
            pltpu.VMEM((mine, width), F32),
            pltpu.VMEM((total, hv), BF),
            pltpu.VMEM((total, units), BF),
            pltpu.VMEM((total, units), BF),
            pltpu.VMEM((total, units), BF),
            pltpu.VMEM((256, units), F32),
        ]
        + [dma((n - 1, count, 2))] * 2
        + [dma((n,))] * 2
        + [dma((micro, n_tp))] * 6
        + [dma((n_tp - 1, micro))] * 4
        + [dma((SLOTS + 1, 4)), dma((8,)), dma((19 + micro,))],
        compiler_params=pltpu.CompilerParams(
            collective_id=1, has_side_effects=True, vmem_limit_bytes=66_500_000
        ),
        cost_estimate=pl.CostEstimate(
            flops=2 * total * width * sum(sizes), bytes_accessed=120_000_000, transcendentals=0
        ),
        name="forward_kernel",
    )(x, cot, gains, cosine, sine, *tables, *weights)


def backward_kernel(
    n,
    n_tp,
    gain_ref,
    col_ref,
    row_ref,
    rate_ref,
    cos_ref,
    sin_ref,
    cot_ref,
    wd_ref,
    value_ref,
    slope_ref,
    hidden_ref,
    second_ref,
    wu_ref,
    wl_ref,
    middle_ref,
    cotf_ref,
    wo_ref,
    q_ref,
    k_ref,
    v_ref,
    g_ref,
    dd_out,
    du_out,
    dl_out,
    sum_out,
    grad_out,
    mall_out,
    gq_out,
    gk_out,
    gv_out,
    gs_out,
    cot_v,
    w_v,
    gu_v,
    gl_v,
    hidden_v,
    second_v,
    wu_s,
    wl_s,
    middle_v,
    cotf_v,
    q_v,
    k_v,
    v_v,
    g_v,
    gs_v,
    gated_v,
    decay_v,
    gk_acc,
    gv_acc,
    back_v,
    own_v,
    got_v,
    mall_v,
    dd_p,
    du_p,
    dl_p,
    dd_s,
    du_s,
    dl_s,
    dd_r,
    du_r,
    dl_r,
    ring_send,
    ring_recv,
    ring_free,
    part_send,
    part_recv,
    share_send,
    share_recv,
    load_sem,
    local_sem,
):
    total, width = cot_v.shape
    mine = own_v.shape[0]
    window = col_ref.shape[0]
    micro = total // window
    rows = mine // micro
    heads = decay_v.shape[0]
    dp, tp, cw, ccw = neighbours(n)
    bits = bits_of(n_tp)
    greet([(cw, tp), (ccw, tp)] + [(dp, partner(tp, bit)) for bit in bits])

    pairs = (
        (hidden_ref, hidden_v),
        (cot_ref, cot_v),
        (wd_ref, w_v),
        (value_ref, gu_v),
        (slope_ref, gl_v),
        (second_ref, second_v),
        (middle_ref, middle_v),
        (cotf_ref, cotf_v),
        (q_ref, q_v),
        (k_ref, k_v),
        (v_ref, v_v),
        (g_ref, g_v),
    )
    loads = [
        pltpu.make_async_copy(source, target, local_sem.at[at])
        for at, (source, target) in enumerate(pairs)
    ]
    for copy in loads:
        copy.start()

    def block_load(i, a):
        source, target = ((wu_ref, wu_s), (wl_ref, wl_s))[a]
        return pltpu.make_async_copy(
            source.at[i % n], target.at[i % 2], load_sem.at[i % 2, a]
        )

    block_load(0, 0).start()
    block_load(0, 1).start()

    def gradient(i, a):
        block = pl.ds(i * BLOCK, BLOCK)
        if a == 0:
            dd_p[...] = tn(hidden_v[...], cot_v[:, block])
        else:
            (du_p, dl_p)[a - 1][...] = tn((gu_v, gl_v)[a - 1][...], second_v[:, block])

    ring = SumRing(
        n,
        tp,
        cw,
        ccw,
        (
            (dd_p, dd_s, dd_r, dd_out),
            (du_p, du_s, du_r, du_out),
            (dl_p, dl_s, dl_r, dl_out),
        ),
        gradient,
        ring_send,
        ring_recv,
        ring_free,
    )
    loads[0].wait()
    loads[1].wait()
    ring.first(0)
    for copy in loads[2:5]:
        copy.wait()
    tile = 256

    @pl.loop(0, total // tile)
    def _(r):
        here = pl.ds(pl.multiple_of(r * tile, tile), tile)
        grad = None
        for i in range(n):
            term = nt(cot_v[here, pl.ds(i * BLOCK, BLOCK)], w_v[i])
            grad = term if grad is None else grad + term
        gu_v[here, :] = (grad * gu_v[here, :].astype(F32)).astype(BF)
        gl_v[here, :] = (grad * gl_v[here, :].astype(F32)).astype(BF)

    wo_load = pltpu.make_async_copy(wo_ref, w_v, local_sem.at[2])
    wo_load.start()
    loads[5].wait()
    ring.first(1)
    ring.first(2)
    ring.prepare()
    collect = Collect(dp, tp, n_tp, micro, rows, back_v, got_v, own_v, part_send, part_recv)
    share = Share(dp, tp, n_tp, micro, rows, mall_v, share_send, share_recv)
    for m in range(micro):
        for i in range(n):
            at = m * n + i
            for a in range(2):
                block_load(at, a).wait()
                if at + 1 < micro * n:
                    block_load(at + 1, a).start()

            @pl.loop(0, window // tile)
            def _(r):
                here = pl.ds(pl.multiple_of(m * window + r * tile, tile), tile)
                back_v[here, pl.ds(i * BLOCK, BLOCK)] = (
                    nn(gu_v[here, :], wu_s[at % 2]) + nn(gl_v[here, :], wl_s[at % 2])
                ).astype(BF)

        collect.start(bits[0], m)
    for at, bit in enumerate(bits[:-1]):
        for m in range(micro):
            collect.add(bit, m)
            collect.start(bits[at + 1], m)
    fill_decay(decay_v, col_ref, row_ref, rate_ref)
    ring.advance()
    ring.prepare()
    loads[6].wait()
    loads[7].wait()
    for m in range(micro):
        collect.add(bits[-1], m)

        @pl.loop(0, rows // STEP)
        def _(r):
            inner = pl.multiple_of(r * STEP, STEP)
            here = pl.ds(pl.multiple_of(m * rows + inner, STEP), STEP)
            there = pl.ds(pl.multiple_of(m * window + inner, STEP), STEP)
            middle = middle_v[here, :]
            scale = lax.rsqrt(jnp.mean(middle * middle, axis=-1, keepdims=True) + EPS)
            scaled = own_v[here, :] * gain_ref[1:2, :]
            inside = jnp.mean(scaled * middle, axis=-1, keepdims=True)
            grad = cotf_v[here, :] + scale * (scaled - middle * (scale * scale * inside))
            cotf_v[here, :] = grad
            mall_v[there, :] = grad.astype(BF)

        share.begin(m)
        ring.advance()
        ring.prepare()
    grad_copy = pltpu.make_async_copy(cotf_v, grad_out, local_sem.at[7])
    grad_copy.start()
    for copy in loads[8:]:
        copy.wait()
    wo_load.wait()
    half = HK // 2
    for m in range(micro):
        share.relay(m)

        @pl.loop(0, window // tile)
        def _(r):
            at = pl.multiple_of(r * tile, tile)
            here = pl.ds(pl.multiple_of(m * window + at, tile), tile)
            grad = None
            for i in range(n):
                term = nt(mall_v[here, pl.ds(i * BLOCK, BLOCK)], w_v[i])
                grad = term if grad is None else grad + term
            gated_v[pl.ds(at, tile), :] = grad

        for h in range(heads):
            ring.advance()
            ring.prepare()
            keys = pl.ds(h * HK, HK)
            values = pl.ds(h * HV, HV)
            inside = pl.ds(m * window, window)
            gk_acc[...] = jnp.zeros_like(gk_acc)
            gv_acc[...] = jnp.zeros_like(gv_acc)

            @pl.loop(0, window // tile)
            def _(r):
                at = pl.multiple_of(r * tile, tile)
                local = pl.ds(at, tile)
                here = pl.ds(pl.multiple_of(m * window + at, tile), tile)
                decay = decay_v[h, local, :]
                query = q_v[here, keys]
                weight = (nt(query, k_v[inside, keys]) * decay).astype(BF)
                kept = nn(weight, v_v[inside, values])
                group = lax.rsqrt(jnp.mean(kept * kept, axis=-1, keepdims=True) + GROUP_EPS)
                gate = g_v[here, values]
                sigmoid = jax.nn.sigmoid(gate)
                grad = gated_v[local, values]
                gs_v[here, values] = (
                    grad * (kept * group) * (sigmoid * (1.0 + gate * (1.0 - sigmoid)))
                ).astype(BF)
                lifted = grad * (gate * sigmoid)
                mean = jnp.mean(lifted * kept, axis=-1, keepdims=True)
                grad_kept = (group * (lifted - kept * (group * group * mean))).astype(BF)
                gv_acc[...] += tn(weight, grad_kept)
                score = (nt(grad_kept, v_v[inside, values]) * decay).astype(BF)
                gk_acc[...] += tn(score, query)
                turned = nn(score, k_v[inside, keys])
                low, high = turned[:, :half], turned[:, half:]
                cosine, sine = cos_ref[local, :], sin_ref[local, :]
                q_v[here, pl.ds(h * HK, half)] = (low * cosine + high * sine).astype(BF)
                q_v[here, pl.ds(h * HK + half, half)] = (high * cosine - low * sine).astype(BF)

            low, high = gk_acc[:, :half], gk_acc[:, half:]
            cosine, sine = cos_ref[...], sin_ref[...]
            k_v[inside, pl.ds(h * HK, half)] = (low * cosine + high * sine).astype(BF)
            k_v[inside, pl.ds(h * HK + half, half)] = (high * cosine - low * sine).astype(BF)
            v_v[inside, values] = gv_acc[...].astype(BF)
    mall_copy = pltpu.make_async_copy(mall_v, mall_out, local_sem.at[6])
    mall_copy.start()
    stores = [
        pltpu.make_async_copy(source, target, local_sem.at[8 + at])
        for at, (source, target) in enumerate(
            ((q_v, gq_out), (k_v, gk_out), (v_v, gv_out), (gs_v, gs_out))
        )
    ]
    for copy in stores:
        copy.start()
    for a in range(2):
        block_load(0, a).start()
    for _ in range(n):
        ring.advance()
    for a in range(2):
        block_load(0, a).wait()
    sums = jnp.sum(wu_s[0].astype(F32) * du_out[...], axis=0, keepdims=True)
    sums += jnp.sum(wl_s[0].astype(F32) * dl_out[...], axis=0, keepdims=True)
    sum_out[...] = jnp.broadcast_to(sums, sum_out.shape)
    ring.finish()
    collect.finish()
    share.finish()
    for copy in stores + [grad_copy, mall_copy]:
        copy.wait()


def mid_backward(n, n_tp, gain, tables, cosine, sine, cot, wd, value, slope, hidden, second,
                 wu, wl, middle, cot_rel, wo, q, k, v, g):
    total, width = cot.shape
    mine = middle.shape[0]
    units, hv, hk = wu.shape[1], v.shape[1], q.shape[1]
    heads = tables[2].shape[0]
    window = tables[0].shape[0]
    micro = total // window
    shape = jax.ShapeDtypeStruct
    dma = pltpu.SemaphoreType.DMA
    block_shapes = ((units, BLOCK),) * 3
    return pl.pallas_call(
        functools.partial(backward_kernel, n, n_tp),
        out_shape=tuple(shape(s, F32) for s in block_shapes)
        + (
            shape((8, BLOCK), F32),
            shape((mine, width), F32),
            shape((total, width), BF),
            shape((total, hk), BF),
            shape((total, hk), BF),
            shape((total, hv), BF),
            shape((total, hv), BF),
        ),
        in_specs=[vmem()] * 6 + [anyspec()] * 15,
        out_specs=(vmem(),) * 4 + (anyspec(),) * 6,
        scratch_shapes=[
            pltpu.VMEM((total, width), BF),
            pltpu.VMEM(wd.shape, BF),
            pltpu.VMEM((total, units), BF),
            pltpu.VMEM((total, units), BF),
            pltpu.VMEM((total, units), BF),
            pltpu.VMEM((total, width), BF),
            pltpu.VMEM((2, units, BLOCK), BF),
            pltpu.VMEM((2, units, BLOCK), BF),
            pltpu.VMEM((mine, width), F32),
            pltpu.VMEM((mine, width), F32),
            pltpu.VMEM((total, hk), BF),
            pltpu.VMEM((total, hk), BF),
            pltpu.VMEM((total, hv), BF),
            pltpu.VMEM((total, hv), F32),
            pltpu.VMEM((total, hv), BF),
            pltpu.VMEM((window, hv), F32),
            pltpu.VMEM((heads, window, window), F32),
            pltpu.VMEM((window, HK), F32),
            pltpu.VMEM((window, HV), F32),
            pltpu.VMEM((total, width), BF),
            pltpu.VMEM((mine, width), F32),
            pltpu.VMEM((n_tp - 1, mine, width), BF),
            pltpu.VMEM((total, width), BF),
        ]
        + [pltpu.VMEM(s, F32) for s in block_shapes]
        + [pltpu.VMEM((2,) + s, BF) for s in block_shapes]
        + [pltpu.VMEM((2,) + s, BF) for s in block_shapes]
        + [
            dma((n - 1, 3, 2)),
            dma((n - 1, 3, 2)),
            pltpu.SemaphoreType.REGULAR((3, 2)),
            dma((n_tp - 1, micro)),
            dma((n_tp - 1, micro)),
            dma((micro, n_tp)),
            dma((micro, n_tp)),
            dma((2, 2)),
            dma((12,)),
        ],
        compiler_params=pltpu.CompilerParams(
            collective_id=4, has_side_effects=True, vmem_limit_bytes=67_000_000
        ),
        cost_estimate=pl.CostEstimate(
            flops=16 * total * width * units, bytes_accessed=80_000_000, transcendentals=0
        ),
        name="backward_kernel",
    )(gain, *tables, cosine, sine, cot, wd, value, slope, hidden, second, wu, wl, middle,
      cot_rel, wo, q, k, v, g)


def out_kernel(
    n,
    n_tp,
    gq_ref,
    gk_ref,
    gv_ref,
    gs_ref,
    gain_ref,
    own_gain_ref,
    sum_ref,
    nall_ref,
    gated_ref,
    mall_ref,
    mid_ref,
    x_ref,
    wq_ref,
    wk_ref,
    wv_ref,
    wg_ref,
    dq_out,
    dk_out,
    dv_out,
    ds_out,
    do_out,
    gain_out,
    rows_out,
    nall_v,
    gated_v,
    mall_v,
    mid_v,
    x_v,
    dq_p,
    dk_p,
    dv_p,
    ds_p,
    do_p,
    dq_s,
    dk_s,
    dv_s,
    ds_s,
    do_s,
    dq_r,
    dk_r,
    dv_r,
    ds_r,
    do_r,
    wq_s,
    wk_s,
    wv_s,
    wg_s,
    back_v,
    own_v,
    got_v,
    ring_send,
    ring_recv,
    ring_free,
    part_send,
    part_recv,
    sum_v,
    sum_send,
    sum_recv,
    load_sem,
    local_sem,
):
    micro, rows, width = rows_out.shape
    total = nall_v.shape[0]
    mine = micro * rows
    dp, tp, cw, ccw = neighbours(n)
    pos = ring_position(dp, n)
    bits = bits_of(n_tp)
    greet([(cw, tp), (ccw, tp)] + [(dp, partner(tp, bit)) for bit in bits])

    grads = (gq_ref, gk_ref, gv_ref, gs_ref)
    outs = (dq_out, dk_out, dv_out, ds_out)
    products = (dq_p, dk_p, dv_p, ds_p)
    wholes = (wq_ref, wk_ref, wv_ref, wg_ref)
    slots = (wq_s, wk_s, wv_s, wg_s)
    loads = [
        pltpu.make_async_copy(source, target, local_sem.at[at])
        for at, (source, target) in enumerate(
            (
                (nall_ref, nall_v),
                (gated_ref, gated_v),
                (mall_ref, mall_v),
                (mid_ref, mid_v),
                (x_ref, x_v),
            )
        )
    ]
    for copy in loads:
        copy.start()

    def load(i, a):
        return pltpu.make_async_copy(
            wholes[a].at[i], slots[a].at[i % 2], load_sem.at[i % 2, a]
        )

    for a in range(4):
        load(0, a).start()

    def gradient(i, a):
        block = pl.ds(i * BLOCK, BLOCK)
        if a < 4:
            products[a][...] = tn(grads[a][...], nall_v[:, block])
        else:
            do_p[...] = tn(gated_v[...], mall_v[:, block])

    ring = SumRing(
        n,
        tp,
        cw,
        ccw,
        (
            (dq_p, dq_s, dq_r, dq_out),
            (dk_p, dk_s, dk_r, dk_out),
            (dv_p, dv_s, dv_r, dv_out),
            (ds_p, ds_s, ds_r, ds_out),
            (do_p, do_s, do_r, do_out),
        ),
        gradient,
        ring_send,
        ring_recv,
        ring_free,
    )
    tile = 256

    def backward(i):
        for a in range(4):
            load(i, a).wait()
            if i + 1 < n:
                load(i + 1, a).start()

        @pl.loop(0, total // tile)
        def _(r):
            here = pl.ds(pl.multiple_of(r * tile, tile), tile)
            block = None
            for a in range(4):
                term = nn(grads[a][here, :], slots[a][i % 2])
                block = term if block is None else block + term
            back_v[here, pl.ds(i * BLOCK, BLOCK)] = block.astype(BF)

    def natural(i, side):
        at = ring_index((pos + (n - i if side == 0 else i)) % n, n) * BLOCK + side * LANE
        return pl.ds(pl.multiple_of(at, LANE), LANE)

    def finish_rows():
        @pl.loop(0, mine // STEP)
        def _(r):
            at = pl.multiple_of(r * STEP, STEP)
            m, inner = at // rows, pl.multiple_of(at % rows, STEP)
            here = pl.ds(at, STEP)
            x = x_v[here, :]
            scale = lax.rsqrt(jnp.mean(x * x, axis=-1, keepdims=True) + EPS)
            inside = jnp.mean(own_v[here, :] * gain_ref[0:1, :] * x, axis=-1, keepdims=True)
            slope = scale * scale * inside
            for i in range(n):
                for side in range(2):
                    lanes = pl.ds(i * BLOCK + side * LANE, LANE)
                    scaled = own_v[here, lanes] * gain_ref[0:1, lanes]
                    rows_out[m, pl.ds(inner, STEP), natural(i, side)] = mid_v[
                        here, lanes
                    ] + scale * (scaled - x_v[here, lanes] * slope)

    collect = Collect(dp, tp, n_tp, micro, rows, back_v, got_v, own_v, part_send, part_recv)
    loads[0].wait()
    for a in range(4):
        ring.first(a)
    loads[1].wait()
    loads[2].wait()
    ring.first(4)
    ring.prepare()
    for i in range(n):
        backward(i)
        if i % 3 == 2:
            ring.advance()
            ring.prepare()
    for m in range(micro):
        collect.start(bits[0], m)
    ring.advance()
    ring.prepare()
    for at, bit in enumerate(bits):
        for m in range(micro):
            collect.add(bit, m)
            if at + 1 < len(bits):
                collect.start(bits[at + 1], m)
        if at + 1 < len(bits):
            ring.advance()
            ring.prepare()
            ring.advance()
            ring.prepare()
    loads[3].wait()
    loads[4].wait()
    finish_rows()
    for a in range(4):
        load(0, a).start()
    for _ in range(n):
        ring.advance()

    sums = None
    for a in range(4):
        load(0, a).wait()
        term = jnp.sum(slots[a][0].astype(F32) * outs[a][...], axis=0, keepdims=True)
        sums = term if sums is None else sums + term
    sum_v[0] = jnp.concatenate([sums, sum_ref[1:8, :]], axis=0)
    for at, bit in enumerate(bits):
        swap = pltpu.make_async_remote_copy(
            src_ref=sum_v.at[2 * at],
            dst_ref=sum_v.at[2 * at + 1],
            send_sem=sum_send.at[at],
            recv_sem=sum_recv.at[at],
            device_id=(dp, partner(tp, bit)),
            device_id_type=MESH,
        )
        swap.start()
        swap.wait()
        sum_v[2 * at + 2] = sum_v[2 * at] + sum_v[2 * at + 1]
    gain_out[...] = sum_v[2 * len(bits)] / own_gain_ref[...]
    ring.finish()
    collect.finish()


def project_back(n, n_tp, rows, grads, gain, own_gain, sums, normed, gated, middle_all, grad_middle, x_rel, weights):
    total, width = normed.shape
    mine = x_rel.shape[0]
    micro = mine // rows
    blocks = [(g.shape[1], BLOCK) for g in grads] + [(gated.shape[1], BLOCK)]
    shape = jax.ShapeDtypeStruct
    dma = pltpu.SemaphoreType.DMA
    return pl.pallas_call(
        functools.partial(out_kernel, n, n_tp),
        out_shape=tuple(shape(s, F32) for s in blocks)
        + (shape((8, BLOCK), F32), shape((micro, rows, width), F32)),
        in_specs=[vmem()] * 7 + [anyspec()] * 9,
        out_specs=(vmem(),) * 7,
        scratch_shapes=[
            pltpu.VMEM((total, width), BF),
            pltpu.VMEM(gated.shape, BF),
            pltpu.VMEM((total, width), BF),
            pltpu.VMEM((mine, width), F32),
            pltpu.VMEM((mine, width), F32),
        ]
        + [pltpu.VMEM(s, F32) for s in blocks]
        + [pltpu.VMEM((2,) + s, BF) for s in blocks]
        + [pltpu.VMEM((2,) + s, BF) for s in blocks]
        + [pltpu.VMEM((2,) + s, BF) for s in blocks[:4]]
        + [
            pltpu.VMEM((total, width), BF),
            pltpu.VMEM((mine, width), F32),
            pltpu.VMEM((n_tp - 1, mine, width), BF),
            dma((n - 1, 5, 2)),
            dma((n - 1, 5, 2)),
            pltpu.SemaphoreType.REGULAR((5, 2)),
            dma((n_tp - 1, micro)),
            dma((n_tp - 1, micro)),
            pltpu.VMEM((2 * len(bits_of(n_tp)) + 1, 8, BLOCK), F32),
            dma((len(bits_of(n_tp)),)),
            dma((len(bits_of(n_tp)),)),
            dma((2, 4)),
            dma((5,)),
        ],
        compiler_params=pltpu.CompilerParams(
            collective_id=2, has_side_effects=True, vmem_limit_bytes=66_000_000
        ),
        cost_estimate=pl.CostEstimate(
            flops=4 * total * width * sum(s[0] for s in blocks),
            bytes_accessed=60_000_000,
            transcendentals=0,
        ),
        name="out_kernel",
    )(*grads, gain, own_gain, sums, normed, gated, middle_all, grad_middle, x_rel, *weights)


def finish_kernel(
    n,
    n_tp,
    passed,
    turned,
    *refs,
):
    sources = refs[: passed + turned]
    middle_ref, near_ref, far_ref = refs[passed + turned : passed + turned + 3]
    targets = refs[passed + turned + 3 : 2 * (passed + turned) + 3]
    block_out = refs[2 * (passed + turned) + 3]
    scratch = refs[2 * (passed + turned) + 4 :]
    held, (middle_v, near_v, far_v, block_v), (sem_in, sem_out) = (
        scratch[: passed + 2 * turned],
        scratch[passed + 2 * turned : passed + 2 * turned + 4],
        scratch[passed + 2 * turned + 4 :],
    )
    micro, rows, width = block_v.shape
    pos = ring_position(lax.axis_index("dp"), n)
    count = passed + turned
    ins = [
        pltpu.make_async_copy(sources[i], held[i], sem_in.at[i]) for i in range(count)
    ] + [
        pltpu.make_async_copy(source, target, sem_in.at[count + i])
        for i, (source, target) in enumerate(
            ((middle_ref, middle_v), (near_ref, near_v), (far_ref, far_v))
        )
    ]
    for copy in ins[count:] + ins[:count]:
        copy.start()
    results = list(held[:passed]) + list(held[count:])
    outs = [pltpu.make_async_copy(results[i], targets[i], sem_out.at[i]) for i in range(count)]
    outs.append(pltpu.make_async_copy(block_v, block_out, sem_out.at[count]))
    for copy in ins[count:]:
        copy.wait()

    @pl.loop(0, micro * rows // STEP)
    def _(r):
        at = pl.multiple_of(r * STEP, STEP)
        m, inner = at // rows, pl.multiple_of(at % rows, STEP)
        here = pl.ds(at, STEP)
        for i in range(n):
            for side in range(2):
                lanes = pl.ds(i * BLOCK + side * LANE, LANE)
                spot = ring_index((pos + (n - i if side == 0 else i)) % n, n)
                there = pl.ds(pl.multiple_of(spot * BLOCK + side * LANE, LANE), LANE)
                block_v[m, pl.ds(inner, STEP), there] = middle_v[here, lanes] + (
                    near_v[here, lanes] + far_v[here, lanes].astype(F32)
                )

    outs[count].start()
    for i in range(passed):
        ins[i].wait()
        outs[i].start()
    for i in range(turned):
        ins[passed + i].wait()
        held[count + i][...] = held[passed + i][...].T
        outs[passed + i].start()
    for copy in outs:
        copy.wait()


def finish(n, n_tp, passed, turned, middle, near, far, block_shape):
    shape = jax.ShapeDtypeStruct
    results = tuple(shape(a.shape, a.dtype) for a in passed) + tuple(
        shape(a.shape[::-1], a.dtype) for a in turned
    )
    count = len(passed) + len(turned)
    return pl.pallas_call(
        functools.partial(finish_kernel, n, n_tp, len(passed), len(turned)),
        out_shape=results + (shape(block_shape, F32),),
        in_specs=[anyspec()] * (count + 3),
        out_specs=(anyspec(),) * (count + 1),
        scratch_shapes=[pltpu.VMEM(a.shape, a.dtype) for a in passed]
        + [pltpu.VMEM(a.shape, a.dtype) for a in turned]
        + [pltpu.VMEM(a.shape[::-1], a.dtype) for a in turned]
        + [
            pltpu.VMEM(middle.shape, F32),
            pltpu.VMEM(near.shape, F32),
            pltpu.VMEM(far.shape, BF),
            pltpu.VMEM(block_shape, F32),
            pltpu.SemaphoreType.DMA((count + 3,)),
            pltpu.SemaphoreType.DMA((count + 1,)),
        ],
        compiler_params=pltpu.CompilerParams(vmem_limit_bytes=66_000_000),
        name="finish_kernel",
    )(*passed, *turned, middle, near, far)


def normalize(row_block, gain_vec):
    row_scale = lax.rsqrt(jnp.mean(row_block * row_block, axis=-1, keepdims=True) + EPS)
    return (row_block * row_scale * gain_vec.astype(jnp.float32), row_scale)


def norm_back(grad_rows, row_block, row_scale, gain_vec):
    scaled_grad = grad_rows * gain_vec.astype(jnp.float32)
    back_rows = row_scale * (
        scaled_grad
        - row_block
        * row_scale
        * row_scale
        * jnp.mean(scaled_grad * row_block, axis=-1, keepdims=True)
    )
    return (back_rows, jnp.sum(grad_rows * row_block * row_scale, axis=0))


def angles(length, feature_width):
    half_width = feature_width // 2
    frequency = jnp.exp(-math.log(10000.0) * jnp.arange(half_width, dtype=jnp.float32) / half_width)
    turns = jnp.arange(length, dtype=jnp.float32)[:, None] * frequency[None, :]
    return (jnp.cos(turns)[:, None, :], jnp.sin(turns)[:, None, :])


def decays(length, head_ids):
    places = jnp.arange(length, dtype=jnp.float32)
    spacing = places[:, None] - places[None, :]
    log_rate = jnp.log(1.0 - jnp.exp2(-5.0 - head_ids))
    return jnp.where(
        spacing[None] >= 0.0,
        jnp.exp(jnp.maximum(spacing, 0.0)[None] * log_rate[:, None, None]),
        0.0,
    )


def rotate(value_vectors, cosine_table, sine_table):
    half_width = value_vectors.shape[-1] // 2
    lower = value_vectors[..., :half_width]
    upper = value_vectors[..., half_width:]
    return jnp.concatenate(
        [lower * cosine_table - upper * sine_table, upper * cosine_table + lower * sine_table],
        axis=-1,
    )


def unrotate(value_vectors, cosine_table, sine_table):
    half_width = value_vectors.shape[-1] // 2
    lower = value_vectors[..., :half_width]
    upper = value_vectors[..., half_width:]
    return jnp.concatenate(
        [lower * cosine_table + upper * sine_table, upper * cosine_table - lower * sine_table],
        axis=-1,
    )


def plain_gelu_parts(pre_act):
    normal_cdf = 0.5 * (1.0 + lax.erf(pre_act * (1.0 / math.sqrt(2.0))))
    density = jnp.exp(-0.5 * pre_act * pre_act) * (1.0 / math.sqrt(2.0 * math.pi))
    return (pre_act * normal_cdf, normal_cdf + pre_act * density)


def inner_rows(left_rows, right_rows):
    return lax.dot_general(
        left_rows, right_rows, (((0,), (0,)), ((), ())), preferred_element_type=jnp.float32
    )


def times_t(left_rows, right_rows):
    return lax.dot_general(
        left_rows, right_rows, (((1,), (1,)), ((), ())), preferred_element_type=jnp.float32
    )


def forward_pass(rows_in, gathered, cosine_table, sine_table, decay_mask):
    (
        first_gain,
        second_gain,
        query_weight,
        key_weight,
        value_weight,
        swish_weight,
        output_weight,
        up_projection_matrix,
        gelu_weight,
        down_weight,
    ) = gathered
    local_heads = decay_mask.shape[0]
    scale_qk = 1.0 / math.sqrt(HK)
    normed, first_scale = normalize(rows_in, first_gain)
    normed_all = lax.all_gather(normed.astype(jnp.bfloat16), "tensor", axis=0, tiled=True)
    total_rows = normed_all.shape[0]
    sequences = total_rows // LEN
    query_turned_rows = rotate(
        jnp.dot(normed_all, query_weight, preferred_element_type=jnp.float32).reshape(
            sequences, LEN, local_heads, HK
        ),
        cosine_table,
        sine_table,
    ).astype(jnp.bfloat16)
    key_turned_rows = rotate(
        jnp.dot(normed_all, key_weight, preferred_element_type=jnp.float32).reshape(
            sequences, LEN, local_heads, HK
        ),
        cosine_table,
        sine_table,
    ).astype(jnp.bfloat16)
    value_rows = (
        jnp.dot(normed_all, value_weight, preferred_element_type=jnp.float32)
        .astype(jnp.bfloat16)
        .reshape(sequences, LEN, local_heads, HV)
    )
    gate_pre = jnp.dot(normed_all, swish_weight, preferred_element_type=jnp.float32)
    unscaled_logits = jnp.einsum(
        "snhd,smhd->shnm", query_turned_rows, key_turned_rows, preferred_element_type=jnp.float32
    )
    weight_bf = (unscaled_logits * (decay_mask * scale_qk)).astype(jnp.bfloat16)
    retained = jnp.einsum(
        "shnm,smhe->snhe", weight_bf, value_rows, preferred_element_type=jnp.float32
    )
    group_scale = lax.rsqrt(jnp.mean(retained * retained, axis=-1, keepdims=True) + GROUP_EPS)
    grouped = (retained * group_scale).reshape(total_rows, local_heads * HV)
    sigmoid_gate = jax.nn.sigmoid(gate_pre)
    swish_val = gate_pre * sigmoid_gate
    gated_rows = (swish_val * grouped).astype(jnp.bfloat16)
    attention = lax.psum_scatter(
        jnp.dot(gated_rows, output_weight, preferred_element_type=jnp.float32),
        "tensor",
        scatter_dimension=0,
        tiled=True,
    )
    middle = rows_in + attention
    second, second_scale = normalize(middle, second_gain)
    second_all = lax.all_gather(second.astype(jnp.bfloat16), "tensor", axis=0, tiled=True)
    up_pre = jnp.dot(second_all, up_projection_matrix, preferred_element_type=jnp.float32)
    gelu_pre = jnp.dot(second_all, gelu_weight, preferred_element_type=jnp.float32)
    gelu_val, gelu_slope = plain_gelu_parts(gelu_pre)
    hidden = (gelu_val * up_pre).astype(jnp.bfloat16)
    block_rows = middle + lax.psum_scatter(
        jnp.dot(hidden, down_weight, preferred_element_type=jnp.float32).astype(jnp.bfloat16),
        "tensor",
        scatter_dimension=0,
        tiled=True,
    ).astype(jnp.float32)
    kept_state = (
        rows_in,
        first_scale,
        normed_all,
        query_turned_rows,
        key_turned_rows,
        value_rows,
        gate_pre,
        weight_bf,
        retained,
        group_scale,
        grouped,
        gated_rows,
        middle,
        second_scale,
        second_all,
        up_pre,
        gelu_val,
        gelu_slope,
        hidden,
    )
    return (block_rows, kept_state)


def backward_pass(kept_state, cot_in, gathered, cosine_table, sine_table, decay_mask):
    (
        first_gain,
        second_gain,
        query_weight,
        key_weight,
        value_weight,
        swish_weight,
        output_weight,
        up_projection_matrix,
        gelu_weight,
        down_weight,
    ) = gathered
    (
        rows_in,
        first_scale,
        normed_all,
        query_turned_rows,
        key_turned_rows,
        value_rows,
        gate_pre,
        weight_bf,
        retained,
        group_scale,
        grouped,
        gated_rows,
        middle,
        second_scale,
        second_all,
        up_pre,
        gelu_val,
        gelu_slope,
        hidden,
    ) = kept_state
    local_heads = decay_mask.shape[0]
    total_rows = normed_all.shape[0]
    scale_qk = 1.0 / math.sqrt(HK)
    cot_all = lax.all_gather(cot_in.astype(jnp.bfloat16), "tensor", axis=0, tiled=True)
    grad_hidden = times_t(cot_all, down_weight)
    grad_down = inner_rows(hidden, cot_all)
    grad_uppre = (grad_hidden * gelu_val).astype(jnp.bfloat16)
    grad_gelupre = (grad_hidden * up_pre * gelu_slope).astype(jnp.bfloat16)
    grad_up = inner_rows(second_all, grad_uppre)
    grad_gelu = inner_rows(second_all, grad_gelupre)
    second_back = lax.psum_scatter(
        times_t(grad_uppre, up_projection_matrix) + times_t(grad_gelupre, gelu_weight),
        "tensor",
        scatter_dimension=0,
        tiled=True,
    )
    middle_back, grad_gain_two = norm_back(second_back, middle, second_scale, second_gain)
    grad_middle = cot_in + middle_back
    middle_all = lax.all_gather(grad_middle.astype(jnp.bfloat16), "tensor", axis=0, tiled=True)
    grad_gated = times_t(middle_all, output_weight)
    grad_out = inner_rows(gated_rows, middle_all)
    sigmoid_gate = jax.nn.sigmoid(gate_pre)
    swish_val = gate_pre * sigmoid_gate
    grad_swishpre = (
        grad_gated * grouped * (sigmoid_gate * (1.0 + gate_pre * (1.0 - sigmoid_gate)))
    ).astype(jnp.bfloat16)
    grad_grouped = (grad_gated * swish_val).reshape(retained.shape)
    grad_retained = (
        group_scale
        * (
            grad_grouped
            - retained
            * group_scale
            * group_scale
            * jnp.mean(grad_grouped * retained, axis=-1, keepdims=True)
        )
    ).astype(jnp.bfloat16)
    grad_valrows = jnp.einsum(
        "shnm,snhe->smhe", weight_bf, grad_retained, preferred_element_type=jnp.float32
    ).astype(jnp.bfloat16)
    grad_weight = jnp.einsum(
        "snhe,smhe->shnm", grad_retained, value_rows, preferred_element_type=jnp.float32
    )
    grad_retention_logits = (grad_weight * (decay_mask * scale_qk)).astype(jnp.bfloat16)
    grad_query_rotated_rows = jnp.einsum(
        "shnm,smhd->snhd",
        grad_retention_logits,
        key_turned_rows,
        preferred_element_type=jnp.float32,
    )
    grad_key_rotated_rows = jnp.einsum(
        "shnm,snhd->smhd",
        grad_retention_logits,
        query_turned_rows,
        preferred_element_type=jnp.float32,
    )
    grad_qpre = (
        unrotate(grad_query_rotated_rows, cosine_table, sine_table)
        .astype(jnp.bfloat16)
        .reshape(total_rows, local_heads * HK)
    )
    grad_kpre = (
        unrotate(grad_key_rotated_rows, cosine_table, sine_table)
        .astype(jnp.bfloat16)
        .reshape(total_rows, local_heads * HK)
    )
    grad_vflat = grad_valrows.reshape(total_rows, local_heads * HV)
    first_back = lax.psum_scatter(
        times_t(grad_qpre, query_weight)
        + times_t(grad_kpre, key_weight)
        + times_t(grad_vflat, value_weight)
        + times_t(grad_swishpre, swish_weight),
        "tensor",
        scatter_dimension=0,
        tiled=True,
    )
    grad_query = inner_rows(normed_all, grad_qpre)
    grad_key = inner_rows(normed_all, grad_kpre)
    grad_value = inner_rows(normed_all, grad_vflat)
    grad_swish = inner_rows(normed_all, grad_swishpre)
    input_back, grad_gain_one = norm_back(first_back, rows_in, first_scale, first_gain)
    grad_rows = grad_middle + input_back
    pieces = (
        grad_gain_one,
        grad_gain_two,
        grad_query,
        grad_key,
        grad_value,
        grad_swish,
        grad_out,
        grad_up,
        grad_gelu,
        grad_down,
    )
    return (grad_rows, pieces)


def plain_body(
    block_input,
    cotangent,
    first_gain,
    second_gain,
    query_weight,
    key_weight,
    value_weight,
    swish_weight,
    output_weight,
    up_projection_matrix,
    gelu_weight,
    down_weight,
):
    local_heads = query_weight.shape[1] // HK
    head_ids = (lax.axis_index("tensor") * local_heads + jnp.arange(local_heads)).astype(
        jnp.float32
    )
    cosine_table, sine_table = angles(LEN, HK)
    decay_mask = decays(LEN, head_ids)
    output_list = []
    grad_list = []
    totals = ()
    for micro_idx in range(block_input.shape[0]):
        forward_set = (
            lax.all_gather(first_gain, "dp", axis=0, tiled=True),
            lax.all_gather(second_gain, "dp", axis=0, tiled=True),
            lax.all_gather(query_weight, "dp", axis=0, tiled=True),
            lax.all_gather(key_weight, "dp", axis=0, tiled=True),
            lax.all_gather(value_weight, "dp", axis=0, tiled=True),
            lax.all_gather(swish_weight, "dp", axis=0, tiled=True),
            lax.all_gather(output_weight, "dp", axis=1, tiled=True),
            lax.all_gather(up_projection_matrix, "dp", axis=0, tiled=True),
            lax.all_gather(gelu_weight, "dp", axis=0, tiled=True),
            lax.all_gather(down_weight, "dp", axis=1, tiled=True),
        )
        block_rows, kept_state = forward_pass(
            block_input[micro_idx], forward_set, cosine_table, sine_table, decay_mask
        )
        held = lax.optimization_barrier(
            (
                (
                    first_gain,
                    second_gain,
                    query_weight,
                    key_weight,
                    value_weight,
                    swish_weight,
                    output_weight,
                    up_projection_matrix,
                    gelu_weight,
                    down_weight,
                ),
                block_rows,
            )
        )[0]
        backward_set = (
            lax.all_gather(held[0], "dp", axis=0, tiled=True),
            lax.all_gather(held[1], "dp", axis=0, tiled=True),
            lax.all_gather(held[2], "dp", axis=0, tiled=True),
            lax.all_gather(held[3], "dp", axis=0, tiled=True),
            lax.all_gather(held[4], "dp", axis=0, tiled=True),
            lax.all_gather(held[5], "dp", axis=0, tiled=True),
            lax.all_gather(held[6], "dp", axis=1, tiled=True),
            lax.all_gather(held[7], "dp", axis=0, tiled=True),
            lax.all_gather(held[8], "dp", axis=0, tiled=True),
            lax.all_gather(held[9], "dp", axis=1, tiled=True),
        )
        grad_rows, pieces = backward_pass(
            kept_state, cotangent[micro_idx], backward_set, cosine_table, sine_table, decay_mask
        )
        output_list.append(block_rows)
        grad_list.append(grad_rows)
        if micro_idx == 0:
            totals = tuple(pieces)
        else:
            totals = tuple((total + piece for total, piece in zip(totals, pieces)))
    totals = (
        lax.psum_scatter(totals[0], "dp", scatter_dimension=0, tiled=True),
        lax.psum_scatter(totals[1], "dp", scatter_dimension=0, tiled=True),
        lax.psum_scatter(totals[2], "dp", scatter_dimension=0, tiled=True),
        lax.psum_scatter(totals[3], "dp", scatter_dimension=0, tiled=True),
        lax.psum_scatter(totals[4], "dp", scatter_dimension=0, tiled=True),
        lax.psum_scatter(totals[5], "dp", scatter_dimension=0, tiled=True),
        lax.psum_scatter(totals[6], "dp", scatter_dimension=1, tiled=True),
        lax.psum_scatter(totals[7], "dp", scatter_dimension=0, tiled=True),
        lax.psum_scatter(totals[8], "dp", scatter_dimension=0, tiled=True),
        lax.psum_scatter(totals[9], "dp", scatter_dimension=1, tiled=True),
    )
    gain_first, gain_second = lax.psum((totals[0], totals[1]), "tensor")
    return (
        jnp.stack(output_list, axis=0),
        jnp.stack(grad_list, axis=0),
        gain_first,
        gain_second,
        totals[2],
        totals[3],
        totals[4],
        totals[5],
        totals[6],
        totals[7],
        totals[8],
        totals[9],
    )


def ring_body(
    n_dp,
    n_tp,
    block_input,
    cotangent,
    first_gain,
    second_gain,
    query_weight,
    key_weight,
    value_weight,
    swish_weight,
    output_weight,
    up_projection_matrix,
    gelu_weight,
    down_weight,
):
    micro, rows, width = block_input.shape
    local_heads = query_weight.shape[1] // HK
    window = n_tp * rows

    me = lax.axis_index("tensor")
    head_ids = (me * local_heads + jnp.arange(local_heads)).astype(F32)
    chunk_of = jnp.arange(n_tp) ^ me
    natural = (chunk_of[:, None] * rows + jnp.arange(rows)[None, :]).reshape(window)
    place = (natural % LEN).astype(F32)
    half_key = HK // 2
    frequency = jnp.exp(-math.log(10000.0) * jnp.arange(half_key, dtype=F32) / half_key)
    turns = place[:, None] * frequency[None, :]
    cosine, sine = jnp.cos(turns), jnp.sin(turns)
    log_rate = jnp.log(1.0 - jnp.exp2(-5.0 - head_ids))
    spots = natural.astype(F32)
    tables = (
        jnp.broadcast_to(spots[:, None], (window, LANE)),
        spots[None, :],
        jnp.broadcast_to(log_rate[:, None], (local_heads, window)),
    )

    gains_own = jnp.stack([first_gain, second_gain]).astype(F32)
    results = forward(
        n_dp,
        n_tp,
        block_input,
        cotangent,
        gains_own,
        cosine,
        sine,
        tables,
        (
            query_weight.T,
            key_weight.T,
            value_weight.T,
            swish_weight.T,
            output_weight,
            up_projection_matrix.T,
            gelu_weight.T,
            down_weight,
        ),
    )
    query, key, value, gate, x_rel, cot_rel, gains, normed, cot_all = results[:9]
    w_in, (w_o, w_u, w_l, w_d) = results[9:13], results[13:17]
    gated, middle, second, hidden, gelu_val, up_slope, near, far = results[17:]

    far = lax.ppermute(far, "tensor", [(i, i ^ (n_tp // 2)) for i in range(n_tp)])

    grad_down, grad_up, grad_gelu, sums, grad_middle, middle_all, *grads = (
        mid_backward(
            n_dp,
            n_tp,
            gains,
            tables,
            cosine,
            sine,
            cot_all,
            w_d,
            gelu_val,
            up_slope,
            hidden,
            second,
            w_u,
            w_l,
            middle,
            cot_rel,
            w_o,
            query,
            key,
            value,
            gate,
        )
    )
    grad_query, grad_key, grad_value, grad_swish, grad_out, gain_grads, grad_rows = project_back(
        n_dp,
        n_tp,
        rows,
        grads,
        gains,
        jnp.pad(gains_own, ((0, 6), (0, 0)), constant_values=1.0),
        sums,
        normed,
        gated,
        middle_all,
        grad_middle,
        x_rel,
        w_in,
    )

    passed = (grad_value, grad_swish, grad_out, grad_up, grad_gelu, grad_down, grad_rows)
    *passed, grad_query, grad_key, block_rows = finish(
        n_dp, n_tp, passed, (grad_query, grad_key), middle, near, far, block_input.shape
    )
    grad_value, grad_swish, grad_out, grad_up, grad_gelu, grad_down, grad_rows = passed

    return (
        block_rows,
        grad_rows,
        gain_grads[0],
        gain_grads[1],
        grad_query,
        grad_key,
        grad_value.T,
        grad_swish.T,
        grad_out,
        grad_up.T,
        grad_gelu.T,
        grad_down,
    )


def solution(mesh):
    rows = P(None, ("dp", "tensor"), None)
    wide, tall, gain = P("dp", "tensor"), P("tensor", "dp"), P("dp")
    n_dp, n_tp = mesh.shape["dp"], mesh.shape["tensor"]

    def run(*arrays):
        blocks = arrays[2].shape[0] == BLOCK and n_dp % 2 == 0 and n_dp > 2
        pairs = n_tp > 1 and n_tp & (n_tp - 1) == 0
        aligned = (n_tp * arrays[0].shape[1]) % LEN == 0 and arrays[0].shape[1] % LANE == 0
        if blocks and pairs and aligned:
            return ring_body(n_dp, n_tp, *arrays)
        return plain_body(*arrays)

    return jax.shard_map(
        run,
        mesh=mesh,
        in_specs=(rows, rows, gain, gain) + (wide,) * 4 + (tall, wide, wide, tall),
        out_specs=(rows, rows, gain, gain) + (wide,) * 4 + (tall, wide, wide, tall),
        check_vma=False,
    )
```

```python
import functools
import math

import jax
import jax.numpy as jnp
from jax import lax
from jax.experimental import pallas as pl
from jax.experimental.pallas import tpu as pltpu
from jax.sharding import PartitionSpec as P

HK = 256
HV = 432
LEN = 512
EPS = 1e-05
GROUP_EPS = 1.0
BF = jnp.bfloat16
F32 = jnp.float32
MESH = pl.DeviceIdType.MESH
LANE = 128
BLOCK = 2 * LANE
SLOTS = 3
STEP = 32


def ring_position(index, count):
    low = index // 2
    return low + (index % 2) * (count - 1 - 2 * low)


def ring_index(position, count):
    high = position // (count // 2)
    return (1 - high) * (2 * position) + high * (2 * (count - 1 - position) + 1)


def bits_of(count):
    return [1 << i for i in range(count.bit_length() - 1)]


def anyspec():
    return pl.BlockSpec(memory_space=pl.ANY)


def vmem():
    return pl.BlockSpec(memory_space=pltpu.VMEM)


def nt(left, right):
    return lax.dot_general(left, right, (((1,), (1,)), ((), ())), preferred_element_type=F32)


def nn(left, right):
    return lax.dot_general(left, right, (((1,), (0,)), ((), ())), preferred_element_type=F32)


def tn(left, right):
    return lax.dot_general(left, right, (((0,), (0,)), ((), ())), preferred_element_type=F32)


def partner(tp, bit):
    return tp + bit - 2 * bit * ((tp // bit) % 2)


def neighbours(n):
    dp, tp = lax.axis_index("dp"), lax.axis_index("tensor")
    pos = ring_position(dp, n)
    return dp, tp, ring_index((pos + 1) % n, n), ring_index((pos + n - 1) % n, n)


def greet(devices):
    barrier = pltpu.get_barrier_semaphore()
    for device in devices:
        pl.semaphore_signal(barrier, inc=1, device_id=device, device_id_type=MESH)
    pl.semaphore_wait(barrier, len(devices))


class Share:
    def __init__(self, dp, tp, n_tp, micro, rows, buf, send, recv):
        self.dp, self.tp, self.n_tp, self.micro, self.rows = dp, tp, n_tp, micro, rows
        self.buf, self.send, self.recv = buf, send, recv
        self.bits = bits_of(n_tp)[::-1]

    def copies(self, bit, m, keys=None):
        window = self.n_tp * self.rows
        for key in range(0, self.n_tp, 2 * bit):
            if keys is None or (key == 0) == keys:
                yield pltpu.make_async_remote_copy(
                    src_ref=self.buf.at[pl.ds(m * window + key * self.rows, self.rows)],
                    dst_ref=self.buf.at[pl.ds(m * window + (key ^ bit) * self.rows, self.rows)],
                    send_sem=self.send.at[m, key ^ bit],
                    recv_sem=self.recv.at[m, key ^ bit],
                    device_id=(self.dp, partner(self.tp, bit)),
                    device_id_type=MESH,
                )

    def begin(self, m):
        for bit in self.bits:
            for copy in self.copies(bit, m, True):
                copy.start()

    def relay(self, m):
        for bit in self.bits:
            for copy in self.copies(bit, m, False):
                copy.start()
            for copy in self.copies(bit, m):
                copy.wait_recv()

    def finish(self):
        for m in range(self.micro):
            for bit in self.bits:
                for copy in self.copies(bit, m):
                    copy.wait_send()


class Collect:
    def __init__(self, dp, tp, n_tp, micro, rows, back, got, own, send, recv):
        self.dp, self.tp, self.n_tp, self.micro, self.rows = dp, tp, n_tp, micro, rows
        self.back, self.got, self.own, self.send, self.recv = back, got, own, send, recv
        self.bits = bits_of(n_tp)

    def keys(self, bit):
        return [key for key in range(0, self.n_tp, bit) if key & bit]

    def copies(self, bit, m):
        window = self.n_tp * self.rows
        for key in self.keys(bit):
            yield pltpu.make_async_remote_copy(
                src_ref=self.back.at[pl.ds(m * window + key * self.rows, self.rows)],
                dst_ref=self.got.at[key - 1, pl.ds(m * self.rows, self.rows)],
                send_sem=self.send.at[key - 1, m],
                recv_sem=self.recv.at[key - 1, m],
                device_id=(self.dp, partner(self.tp, bit)),
                device_id_type=MESH,
            )

    def start(self, bit, m):
        for copy in self.copies(bit, m):
            copy.start()

    def add(self, bit, m):
        window = self.n_tp * self.rows
        for copy in self.copies(bit, m):
            copy.wait_recv()
        for key in self.keys(bit):
            target = key ^ bit

            @pl.loop(0, self.rows // STEP)
            def _(r):
                inner = pl.multiple_of(r * STEP, STEP)
                here = pl.ds(pl.multiple_of(m * self.rows + inner, STEP), STEP)
                there = pl.ds(pl.multiple_of(m * window + target * self.rows + inner, STEP), STEP)
                got = self.got[key - 1, here, :].astype(F32)
                if target == 0:
                    held = self.back[there, :].astype(F32) if bit == 1 else self.own[here, :]
                    self.own[here, :] = held + got
                else:
                    self.back[there, :] = (self.back[there, :].astype(F32) + got).astype(BF)

    def finish(self, bits=None):
        for m in range(self.micro):
            for bit in self.bits if bits is None else bits:
                for copy in self.copies(bit, m):
                    copy.wait_send()


def fill_decay(decay_v, col_ref, row_ref, rate_ref):
    heads, window, _ = decay_v.shape
    scale_qk = 1.0 / math.sqrt(HK)
    for h in range(heads):

        @pl.loop(0, window // LANE)
        def _(r):
            here = pl.ds(pl.multiple_of(r * LANE, LANE), LANE)
            col, row = col_ref[here, 0:1], row_ref[...]
            spacing = col - row
            same = jnp.floor(col * (1.0 / LEN)) == jnp.floor(row * (1.0 / LEN))
            kept = jnp.exp(jnp.maximum(spacing, 0.0) * rate_ref[h : h + 1, :]) * scale_qk
            decay_v[h, here, :] = jnp.where((spacing >= 0.0) & same, kept, 0.0)


def gelu_parts(pre_act):
    normal_cdf = 0.5 * (1.0 + lax.erf(pre_act * (1.0 / math.sqrt(2.0))))
    density = jnp.exp(-0.5 * pre_act * pre_act) * (1.0 / math.sqrt(2.0 * math.pi))
    return (pre_act * normal_cdf, normal_cdf + pre_act * density)


def forward_kernel(
    n,
    n_tp,
    x_ref,
    cot_ref,
    gains_ref,
    cos_ref,
    sin_ref,
    col_ref,
    row_ref,
    rate_ref,
    *refs,
):
    shards, refs = refs[:8], refs[8:]
    q_out, k_out, v_out, g_out, xr_out, cr_out, gain_out, nall_out, call_out = refs[:9]
    whole_outs, refs = refs[9:17], refs[17:]
    gated_out, middle_out, second_out, hidden_out, value_out, slope_out, near_out, far_out = refs[:8]
    nall_v, row_v, cot_v, gain_v, q_v, k_v, v_v, g_v, decay_v, got_v = refs[8:18]
    held, refs = refs[18:22], refs[22:]
    x_v, q_acc, k_acc, v_acc, wq_s, wk_s, wv_s, wg_s = refs[:8]
    back_v, own_v, gated_v, hidden_v, value_v, slope_v, up_v = refs[8:15]
    refs = refs[15:]
    ring_send, ring_recv, gain_send, gain_recv = refs[:4]
    first_send, first_recv, cot_send, cot_recv, share_send, share_recv = refs[4:10]
    part_send, part_recv, last_send, last_recv, load_sem, local_sem, out_sem = refs[10:]

    micro, rows, width = x_ref.shape
    window = n_tp * rows
    total, mine = micro * window, micro * rows
    dp, tp, cw, ccw = neighbours(n)
    pos = ring_position(dp, n)
    bits = bits_of(n_tp)
    heads = decay_v.shape[0]
    tile = 256
    half = HK // 2
    greet(
        [(ring_index((pos + k) % n, n), tp) for k in range(1, n)]
        + [(dp, partner(tp, bit)) for bit in bits]
    )

    wholes = tuple(whole_outs[:4]) + tuple(held)
    pieces = [(a, 0, shards[a].shape[0]) for a in range(4)]
    groups = [(0, 1, 2, 3)]
    for pair in ((4,), (5, 6), (7,)):
        group = []
        for a in pair:
            size = shards[a].shape[0]
            cut = size // 2 // 16 * 16 if len(pair) == 1 else size
            group.append(len(pieces))
            pieces.append((a, 0, cut))
            if cut < size:
                group.append(len(pieces))
                pieces.append((a, cut, size - cut))
        groups.append(tuple(group))
    ring_a, ring_b, ring_c, ring_d = groups

    def hop(i, p, side):
        a, low, size = pieces[p]
        span, lanes = pl.ds(low, size), pl.ds(side * LANE, LANE)
        own = isinstance(i, int) and i == 0
        return pltpu.make_async_remote_copy(
            src_ref=shards[a].at[span, lanes] if own else wholes[a].at[i, span, lanes],
            dst_ref=wholes[a].at[i + 1, span, lanes],
            send_sem=ring_send.at[i, p, side],
            recv_sem=ring_recv.at[i, p, side],
            device_id=((cw, ccw)[side], tp),
            device_id_type=MESH,
        )

    def ring_start(group):
        for p in group:
            for side in range(2):
                hop(0, p, side).start()

    def ring_pass(s, p):
        for side in range(2):
            hop(s - 1, p, side).wait_recv()
            if isinstance(s, int):
                if s < n - 1:
                    hop(s, p, side).start()
            else:

                @pl.when(s < n - 1)
                def _():
                    hop(s, p, side).start()

    def ring_step(s, group, following=()):
        for p in group:
            ring_pass(s, p)
        if isinstance(s, int) and s == n - 2:
            ring_start(following)

    def store(source, target):
        copy = pltpu.make_async_copy(source, target, out_sem.at[len(stores)])
        copy.start()
        stores.append(copy)

    stores = []
    ring_start(ring_a)
    own_blocks = [
        pltpu.make_async_copy(shards[4 + i], held[i].at[0], local_sem.at[4 + i]) for i in range(4)
    ]

    def natural(i, side):
        at = ring_index((pos + (n - i if side == 0 else i)) % n, n) * BLOCK + side * LANE
        return pl.ds(pl.multiple_of(at, LANE), LANE)

    first = Share(dp, tp, n_tp, micro, rows, nall_v, first_send, first_recv)
    share = Share(dp, tp, n_tp, micro, rows, nall_v, share_send, share_recv)

    def cot_copy(bit, m, key):
        source = cot_v.at[pl.ds(m * rows, rows)]
        if key:
            source = call_out.at[pl.ds(m * window + key * rows, rows)]
        return pltpu.make_async_remote_copy(
            src_ref=source,
            dst_ref=call_out.at[pl.ds(m * window + (key ^ bit) * rows, rows)],
            send_sem=cot_send.at[m, key ^ bit],
            recv_sem=cot_recv.at[m, key ^ bit],
            device_id=(dp, partner(tp, bit)),
            device_id_type=MESH,
        )

    def cot_copies(bit, keys=None):
        for m in range(micro):
            for key in range(0, n_tp, 2 * bit):
                if keys is None or (key == 0) == keys:
                    yield cot_copy(bit, m, key)

    def project():
        cot_rel_v = own_v
        slots = (wq_s, wk_s, wv_s, wg_s)
        accs = (q_acc, k_acc, v_acc, g_v)

        def load(i, a):
            source = shards[a] if i == 0 else wholes[a].at[i]
            return pltpu.make_async_copy(
                source, slots[a].at[i % SLOTS], load_sem.at[i % SLOTS, a]
            )

        x_copy = pltpu.make_async_copy(x_ref, x_v, local_sem.at[0])
        x_copy.start()
        for a in range(4):
            load(0, a).start()

        def gain_copy(k):
            return pltpu.make_async_remote_copy(
                src_ref=gains_ref,
                dst_ref=gain_v.at[k],
                send_sem=gain_send.at[k],
                recv_sem=gain_recv.at[k],
                device_id=(ring_index((pos + k) % n, n), tp),
                device_id_type=MESH,
            )

        own_gain = pltpu.make_async_copy(gains_ref, gain_v.at[0], local_sem.at[1])
        own_gain.start()
        for k in range(1, n):
            gain_copy(k).start()
        own_gain.wait()
        for k in range(1, n):
            gain_copy(k).wait()
        for i in range(n):
            gain_out[:, pl.ds(i * BLOCK, LANE)] = gain_v[i, :, pl.ds(0, LANE)]
            gain_out[:, pl.ds(i * BLOCK + LANE, LANE)] = gain_v[(n - i) % n, :, pl.ds(LANE, LANE)]
        x_copy.wait()

        def each_part(work):
            @pl.loop(0, mine // STEP)
            def _(r):
                at = pl.multiple_of(r * STEP, STEP)
                m, inner = at // rows, pl.multiple_of(at % rows, STEP)
                work(at, m, inner)

        def normalize_part(at, m, inner):
            chunk = x_v[m, pl.ds(inner, STEP), :]
            scale = lax.rsqrt(jnp.mean(chunk * chunk, axis=-1, keepdims=True) + EPS)
            there = pl.ds(pl.multiple_of(m * window + inner, STEP), STEP)
            for i in range(n):
                for side in range(2):
                    lanes = pl.ds(i * BLOCK + side * LANE, LANE)
                    part = x_v[m, pl.ds(inner, STEP), natural(i, side)]
                    row_v[pl.ds(at, STEP), lanes] = part
                    nall_v[there, lanes] = (part * scale * gain_out[0:1, lanes]).astype(BF)

        each_part(normalize_part)
        for m in range(micro):
            first.begin(m)
        store(row_v, xr_out)
        c_copy = pltpu.make_async_copy(cot_ref, x_v, local_sem.at[0])
        c_copy.start()
        c_copy.wait()

        def cot_part(at, m, inner):
            for i in range(n):
                for side in range(2):
                    lanes = pl.ds(i * BLOCK + side * LANE, LANE)
                    part = x_v[m, pl.ds(inner, STEP), natural(i, side)]
                    cot_rel_v[pl.ds(at, STEP), lanes] = part
                    cot_v[pl.ds(at, STEP), lanes] = part.astype(BF)

        each_part(cot_part)
        cot_rel = pltpu.make_async_copy(cot_rel_v, cr_out, local_sem.at[1])
        cot_rel.start()
        for m in range(micro):
            store(cot_v.at[pl.ds(m * rows, rows)], call_out.at[pl.ds(m * window, rows)])
        for copy in own_blocks:
            copy.start()

        def product(j, a, last):
            load(j, a).wait()
            if j == 0:
                pltpu.make_async_copy(
                    slots[a].at[0], wholes[a].at[0], load_sem.at[SLOTS, a]
                ).start()

            @pl.loop(0, total // tile)
            def _(r):
                at = pl.multiple_of(r * tile, tile)
                here = pl.ds(at, tile)
                part = nt(nall_v[here, pl.ds(j * BLOCK, BLOCK)], slots[a][j % SLOTS])
                if j > 0:
                    part = accs[a][here, :] + part
                if not last or a == 3:
                    accs[a][here, :] = part
                elif a == 2:
                    v_v[here, :] = part.astype(BF)
                else:
                    place = pl.ds(pl.multiple_of(at % window, tile), tile)
                    cosine, sine = cos_ref[place, :], sin_ref[place, :]
                    out = (q_v, k_v)[a]
                    for h in range(heads):
                        low = part[:, h * HK : h * HK + half]
                        high = part[:, h * HK + half : (h + 1) * HK]
                        out[here, pl.ds(h * HK, half)] = (low * cosine - high * sine).astype(BF)
                        out[here, pl.ds(h * HK + half, half)] = (
                            high * cosine + low * sine
                        ).astype(BF)

            if j == 0:
                pltpu.make_async_copy(
                    slots[a].at[0], wholes[a].at[0], load_sem.at[SLOTS, a]
                ).wait()

        start_at, done = 3, 0
        for i in range(n + 1):
            if i == 2:
                fill_decay(decay_v, col_ref, row_ref, rate_ref)
            if i == start_at:
                for m in range(micro):
                    first.relay(m)
                store(nall_v, nall_out)
                for bit in bits[::-1]:
                    for copy in cot_copies(bit, True):
                        copy.start()
            if i == n - 1:
                for bit in bits[::-1]:
                    for copy in cot_copies(bit, False):
                        copy.start()
                    for copy in cot_copies(bit):
                        copy.wait_recv()
            todo = []
            if i >= start_at:
                goal = min(i - 1, done + 1) if i < n else n - 1
                todo = list(range(done, goal + 1))
                done = goal + 1
            for a in range(4):
                if 0 < i < n:
                    ring_pass(i, a)
                if i == n - 2 and a == 3:
                    ring_start(ring_b)
                for j in todo:
                    product(j, a, j == n - 1)
                if 0 < i < n:
                    load(i, a).start()
                if i == n:
                    source, target = ((q_v, q_out), (k_v, k_out), (v_v, v_out), (g_v, g_out))[a]
                    store(source, target)
        cot_rel.wait()

    project()
    wo_v, wu_v, wl_v, wd_v = held
    units = shards[7].shape[0]

    def middle_part():
        for copy in own_blocks:
            copy.wait()

        def attend(m, h):
            keys = pl.ds(h * HK, HK)
            values = pl.ds(h * HV, HV)
            inside = pl.ds(m * window, window)

            @pl.loop(0, window // tile)
            def _(r):
                at = pl.multiple_of(r * tile, tile)
                here = pl.ds(pl.multiple_of(m * window + at, tile), tile)
                scores = nt(q_v[here, keys], k_v[inside, keys])
                weight = (scores * decay_v[h, pl.ds(at, tile), :]).astype(BF)
                kept = nn(weight, v_v[inside, values])
                group = lax.rsqrt(jnp.mean(kept * kept, axis=-1, keepdims=True) + GROUP_EPS)
                gate = g_v[here, values]
                gated_v[here, values] = (gate * jax.nn.sigmoid(gate) * (kept * group)).astype(BF)

        def times_block(left, weights, i):
            @pl.loop(0, total // tile)
            def _(r):
                here = pl.ds(pl.multiple_of(r * tile, tile), tile)
                back_v[here, pl.ds(i * BLOCK, BLOCK)] = nn(left[here, :], weights[i]).astype(BF)

        collect = Collect(dp, tp, n_tp, micro, rows, back_v, got_v, own_v, part_send, part_recv)
        jobs = [(m, h) for m in range(micro) for h in range(heads)]
        reached = 0
        while jobs:
            if reached < n - 1:
                reached += 1
                ring_step(reached, ring_b, ring_c)
            attend(*jobs.pop(0))
        store(gated_v, gated_out)
        ready = 0
        while ready < n:
            if reached < n - 1:
                reached += 1
                ring_step(reached, ring_b, ring_c)
            for _ in range(2 if reached < n - 1 else n):
                if ready < min(n, reached + 1):
                    times_block(gated_v, wo_v, ready)
                    ready += 1
        store(wo_v, whole_outs[4])
        first.finish()
        stores[0].wait()
        stores[micro + 1].wait()
        for m in range(micro):
            collect.start(bits[0], m)
        passed = [0]

        def pairs_to(goal):
            while passed[0] < min(goal, n - 1):
                passed[0] += 1
                ring_step(passed[0], ring_c, ring_d)

        for at, bit in enumerate(bits[:-1]):
            for m in range(micro):
                collect.add(bit, m)
                collect.start(bits[at + 1], m)
        pairs_to(1)
        for m in range(micro):
            pairs_to(2 + m)
            collect.add(bits[-1], m)

            @pl.loop(0, rows // STEP)
            def _(r):
                inner = pl.multiple_of(r * STEP, STEP)
                here = pl.ds(pl.multiple_of(m * rows + inner, STEP), STEP)
                there = pl.ds(pl.multiple_of(m * window + inner, STEP), STEP)
                middle = row_v[here, :] + own_v[here, :]
                row_v[here, :] = middle
                scale = lax.rsqrt(jnp.mean(middle * middle, axis=-1, keepdims=True) + EPS)
                nall_v[there, :] = (middle * scale * gain_out[1:2, :]).astype(BF)

            share.begin(m)
        store(row_v, middle_out)
        pairs_to(4)
        for m in range(micro):
            share.relay(m)
            pairs_to(5 + m)
        pairs_to(n - 1)
        store(nall_v, second_out)
        store(wu_v, whole_outs[5])
        store(wl_v, whole_outs[6])

        def rows_by(weights, here):
            result = None
            for i in range(n):
                term = nt(nall_v[here, pl.ds(i * BLOCK, BLOCK)], weights[i])
                result = term if result is None else result + term
            return result

        tiles = total // tile
        every = max(1, tiles // 2)
        inside_loop = min(tiles // every, n - 1)

        @pl.loop(0, tiles)
        def _(r):
            here = pl.ds(pl.multiple_of(r * tile, tile), tile)
            up_v[...] = rows_by(wu_v, here)
            gelu_val, gelu_slope = gelu_parts(rows_by(wl_v, here))
            up = up_v[...]
            hidden_v[here, :] = (gelu_val * up).astype(BF)
            value_v[here, :] = gelu_val.astype(BF)
            slope_v[here, :] = (up * gelu_slope).astype(BF)

            @pl.when((r % every == every - 1) & (r // every < inside_loop))
            def _():
                ring_step(r // every + 1, ring_d)

        store(hidden_v, hidden_out)
        store(value_v, value_out)
        store(slope_v, slope_out)
        collect.finish()
        ready = 0
        for s in range(inside_loop, n):
            if s > inside_loop:
                ring_step(s, ring_d)
            for _ in range(2 if s < n - 1 else n):
                if ready <= s and ready < n:
                    times_block(hidden_v, wd_v, ready)
                    ready += 1
        store(wd_v, whole_outs[7])
        last = Collect(dp, tp, n_tp, micro, rows, back_v, got_v, own_v, last_send, last_recv)
        for at, bit in enumerate(bits[:-1]):
            for m in range(micro):
                last.start(bit, m)
            for m in range(micro):
                last.add(bit, m)
        store(own_v, near_out)
        for m in range(micro):
            store(
                back_v.at[pl.ds(m * window + bits[-1] * rows, rows)],
                far_out.at[pl.ds(m * rows, rows)],
            )
        last.finish(bits[:-1])
        for i in range(n - 1):
            for p in range(len(pieces)):
                hop(i, p, 0).wait_send()
                hop(i, p, 1).wait_send()
        share.finish()
        for bit in bits:
            for copy in cot_copies(bit):
                copy.wait_send()
        for at, copy in enumerate(stores):
            if at not in waited:
                copy.wait()

    waited = (0, micro + 1)
    middle_part()


def forward(n, n_tp, x, cot, gains, cosine, sine, tables, weights):
    micro, rows, width = x.shape
    window = n_tp * rows
    total, mine = micro * window, micro * rows
    sizes = [w.shape[0] for w in weights]
    hv, units = sizes[2], sizes[7]
    shape = jax.ShapeDtypeStruct
    dma = pltpu.SemaphoreType.DMA
    count = 4 + 2 + 2 + 2
    return pl.pallas_call(
        functools.partial(forward_kernel, n, n_tp),
        out_shape=(
            shape((total, sizes[0]), BF),
            shape((total, sizes[1]), BF),
            shape((total, hv), BF),
            shape((total, sizes[3]), F32),
            shape((mine, width), F32),
            shape((mine, width), F32),
            shape((2, width), F32),
            shape((total, width), BF),
            shape((total, width), BF),
        )
        + tuple(shape((n, s, BLOCK), BF) for s in sizes)
        + (
            shape((total, hv), BF),
            shape((mine, width), F32),
            shape((total, width), BF),
            shape((total, units), BF),
            shape((total, units), BF),
            shape((total, units), BF),
            shape((mine, width), F32),
            shape((mine, width), BF),
        ),
        in_specs=[anyspec()] * 3 + [vmem()] * 5 + [anyspec()] * 8,
        out_specs=(anyspec(),) * 6 + (vmem(),) + (anyspec(),) * 18,
        scratch_shapes=[
            pltpu.VMEM((total, width), BF),
            pltpu.VMEM((mine, width), F32),
            pltpu.VMEM((mine, width), BF),
            pltpu.VMEM((n, 2, BLOCK), F32),
            pltpu.VMEM((total, sizes[0]), BF),
            pltpu.VMEM((total, sizes[1]), BF),
            pltpu.VMEM((total, hv), BF),
            pltpu.VMEM((total, sizes[3]), F32),
            pltpu.VMEM((tables[2].shape[0], window, window), F32),
            pltpu.VMEM((n_tp - 1, mine, width), BF),
        ]
        + [pltpu.VMEM((n, s, BLOCK), BF) for s in sizes[4:]]
        + [pltpu.VMEM((micro, rows, width), F32)]
        + [pltpu.VMEM((total, s), F32) for s in sizes[:3]]
        + [pltpu.VMEM((SLOTS, s, BLOCK), BF) for s in sizes[:4]]
        + [
            pltpu.VMEM((total, width), BF),
            pltpu.VMEM((mine, width), F32),
            pltpu.VMEM((total, hv), BF),
            pltpu.VMEM((total, units), BF),
            pltpu.VMEM((total, units), BF),
            pltpu.VMEM((total, units), BF),
            pltpu.VMEM((256, units), F32),
        ]
        + [dma((n - 1, count, 2))] * 2
        + [dma((n,))] * 2
        + [dma((micro, n_tp))] * 6
        + [dma((n_tp - 1, micro))] * 4
        + [dma((SLOTS + 1, 4)), dma((8,)), dma((19 + micro,))],
        compiler_params=pltpu.CompilerParams(
            collective_id=1, has_side_effects=True, vmem_limit_bytes=66_500_000
        ),
        cost_estimate=pl.CostEstimate(
            flops=2 * total * width * sum(sizes), bytes_accessed=120_000_000, transcendentals=0
        ),
        name="forward_kernel",
    )(x, cot, gains, cosine, sine, *tables, *weights)


class LaneRing:
    def __init__(self, n, tp, cw, ccw, lanes, fresh, free, done):
        self.n, self.tp, self.ways, self.lanes = n, tp, (cw, ccw), lanes
        self.fresh, self.free, self.done = fresh, free, done
        self.state = [dict(job=0, step=1, firsts=0, ready=False) for _ in lanes]
        self.allowed = [0 for _ in lanes]

    def hop(self, p, t):
        lane = self.lanes[p]
        size = lane["jobs"][t // (self.n - 1)][0]
        slots = lane["recv"].shape[0]
        copies = []
        for side in range(2):
            lanes = pl.ds(side * LANE, LANE)
            copies.append(
                pltpu.make_async_remote_copy(
                    src_ref=lane["send"].at[t % 2, pl.ds(0, size), lanes],
                    dst_ref=lane["recv"].at[t % slots, pl.ds(0, size), lanes],
                    send_sem=lane["send_sem"].at[t, side],
                    recv_sem=lane["recv_sem"].at[t, side],
                    device_id=(self.ways[side], self.tp),
                    device_id_type=MESH,
                )
            )
        return copies

    def post(self, p, t, total):
        lane = self.lanes[p]
        slots = lane["recv"].shape[0]
        if t >= 2:
            for copy in self.hop(p, t - 2):
                copy.wait_send()
        lane["send"][t % 2, pl.ds(0, total.shape[0]), :] = total.astype(BF)
        for side, copy in enumerate(self.hop(p, t)):
            if t >= slots:
                pl.semaphore_wait(self.free.at[p, side], 1)
            copy.start()

    def first(self, p):
        lane, state = self.lanes[p], self.state[p]
        job = state["firsts"]
        size, gradient, _ = lane["jobs"][job]
        state["firsts"] += 1
        gradient(1 % self.n, self.fresh.at[pl.ds(0, size)])
        self.post(p, job * (self.n - 1), self.fresh[pl.ds(0, size), :])

    def prepare(self):
        for p, lane in enumerate(self.lanes):
            state = self.state[p]
            if state["job"] < state["firsts"] and not state["ready"]:
                size, gradient, _ = lane["jobs"][state["job"]]
                gradient((state["step"] + 1) % self.n, lane["part"].at[pl.ds(0, size)])
                state["ready"] = True

    def advance(self):
        n = self.n
        self.prepare()
        for p, lane in enumerate(self.lanes):
            state = self.state[p]
            job, step = state["job"], state["step"]
            count = len(lane["jobs"])
            if job >= state["firsts"]:
                if job < min(count, self.allowed[p]):
                    self.first(p)
                continue
            if step == n - 1 and state["firsts"] == job + 1 < min(count, self.allowed[p]):
                self.first(p)
            size, _, out = lane["jobs"][job]
            t = job * (n - 1) + step - 1
            slots = lane["recv"].shape[0]
            for copy in self.hop(p, t):
                copy.wait_recv()
            total = lane["part"][pl.ds(0, size), :] + lane["recv"][
                t % slots, pl.ds(0, size), :
            ].astype(F32)
            state["ready"] = False
            if step == n - 1:
                self.done(p, job, total, out)
                state["job"], state["step"] = job + 1, 1
            if t + slots < count * (n - 1):
                for side in range(2):
                    pl.semaphore_signal(
                        self.free.at[p, side],
                        inc=1,
                        device_id=(self.ways[1 - side], self.tp),
                        device_id_type=MESH,
                    )
            if step < n - 1:
                self.post(p, t + 1, total)
                state["step"] = step + 1

    def busy(self):
        return any(s["job"] < len(lane["jobs"]) for s, lane in zip(self.state, self.lanes))

    def finish(self):
        for p, lane in enumerate(self.lanes):
            last = len(lane["jobs"]) * (self.n - 1)
            for t in range(max(0, last - 2), last):
                for copy in self.hop(p, t):
                    copy.wait_send()


def backward_kernel(
    n,
    n_tp,
    gain_ref,
    own_gain_ref,
    col_ref,
    row_ref,
    rate_ref,
    cos_ref,
    sin_ref,
    *refs,
):
    hidden_ref, cot_ref, value_ref, slope_ref, second_ref, middle_ref, cotf_ref = refs[:7]
    q_ref, k_ref, v_ref, g_ref, gated_ref, nall_ref, x_ref = refs[7:14]
    wq_ref, wk_ref, wv_ref, wg_ref, wo_ref, wu_ref, wl_ref, wd_ref = refs[14:22]
    refs = refs[22:]
    dd_out, du_out, dl_out, do_out, ds_out, dv_out, dq_out, dk_out, sum_out, rows_out = refs[:10]
    cot_v, w_v, gu_v, gl_v, hidden_v, second_v, wu_s, wl_s, middle_v, cotf_v = refs[10:20]
    q_v, k_v, v_v, g_v, gs_v, gated_v, decay_v, gk_acc, gv_acc = refs[20:29]
    back_v, own_v, got_v, mall_v, rows_v, part0, part1, fresh_v = refs[29:37]
    send0, send1, recv0, recv1, done_v, own_w, sum_v = refs[37:44]
    ring_send0, ring_send1, ring_recv0, ring_recv1, ring_free = refs[44:49]
    part_send, part_recv, last_send, last_recv, share_send, share_recv = refs[49:55]
    sum_send, sum_recv, load_sem, done_sem, own_sem, local_sem = refs[55:]

    total, width = cot_v.shape
    mine = own_v.shape[0]
    window = col_ref.shape[0]
    micro = total // window
    rows = mine // micro
    heads = decay_v.shape[0]
    dp, tp, cw, ccw = neighbours(n)
    pos = ring_position(dp, n)
    bits = bits_of(n_tp)
    tile = 256
    half = HK // 2
    greet([(cw, tp), (ccw, tp)] + [(dp, partner(tp, bit)) for bit in bits])

    pairs = (
        (hidden_ref, hidden_v),
        (cot_ref, cot_v),
        (wd_ref, w_v),
        (value_ref, gu_v),
        (slope_ref, gl_v),
        (second_ref, second_v),
        (middle_ref, middle_v),
        (cotf_ref, cotf_v),
        (q_ref, q_v),
        (k_ref, k_v),
        (v_ref, v_v),
        (g_ref, g_v),
    )
    loads = [
        pltpu.make_async_copy(source, target, local_sem.at[at])
        for at, (source, target) in enumerate(pairs)
    ]
    for copy in loads:
        copy.start()

    def block_load(i, a):
        source, target = ((wu_ref, wu_s), (wl_ref, wl_s))[a]
        return pltpu.make_async_copy(
            source.at[i % n], target.at[i % 2], load_sem.at[i % 2, a]
        )

    block_load(0, 0).start()
    block_load(0, 1).start()

    def product(left, right):
        def gradient(i, target):
            target[...] = tn(left[...], right[:, pl.ds(i * BLOCK, BLOCK)])

        return gradient

    units, hv, hk = gu_v.shape[1], v_v.shape[1], q_v.shape[1]
    lanes = (
        dict(
            jobs=(
                (units, product(hidden_v, cot_v), (dd_out, None)),
                (units, product(gl_v, second_v), (dl_out, wl_ref)),
                (hv, product(gs_v, cot_v), (ds_out, wg_ref)),
                (hk, product(q_v, cot_v), (dq_out, wq_ref)),
            ),
            part=part0,
            send=send0,
            recv=recv0,
            send_sem=ring_send0,
            recv_sem=ring_recv0,
        ),
        dict(
            jobs=(
                (units, product(gu_v, second_v), (du_out, wu_ref)),
                (hv, product(hidden_v, mall_v), (do_out, None)),
                (hv, product(v_v, cot_v), (dv_out, wv_ref)),
                (hk, product(k_v, cot_v), (dk_out, wk_ref)),
            ),
            part=part1,
            send=send1,
            recv=recv1,
            send_sem=ring_send1,
            recv_sem=ring_recv1,
        ),
    )
    pending = {}

    def done(p, job, result, out):
        target, weight = out
        size = result.shape[0]
        if p in pending:
            pending.pop(p).wait()
        done_v[p, pl.ds(0, size), :] = result
        pending[p] = pltpu.make_async_copy(
            done_v.at[p, pl.ds(0, size)], target, done_sem.at[p]
        )
        pending[p].start()
        if weight is not None:
            own = pltpu.make_async_copy(
                weight.at[0], own_w.at[p, pl.ds(0, size)], own_sem.at[p]
            )
            own.start()
            own.wait()
            line = jnp.sum(
                own_w[p, pl.ds(0, size), :].astype(F32) * done_v[p, pl.ds(0, size), :],
                axis=0,
                keepdims=True,
            )
            at = 1 if job < 2 else 0
            sum_v[0, at : at + 1, :] = sum_v[0, at : at + 1, :] + line

    sum_v[...] = jnp.zeros_like(sum_v)
    ring = LaneRing(n, tp, cw, ccw, lanes, fresh_v, ring_free, done)
    loads[0].wait()
    loads[1].wait()
    ring.allowed = [1, 0]
    ring.first(0)
    for copy in loads[2:5]:
        copy.wait()

    @pl.loop(0, total // tile)
    def _(r):
        here = pl.ds(pl.multiple_of(r * tile, tile), tile)
        grad = None
        for i in range(n):
            term = nt(cot_v[here, pl.ds(i * BLOCK, BLOCK)], w_v[i])
            grad = term if grad is None else grad + term
        gu_v[here, :] = (grad * gu_v[here, :].astype(F32)).astype(BF)
        gl_v[here, :] = (grad * gl_v[here, :].astype(F32)).astype(BF)

    wo_load = pltpu.make_async_copy(wo_ref, w_v, local_sem.at[2])
    wo_load.start()
    loads[5].wait()
    ring.allowed = [2, 1]
    ring.first(1)
    ring.prepare()
    collect = Collect(dp, tp, n_tp, micro, rows, back_v, got_v, own_v, part_send, part_recv)
    share = Share(dp, tp, n_tp, micro, rows, mall_v, share_send, share_recv)
    for m in range(micro):
        for i in range(n):
            at = m * n + i
            for a in range(2):
                block_load(at, a).wait()
                if at + 1 < micro * n:
                    block_load(at + 1, a).start()

            @pl.loop(0, window // tile)
            def _(r):
                here = pl.ds(pl.multiple_of(m * window + r * tile, tile), tile)
                back_v[here, pl.ds(i * BLOCK, BLOCK)] = (
                    nn(gu_v[here, :], wu_s[at % 2]) + nn(gl_v[here, :], wl_s[at % 2])
                ).astype(BF)

        collect.start(bits[0], m)
    ring.advance()
    ring.prepare()
    for at, bit in enumerate(bits[:-1]):
        for m in range(micro):
            collect.add(bit, m)
            collect.start(bits[at + 1], m)
    fill_decay(decay_v, col_ref, row_ref, rate_ref)
    loads[6].wait()
    loads[7].wait()
    for m in range(micro):
        ring.advance()
        ring.prepare()
        collect.add(bits[-1], m)

        @pl.loop(0, rows // STEP)
        def _(r):
            inner = pl.multiple_of(r * STEP, STEP)
            here = pl.ds(pl.multiple_of(m * rows + inner, STEP), STEP)
            there = pl.ds(pl.multiple_of(m * window + inner, STEP), STEP)
            middle = middle_v[here, :]
            scale = lax.rsqrt(jnp.mean(middle * middle, axis=-1, keepdims=True) + EPS)
            scaled = own_v[here, :] * gain_ref[1:2, :]
            inside = jnp.mean(scaled * middle, axis=-1, keepdims=True)
            grad = cotf_v[here, :] + scale * (scaled - middle * (scale * scale * inside))
            cotf_v[here, :] = grad
            mall_v[there, :] = grad.astype(BF)

        share.begin(m)
    x_load = pltpu.make_async_copy(x_ref, middle_v, local_sem.at[6])
    x_load.start()
    collect.finish()
    ring.advance()
    ring.prepare()
    for copy in loads[8:]:
        copy.wait()
    wo_load.wait()
    gated_load = None
    for m in range(micro):
        share.relay(m)
        if m == micro - 1 and gated_load is not None:
            gated_load.wait()
            ring.allowed = [2, 2]
        ring.advance()
        ring.prepare()
        for h in range(heads):
            keys = pl.ds(h * HK, HK)
            values = pl.ds(h * HV, HV)
            inside = pl.ds(m * window, window)
            gk_acc[...] = jnp.zeros_like(gk_acc)
            gv_acc[...] = jnp.zeros_like(gv_acc)

            @pl.loop(0, window // tile)
            def _(r):
                at = pl.multiple_of(r * tile, tile)
                here = pl.ds(pl.multiple_of(m * window + at, tile), tile)
                grad = None
                for i in range(n):
                    term = nt(mall_v[here, pl.ds(i * BLOCK, BLOCK)], w_v[i, values, :])
                    grad = term if grad is None else grad + term
                gated_v[pl.ds(at, tile), :] = grad

            @pl.loop(0, window // tile)
            def _(r):
                at = pl.multiple_of(r * tile, tile)
                local = pl.ds(at, tile)
                here = pl.ds(pl.multiple_of(m * window + at, tile), tile)
                decay = decay_v[h, local, :]
                query = q_v[here, keys]
                weight = (nt(query, k_v[inside, keys]) * decay).astype(BF)
                kept = nn(weight, v_v[inside, values])
                group = lax.rsqrt(jnp.mean(kept * kept, axis=-1, keepdims=True) + GROUP_EPS)
                gate = g_v[here, values]
                sigmoid = jax.nn.sigmoid(gate)
                grad = gated_v[local, :]
                gs_v[here, values] = (
                    grad * (kept * group) * (sigmoid * (1.0 + gate * (1.0 - sigmoid)))
                ).astype(BF)
                lifted = grad * (gate * sigmoid)
                mean = jnp.mean(lifted * kept, axis=-1, keepdims=True)
                grad_kept = (group * (lifted - kept * (group * group * mean))).astype(BF)
                gv_acc[...] += tn(weight, grad_kept)
                score = (nt(grad_kept, v_v[inside, values]) * decay).astype(BF)
                gk_acc[...] += tn(score, query)
                turned = nn(score, k_v[inside, keys])
                low, high = turned[:, :half], turned[:, half:]
                cosine, sine = cos_ref[local, :], sin_ref[local, :]
                q_v[here, pl.ds(h * HK, half)] = (low * cosine + high * sine).astype(BF)
                q_v[here, pl.ds(h * HK + half, half)] = (high * cosine - low * sine).astype(BF)

            low, high = gk_acc[:, :half], gk_acc[:, half:]
            cosine, sine = cos_ref[...], sin_ref[...]
            k_v[inside, pl.ds(h * HK, half)] = (low * cosine + high * sine).astype(BF)
            k_v[inside, pl.ds(h * HK + half, half)] = (high * cosine - low * sine).astype(BF)
            v_v[inside, values] = gv_acc[...].astype(BF)
            ring.advance()
            if ring.state[0]["job"] > 0 and gated_load is None:
                gated_load = pltpu.make_async_copy(gated_ref, hidden_v, local_sem.at[0])
                gated_load.start()
                nall_load = pltpu.make_async_copy(nall_ref, cot_v, local_sem.at[1])
                nall_load.start()
            ring.prepare()

    def settle():
        while ring.state[0]["job"] == 0:
            ring.advance()

    if gated_load is None:
        settle()
        gated_load = pltpu.make_async_copy(gated_ref, hidden_v, local_sem.at[0])
        gated_load.start()
        nall_load = pltpu.make_async_copy(nall_ref, cot_v, local_sem.at[1])
        nall_load.start()
    if ring.allowed[1] < 2:
        gated_load.wait()
    nall_load.wait()
    ring.allowed = [4, 4]

    wholes = (wq_ref, wk_ref, wv_ref, wg_ref)
    grads = (q_v, k_v, v_v, gs_v)
    sizes = (hk, hk, hv, hv)

    def weight_slot(i, a):
        return w_v.at[2 * a + i % 2, pl.ds(0, sizes[a])]

    def weight_load(i, a):
        return pltpu.make_async_copy(
            wholes[a].at[i], weight_slot(i, a), load_sem.at[2 + i % 2, a]
        )

    for a in range(4):
        weight_load(0, a).start()
    ring.advance()
    ring.prepare()
    for i in range(n):
        for a in range(4):
            weight_load(i, a).wait()
            if i + 1 < n:
                weight_load(i + 1, a).start()

        @pl.loop(0, total // tile)
        def _(r):
            here = pl.ds(pl.multiple_of(r * tile, tile), tile)
            block = None
            for a in range(4):
                term = nn(grads[a][here, :], weight_slot(i, a)[...])
                block = term if block is None else block + term
            back_v[here, pl.ds(i * BLOCK, BLOCK)] = block.astype(BF)

        if i % 2 == 1:
            ring.advance()
            ring.prepare()
    last = Collect(dp, tp, n_tp, micro, rows, back_v, got_v, own_v, last_send, last_recv)
    for m in range(micro):
        last.start(bits[0], m)
    ring.advance()
    ring.prepare()
    for at, bit in enumerate(bits):
        for m in range(micro):
            last.add(bit, m)
            if at + 1 < len(bits):
                last.start(bits[at + 1], m)
        if at + 1 < len(bits):
            for _ in range(3):
                ring.advance()
                ring.prepare()
    x_load.wait()

    def natural(i, side):
        at = ring_index((pos + (n - i if side == 0 else i)) % n, n) * BLOCK + side * LANE
        return pl.ds(pl.multiple_of(at, LANE), LANE)

    @pl.loop(0, mine // STEP)
    def _(r):
        at = pl.multiple_of(r * STEP, STEP)
        m, inner = at // rows, pl.multiple_of(at % rows, STEP)
        here = pl.ds(at, STEP)
        x = middle_v[here, :]
        scale = lax.rsqrt(jnp.mean(x * x, axis=-1, keepdims=True) + EPS)
        inside = jnp.mean(own_v[here, :] * gain_ref[0:1, :] * x, axis=-1, keepdims=True)
        slope = scale * scale * inside
        for i in range(n):
            for side in range(2):
                lanes = pl.ds(i * BLOCK + side * LANE, LANE)
                scaled = own_v[here, lanes] * gain_ref[0:1, lanes]
                rows_v[m, pl.ds(inner, STEP), natural(i, side)] = cotf_v[
                    here, lanes
                ] + scale * (scaled - middle_v[here, lanes] * slope)

    rows_copy = pltpu.make_async_copy(rows_v, rows_out, local_sem.at[2])
    rows_copy.start()
    while ring.busy():
        ring.advance()
        ring.prepare()
    for at, bit in enumerate(bits):
        swap = pltpu.make_async_remote_copy(
            src_ref=sum_v.at[2 * at],
            dst_ref=sum_v.at[2 * at + 1],
            send_sem=sum_send.at[at],
            recv_sem=sum_recv.at[at],
            device_id=(dp, partner(tp, bit)),
            device_id_type=MESH,
        )
        swap.start()
        swap.wait()
        sum_v[2 * at + 2] = sum_v[2 * at] + sum_v[2 * at + 1]
    sum_out[...] = sum_v[2 * len(bits)] / own_gain_ref[...]
    ring.finish()
    share.finish()
    last.finish()
    rows_copy.wait()
    for copy in pending.values():
        copy.wait()


def backward(n, n_tp, rows, gain, own_gain, tables, cosine, sine, arrays, weights):
    total, width = arrays[1].shape
    mine = arrays[5].shape[0]
    units, hk, hv = arrays[0].shape[1], arrays[7].shape[1], arrays[9].shape[1]
    heads = tables[2].shape[0]
    window = tables[0].shape[0]
    micro = total // window
    tall = max(units, hv, hk)
    hops = 4 * (n - 1)
    count = len(bits_of(n_tp))
    shape = jax.ShapeDtypeStruct
    dma = pltpu.SemaphoreType.DMA
    sizes = (units, units, units, hv, hv, hv, hk, hk)
    return pl.pallas_call(
        functools.partial(backward_kernel, n, n_tp),
        out_shape=tuple(shape((s, BLOCK), F32) for s in sizes)
        + (shape((8, BLOCK), F32), shape((micro, rows, width), F32)),
        in_specs=[vmem()] * 7 + [anyspec()] * 22,
        out_specs=(anyspec(),) * 8 + (vmem(), anyspec()),
        scratch_shapes=[
            pltpu.VMEM((total, width), BF),
            pltpu.VMEM((n, tall, BLOCK), BF),
            pltpu.VMEM((total, units), BF),
            pltpu.VMEM((total, units), BF),
            pltpu.VMEM((total, units), BF),
            pltpu.VMEM((total, width), BF),
            pltpu.VMEM((2, units, BLOCK), BF),
            pltpu.VMEM((2, units, BLOCK), BF),
            pltpu.VMEM((mine, width), F32),
            pltpu.VMEM((mine, width), F32),
            pltpu.VMEM((total, hk), BF),
            pltpu.VMEM((total, hk), BF),
            pltpu.VMEM((total, hv), BF),
            pltpu.VMEM((total, hv), F32),
            pltpu.VMEM((total, hv), BF),
            pltpu.VMEM((window, HV), F32),
            pltpu.VMEM((heads, window, window), F32),
            pltpu.VMEM((window, HK), F32),
            pltpu.VMEM((window, HV), F32),
            pltpu.VMEM((total, width), BF),
            pltpu.VMEM((mine, width), F32),
            pltpu.VMEM((n_tp - 1, mine, width), BF),
            pltpu.VMEM((total, width), BF),
            pltpu.VMEM((micro, rows, width), F32),
            pltpu.VMEM((tall, BLOCK), F32),
            pltpu.VMEM((tall, BLOCK), F32),
            pltpu.VMEM((tall, BLOCK), F32),
            pltpu.VMEM((2, tall, BLOCK), BF),
            pltpu.VMEM((2, tall, BLOCK), BF),
            pltpu.VMEM((2, tall, BLOCK), BF),
            pltpu.VMEM((2, tall, BLOCK), BF),
            pltpu.VMEM((2, tall, BLOCK), F32),
            pltpu.VMEM((2, tall, BLOCK), BF),
            pltpu.VMEM((2 * count + 1, 8, BLOCK), F32),
        ]
        + [dma((hops, 2))] * 4
        + [pltpu.SemaphoreType.REGULAR((2, 2))]
        + [dma((n_tp - 1, micro))] * 4
        + [dma((micro, n_tp))] * 2
        + [dma((count,))] * 2
        + [dma((4, 4)), dma((2,)), dma((2,)), dma((12,))],
        compiler_params=pltpu.CompilerParams(
            collective_id=2, has_side_effects=True, vmem_limit_bytes=67_000_000
        ),
        cost_estimate=pl.CostEstimate(
            flops=4 * total * width * sum(sizes), bytes_accessed=120_000_000, transcendentals=0
        ),
        name="backward_kernel",
    )(gain, own_gain, *tables, cosine, sine, *arrays, *weights)


def finish_kernel(
    n,
    n_tp,
    passed,
    turned,
    *refs,
):
    sources = refs[: passed + turned]
    middle_ref, near_ref, far_ref = refs[passed + turned : passed + turned + 3]
    targets = refs[passed + turned + 3 : 2 * (passed + turned) + 3]
    block_out = refs[2 * (passed + turned) + 3]
    scratch = refs[2 * (passed + turned) + 4 :]
    held, (middle_v, near_v, far_v, block_v), (sem_in, sem_out) = (
        scratch[: passed + 2 * turned],
        scratch[passed + 2 * turned : passed + 2 * turned + 4],
        scratch[passed + 2 * turned + 4 :],
    )
    micro, rows, width = block_v.shape
    pos = ring_position(lax.axis_index("dp"), n)
    count = passed + turned
    ins = [
        pltpu.make_async_copy(sources[i], held[i], sem_in.at[i]) for i in range(count)
    ] + [
        pltpu.make_async_copy(source, target, sem_in.at[count + i])
        for i, (source, target) in enumerate(
            ((middle_ref, middle_v), (near_ref, near_v), (far_ref, far_v))
        )
    ]
    for copy in ins[count:] + ins[:count]:
        copy.start()
    results = list(held[:passed]) + list(held[count:])
    outs = [pltpu.make_async_copy(results[i], targets[i], sem_out.at[i]) for i in range(count)]
    outs.append(pltpu.make_async_copy(block_v, block_out, sem_out.at[count]))
    for copy in ins[count:]:
        copy.wait()

    @pl.loop(0, micro * rows // STEP)
    def _(r):
        at = pl.multiple_of(r * STEP, STEP)
        m, inner = at // rows, pl.multiple_of(at % rows, STEP)
        here = pl.ds(at, STEP)
        for i in range(n):
            for side in range(2):
                lanes = pl.ds(i * BLOCK + side * LANE, LANE)
                spot = ring_index((pos + (n - i if side == 0 else i)) % n, n)
                there = pl.ds(pl.multiple_of(spot * BLOCK + side * LANE, LANE), LANE)
                block_v[m, pl.ds(inner, STEP), there] = middle_v[here, lanes] + (
                    near_v[here, lanes] + far_v[here, lanes].astype(F32)
                )

    outs[count].start()
    for i in range(passed):
        ins[i].wait()
        outs[i].start()
    for i in range(turned):
        ins[passed + i].wait()
        held[count + i][...] = held[passed + i][...].T
        outs[passed + i].start()
    for copy in outs:
        copy.wait()


def finish(n, n_tp, passed, turned, middle, near, far, block_shape):
    shape = jax.ShapeDtypeStruct
    results = tuple(shape(a.shape, a.dtype) for a in passed) + tuple(
        shape(a.shape[::-1], a.dtype) for a in turned
    )
    count = len(passed) + len(turned)
    return pl.pallas_call(
        functools.partial(finish_kernel, n, n_tp, len(passed), len(turned)),
        out_shape=results + (shape(block_shape, F32),),
        in_specs=[anyspec()] * (count + 3),
        out_specs=(anyspec(),) * (count + 1),
        scratch_shapes=[pltpu.VMEM(a.shape, a.dtype) for a in passed]
        + [pltpu.VMEM(a.shape, a.dtype) for a in turned]
        + [pltpu.VMEM(a.shape[::-1], a.dtype) for a in turned]
        + [
            pltpu.VMEM(middle.shape, F32),
            pltpu.VMEM(near.shape, F32),
            pltpu.VMEM(far.shape, BF),
            pltpu.VMEM(block_shape, F32),
            pltpu.SemaphoreType.DMA((count + 3,)),
            pltpu.SemaphoreType.DMA((count + 1,)),
        ],
        compiler_params=pltpu.CompilerParams(vmem_limit_bytes=66_000_000),
        name="finish_kernel",
    )(*passed, *turned, middle, near, far)


def normalize(row_block, gain_vec):
    row_scale = lax.rsqrt(jnp.mean(row_block * row_block, axis=-1, keepdims=True) + EPS)
    return (row_block * row_scale * gain_vec.astype(jnp.float32), row_scale)


def norm_back(grad_rows, row_block, row_scale, gain_vec):
    scaled_grad = grad_rows * gain_vec.astype(jnp.float32)
    back_rows = row_scale * (
        scaled_grad
        - row_block
        * row_scale
        * row_scale
        * jnp.mean(scaled_grad * row_block, axis=-1, keepdims=True)
    )
    return (back_rows, jnp.sum(grad_rows * row_block * row_scale, axis=0))


def angles(length, feature_width):
    half_width = feature_width // 2
    frequency = jnp.exp(-math.log(10000.0) * jnp.arange(half_width, dtype=jnp.float32) / half_width)
    turns = jnp.arange(length, dtype=jnp.float32)[:, None] * frequency[None, :]
    return (jnp.cos(turns)[:, None, :], jnp.sin(turns)[:, None, :])


def decays(length, head_ids):
    places = jnp.arange(length, dtype=jnp.float32)
    spacing = places[:, None] - places[None, :]
    log_rate = jnp.log(1.0 - jnp.exp2(-5.0 - head_ids))
    return jnp.where(
        spacing[None] >= 0.0,
        jnp.exp(jnp.maximum(spacing, 0.0)[None] * log_rate[:, None, None]),
        0.0,
    )


def rotate(value_vectors, cosine_table, sine_table):
    half_width = value_vectors.shape[-1] // 2
    lower = value_vectors[..., :half_width]
    upper = value_vectors[..., half_width:]
    return jnp.concatenate(
        [lower * cosine_table - upper * sine_table, upper * cosine_table + lower * sine_table],
        axis=-1,
    )


def unrotate(value_vectors, cosine_table, sine_table):
    half_width = value_vectors.shape[-1] // 2
    lower = value_vectors[..., :half_width]
    upper = value_vectors[..., half_width:]
    return jnp.concatenate(
        [lower * cosine_table + upper * sine_table, upper * cosine_table - lower * sine_table],
        axis=-1,
    )


def plain_gelu_parts(pre_act):
    normal_cdf = 0.5 * (1.0 + lax.erf(pre_act * (1.0 / math.sqrt(2.0))))
    density = jnp.exp(-0.5 * pre_act * pre_act) * (1.0 / math.sqrt(2.0 * math.pi))
    return (pre_act * normal_cdf, normal_cdf + pre_act * density)


def inner_rows(left_rows, right_rows):
    return lax.dot_general(
        left_rows, right_rows, (((0,), (0,)), ((), ())), preferred_element_type=jnp.float32
    )


def times_t(left_rows, right_rows):
    return lax.dot_general(
        left_rows, right_rows, (((1,), (1,)), ((), ())), preferred_element_type=jnp.float32
    )


def forward_pass(rows_in, gathered, cosine_table, sine_table, decay_mask):
    (
        first_gain,
        second_gain,
        query_weight,
        key_weight,
        value_weight,
        swish_weight,
        output_weight,
        up_projection_matrix,
        gelu_weight,
        down_weight,
    ) = gathered
    local_heads = decay_mask.shape[0]
    scale_qk = 1.0 / math.sqrt(HK)
    normed, first_scale = normalize(rows_in, first_gain)
    normed_all = lax.all_gather(normed.astype(jnp.bfloat16), "tensor", axis=0, tiled=True)
    total_rows = normed_all.shape[0]
    sequences = total_rows // LEN
    query_turned_rows = rotate(
        jnp.dot(normed_all, query_weight, preferred_element_type=jnp.float32).reshape(
            sequences, LEN, local_heads, HK
        ),
        cosine_table,
        sine_table,
    ).astype(jnp.bfloat16)
    key_turned_rows = rotate(
        jnp.dot(normed_all, key_weight, preferred_element_type=jnp.float32).reshape(
            sequences, LEN, local_heads, HK
        ),
        cosine_table,
        sine_table,
    ).astype(jnp.bfloat16)
    value_rows = (
        jnp.dot(normed_all, value_weight, preferred_element_type=jnp.float32)
        .astype(jnp.bfloat16)
        .reshape(sequences, LEN, local_heads, HV)
    )
    gate_pre = jnp.dot(normed_all, swish_weight, preferred_element_type=jnp.float32)
    unscaled_logits = jnp.einsum(
        "snhd,smhd->shnm", query_turned_rows, key_turned_rows, preferred_element_type=jnp.float32
    )
    weight_bf = (unscaled_logits * (decay_mask * scale_qk)).astype(jnp.bfloat16)
    retained = jnp.einsum(
        "shnm,smhe->snhe", weight_bf, value_rows, preferred_element_type=jnp.float32
    )
    group_scale = lax.rsqrt(jnp.mean(retained * retained, axis=-1, keepdims=True) + GROUP_EPS)
    grouped = (retained * group_scale).reshape(total_rows, local_heads * HV)
    sigmoid_gate = jax.nn.sigmoid(gate_pre)
    swish_val = gate_pre * sigmoid_gate
    gated_rows = (swish_val * grouped).astype(jnp.bfloat16)
    attention = lax.psum_scatter(
        jnp.dot(gated_rows, output_weight, preferred_element_type=jnp.float32),
        "tensor",
        scatter_dimension=0,
        tiled=True,
    )
    middle = rows_in + attention
    second, second_scale = normalize(middle, second_gain)
    second_all = lax.all_gather(second.astype(jnp.bfloat16), "tensor", axis=0, tiled=True)
    up_pre = jnp.dot(second_all, up_projection_matrix, preferred_element_type=jnp.float32)
    gelu_pre = jnp.dot(second_all, gelu_weight, preferred_element_type=jnp.float32)
    gelu_val, gelu_slope = plain_gelu_parts(gelu_pre)
    hidden = (gelu_val * up_pre).astype(jnp.bfloat16)
    block_rows = middle + lax.psum_scatter(
        jnp.dot(hidden, down_weight, preferred_element_type=jnp.float32).astype(jnp.bfloat16),
        "tensor",
        scatter_dimension=0,
        tiled=True,
    ).astype(jnp.float32)
    kept_state = (
        rows_in,
        first_scale,
        normed_all,
        query_turned_rows,
        key_turned_rows,
        value_rows,
        gate_pre,
        weight_bf,
        retained,
        group_scale,
        grouped,
        gated_rows,
        middle,
        second_scale,
        second_all,
        up_pre,
        gelu_val,
        gelu_slope,
        hidden,
    )
    return (block_rows, kept_state)


def backward_pass(kept_state, cot_in, gathered, cosine_table, sine_table, decay_mask):
    (
        first_gain,
        second_gain,
        query_weight,
        key_weight,
        value_weight,
        swish_weight,
        output_weight,
        up_projection_matrix,
        gelu_weight,
        down_weight,
    ) = gathered
    (
        rows_in,
        first_scale,
        normed_all,
        query_turned_rows,
        key_turned_rows,
        value_rows,
        gate_pre,
        weight_bf,
        retained,
        group_scale,
        grouped,
        gated_rows,
        middle,
        second_scale,
        second_all,
        up_pre,
        gelu_val,
        gelu_slope,
        hidden,
    ) = kept_state
    local_heads = decay_mask.shape[0]
    total_rows = normed_all.shape[0]
    scale_qk = 1.0 / math.sqrt(HK)
    cot_all = lax.all_gather(cot_in.astype(jnp.bfloat16), "tensor", axis=0, tiled=True)
    grad_hidden = times_t(cot_all, down_weight)
    grad_down = inner_rows(hidden, cot_all)
    grad_uppre = (grad_hidden * gelu_val).astype(jnp.bfloat16)
    grad_gelupre = (grad_hidden * up_pre * gelu_slope).astype(jnp.bfloat16)
    grad_up = inner_rows(second_all, grad_uppre)
    grad_gelu = inner_rows(second_all, grad_gelupre)
    second_back = lax.psum_scatter(
        times_t(grad_uppre, up_projection_matrix) + times_t(grad_gelupre, gelu_weight),
        "tensor",
        scatter_dimension=0,
        tiled=True,
    )
    middle_back, grad_gain_two = norm_back(second_back, middle, second_scale, second_gain)
    grad_middle = cot_in + middle_back
    middle_all = lax.all_gather(grad_middle.astype(jnp.bfloat16), "tensor", axis=0, tiled=True)
    grad_gated = times_t(middle_all, output_weight)
    grad_out = inner_rows(gated_rows, middle_all)
    sigmoid_gate = jax.nn.sigmoid(gate_pre)
    swish_val = gate_pre * sigmoid_gate
    grad_swishpre = (
        grad_gated * grouped * (sigmoid_gate * (1.0 + gate_pre * (1.0 - sigmoid_gate)))
    ).astype(jnp.bfloat16)
    grad_grouped = (grad_gated * swish_val).reshape(retained.shape)
    grad_retained = (
        group_scale
        * (
            grad_grouped
            - retained
            * group_scale
            * group_scale
            * jnp.mean(grad_grouped * retained, axis=-1, keepdims=True)
        )
    ).astype(jnp.bfloat16)
    grad_valrows = jnp.einsum(
        "shnm,snhe->smhe", weight_bf, grad_retained, preferred_element_type=jnp.float32
    ).astype(jnp.bfloat16)
    grad_weight = jnp.einsum(
        "snhe,smhe->shnm", grad_retained, value_rows, preferred_element_type=jnp.float32
    )
    grad_retention_logits = (grad_weight * (decay_mask * scale_qk)).astype(jnp.bfloat16)
    grad_query_rotated_rows = jnp.einsum(
        "shnm,smhd->snhd",
        grad_retention_logits,
        key_turned_rows,
        preferred_element_type=jnp.float32,
    )
    grad_key_rotated_rows = jnp.einsum(
        "shnm,snhd->smhd",
        grad_retention_logits,
        query_turned_rows,
        preferred_element_type=jnp.float32,
    )
    grad_qpre = (
        unrotate(grad_query_rotated_rows, cosine_table, sine_table)
        .astype(jnp.bfloat16)
        .reshape(total_rows, local_heads * HK)
    )
    grad_kpre = (
        unrotate(grad_key_rotated_rows, cosine_table, sine_table)
        .astype(jnp.bfloat16)
        .reshape(total_rows, local_heads * HK)
    )
    grad_vflat = grad_valrows.reshape(total_rows, local_heads * HV)
    first_back = lax.psum_scatter(
        times_t(grad_qpre, query_weight)
        + times_t(grad_kpre, key_weight)
        + times_t(grad_vflat, value_weight)
        + times_t(grad_swishpre, swish_weight),
        "tensor",
        scatter_dimension=0,
        tiled=True,
    )
    grad_query = inner_rows(normed_all, grad_qpre)
    grad_key = inner_rows(normed_all, grad_kpre)
    grad_value = inner_rows(normed_all, grad_vflat)
    grad_swish = inner_rows(normed_all, grad_swishpre)
    input_back, grad_gain_one = norm_back(first_back, rows_in, first_scale, first_gain)
    grad_rows = grad_middle + input_back
    pieces = (
        grad_gain_one,
        grad_gain_two,
        grad_query,
        grad_key,
        grad_value,
        grad_swish,
        grad_out,
        grad_up,
        grad_gelu,
        grad_down,
    )
    return (grad_rows, pieces)


def plain_body(
    block_input,
    cotangent,
    first_gain,
    second_gain,
    query_weight,
    key_weight,
    value_weight,
    swish_weight,
    output_weight,
    up_projection_matrix,
    gelu_weight,
    down_weight,
):
    local_heads = query_weight.shape[1] // HK
    head_ids = (lax.axis_index("tensor") * local_heads + jnp.arange(local_heads)).astype(
        jnp.float32
    )
    cosine_table, sine_table = angles(LEN, HK)
    decay_mask = decays(LEN, head_ids)
    output_list = []
    grad_list = []
    totals = ()
    for micro_idx in range(block_input.shape[0]):
        forward_set = (
            lax.all_gather(first_gain, "dp", axis=0, tiled=True),
            lax.all_gather(second_gain, "dp", axis=0, tiled=True),
            lax.all_gather(query_weight, "dp", axis=0, tiled=True),
            lax.all_gather(key_weight, "dp", axis=0, tiled=True),
            lax.all_gather(value_weight, "dp", axis=0, tiled=True),
            lax.all_gather(swish_weight, "dp", axis=0, tiled=True),
            lax.all_gather(output_weight, "dp", axis=1, tiled=True),
            lax.all_gather(up_projection_matrix, "dp", axis=0, tiled=True),
            lax.all_gather(gelu_weight, "dp", axis=0, tiled=True),
            lax.all_gather(down_weight, "dp", axis=1, tiled=True),
        )
        block_rows, kept_state = forward_pass(
            block_input[micro_idx], forward_set, cosine_table, sine_table, decay_mask
        )
        held = lax.optimization_barrier(
            (
                (
                    first_gain,
                    second_gain,
                    query_weight,
                    key_weight,
                    value_weight,
                    swish_weight,
                    output_weight,
                    up_projection_matrix,
                    gelu_weight,
                    down_weight,
                ),
                block_rows,
            )
        )[0]
        backward_set = (
            lax.all_gather(held[0], "dp", axis=0, tiled=True),
            lax.all_gather(held[1], "dp", axis=0, tiled=True),
            lax.all_gather(held[2], "dp", axis=0, tiled=True),
            lax.all_gather(held[3], "dp", axis=0, tiled=True),
            lax.all_gather(held[4], "dp", axis=0, tiled=True),
            lax.all_gather(held[5], "dp", axis=0, tiled=True),
            lax.all_gather(held[6], "dp", axis=1, tiled=True),
            lax.all_gather(held[7], "dp", axis=0, tiled=True),
            lax.all_gather(held[8], "dp", axis=0, tiled=True),
            lax.all_gather(held[9], "dp", axis=1, tiled=True),
        )
        grad_rows, pieces = backward_pass(
            kept_state, cotangent[micro_idx], backward_set, cosine_table, sine_table, decay_mask
        )
        output_list.append(block_rows)
        grad_list.append(grad_rows)
        if micro_idx == 0:
            totals = tuple(pieces)
        else:
            totals = tuple((total + piece for total, piece in zip(totals, pieces)))
    totals = (
        lax.psum_scatter(totals[0], "dp", scatter_dimension=0, tiled=True),
        lax.psum_scatter(totals[1], "dp", scatter_dimension=0, tiled=True),
        lax.psum_scatter(totals[2], "dp", scatter_dimension=0, tiled=True),
        lax.psum_scatter(totals[3], "dp", scatter_dimension=0, tiled=True),
        lax.psum_scatter(totals[4], "dp", scatter_dimension=0, tiled=True),
        lax.psum_scatter(totals[5], "dp", scatter_dimension=0, tiled=True),
        lax.psum_scatter(totals[6], "dp", scatter_dimension=1, tiled=True),
        lax.psum_scatter(totals[7], "dp", scatter_dimension=0, tiled=True),
        lax.psum_scatter(totals[8], "dp", scatter_dimension=0, tiled=True),
        lax.psum_scatter(totals[9], "dp", scatter_dimension=1, tiled=True),
    )
    gain_first, gain_second = lax.psum((totals[0], totals[1]), "tensor")
    return (
        jnp.stack(output_list, axis=0),
        jnp.stack(grad_list, axis=0),
        gain_first,
        gain_second,
        totals[2],
        totals[3],
        totals[4],
        totals[5],
        totals[6],
        totals[7],
        totals[8],
        totals[9],
    )


def ring_body(
    n_dp,
    n_tp,
    block_input,
    cotangent,
    first_gain,
    second_gain,
    query_weight,
    key_weight,
    value_weight,
    swish_weight,
    output_weight,
    up_projection_matrix,
    gelu_weight,
    down_weight,
):
    micro, rows, width = block_input.shape
    local_heads = query_weight.shape[1] // HK
    window = n_tp * rows

    me = lax.axis_index("tensor")
    head_ids = (me * local_heads + jnp.arange(local_heads)).astype(F32)
    chunk_of = jnp.arange(n_tp) ^ me
    natural = (chunk_of[:, None] * rows + jnp.arange(rows)[None, :]).reshape(window)
    place = (natural % LEN).astype(F32)
    half_key = HK // 2
    frequency = jnp.exp(-math.log(10000.0) * jnp.arange(half_key, dtype=F32) / half_key)
    turns = place[:, None] * frequency[None, :]
    cosine, sine = jnp.cos(turns), jnp.sin(turns)
    log_rate = jnp.log(1.0 - jnp.exp2(-5.0 - head_ids))
    spots = natural.astype(F32)
    tables = (
        jnp.broadcast_to(spots[:, None], (window, LANE)),
        spots[None, :],
        jnp.broadcast_to(log_rate[:, None], (local_heads, window)),
    )

    gains_own = jnp.stack([first_gain, second_gain]).astype(F32)
    results = forward(
        n_dp,
        n_tp,
        block_input,
        cotangent,
        gains_own,
        cosine,
        sine,
        tables,
        (
            query_weight.T,
            key_weight.T,
            value_weight.T,
            swish_weight.T,
            output_weight,
            up_projection_matrix.T,
            gelu_weight.T,
            down_weight,
        ),
    )
    query, key, value, gate, x_rel, cot_rel, gains, normed, cot_all = results[:9]
    w_in, (w_o, w_u, w_l, w_d) = results[9:13], results[13:17]
    gated, middle, second, hidden, gelu_val, up_slope, near, far = results[17:]

    far = lax.ppermute(far, "tensor", [(i, i ^ (n_tp // 2)) for i in range(n_tp)])

    (
        grad_down,
        grad_up,
        grad_gelu,
        grad_out,
        grad_swish,
        grad_value,
        grad_query,
        grad_key,
        gain_grads,
        grad_rows,
    ) = backward(
        n_dp,
        n_tp,
        rows,
        gains,
        jnp.pad(gains_own, ((0, 6), (0, 0)), constant_values=1.0),
        tables,
        cosine,
        sine,
        (
            hidden,
            cot_all,
            gelu_val,
            up_slope,
            second,
            middle,
            cot_rel,
            query,
            key,
            value,
            gate,
            gated,
            normed,
            x_rel,
        ),
        (*w_in, w_o, w_u, w_l, w_d),
    )
    passed = (grad_value, grad_swish, grad_out, grad_up, grad_gelu, grad_down, grad_rows)
    *passed, grad_query, grad_key, block_rows = finish(
        n_dp, n_tp, passed, (grad_query, grad_key), middle, near, far, block_input.shape
    )
    grad_value, grad_swish, grad_out, grad_up, grad_gelu, grad_down, grad_rows = passed

    return (
        block_rows,
        grad_rows,
        gain_grads[0],
        gain_grads[1],
        grad_query,
        grad_key,
        grad_value.T,
        grad_swish.T,
        grad_out,
        grad_up.T,
        grad_gelu.T,
        grad_down,
    )


def solution(mesh):
    rows = P(None, ("dp", "tensor"), None)
    wide, tall, gain = P("dp", "tensor"), P("tensor", "dp"), P("dp")
    n_dp, n_tp = mesh.shape["dp"], mesh.shape["tensor"]

    def run(*arrays):
        blocks = arrays[2].shape[0] == BLOCK and n_dp % 2 == 0 and n_dp > 2
        pairs = n_tp > 1 and n_tp & (n_tp - 1) == 0
        aligned = (n_tp * arrays[0].shape[1]) % LEN == 0 and arrays[0].shape[1] % LANE == 0
        equal = arrays[6].shape[1] == arrays[9].shape[1]
        if blocks and pairs and aligned and equal:
            return ring_body(n_dp, n_tp, *arrays)
        return plain_body(*arrays)

    return jax.shard_map(
        run,
        mesh=mesh,
        in_specs=(rows, rows, gain, gain) + (wide,) * 4 + (tall, wide, wide, tall),
        out_specs=(rows, rows, gain, gain) + (wide,) * 4 + (tall, wide, wide, tall),
        check_vma=False,
    )
```

```python
import functools
import math

import jax
import jax.numpy as jnp
from jax import lax
from jax.experimental import pallas as pl
from jax.experimental.pallas import tpu as pltpu
from jax.sharding import PartitionSpec as P

HK = 256
HV = 432
LEN = 512
EPS = 1e-05
GROUP_EPS = 1.0
BF = jnp.bfloat16
F32 = jnp.float32
MESH = pl.DeviceIdType.MESH
LANE = 128
BLOCK = 2 * LANE
SLOTS = 3
STEP = 32
SPLIT = 2


def ring_position(index, count):
    low = index // 2
    return low + (index % 2) * (count - 1 - 2 * low)


def ring_index(position, count):
    high = position // (count // 2)
    return (1 - high) * (2 * position) + high * (2 * (count - 1 - position) + 1)


def bits_of(count):
    return [1 << i for i in range(count.bit_length() - 1)]


def anyspec():
    return pl.BlockSpec(memory_space=pl.ANY)


def vmem():
    return pl.BlockSpec(memory_space=pltpu.VMEM)


def nt(left, right):
    return lax.dot_general(left, right, (((1,), (1,)), ((), ())), preferred_element_type=F32)


def nn(left, right):
    return lax.dot_general(left, right, (((1,), (0,)), ((), ())), preferred_element_type=F32)


def tn(left, right):
    return lax.dot_general(left, right, (((0,), (0,)), ((), ())), preferred_element_type=F32)


def partner(tp, bit):
    return tp + bit - 2 * bit * ((tp // bit) % 2)


def neighbours(n):
    dp, tp = lax.axis_index("dp"), lax.axis_index("tensor")
    pos = ring_position(dp, n)
    return dp, tp, ring_index((pos + 1) % n, n), ring_index((pos + n - 1) % n, n)


def greet(devices):
    barrier = pltpu.get_barrier_semaphore()
    for device in devices:
        pl.semaphore_signal(barrier, inc=1, device_id=device, device_id_type=MESH)
    pl.semaphore_wait(barrier, len(devices))


class Share:
    def __init__(self, dp, tp, n_tp, micro, rows, buf, send, recv):
        self.dp, self.tp, self.n_tp, self.micro, self.rows = dp, tp, n_tp, micro, rows
        self.buf, self.send, self.recv = buf, send, recv
        self.bits = bits_of(n_tp)[::-1]

    def copies(self, bit, m, keys=None):
        window = self.n_tp * self.rows
        for key in range(0, self.n_tp, 2 * bit):
            if keys is None or (key == 0) == keys:
                yield pltpu.make_async_remote_copy(
                    src_ref=self.buf.at[pl.ds(m * window + key * self.rows, self.rows)],
                    dst_ref=self.buf.at[pl.ds(m * window + (key ^ bit) * self.rows, self.rows)],
                    send_sem=self.send.at[m, key ^ bit],
                    recv_sem=self.recv.at[m, key ^ bit],
                    device_id=(self.dp, partner(self.tp, bit)),
                    device_id_type=MESH,
                )

    def begin(self, m):
        for bit in self.bits:
            for copy in self.copies(bit, m, True):
                copy.start()

    def relay(self, m):
        for bit in self.bits:
            for copy in self.copies(bit, m, False):
                copy.start()
            for copy in self.copies(bit, m):
                copy.wait_recv()

    def finish(self):
        for m in range(self.micro):
            for bit in self.bits:
                for copy in self.copies(bit, m):
                    copy.wait_send()


class Collect:
    def __init__(self, dp, tp, n_tp, micro, rows, back, got, own, send, recv):
        self.dp, self.tp, self.n_tp, self.micro, self.rows = dp, tp, n_tp, micro, rows
        self.back, self.got, self.own, self.send, self.recv = back, got, own, send, recv
        self.bits = bits_of(n_tp)

    def keys(self, bit):
        return [key for key in range(0, self.n_tp, bit) if key & bit]

    def copies(self, bit, m):
        window = self.n_tp * self.rows
        for key in self.keys(bit):
            yield pltpu.make_async_remote_copy(
                src_ref=self.back.at[pl.ds(m * window + key * self.rows, self.rows)],
                dst_ref=self.got.at[key - 1, pl.ds(m * self.rows, self.rows)],
                send_sem=self.send.at[key - 1, m],
                recv_sem=self.recv.at[key - 1, m],
                device_id=(self.dp, partner(self.tp, bit)),
                device_id_type=MESH,
            )

    def start(self, bit, m):
        for copy in self.copies(bit, m):
            copy.start()

    def add(self, bit, m):
        window = self.n_tp * self.rows
        for copy in self.copies(bit, m):
            copy.wait_recv()
        for key in self.keys(bit):
            target = key ^ bit

            @pl.loop(0, self.rows // STEP)
            def _(r):
                inner = pl.multiple_of(r * STEP, STEP)
                here = pl.ds(pl.multiple_of(m * self.rows + inner, STEP), STEP)
                there = pl.ds(pl.multiple_of(m * window + target * self.rows + inner, STEP), STEP)
                got = self.got[key - 1, here, :].astype(F32)
                if target == 0:
                    held = self.back[there, :].astype(F32) if bit == 1 else self.own[here, :]
                    self.own[here, :] = held + got
                else:
                    self.back[there, :] = (self.back[there, :].astype(F32) + got).astype(BF)

    def finish(self, bits=None):
        for m in range(self.micro):
            for bit in self.bits if bits is None else bits:
                for copy in self.copies(bit, m):
                    copy.wait_send()


def fill_decay(decay_v, col_ref, row_ref, rate_ref):
    heads, window, _ = decay_v.shape
    scale_qk = 1.0 / math.sqrt(HK)
    for h in range(heads):

        @pl.loop(0, window // LANE)
        def _(r):
            here = pl.ds(pl.multiple_of(r * LANE, LANE), LANE)
            col, row = col_ref[here, 0:1], row_ref[...]
            spacing = col - row
            same = jnp.floor(col * (1.0 / LEN)) == jnp.floor(row * (1.0 / LEN))
            kept = jnp.exp(jnp.maximum(spacing, 0.0) * rate_ref[h : h + 1, :]) * scale_qk
            decay_v[h, here, :] = jnp.where((spacing >= 0.0) & same, kept, 0.0)


def gelu_parts(pre_act):
    normal_cdf = 0.5 * (1.0 + lax.erf(pre_act * (1.0 / math.sqrt(2.0))))
    density = jnp.exp(-0.5 * pre_act * pre_act) * (1.0 / math.sqrt(2.0 * math.pi))
    return (pre_act * normal_cdf, normal_cdf + pre_act * density)


def forward_kernel(
    n,
    n_tp,
    x_ref,
    cot_ref,
    gains_ref,
    cos_ref,
    sin_ref,
    col_ref,
    row_ref,
    rate_ref,
    *refs,
):
    shards, refs = refs[:8], refs[8:]
    q_out, k_out, v_out, g_out, xr_out, cr_out, gain_out, nall_out, call_out = refs[:9]
    whole_outs, refs = refs[9:17], refs[17:]
    gated_out, middle_out, second_out, hidden_out, value_out, slope_out, near_out, far_out = refs[:8]
    nall_v, row_v, cot_v, gain_v, q_v, k_v, v_v, g_v, decay_v, got_v = refs[8:18]
    held, refs = refs[18:22], refs[22:]
    x_v, q_acc, k_acc, v_acc, wq_s, wk_s, wv_s, wg_s = refs[:8]
    back_v, own_v, gated_v, hidden_v, value_v, slope_v, up_v = refs[8:15]
    refs = refs[15:]
    ring_send, ring_recv, gain_send, gain_recv = refs[:4]
    first_send, first_recv, cot_send, cot_recv, share_send, share_recv = refs[4:10]
    part_send, part_recv, last_send, last_recv, load_sem, local_sem, out_sem = refs[10:]

    micro, rows, width = x_ref.shape
    window = n_tp * rows
    total, mine = micro * window, micro * rows
    dp, tp, cw, ccw = neighbours(n)
    pos = ring_position(dp, n)
    bits = bits_of(n_tp)
    heads = decay_v.shape[0]
    tile = 256
    half = HK // 2
    greet(
        [(ring_index((pos + k) % n, n), tp) for k in range(1, n)]
        + [(dp, partner(tp, bit)) for bit in bits]
    )

    wholes = tuple(whole_outs[:4]) + tuple(held)
    slots = (wq_s, wk_s, wv_s, wg_s)
    pieces = [(a, 0, slots[a].shape[1]) for a in range(4)]
    groups = [(0, 1, 2, 3)]
    for pair in ((4,), (5, 6), (7,)):
        group = []
        for a in pair:
            size = shards[a].shape[0]
            parts = SPLIT if len(pair) == 1 else 1
            cuts = [size * j // parts // 16 * 16 for j in range(parts)] + [size]
            for low, high in zip(cuts, cuts[1:]):
                group.append(len(pieces))
                pieces.append((a, low, high - low))
        groups.append(tuple(group))
    ring_a, ring_b, ring_c, ring_d = groups

    def hop(i, p, side):
        a, low, size = pieces[p]
        span, lanes = pl.ds(low, size), pl.ds(side * LANE, LANE)
        if not (isinstance(i, int) and i == 0):
            source = wholes[a].at[i, span, lanes]
        elif a < 2:
            source = slots[a].at[0, span, lanes]
        else:
            source = shards[a].at[span, lanes]
        return pltpu.make_async_remote_copy(
            src_ref=source,
            dst_ref=wholes[a].at[i + 1, span, lanes],
            send_sem=ring_send.at[i, p, side],
            recv_sem=ring_recv.at[i, p, side],
            device_id=((cw, ccw)[side], tp),
            device_id_type=MESH,
        )

    def ring_start(group):
        for p in group:
            for side in range(2):
                hop(0, p, side).start()

    def ring_pass(s, p):
        for side in range(2):
            hop(s - 1, p, side).wait_recv()
            if isinstance(s, int):
                if s < n - 1:
                    hop(s, p, side).start()
            else:

                @pl.when(s < n - 1)
                def _():
                    hop(s, p, side).start()

    def ring_step(s, group, following=()):
        for p in group:
            ring_pass(s, p)
        if isinstance(s, int) and s == n - 2:
            ring_start(following)

    def store(source, target):
        copy = pltpu.make_async_copy(source, target, out_sem.at[len(stores)])
        copy.start()
        stores.append(copy)

    stores = []
    turned = [
        pltpu.make_async_copy(shards[a], (q_v, k_v)[a].at[pl.ds(0, BLOCK)], local_sem.at[2 + a])
        for a in range(2)
    ]
    for copy in turned:
        copy.start()
    ring_start(ring_a[2:])
    for a in range(2):
        turned[a].wait()
        natural_block = (q_v, k_v)[a][pl.ds(0, BLOCK), :]
        slots[a][0] = natural_block.astype(F32).T.astype(BF)
        ring_start(ring_a[a : a + 1])
    own_blocks = [
        pltpu.make_async_copy(shards[4 + i], held[i].at[0], local_sem.at[4 + i]) for i in range(4)
    ]

    def natural(i, side):
        at = ring_index((pos + (n - i if side == 0 else i)) % n, n) * BLOCK + side * LANE
        return pl.ds(pl.multiple_of(at, LANE), LANE)

    first = Share(dp, tp, n_tp, micro, rows, nall_v, first_send, first_recv)
    share = Share(dp, tp, n_tp, micro, rows, nall_v, share_send, share_recv)

    def cot_copy(bit, m, key):
        source = cot_v.at[pl.ds(m * rows, rows)]
        if key:
            source = call_out.at[pl.ds(m * window + key * rows, rows)]
        return pltpu.make_async_remote_copy(
            src_ref=source,
            dst_ref=call_out.at[pl.ds(m * window + (key ^ bit) * rows, rows)],
            send_sem=cot_send.at[m, key ^ bit],
            recv_sem=cot_recv.at[m, key ^ bit],
            device_id=(dp, partner(tp, bit)),
            device_id_type=MESH,
        )

    def cot_copies(bit, keys=None):
        for m in range(micro):
            for key in range(0, n_tp, 2 * bit):
                if keys is None or (key == 0) == keys:
                    yield cot_copy(bit, m, key)

    def project():
        cot_rel_v = own_v
        accs = (q_acc, k_acc, v_acc, g_v)

        def load(i, a):
            source = shards[a] if i == 0 else wholes[a].at[i]
            return pltpu.make_async_copy(
                source, slots[a].at[i % SLOTS], load_sem.at[i % SLOTS, a]
            )

        x_copy = pltpu.make_async_copy(x_ref, x_v, local_sem.at[0])
        x_copy.start()
        for a in range(2, 4):
            load(0, a).start()

        def gain_copy(k):
            return pltpu.make_async_remote_copy(
                src_ref=gains_ref,
                dst_ref=gain_v.at[k],
                send_sem=gain_send.at[k],
                recv_sem=gain_recv.at[k],
                device_id=(ring_index((pos + k) % n, n), tp),
                device_id_type=MESH,
            )

        own_gain = pltpu.make_async_copy(gains_ref, gain_v.at[0], local_sem.at[1])
        own_gain.start()
        for k in range(1, n):
            gain_copy(k).start()
        own_gain.wait()
        for k in range(1, n):
            gain_copy(k).wait()
        for i in range(n):
            gain_out[:, pl.ds(i * BLOCK, LANE)] = gain_v[i, :, pl.ds(0, LANE)]
            gain_out[:, pl.ds(i * BLOCK + LANE, LANE)] = gain_v[(n - i) % n, :, pl.ds(LANE, LANE)]
        x_copy.wait()

        def each_part(work):
            @pl.loop(0, mine // STEP)
            def _(r):
                at = pl.multiple_of(r * STEP, STEP)
                m, inner = at // rows, pl.multiple_of(at % rows, STEP)
                work(at, m, inner)

        def normalize_part(at, m, inner):
            chunk = x_v[m, pl.ds(inner, STEP), :]
            scale = lax.rsqrt(jnp.mean(chunk * chunk, axis=-1, keepdims=True) + EPS)
            there = pl.ds(pl.multiple_of(m * window + inner, STEP), STEP)
            for i in range(n):
                for side in range(2):
                    lanes = pl.ds(i * BLOCK + side * LANE, LANE)
                    part = x_v[m, pl.ds(inner, STEP), natural(i, side)]
                    row_v[pl.ds(at, STEP), lanes] = part
                    nall_v[there, lanes] = (part * scale * gain_out[0:1, lanes]).astype(BF)

        each_part(normalize_part)
        for m in range(micro):
            first.begin(m)
        store(row_v, xr_out)
        c_copy = pltpu.make_async_copy(cot_ref, x_v, local_sem.at[0])
        c_copy.start()
        cot_rel = pltpu.make_async_copy(cot_rel_v, cr_out, local_sem.at[1])

        def cot_part(at, m, inner):
            for i in range(n):
                for side in range(2):
                    lanes = pl.ds(i * BLOCK + side * LANE, LANE)
                    part = x_v[m, pl.ds(inner, STEP), natural(i, side)]
                    cot_rel_v[pl.ds(at, STEP), lanes] = part
                    cot_v[pl.ds(at, STEP), lanes] = part.astype(BF)

        def take_cot():
            c_copy.wait()
            each_part(cot_part)
            cot_rel.start()
            for m in range(micro):
                store(cot_v.at[pl.ds(m * rows, rows)], call_out.at[pl.ds(m * window, rows)])
            for copy in own_blocks:
                copy.start()

        def product(j, a, last):
            if j > 0 or a > 1:
                load(j, a).wait()
            if j == 0:
                pltpu.make_async_copy(
                    slots[a].at[0], wholes[a].at[0], load_sem.at[SLOTS, a]
                ).start()

            @pl.loop(0, total // tile)
            def _(r):
                at = pl.multiple_of(r * tile, tile)
                here = pl.ds(at, tile)
                part = nt(nall_v[here, pl.ds(j * BLOCK, BLOCK)], slots[a][j % SLOTS])
                if j > 0:
                    part = accs[a][here, :] + part
                if not last or a == 3:
                    accs[a][here, :] = part
                elif a == 2:
                    v_v[here, :] = part.astype(BF)
                else:
                    place = pl.ds(pl.multiple_of(at % window, tile), tile)
                    cosine, sine = cos_ref[place, :], sin_ref[place, :]
                    out = (q_v, k_v)[a]
                    for h in range(heads):
                        low = part[:, h * HK : h * HK + half]
                        high = part[:, h * HK + half : (h + 1) * HK]
                        out[here, pl.ds(h * HK, half)] = (low * cosine - high * sine).astype(BF)
                        out[here, pl.ds(h * HK + half, half)] = (
                            high * cosine + low * sine
                        ).astype(BF)

            if j == 0:
                pltpu.make_async_copy(
                    slots[a].at[0], wholes[a].at[0], load_sem.at[SLOTS, a]
                ).wait()

        start_at, done = 3, 0
        for i in range(n + 1):
            if i == 2:
                take_cot()
                fill_decay(decay_v, col_ref, row_ref, rate_ref)
            if i == start_at:
                for m in range(micro):
                    first.relay(m)
                store(nall_v, nall_out)
                for bit in bits[::-1]:
                    for copy in cot_copies(bit, True):
                        copy.start()
            if i == n - 1:
                for bit in bits[::-1]:
                    for copy in cot_copies(bit, False):
                        copy.start()
                    for copy in cot_copies(bit):
                        copy.wait_recv()
            todo = []
            if i >= start_at:
                goal = min(i - 1, done + 1) if i < n else n - 1
                todo = list(range(done, goal + 1))
                done = goal + 1
            for a in range(4):
                if 0 < i < n:
                    ring_pass(i, a)
                if i == n - 2 and a == 3:
                    ring_start(ring_b)
                for j in todo:
                    product(j, a, j == n - 1)
                if 0 < i < n:
                    if i == SLOTS and a < 2:
                        hop(0, a, 0).wait_send()
                        hop(0, a, 1).wait_send()
                    load(i, a).start()
                if i == n:
                    source, target = ((q_v, q_out), (k_v, k_out), (v_v, v_out), (g_v, g_out))[a]
                    store(source, target)
        cot_rel.wait()

    project()
    wo_v, wu_v, wl_v, wd_v = held
    units = shards[7].shape[0]

    def middle_part():
        for copy in own_blocks:
            copy.wait()

        def attend(m, h):
            keys = pl.ds(h * HK, HK)
            values = pl.ds(h * HV, HV)
            inside = pl.ds(m * window, window)

            @pl.loop(0, window // tile)
            def _(r):
                at = pl.multiple_of(r * tile, tile)
                here = pl.ds(pl.multiple_of(m * window + at, tile), tile)
                scores = nt(q_v[here, keys], k_v[inside, keys])
                weight = (scores * decay_v[h, pl.ds(at, tile), :]).astype(BF)
                kept = nn(weight, v_v[inside, values])
                group = lax.rsqrt(jnp.mean(kept * kept, axis=-1, keepdims=True) + GROUP_EPS)
                gate = g_v[here, values]
                gated_v[here, values] = (gate * jax.nn.sigmoid(gate) * (kept * group)).astype(BF)

        def times_block(left, weights, i):
            @pl.loop(0, total // tile)
            def _(r):
                here = pl.ds(pl.multiple_of(r * tile, tile), tile)
                back_v[here, pl.ds(i * BLOCK, BLOCK)] = nn(left[here, :], weights[i]).astype(BF)

        collect = Collect(dp, tp, n_tp, micro, rows, back_v, got_v, own_v, part_send, part_recv)
        jobs = [(m, h) for m in range(micro) for h in range(heads)]
        reached = 0
        while jobs:
            if reached < n - 1:
                reached += 1
                ring_step(reached, ring_b, ring_c)
            attend(*jobs.pop(0))
        store(gated_v, gated_out)
        ready = 0
        while ready < n:
            if reached < n - 1:
                reached += 1
                ring_step(reached, ring_b, ring_c)
            for _ in range(2 if reached < n - 1 else n):
                if ready < min(n, reached + 1):
                    times_block(gated_v, wo_v, ready)
                    ready += 1
        store(wo_v, whole_outs[4])
        first.finish()
        stores[0].wait()
        stores[micro + 1].wait()
        for m in range(micro):
            collect.start(bits[0], m)
        passed = [0]

        def pairs_to(goal):
            while passed[0] < min(goal, n - 1):
                passed[0] += 1
                ring_step(passed[0], ring_c, ring_d)

        for at, bit in enumerate(bits[:-1]):
            for m in range(micro):
                collect.add(bit, m)
                collect.start(bits[at + 1], m)
        pairs_to(1)
        for m in range(micro):
            pairs_to(2 + m)
            collect.add(bits[-1], m)

            @pl.loop(0, rows // STEP)
            def _(r):
                inner = pl.multiple_of(r * STEP, STEP)
                here = pl.ds(pl.multiple_of(m * rows + inner, STEP), STEP)
                there = pl.ds(pl.multiple_of(m * window + inner, STEP), STEP)
                middle = row_v[here, :] + own_v[here, :]
                row_v[here, :] = middle
                scale = lax.rsqrt(jnp.mean(middle * middle, axis=-1, keepdims=True) + EPS)
                nall_v[there, :] = (middle * scale * gain_out[1:2, :]).astype(BF)

            share.begin(m)
        store(row_v, middle_out)
        pairs_to(4)
        for m in range(micro):
            share.relay(m)
            pairs_to(5 + m)
        pairs_to(n - 1)
        store(nall_v, second_out)
        store(wu_v, whole_outs[5])
        store(wl_v, whole_outs[6])

        def rows_by(weights, here):
            result = None
            for i in range(n):
                term = nt(nall_v[here, pl.ds(i * BLOCK, BLOCK)], weights[i])
                result = term if result is None else result + term
            return result

        tiles = total // tile
        every = max(1, tiles // 2)
        inside_loop = min(tiles // every, n - 1)

        @pl.loop(0, tiles)
        def _(r):
            here = pl.ds(pl.multiple_of(r * tile, tile), tile)
            up_v[...] = rows_by(wu_v, here)
            gelu_val, gelu_slope = gelu_parts(rows_by(wl_v, here))
            up = up_v[...]
            hidden_v[here, :] = (gelu_val * up).astype(BF)
            value_v[here, :] = gelu_val.astype(BF)
            slope_v[here, :] = (up * gelu_slope).astype(BF)

            @pl.when((r % every == every - 1) & (r // every < inside_loop))
            def _():
                ring_step(r // every + 1, ring_d)

        store(hidden_v, hidden_out)
        store(value_v, value_out)
        store(slope_v, slope_out)
        collect.finish()
        ready = 0
        for s in range(inside_loop, n):
            if s > inside_loop:
                ring_step(s, ring_d)
            for _ in range(2 if s < n - 1 else n):
                if ready <= s and ready < n:
                    times_block(hidden_v, wd_v, ready)
                    ready += 1
        store(wd_v, whole_outs[7])
        last = Collect(dp, tp, n_tp, micro, rows, back_v, got_v, own_v, last_send, last_recv)
        for at, bit in enumerate(bits[:-1]):
            for m in range(micro):
                last.start(bit, m)
            for m in range(micro):
                last.add(bit, m)
        store(own_v, near_out)
        for m in range(micro):
            store(
                back_v.at[pl.ds(m * window + bits[-1] * rows, rows)],
                far_out.at[pl.ds(m * rows, rows)],
            )
        last.finish(bits[:-1])
        for i in range(n - 1):
            for p in range(0 if i > 0 else 2, len(pieces)):
                hop(i, p, 0).wait_send()
                hop(i, p, 1).wait_send()
        share.finish()
        for bit in bits:
            for copy in cot_copies(bit):
                copy.wait_send()
        for at, copy in enumerate(stores):
            if at not in waited:
                copy.wait()

    waited = (0, micro + 1)
    middle_part()


def forward(n, n_tp, x, cot, gains, cosine, sine, tables, weights):
    micro, rows, width = x.shape
    window = n_tp * rows
    total, mine = micro * window, micro * rows
    sizes = [w.shape[1] for w in weights[:2]] + [w.shape[0] for w in weights[2:]]
    hv, units = sizes[2], sizes[7]
    shape = jax.ShapeDtypeStruct
    dma = pltpu.SemaphoreType.DMA
    count = 4 + SPLIT + 2 + SPLIT
    return pl.pallas_call(
        functools.partial(forward_kernel, n, n_tp),
        out_shape=(
            shape((total, sizes[0]), BF),
            shape((total, sizes[1]), BF),
            shape((total, hv), BF),
            shape((total, sizes[3]), F32),
            shape((mine, width), F32),
            shape((mine, width), F32),
            shape((2, width), F32),
            shape((total, width), BF),
            shape((total, width), BF),
        )
        + tuple(shape((n, s, BLOCK), BF) for s in sizes)
        + (
            shape((total, hv), BF),
            shape((mine, width), F32),
            shape((total, width), BF),
            shape((total, units), BF),
            shape((total, units), BF),
            shape((total, units), BF),
            shape((mine, width), F32),
            shape((mine, width), BF),
        ),
        in_specs=[anyspec()] * 3 + [vmem()] * 5 + [anyspec()] * 8,
        out_specs=(anyspec(),) * 6 + (vmem(),) + (anyspec(),) * 18,
        scratch_shapes=[
            pltpu.VMEM((total, width), BF),
            pltpu.VMEM((mine, width), F32),
            pltpu.VMEM((mine, width), BF),
            pltpu.VMEM((n, 2, BLOCK), F32),
            pltpu.VMEM((total, sizes[0]), BF),
            pltpu.VMEM((total, sizes[1]), BF),
            pltpu.VMEM((total, hv), BF),
            pltpu.VMEM((total, sizes[3]), F32),
            pltpu.VMEM((tables[2].shape[0], window, window), F32),
            pltpu.VMEM((n_tp - 1, mine, width), BF),
        ]
        + [pltpu.VMEM((n, s, BLOCK), BF) for s in sizes[4:]]
        + [pltpu.VMEM((micro, rows, width), F32)]
        + [pltpu.VMEM((total, s), F32) for s in sizes[:3]]
        + [pltpu.VMEM((SLOTS, s, BLOCK), BF) for s in sizes[:4]]
        + [
            pltpu.VMEM((total, width), BF),
            pltpu.VMEM((mine, width), F32),
            pltpu.VMEM((total, hv), BF),
            pltpu.VMEM((total, units), BF),
            pltpu.VMEM((total, units), BF),
            pltpu.VMEM((total, units), BF),
            pltpu.VMEM((256, units), F32),
        ]
        + [dma((n - 1, count, 2))] * 2
        + [dma((n,))] * 2
        + [dma((micro, n_tp))] * 6
        + [dma((n_tp - 1, micro))] * 4
        + [dma((SLOTS + 1, 4)), dma((8,)), dma((19 + micro,))],
        compiler_params=pltpu.CompilerParams(
            collective_id=1, has_side_effects=True, vmem_limit_bytes=66_500_000
        ),
        cost_estimate=pl.CostEstimate(
            flops=2 * total * width * sum(sizes), bytes_accessed=120_000_000, transcendentals=0
        ),
        name="forward_kernel",
    )(x, cot, gains, cosine, sine, *tables, *weights)


class LaneRing:
    def __init__(self, n, tp, cw, ccw, lanes, fresh, free, soon, done):
        self.n, self.tp, self.ways, self.lanes = n, tp, (cw, ccw), lanes
        self.fresh, self.free, self.soon, self.done = fresh, free, soon, done
        self.state = [dict(job=0, step=1, firsts=0, ready=False) for _ in lanes]
        self.allowed = [0 for _ in lanes]

    def hop(self, p, t):
        lane = self.lanes[p]
        size = lane["jobs"][t // (self.n - 1)][0]
        slots = lane["recv"].shape[0]
        copies = []
        for side in range(2):
            lanes = pl.ds(side * LANE, LANE)
            copies.append(
                pltpu.make_async_remote_copy(
                    src_ref=lane["send"].at[t % 2, pl.ds(0, size), lanes],
                    dst_ref=lane["recv"].at[t % slots, pl.ds(0, size), lanes],
                    send_sem=lane["send_sem"].at[t, side],
                    recv_sem=lane["recv_sem"].at[t, side],
                    device_id=(self.ways[side], self.tp),
                    device_id_type=MESH,
                )
            )
        return copies

    def post(self, p, t, total):
        lane = self.lanes[p]
        slots = lane["recv"].shape[0]
        if t >= 2:
            for copy in self.hop(p, t - 2):
                copy.wait_send()
        lane["send"][t % 2, pl.ds(0, total.shape[0]), :] = total.astype(BF)
        for side, copy in enumerate(self.hop(p, t)):
            if t >= slots:
                pl.semaphore_wait(self.free.at[p, side], 1)
            copy.start()

    def first(self, p):
        lane, state = self.lanes[p], self.state[p]
        job = state["firsts"]
        size, gradient, _ = lane["jobs"][job]
        state["firsts"] += 1
        gradient(1 % self.n, self.fresh.at[pl.ds(0, size)])
        self.post(p, job * (self.n - 1), self.fresh[pl.ds(0, size), :])

    def prepare(self):
        for p, lane in enumerate(self.lanes):
            state = self.state[p]
            if state["job"] < state["firsts"] and not state["ready"]:
                size, gradient, _ = lane["jobs"][state["job"]]
                gradient((state["step"] + 1) % self.n, lane["part"].at[pl.ds(0, size)])
                state["ready"] = True

    def advance(self, only=(0, 1)):
        n = self.n
        self.prepare()
        for p in only:
            lane = self.lanes[p]
            state = self.state[p]
            job, step = state["job"], state["step"]
            count = len(lane["jobs"])
            if job >= state["firsts"]:
                if job < min(count, self.allowed[p]):
                    self.first(p)
                continue
            if step == n - 1 and state["firsts"] == job + 1 < min(count, self.allowed[p]):
                self.first(p)
            size, _, out = lane["jobs"][job]
            t = job * (n - 1) + step - 1
            slots = lane["recv"].shape[0]
            for copy in self.hop(p, t):
                copy.wait_recv()
            total = lane["part"][pl.ds(0, size), :] + lane["recv"][
                t % slots, pl.ds(0, size), :
            ].astype(F32)
            state["ready"] = False
            if step == n - 1:
                self.done(p, job, total, out)
                state["job"], state["step"] = job + 1, 1
            if t + slots < count * (n - 1):
                for side in range(2):
                    pl.semaphore_signal(
                        self.free.at[p, side],
                        inc=1,
                        device_id=(self.ways[1 - side], self.tp),
                        device_id_type=MESH,
                    )
            if step < n - 1:
                self.post(p, t + 1, total)
                state["step"] = step + 1
                if step == n - 2:
                    self.soon(p, out)

    def busy(self):
        return any(s["job"] < len(lane["jobs"]) for s, lane in zip(self.state, self.lanes))

    def finish(self):
        for p, lane in enumerate(self.lanes):
            last = len(lane["jobs"]) * (self.n - 1)
            for t in range(max(0, last - 2), last):
                for copy in self.hop(p, t):
                    copy.wait_send()


def backward_kernel(
    n,
    n_tp,
    gain_ref,
    own_gain_ref,
    col_ref,
    row_ref,
    rate_ref,
    cos_ref,
    sin_ref,
    *refs,
):
    hidden_ref, cot_ref, value_ref, slope_ref, second_ref, middle_ref, cotf_ref = refs[:7]
    q_ref, k_ref, v_ref, g_ref, gated_ref, nall_ref, x_ref = refs[7:14]
    wq_ref, wk_ref, wv_ref, wg_ref, wo_ref, wu_ref, wl_ref, wd_ref = refs[14:22]
    refs = refs[22:]
    dd_out, du_out, dl_out, do_out, ds_out, dv_out, dq_out, dk_out, sum_out, rows_out = refs[:10]
    cot_v, w_v, gu_v, gl_v, hidden_v, second_v, wu_s, wl_s, middle_v, cotf_v = refs[10:20]
    q_v, k_v, v_v, g_v, gs_v, gated_v, decay_v, gk_acc, gv_acc = refs[20:29]
    back_v, own_v, got_v, mall_v, rows_v, part0, part1, fresh_v = refs[29:37]
    send0, send1, recv0, recv1, done_v, own_w, sum_v = refs[37:44]
    ring_send0, ring_send1, ring_recv0, ring_recv1, ring_free = refs[44:49]
    part_send, part_recv, last_send, last_recv, share_send, share_recv = refs[49:55]
    sum_send, sum_recv, load_sem, done_sem, own_sem, local_sem = refs[55:]

    total, width = cot_v.shape
    mine = own_v.shape[0]
    window = col_ref.shape[0]
    micro = total // window
    rows = mine // micro
    heads = decay_v.shape[0]
    dp, tp, cw, ccw = neighbours(n)
    pos = ring_position(dp, n)
    bits = bits_of(n_tp)
    tile = 256
    half = HK // 2
    greet([(cw, tp), (ccw, tp)] + [(dp, partner(tp, bit)) for bit in bits])

    pairs = (
        (hidden_ref, hidden_v),
        (cot_ref, cot_v),
        (wd_ref, w_v),
        (value_ref, gu_v),
        (slope_ref, gl_v),
        (second_ref, second_v),
        (middle_ref, middle_v),
        (cotf_ref, cotf_v),
        (q_ref, q_v),
        (k_ref, k_v),
        (v_ref, v_v),
        (g_ref, g_v),
    )
    loads = [
        pltpu.make_async_copy(source, target, local_sem.at[at])
        for at, (source, target) in enumerate(pairs)
    ]
    for copy in loads[:2]:
        copy.start()

    def block_load(i, a):
        source, target = ((wu_ref, wu_s), (wl_ref, wl_s))[a]
        return pltpu.make_async_copy(
            source.at[i % n], target.at[i % 2], load_sem.at[i % 2, a]
        )

    def product(left, right):
        def gradient(i, target):
            target[...] = tn(left[...], right[:, pl.ds(i * BLOCK, BLOCK)])

        return gradient

    units, hv, hk = gu_v.shape[1], v_v.shape[1], q_v.shape[1]
    lanes = (
        dict(
            jobs=(
                (units, product(hidden_v, cot_v), (dd_out, None)),
                (units, product(gl_v, second_v), (dl_out, wl_ref)),
                (hv, product(gs_v, cot_v), (ds_out, wg_ref)),
                (hk, product(q_v, cot_v), (dq_out, wq_ref)),
            ),
            part=part0,
            send=send0,
            recv=recv0,
            send_sem=ring_send0,
            recv_sem=ring_recv0,
        ),
        dict(
            jobs=(
                (units, product(gu_v, second_v), (du_out, wu_ref)),
                (hv, product(hidden_v, mall_v), (do_out, None)),
                (hv, product(v_v, cot_v), (dv_out, wv_ref)),
                (hk, product(k_v, cot_v), (dk_out, wk_ref)),
            ),
            part=part1,
            send=send1,
            recv=recv1,
            send_sem=ring_send1,
            recv_sem=ring_recv1,
        ),
    )
    pending = {}

    def own_copy(p, weight):
        held = own_w.at[p, pl.ds(0, weight.shape[1])]
        return pltpu.make_async_copy(weight.at[0], held, own_sem.at[p])

    def soon(p, out):
        if out[1] is not None:
            own_copy(p, out[1]).start()

    def done(p, job, result, out):
        target, weight = out
        size = result.shape[0]
        if p in pending:
            pending.pop(p).wait()
        done_v[p, pl.ds(0, size), :] = result
        pending[p] = pltpu.make_async_copy(
            done_v.at[p, pl.ds(0, size)], target, done_sem.at[p]
        )
        pending[p].start()
        if weight is not None:
            own_copy(p, weight).wait()
            line = jnp.sum(
                own_w[p, pl.ds(0, size), :].astype(F32) * done_v[p, pl.ds(0, size), :],
                axis=0,
                keepdims=True,
            )
            at = 1 if job < 2 else 0
            sum_v[0, at : at + 1, :] = sum_v[0, at : at + 1, :] + line

    sum_v[...] = jnp.zeros_like(sum_v)
    ring = LaneRing(n, tp, cw, ccw, lanes, fresh_v, ring_free, soon, done)
    loads[0].wait()
    loads[1].wait()
    for copy in loads[2:5]:
        copy.start()
    ring.allowed = [1, 0]
    ring.first(0)
    for copy in loads[2:5]:
        copy.wait()
    block_load(0, 0).start()
    block_load(0, 1).start()
    for copy in loads[5:]:
        copy.start()

    @pl.loop(0, total // tile)
    def _(r):
        here = pl.ds(pl.multiple_of(r * tile, tile), tile)
        grad = None
        for i in range(n):
            term = nt(cot_v[here, pl.ds(i * BLOCK, BLOCK)], w_v[i])
            grad = term if grad is None else grad + term
        gu_v[here, :] = (grad * gu_v[here, :].astype(F32)).astype(BF)
        gl_v[here, :] = (grad * gl_v[here, :].astype(F32)).astype(BF)

    wo_load = pltpu.make_async_copy(wo_ref, w_v, local_sem.at[2])
    wo_load.start()
    ring.advance((0,))
    loads[5].wait()
    ring.allowed = [2, 1]
    ring.first(1)
    ring.prepare()
    collect = Collect(dp, tp, n_tp, micro, rows, back_v, got_v, own_v, part_send, part_recv)
    share = Share(dp, tp, n_tp, micro, rows, mall_v, share_send, share_recv)
    for m in range(micro):
        for i in range(n):
            at = m * n + i
            for a in range(2):
                block_load(at, a).wait()
                if at + 1 < micro * n:
                    block_load(at + 1, a).start()

            @pl.loop(0, window // tile)
            def _(r):
                here = pl.ds(pl.multiple_of(m * window + r * tile, tile), tile)
                back_v[here, pl.ds(i * BLOCK, BLOCK)] = (
                    nn(gu_v[here, :], wu_s[at % 2]) + nn(gl_v[here, :], wl_s[at % 2])
                ).astype(BF)

        collect.start(bits[0], m)
        ring.advance()
        ring.prepare()
    for at, bit in enumerate(bits[:-1]):
        for m in range(micro):
            collect.add(bit, m)
            collect.start(bits[at + 1], m)
    fill_decay(decay_v, col_ref, row_ref, rate_ref)
    loads[6].wait()
    loads[7].wait()
    for m in range(micro):
        ring.advance()
        ring.prepare()
        collect.add(bits[-1], m)

        @pl.loop(0, rows // STEP)
        def _(r):
            inner = pl.multiple_of(r * STEP, STEP)
            here = pl.ds(pl.multiple_of(m * rows + inner, STEP), STEP)
            there = pl.ds(pl.multiple_of(m * window + inner, STEP), STEP)
            middle = middle_v[here, :]
            scale = lax.rsqrt(jnp.mean(middle * middle, axis=-1, keepdims=True) + EPS)
            scaled = own_v[here, :] * gain_ref[1:2, :]
            inside = jnp.mean(scaled * middle, axis=-1, keepdims=True)
            grad = cotf_v[here, :] + scale * (scaled - middle * (scale * scale * inside))
            cotf_v[here, :] = grad
            mall_v[there, :] = grad.astype(BF)

        share.begin(m)
    x_load = pltpu.make_async_copy(x_ref, middle_v, local_sem.at[6])
    x_load.start()
    collect.finish()
    ring.advance()
    ring.prepare()
    for copy in loads[8:]:
        copy.wait()
    wo_load.wait()
    gated_load = None
    for m in range(micro):
        share.relay(m)
        if m == micro - 1 and gated_load is not None:
            gated_load.wait()
            ring.allowed = [2, 2]
        ring.advance()
        ring.prepare()
        for h in range(heads):
            keys = pl.ds(h * HK, HK)
            values = pl.ds(h * HV, HV)
            inside = pl.ds(m * window, window)
            gk_acc[...] = jnp.zeros_like(gk_acc)
            gv_acc[...] = jnp.zeros_like(gv_acc)

            @pl.loop(0, window // tile)
            def _(r):
                at = pl.multiple_of(r * tile, tile)
                here = pl.ds(pl.multiple_of(m * window + at, tile), tile)
                grad = None
                for i in range(n):
                    term = nt(mall_v[here, pl.ds(i * BLOCK, BLOCK)], w_v[i, values, :])
                    grad = term if grad is None else grad + term
                gated_v[pl.ds(at, tile), :] = grad

            @pl.loop(0, window // tile)
            def _(r):
                at = pl.multiple_of(r * tile, tile)
                local = pl.ds(at, tile)
                here = pl.ds(pl.multiple_of(m * window + at, tile), tile)
                decay = decay_v[h, local, :]
                query = q_v[here, keys]
                weight = (nt(query, k_v[inside, keys]) * decay).astype(BF)
                kept = nn(weight, v_v[inside, values])
                group = lax.rsqrt(jnp.mean(kept * kept, axis=-1, keepdims=True) + GROUP_EPS)
                gate = g_v[here, values]
                sigmoid = jax.nn.sigmoid(gate)
                grad = gated_v[local, :]
                gs_v[here, values] = (
                    grad * (kept * group) * (sigmoid * (1.0 + gate * (1.0 - sigmoid)))
                ).astype(BF)
                lifted = grad * (gate * sigmoid)
                mean = jnp.mean(lifted * kept, axis=-1, keepdims=True)
                grad_kept = (group * (lifted - kept * (group * group * mean))).astype(BF)
                gv_acc[...] += tn(weight, grad_kept)
                score = (nt(grad_kept, v_v[inside, values]) * decay).astype(BF)
                gk_acc[...] += tn(score, query)
                turned = nn(score, k_v[inside, keys])
                low, high = turned[:, :half], turned[:, half:]
                cosine, sine = cos_ref[local, :], sin_ref[local, :]
                q_v[here, pl.ds(h * HK, half)] = (low * cosine + high * sine).astype(BF)
                q_v[here, pl.ds(h * HK + half, half)] = (high * cosine - low * sine).astype(BF)

            low, high = gk_acc[:, :half], gk_acc[:, half:]
            cosine, sine = cos_ref[...], sin_ref[...]
            k_v[inside, pl.ds(h * HK, half)] = (low * cosine + high * sine).astype(BF)
            k_v[inside, pl.ds(h * HK + half, half)] = (high * cosine - low * sine).astype(BF)
            v_v[inside, values] = gv_acc[...].astype(BF)
            ring.advance()
            if ring.state[0]["job"] > 0 and gated_load is None:
                gated_load = pltpu.make_async_copy(gated_ref, hidden_v, local_sem.at[0])
                gated_load.start()
                nall_load = pltpu.make_async_copy(nall_ref, cot_v, local_sem.at[1])
                nall_load.start()
            ring.prepare()

    def settle():
        while ring.state[0]["job"] == 0:
            ring.advance()

    if gated_load is None:
        settle()
        gated_load = pltpu.make_async_copy(gated_ref, hidden_v, local_sem.at[0])
        gated_load.start()
        nall_load = pltpu.make_async_copy(nall_ref, cot_v, local_sem.at[1])
        nall_load.start()
    if ring.allowed[1] < 2:
        gated_load.wait()
    nall_load.wait()
    ring.allowed = [4, 4]

    wholes = (wq_ref, wk_ref, wv_ref, wg_ref)
    grads = (q_v, k_v, v_v, gs_v)
    sizes = (hk, hk, hv, hv)

    def weight_slot(i, a):
        return w_v.at[2 * a + i % 2, pl.ds(0, sizes[a])]

    def weight_load(i, a):
        return pltpu.make_async_copy(
            wholes[a].at[i], weight_slot(i, a), load_sem.at[2 + i % 2, a]
        )

    for a in range(4):
        weight_load(0, a).start()
    ring.advance()
    ring.prepare()
    for i in range(n):
        for a in range(4):
            weight_load(i, a).wait()
            if i + 1 < n:
                weight_load(i + 1, a).start()

        @pl.loop(0, total // tile)
        def _(r):
            here = pl.ds(pl.multiple_of(r * tile, tile), tile)
            block = None
            for a in range(4):
                term = nn(grads[a][here, :], weight_slot(i, a)[...])
                block = term if block is None else block + term
            back_v[here, pl.ds(i * BLOCK, BLOCK)] = block.astype(BF)

        if i % 2 == 1:
            ring.advance()
            ring.prepare()
    last = Collect(dp, tp, n_tp, micro, rows, back_v, got_v, own_v, last_send, last_recv)
    for m in range(micro):
        last.start(bits[0], m)
    ring.advance()
    ring.prepare()
    for at, bit in enumerate(bits):
        for m in range(micro):
            last.add(bit, m)
            if at + 1 < len(bits):
                last.start(bits[at + 1], m)
        if at + 1 < len(bits):
            for _ in range(3):
                ring.advance()
                ring.prepare()
    x_load.wait()

    def natural(i, side):
        at = ring_index((pos + (n - i if side == 0 else i)) % n, n) * BLOCK + side * LANE
        return pl.ds(pl.multiple_of(at, LANE), LANE)

    @pl.loop(0, mine // STEP)
    def _(r):
        at = pl.multiple_of(r * STEP, STEP)
        m, inner = at // rows, pl.multiple_of(at % rows, STEP)
        here = pl.ds(at, STEP)
        x = middle_v[here, :]
        scale = lax.rsqrt(jnp.mean(x * x, axis=-1, keepdims=True) + EPS)
        inside = jnp.mean(own_v[here, :] * gain_ref[0:1, :] * x, axis=-1, keepdims=True)
        slope = scale * scale * inside
        for i in range(n):
            for side in range(2):
                lanes = pl.ds(i * BLOCK + side * LANE, LANE)
                scaled = own_v[here, lanes] * gain_ref[0:1, lanes]
                rows_v[m, pl.ds(inner, STEP), natural(i, side)] = cotf_v[
                    here, lanes
                ] + scale * (scaled - middle_v[here, lanes] * slope)

    rows_copy = pltpu.make_async_copy(rows_v, rows_out, local_sem.at[2])
    rows_copy.start()
    while ring.busy():
        ring.advance()
        ring.prepare()
    for at, bit in enumerate(bits):
        swap = pltpu.make_async_remote_copy(
            src_ref=sum_v.at[2 * at],
            dst_ref=sum_v.at[2 * at + 1],
            send_sem=sum_send.at[at],
            recv_sem=sum_recv.at[at],
            device_id=(dp, partner(tp, bit)),
            device_id_type=MESH,
        )
        swap.start()
        swap.wait()
        sum_v[2 * at + 2] = sum_v[2 * at] + sum_v[2 * at + 1]
    sum_out[...] = sum_v[2 * len(bits)] / own_gain_ref[...]
    ring.finish()
    share.finish()
    last.finish()
    rows_copy.wait()
    for copy in pending.values():
        copy.wait()


def backward(n, n_tp, rows, gain, own_gain, tables, cosine, sine, arrays, weights):
    total, width = arrays[1].shape
    mine = arrays[5].shape[0]
    units, hk, hv = arrays[0].shape[1], arrays[7].shape[1], arrays[9].shape[1]
    heads = tables[2].shape[0]
    window = tables[0].shape[0]
    micro = total // window
    tall = max(units, hv, hk)
    hops = 4 * (n - 1)
    count = len(bits_of(n_tp))
    shape = jax.ShapeDtypeStruct
    dma = pltpu.SemaphoreType.DMA
    sizes = (units, units, units, hv, hv, hv, hk, hk)
    return pl.pallas_call(
        functools.partial(backward_kernel, n, n_tp),
        out_shape=tuple(shape((s, BLOCK), F32) for s in sizes)
        + (shape((8, BLOCK), F32), shape((micro, rows, width), F32)),
        in_specs=[vmem()] * 7 + [anyspec()] * 22,
        out_specs=(anyspec(),) * 8 + (vmem(), anyspec()),
        scratch_shapes=[
            pltpu.VMEM((total, width), BF),
            pltpu.VMEM((n, tall, BLOCK), BF),
            pltpu.VMEM((total, units), BF),
            pltpu.VMEM((total, units), BF),
            pltpu.VMEM((total, units), BF),
            pltpu.VMEM((total, width), BF),
            pltpu.VMEM((2, units, BLOCK), BF),
            pltpu.VMEM((2, units, BLOCK), BF),
            pltpu.VMEM((mine, width), F32),
            pltpu.VMEM((mine, width), F32),
            pltpu.VMEM((total, hk), BF),
            pltpu.VMEM((total, hk), BF),
            pltpu.VMEM((total, hv), BF),
            pltpu.VMEM((total, hv), F32),
            pltpu.VMEM((total, hv), BF),
            pltpu.VMEM((window, HV), F32),
            pltpu.VMEM((heads, window, window), F32),
            pltpu.VMEM((window, HK), F32),
            pltpu.VMEM((window, HV), F32),
            pltpu.VMEM((total, width), BF),
            pltpu.VMEM((mine, width), F32),
            pltpu.VMEM((n_tp - 1, mine, width), BF),
            pltpu.VMEM((total, width), BF),
            pltpu.VMEM((micro, rows, width), F32),
            pltpu.VMEM((tall, BLOCK), F32),
            pltpu.VMEM((tall, BLOCK), F32),
            pltpu.VMEM((tall, BLOCK), F32),
            pltpu.VMEM((2, tall, BLOCK), BF),
            pltpu.VMEM((2, tall, BLOCK), BF),
            pltpu.VMEM((2, tall, BLOCK), BF),
            pltpu.VMEM((2, tall, BLOCK), BF),
            pltpu.VMEM((2, tall, BLOCK), F32),
            pltpu.VMEM((2, tall, BLOCK), BF),
            pltpu.VMEM((2 * count + 1, 8, BLOCK), F32),
        ]
        + [dma((hops, 2))] * 4
        + [pltpu.SemaphoreType.REGULAR((2, 2))]
        + [dma((n_tp - 1, micro))] * 4
        + [dma((micro, n_tp))] * 2
        + [dma((count,))] * 2
        + [dma((4, 4)), dma((2,)), dma((2,)), dma((12,))],
        compiler_params=pltpu.CompilerParams(
            collective_id=2, has_side_effects=True, vmem_limit_bytes=67_000_000
        ),
        cost_estimate=pl.CostEstimate(
            flops=4 * total * width * sum(sizes), bytes_accessed=120_000_000, transcendentals=0
        ),
        name="backward_kernel",
    )(gain, own_gain, *tables, cosine, sine, *arrays, *weights)


def finish_kernel(
    n,
    n_tp,
    passed,
    turned,
    *refs,
):
    sources = refs[: passed + turned]
    middle_ref, near_ref, far_ref = refs[passed + turned : passed + turned + 3]
    targets = refs[passed + turned + 3 : 2 * (passed + turned) + 3]
    block_out = refs[2 * (passed + turned) + 3]
    scratch = refs[2 * (passed + turned) + 4 :]
    held, (middle_v, near_v, far_v, block_v), (sem_in, sem_out) = (
        scratch[: passed + 2 * turned],
        scratch[passed + 2 * turned : passed + 2 * turned + 4],
        scratch[passed + 2 * turned + 4 :],
    )
    micro, rows, width = block_v.shape
    pos = ring_position(lax.axis_index("dp"), n)
    count = passed + turned
    ins = [
        pltpu.make_async_copy(sources[i], held[i], sem_in.at[i]) for i in range(count)
    ] + [
        pltpu.make_async_copy(source, target, sem_in.at[count + i])
        for i, (source, target) in enumerate(
            ((middle_ref, middle_v), (near_ref, near_v), (far_ref, far_v))
        )
    ]
    for copy in ins[count:] + ins[:count]:
        copy.start()
    results = list(held[:passed]) + list(held[count:])
    outs = [pltpu.make_async_copy(results[i], targets[i], sem_out.at[i]) for i in range(count)]
    outs.append(pltpu.make_async_copy(block_v, block_out, sem_out.at[count]))
    for copy in ins[count:]:
        copy.wait()

    @pl.loop(0, micro * rows // STEP)
    def _(r):
        at = pl.multiple_of(r * STEP, STEP)
        m, inner = at // rows, pl.multiple_of(at % rows, STEP)
        here = pl.ds(at, STEP)
        for i in range(n):
            for side in range(2):
                lanes = pl.ds(i * BLOCK + side * LANE, LANE)
                spot = ring_index((pos + (n - i if side == 0 else i)) % n, n)
                there = pl.ds(pl.multiple_of(spot * BLOCK + side * LANE, LANE), LANE)
                block_v[m, pl.ds(inner, STEP), there] = middle_v[here, lanes] + (
                    near_v[here, lanes] + far_v[here, lanes].astype(F32)
                )

    outs[count].start()
    for i in range(passed):
        ins[i].wait()
        outs[i].start()
    for i in range(turned):
        ins[passed + i].wait()
        held[count + i][...] = held[passed + i][...].T
        outs[passed + i].start()
    for copy in outs:
        copy.wait()


def finish(n, n_tp, passed, turned, middle, near, far, block_shape):
    shape = jax.ShapeDtypeStruct
    results = tuple(shape(a.shape, a.dtype) for a in passed) + tuple(
        shape(a.shape[::-1], a.dtype) for a in turned
    )
    count = len(passed) + len(turned)
    return pl.pallas_call(
        functools.partial(finish_kernel, n, n_tp, len(passed), len(turned)),
        out_shape=results + (shape(block_shape, F32),),
        in_specs=[anyspec()] * (count + 3),
        out_specs=(anyspec(),) * (count + 1),
        scratch_shapes=[pltpu.VMEM(a.shape, a.dtype) for a in passed]
        + [pltpu.VMEM(a.shape, a.dtype) for a in turned]
        + [pltpu.VMEM(a.shape[::-1], a.dtype) for a in turned]
        + [
            pltpu.VMEM(middle.shape, F32),
            pltpu.VMEM(near.shape, F32),
            pltpu.VMEM(far.shape, BF),
            pltpu.VMEM(block_shape, F32),
            pltpu.SemaphoreType.DMA((count + 3,)),
            pltpu.SemaphoreType.DMA((count + 1,)),
        ],
        compiler_params=pltpu.CompilerParams(vmem_limit_bytes=66_000_000),
        name="finish_kernel",
    )(*passed, *turned, middle, near, far)


def normalize(row_block, gain_vec):
    row_scale = lax.rsqrt(jnp.mean(row_block * row_block, axis=-1, keepdims=True) + EPS)
    return (row_block * row_scale * gain_vec.astype(jnp.float32), row_scale)


def norm_back(grad_rows, row_block, row_scale, gain_vec):
    scaled_grad = grad_rows * gain_vec.astype(jnp.float32)
    back_rows = row_scale * (
        scaled_grad
        - row_block
        * row_scale
        * row_scale
        * jnp.mean(scaled_grad * row_block, axis=-1, keepdims=True)
    )
    return (back_rows, jnp.sum(grad_rows * row_block * row_scale, axis=0))


def angles(length, feature_width):
    half_width = feature_width // 2
    frequency = jnp.exp(-math.log(10000.0) * jnp.arange(half_width, dtype=jnp.float32) / half_width)
    turns = jnp.arange(length, dtype=jnp.float32)[:, None] * frequency[None, :]
    return (jnp.cos(turns)[:, None, :], jnp.sin(turns)[:, None, :])


def decays(length, head_ids):
    places = jnp.arange(length, dtype=jnp.float32)
    spacing = places[:, None] - places[None, :]
    log_rate = jnp.log(1.0 - jnp.exp2(-5.0 - head_ids))
    return jnp.where(
        spacing[None] >= 0.0,
        jnp.exp(jnp.maximum(spacing, 0.0)[None] * log_rate[:, None, None]),
        0.0,
    )


def rotate(value_vectors, cosine_table, sine_table):
    half_width = value_vectors.shape[-1] // 2
    lower = value_vectors[..., :half_width]
    upper = value_vectors[..., half_width:]
    return jnp.concatenate(
        [lower * cosine_table - upper * sine_table, upper * cosine_table + lower * sine_table],
        axis=-1,
    )


def unrotate(value_vectors, cosine_table, sine_table):
    half_width = value_vectors.shape[-1] // 2
    lower = value_vectors[..., :half_width]
    upper = value_vectors[..., half_width:]
    return jnp.concatenate(
        [lower * cosine_table + upper * sine_table, upper * cosine_table - lower * sine_table],
        axis=-1,
    )


def plain_gelu_parts(pre_act):
    normal_cdf = 0.5 * (1.0 + lax.erf(pre_act * (1.0 / math.sqrt(2.0))))
    density = jnp.exp(-0.5 * pre_act * pre_act) * (1.0 / math.sqrt(2.0 * math.pi))
    return (pre_act * normal_cdf, normal_cdf + pre_act * density)


def inner_rows(left_rows, right_rows):
    return lax.dot_general(
        left_rows, right_rows, (((0,), (0,)), ((), ())), preferred_element_type=jnp.float32
    )


def times_t(left_rows, right_rows):
    return lax.dot_general(
        left_rows, right_rows, (((1,), (1,)), ((), ())), preferred_element_type=jnp.float32
    )


def forward_pass(rows_in, gathered, cosine_table, sine_table, decay_mask):
    (
        first_gain,
        second_gain,
        query_weight,
        key_weight,
        value_weight,
        swish_weight,
        output_weight,
        up_projection_matrix,
        gelu_weight,
        down_weight,
    ) = gathered
    local_heads = decay_mask.shape[0]
    scale_qk = 1.0 / math.sqrt(HK)
    normed, first_scale = normalize(rows_in, first_gain)
    normed_all = lax.all_gather(normed.astype(jnp.bfloat16), "tensor", axis=0, tiled=True)
    total_rows = normed_all.shape[0]
    sequences = total_rows // LEN
    query_turned_rows = rotate(
        jnp.dot(normed_all, query_weight, preferred_element_type=jnp.float32).reshape(
            sequences, LEN, local_heads, HK
        ),
        cosine_table,
        sine_table,
    ).astype(jnp.bfloat16)
    key_turned_rows = rotate(
        jnp.dot(normed_all, key_weight, preferred_element_type=jnp.float32).reshape(
            sequences, LEN, local_heads, HK
        ),
        cosine_table,
        sine_table,
    ).astype(jnp.bfloat16)
    value_rows = (
        jnp.dot(normed_all, value_weight, preferred_element_type=jnp.float32)
        .astype(jnp.bfloat16)
        .reshape(sequences, LEN, local_heads, HV)
    )
    gate_pre = jnp.dot(normed_all, swish_weight, preferred_element_type=jnp.float32)
    unscaled_logits = jnp.einsum(
        "snhd,smhd->shnm", query_turned_rows, key_turned_rows, preferred_element_type=jnp.float32
    )
    weight_bf = (unscaled_logits * (decay_mask * scale_qk)).astype(jnp.bfloat16)
    retained = jnp.einsum(
        "shnm,smhe->snhe", weight_bf, value_rows, preferred_element_type=jnp.float32
    )
    group_scale = lax.rsqrt(jnp.mean(retained * retained, axis=-1, keepdims=True) + GROUP_EPS)
    grouped = (retained * group_scale).reshape(total_rows, local_heads * HV)
    sigmoid_gate = jax.nn.sigmoid(gate_pre)
    swish_val = gate_pre * sigmoid_gate
    gated_rows = (swish_val * grouped).astype(jnp.bfloat16)
    attention = lax.psum_scatter(
        jnp.dot(gated_rows, output_weight, preferred_element_type=jnp.float32),
        "tensor",
        scatter_dimension=0,
        tiled=True,
    )
    middle = rows_in + attention
    second, second_scale = normalize(middle, second_gain)
    second_all = lax.all_gather(second.astype(jnp.bfloat16), "tensor", axis=0, tiled=True)
    up_pre = jnp.dot(second_all, up_projection_matrix, preferred_element_type=jnp.float32)
    gelu_pre = jnp.dot(second_all, gelu_weight, preferred_element_type=jnp.float32)
    gelu_val, gelu_slope = plain_gelu_parts(gelu_pre)
    hidden = (gelu_val * up_pre).astype(jnp.bfloat16)
    block_rows = middle + lax.psum_scatter(
        jnp.dot(hidden, down_weight, preferred_element_type=jnp.float32).astype(jnp.bfloat16),
        "tensor",
        scatter_dimension=0,
        tiled=True,
    ).astype(jnp.float32)
    kept_state = (
        rows_in,
        first_scale,
        normed_all,
        query_turned_rows,
        key_turned_rows,
        value_rows,
        gate_pre,
        weight_bf,
        retained,
        group_scale,
        grouped,
        gated_rows,
        middle,
        second_scale,
        second_all,
        up_pre,
        gelu_val,
        gelu_slope,
        hidden,
    )
    return (block_rows, kept_state)


def backward_pass(kept_state, cot_in, gathered, cosine_table, sine_table, decay_mask):
    (
        first_gain,
        second_gain,
        query_weight,
        key_weight,
        value_weight,
        swish_weight,
        output_weight,
        up_projection_matrix,
        gelu_weight,
        down_weight,
    ) = gathered
    (
        rows_in,
        first_scale,
        normed_all,
        query_turned_rows,
        key_turned_rows,
        value_rows,
        gate_pre,
        weight_bf,
        retained,
        group_scale,
        grouped,
        gated_rows,
        middle,
        second_scale,
        second_all,
        up_pre,
        gelu_val,
        gelu_slope,
        hidden,
    ) = kept_state
    local_heads = decay_mask.shape[0]
    total_rows = normed_all.shape[0]
    scale_qk = 1.0 / math.sqrt(HK)
    cot_all = lax.all_gather(cot_in.astype(jnp.bfloat16), "tensor", axis=0, tiled=True)
    grad_hidden = times_t(cot_all, down_weight)
    grad_down = inner_rows(hidden, cot_all)
    grad_uppre = (grad_hidden * gelu_val).astype(jnp.bfloat16)
    grad_gelupre = (grad_hidden * up_pre * gelu_slope).astype(jnp.bfloat16)
    grad_up = inner_rows(second_all, grad_uppre)
    grad_gelu = inner_rows(second_all, grad_gelupre)
    second_back = lax.psum_scatter(
        times_t(grad_uppre, up_projection_matrix) + times_t(grad_gelupre, gelu_weight),
        "tensor",
        scatter_dimension=0,
        tiled=True,
    )
    middle_back, grad_gain_two = norm_back(second_back, middle, second_scale, second_gain)
    grad_middle = cot_in + middle_back
    middle_all = lax.all_gather(grad_middle.astype(jnp.bfloat16), "tensor", axis=0, tiled=True)
    grad_gated = times_t(middle_all, output_weight)
    grad_out = inner_rows(gated_rows, middle_all)
    sigmoid_gate = jax.nn.sigmoid(gate_pre)
    swish_val = gate_pre * sigmoid_gate
    grad_swishpre = (
        grad_gated * grouped * (sigmoid_gate * (1.0 + gate_pre * (1.0 - sigmoid_gate)))
    ).astype(jnp.bfloat16)
    grad_grouped = (grad_gated * swish_val).reshape(retained.shape)
    grad_retained = (
        group_scale
        * (
            grad_grouped
            - retained
            * group_scale
            * group_scale
            * jnp.mean(grad_grouped * retained, axis=-1, keepdims=True)
        )
    ).astype(jnp.bfloat16)
    grad_valrows = jnp.einsum(
        "shnm,snhe->smhe", weight_bf, grad_retained, preferred_element_type=jnp.float32
    ).astype(jnp.bfloat16)
    grad_weight = jnp.einsum(
        "snhe,smhe->shnm", grad_retained, value_rows, preferred_element_type=jnp.float32
    )
    grad_retention_logits = (grad_weight * (decay_mask * scale_qk)).astype(jnp.bfloat16)
    grad_query_rotated_rows = jnp.einsum(
        "shnm,smhd->snhd",
        grad_retention_logits,
        key_turned_rows,
        preferred_element_type=jnp.float32,
    )
    grad_key_rotated_rows = jnp.einsum(
        "shnm,snhd->smhd",
        grad_retention_logits,
        query_turned_rows,
        preferred_element_type=jnp.float32,
    )
    grad_qpre = (
        unrotate(grad_query_rotated_rows, cosine_table, sine_table)
        .astype(jnp.bfloat16)
        .reshape(total_rows, local_heads * HK)
    )
    grad_kpre = (
        unrotate(grad_key_rotated_rows, cosine_table, sine_table)
        .astype(jnp.bfloat16)
        .reshape(total_rows, local_heads * HK)
    )
    grad_vflat = grad_valrows.reshape(total_rows, local_heads * HV)
    first_back = lax.psum_scatter(
        times_t(grad_qpre, query_weight)
        + times_t(grad_kpre, key_weight)
        + times_t(grad_vflat, value_weight)
        + times_t(grad_swishpre, swish_weight),
        "tensor",
        scatter_dimension=0,
        tiled=True,
    )
    grad_query = inner_rows(normed_all, grad_qpre)
    grad_key = inner_rows(normed_all, grad_kpre)
    grad_value = inner_rows(normed_all, grad_vflat)
    grad_swish = inner_rows(normed_all, grad_swishpre)
    input_back, grad_gain_one = norm_back(first_back, rows_in, first_scale, first_gain)
    grad_rows = grad_middle + input_back
    pieces = (
        grad_gain_one,
        grad_gain_two,
        grad_query,
        grad_key,
        grad_value,
        grad_swish,
        grad_out,
        grad_up,
        grad_gelu,
        grad_down,
    )
    return (grad_rows, pieces)


def plain_body(
    block_input,
    cotangent,
    first_gain,
    second_gain,
    query_weight,
    key_weight,
    value_weight,
    swish_weight,
    output_weight,
    up_projection_matrix,
    gelu_weight,
    down_weight,
):
    local_heads = query_weight.shape[1] // HK
    head_ids = (lax.axis_index("tensor") * local_heads + jnp.arange(local_heads)).astype(
        jnp.float32
    )
    cosine_table, sine_table = angles(LEN, HK)
    decay_mask = decays(LEN, head_ids)
    output_list = []
    grad_list = []
    totals = ()
    for micro_idx in range(block_input.shape[0]):
        forward_set = (
            lax.all_gather(first_gain, "dp", axis=0, tiled=True),
            lax.all_gather(second_gain, "dp", axis=0, tiled=True),
            lax.all_gather(query_weight, "dp", axis=0, tiled=True),
            lax.all_gather(key_weight, "dp", axis=0, tiled=True),
            lax.all_gather(value_weight, "dp", axis=0, tiled=True),
            lax.all_gather(swish_weight, "dp", axis=0, tiled=True),
            lax.all_gather(output_weight, "dp", axis=1, tiled=True),
            lax.all_gather(up_projection_matrix, "dp", axis=0, tiled=True),
            lax.all_gather(gelu_weight, "dp", axis=0, tiled=True),
            lax.all_gather(down_weight, "dp", axis=1, tiled=True),
        )
        block_rows, kept_state = forward_pass(
            block_input[micro_idx], forward_set, cosine_table, sine_table, decay_mask
        )
        held = lax.optimization_barrier(
            (
                (
                    first_gain,
                    second_gain,
                    query_weight,
                    key_weight,
                    value_weight,
                    swish_weight,
                    output_weight,
                    up_projection_matrix,
                    gelu_weight,
                    down_weight,
                ),
                block_rows,
            )
        )[0]
        backward_set = (
            lax.all_gather(held[0], "dp", axis=0, tiled=True),
            lax.all_gather(held[1], "dp", axis=0, tiled=True),
            lax.all_gather(held[2], "dp", axis=0, tiled=True),
            lax.all_gather(held[3], "dp", axis=0, tiled=True),
            lax.all_gather(held[4], "dp", axis=0, tiled=True),
            lax.all_gather(held[5], "dp", axis=0, tiled=True),
            lax.all_gather(held[6], "dp", axis=1, tiled=True),
            lax.all_gather(held[7], "dp", axis=0, tiled=True),
            lax.all_gather(held[8], "dp", axis=0, tiled=True),
            lax.all_gather(held[9], "dp", axis=1, tiled=True),
        )
        grad_rows, pieces = backward_pass(
            kept_state, cotangent[micro_idx], backward_set, cosine_table, sine_table, decay_mask
        )
        output_list.append(block_rows)
        grad_list.append(grad_rows)
        if micro_idx == 0:
            totals = tuple(pieces)
        else:
            totals = tuple((total + piece for total, piece in zip(totals, pieces)))
    totals = (
        lax.psum_scatter(totals[0], "dp", scatter_dimension=0, tiled=True),
        lax.psum_scatter(totals[1], "dp", scatter_dimension=0, tiled=True),
        lax.psum_scatter(totals[2], "dp", scatter_dimension=0, tiled=True),
        lax.psum_scatter(totals[3], "dp", scatter_dimension=0, tiled=True),
        lax.psum_scatter(totals[4], "dp", scatter_dimension=0, tiled=True),
        lax.psum_scatter(totals[5], "dp", scatter_dimension=0, tiled=True),
        lax.psum_scatter(totals[6], "dp", scatter_dimension=1, tiled=True),
        lax.psum_scatter(totals[7], "dp", scatter_dimension=0, tiled=True),
        lax.psum_scatter(totals[8], "dp", scatter_dimension=0, tiled=True),
        lax.psum_scatter(totals[9], "dp", scatter_dimension=1, tiled=True),
    )
    gain_first, gain_second = lax.psum((totals[0], totals[1]), "tensor")
    return (
        jnp.stack(output_list, axis=0),
        jnp.stack(grad_list, axis=0),
        gain_first,
        gain_second,
        totals[2],
        totals[3],
        totals[4],
        totals[5],
        totals[6],
        totals[7],
        totals[8],
        totals[9],
    )


def ring_body(
    n_dp,
    n_tp,
    block_input,
    cotangent,
    first_gain,
    second_gain,
    query_weight,
    key_weight,
    value_weight,
    swish_weight,
    output_weight,
    up_projection_matrix,
    gelu_weight,
    down_weight,
):
    micro, rows, width = block_input.shape
    local_heads = query_weight.shape[1] // HK
    window = n_tp * rows

    me = lax.axis_index("tensor")
    head_ids = (me * local_heads + jnp.arange(local_heads)).astype(F32)
    chunk_of = jnp.arange(n_tp) ^ me
    natural = (chunk_of[:, None] * rows + jnp.arange(rows)[None, :]).reshape(window)
    place = (natural % LEN).astype(F32)
    half_key = HK // 2
    frequency = jnp.exp(-math.log(10000.0) * jnp.arange(half_key, dtype=F32) / half_key)
    turns = place[:, None] * frequency[None, :]
    cosine, sine = jnp.cos(turns), jnp.sin(turns)
    log_rate = jnp.log(1.0 - jnp.exp2(-5.0 - head_ids))
    spots = natural.astype(F32)
    tables = (
        jnp.broadcast_to(spots[:, None], (window, LANE)),
        spots[None, :],
        jnp.broadcast_to(log_rate[:, None], (local_heads, window)),
    )

    gains_own = jnp.stack([first_gain, second_gain]).astype(F32)
    results = forward(
        n_dp,
        n_tp,
        block_input,
        cotangent,
        gains_own,
        cosine,
        sine,
        tables,
        (
            query_weight,
            key_weight,
            value_weight.T,
            swish_weight.T,
            output_weight,
            up_projection_matrix.T,
            gelu_weight.T,
            down_weight,
        ),
    )
    query, key, value, gate, x_rel, cot_rel, gains, normed, cot_all = results[:9]
    w_in, (w_o, w_u, w_l, w_d) = results[9:13], results[13:17]
    gated, middle, second, hidden, gelu_val, up_slope, near, far = results[17:]

    far = lax.ppermute(far, "tensor", [(i, i ^ (n_tp // 2)) for i in range(n_tp)])

    (
        grad_down,
        grad_up,
        grad_gelu,
        grad_out,
        grad_swish,
        grad_value,
        grad_query,
        grad_key,
        gain_grads,
        grad_rows,
    ) = backward(
        n_dp,
        n_tp,
        rows,
        gains,
        jnp.pad(gains_own, ((0, 6), (0, 0)), constant_values=1.0),
        tables,
        cosine,
        sine,
        (
            hidden,
            cot_all,
            gelu_val,
            up_slope,
            second,
            middle,
            cot_rel,
            query,
            key,
            value,
            gate,
            gated,
            normed,
            x_rel,
        ),
        (*w_in, w_o, w_u, w_l, w_d),
    )
    passed = (grad_value, grad_swish, grad_out, grad_up, grad_gelu, grad_down, grad_rows)
    *passed, grad_query, grad_key, block_rows = finish(
        n_dp, n_tp, passed, (grad_query, grad_key), middle, near, far, block_input.shape
    )
    grad_value, grad_swish, grad_out, grad_up, grad_gelu, grad_down, grad_rows = passed

    return (
        block_rows,
        grad_rows,
        gain_grads[0],
        gain_grads[1],
        grad_query,
        grad_key,
        grad_value.T,
        grad_swish.T,
        grad_out,
        grad_up.T,
        grad_gelu.T,
        grad_down,
    )


def solution(mesh):
    rows = P(None, ("dp", "tensor"), None)
    wide, tall, gain = P("dp", "tensor"), P("tensor", "dp"), P("dp")
    n_dp, n_tp = mesh.shape["dp"], mesh.shape["tensor"]

    def run(*arrays):
        blocks = arrays[2].shape[0] == BLOCK and n_dp % 2 == 0 and n_dp > 2
        pairs = n_tp > 1 and n_tp & (n_tp - 1) == 0
        aligned = (n_tp * arrays[0].shape[1]) % LEN == 0 and arrays[0].shape[1] % LANE == 0
        equal = arrays[6].shape[1] == arrays[9].shape[1]
        if blocks and pairs and aligned and equal:
            return ring_body(n_dp, n_tp, *arrays)
        return plain_body(*arrays)

    return jax.shard_map(
        run,
        mesh=mesh,
        in_specs=(rows, rows, gain, gain) + (wide,) * 4 + (tall, wide, wide, tall),
        out_specs=(rows, rows, gain, gain) + (wide,) * 4 + (tall, wide, wide, tall),
        check_vma=False,
    )
```

```python
import functools
import math

import jax
import jax.numpy as jnp
from jax import lax
from jax.experimental import pallas as pl
from jax.experimental.pallas import tpu as pltpu
from jax.sharding import PartitionSpec as P

HK = 256
HV = 432
LEN = 512
EPS = 1e-05
GROUP_EPS = 1.0
BF = jnp.bfloat16
F32 = jnp.float32
MESH = pl.DeviceIdType.MESH
LANE = 128
BLOCK = 2 * LANE
SLOTS = 3
STEP = 32
SPLIT = 2


def ring_position(index, count):
    low = index // 2
    return low + (index % 2) * (count - 1 - 2 * low)


def ring_index(position, count):
    high = position // (count // 2)
    return (1 - high) * (2 * position) + high * (2 * (count - 1 - position) + 1)


def bits_of(count):
    return [1 << i for i in range(count.bit_length() - 1)]


def anyspec():
    return pl.BlockSpec(memory_space=pl.ANY)


def vmem():
    return pl.BlockSpec(memory_space=pltpu.VMEM)


def nt(left, right):
    return lax.dot_general(left, right, (((1,), (1,)), ((), ())), preferred_element_type=F32)


def nn(left, right):
    return lax.dot_general(left, right, (((1,), (0,)), ((), ())), preferred_element_type=F32)


def tn(left, right):
    return lax.dot_general(left, right, (((0,), (0,)), ((), ())), preferred_element_type=F32)


def partner(tp, bit):
    return tp + bit - 2 * bit * ((tp // bit) % 2)


def neighbours(n):
    dp, tp = lax.axis_index("dp"), lax.axis_index("tensor")
    pos = ring_position(dp, n)
    return dp, tp, ring_index((pos + 1) % n, n), ring_index((pos + n - 1) % n, n)


def greet(devices):
    barrier = pltpu.get_barrier_semaphore()
    for device in devices:
        pl.semaphore_signal(barrier, inc=1, device_id=device, device_id_type=MESH)
    pl.semaphore_wait(barrier, len(devices))


class Share:
    def __init__(self, dp, tp, n_tp, micro, rows, buf, send, recv):
        self.dp, self.tp, self.n_tp, self.micro, self.rows = dp, tp, n_tp, micro, rows
        self.buf, self.send, self.recv = buf, send, recv
        self.bits = bits_of(n_tp)[::-1]

    def copies(self, bit, m, keys=None):
        window = self.n_tp * self.rows
        for key in range(0, self.n_tp, 2 * bit):
            if keys is None or (key == 0) == keys:
                yield pltpu.make_async_remote_copy(
                    src_ref=self.buf.at[pl.ds(m * window + key * self.rows, self.rows)],
                    dst_ref=self.buf.at[pl.ds(m * window + (key ^ bit) * self.rows, self.rows)],
                    send_sem=self.send.at[m, key ^ bit],
                    recv_sem=self.recv.at[m, key ^ bit],
                    device_id=(self.dp, partner(self.tp, bit)),
                    device_id_type=MESH,
                )

    def begin(self, m):
        for bit in self.bits:
            for copy in self.copies(bit, m, True):
                copy.start()

    def relay(self, m):
        for bit in self.bits:
            for copy in self.copies(bit, m, False):
                copy.start()
            for copy in self.copies(bit, m):
                copy.wait_recv()

    def finish(self):
        for m in range(self.micro):
            for bit in self.bits:
                for copy in self.copies(bit, m):
                    copy.wait_send()


class Collect:
    def __init__(self, dp, tp, n_tp, micro, rows, back, got, own, send, recv):
        self.dp, self.tp, self.n_tp, self.micro, self.rows = dp, tp, n_tp, micro, rows
        self.back, self.got, self.own, self.send, self.recv = back, got, own, send, recv
        self.bits = bits_of(n_tp)

    def keys(self, bit):
        return [key for key in range(0, self.n_tp, bit) if key & bit]

    def copies(self, bit, m):
        window = self.n_tp * self.rows
        for key in self.keys(bit):
            yield pltpu.make_async_remote_copy(
                src_ref=self.back.at[pl.ds(m * window + key * self.rows, self.rows)],
                dst_ref=self.got.at[key - 1, pl.ds(m * self.rows, self.rows)],
                send_sem=self.send.at[key - 1, m],
                recv_sem=self.recv.at[key - 1, m],
                device_id=(self.dp, partner(self.tp, bit)),
                device_id_type=MESH,
            )

    def start(self, bit, m):
        for copy in self.copies(bit, m):
            copy.start()

    def add(self, bit, m):
        window = self.n_tp * self.rows
        for copy in self.copies(bit, m):
            copy.wait_recv()
        for key in self.keys(bit):
            target = key ^ bit

            @pl.loop(0, self.rows // STEP)
            def _(r):
                inner = pl.multiple_of(r * STEP, STEP)
                here = pl.ds(pl.multiple_of(m * self.rows + inner, STEP), STEP)
                there = pl.ds(pl.multiple_of(m * window + target * self.rows + inner, STEP), STEP)
                got = self.got[key - 1, here, :].astype(F32)
                if target == 0:
                    held = self.back[there, :].astype(F32) if bit == 1 else self.own[here, :]
                    self.own[here, :] = held + got
                else:
                    self.back[there, :] = (self.back[there, :].astype(F32) + got).astype(BF)

    def finish(self, bits=None):
        for m in range(self.micro):
            for bit in self.bits if bits is None else bits:
                for copy in self.copies(bit, m):
                    copy.wait_send()


def fill_decay(decay_v, col_ref, row_ref, rate_ref):
    heads, window, _ = decay_v.shape
    scale_qk = 1.0 / math.sqrt(HK)
    for h in range(heads):

        @pl.loop(0, window // LANE)
        def _(r):
            here = pl.ds(pl.multiple_of(r * LANE, LANE), LANE)
            col, row = col_ref[here, 0:1], row_ref[...]
            spacing = col - row
            same = jnp.floor(col * (1.0 / LEN)) == jnp.floor(row * (1.0 / LEN))
            kept = jnp.exp(jnp.maximum(spacing, 0.0) * rate_ref[h : h + 1, :]) * scale_qk
            decay_v[h, here, :] = jnp.where((spacing >= 0.0) & same, kept, 0.0)


def gelu_parts(pre_act):
    normal_cdf = 0.5 * (1.0 + lax.erf(pre_act * (1.0 / math.sqrt(2.0))))
    density = jnp.exp(-0.5 * pre_act * pre_act) * (1.0 / math.sqrt(2.0 * math.pi))
    return (pre_act * normal_cdf, normal_cdf + pre_act * density)


def forward_kernel(
    n,
    n_tp,
    x_ref,
    cot_ref,
    gains_ref,
    cos_ref,
    sin_ref,
    col_ref,
    row_ref,
    rate_ref,
    *refs,
):
    shards, refs = refs[:8], refs[8:]
    q_out, k_out, v_out, g_out, xr_out, cr_out, gain_out, nall_out, call_out = refs[:9]
    whole_outs, refs = refs[9:17], refs[17:]
    gated_out, middle_out, second_out, hidden_out, value_out, slope_out, near_out, far_out = refs[:8]
    nall_v, row_v, cot_v, gain_v, q_v, k_v, v_v, g_v, decay_v, got_v = refs[8:18]
    held, refs = refs[18:22], refs[22:]
    x_v, q_acc, k_acc, v_acc, wq_s, wk_s, wv_s, wg_s = refs[:8]
    back_v, own_v, gated_v, hidden_v, value_v, slope_v, up_v = refs[8:15]
    refs = refs[15:]
    ring_send, ring_recv, gain_send, gain_recv = refs[:4]
    first_send, first_recv, cot_send, cot_recv, share_send, share_recv = refs[4:10]
    part_send, part_recv, last_send, last_recv, load_sem, local_sem, out_sem = refs[10:]

    micro, rows, width = x_ref.shape
    window = n_tp * rows
    total, mine = micro * window, micro * rows
    dp, tp, cw, ccw = neighbours(n)
    pos = ring_position(dp, n)
    bits = bits_of(n_tp)
    heads = decay_v.shape[0]
    tile = 256
    half = HK // 2
    greet(
        [(ring_index((pos + k) % n, n), tp) for k in range(1, n)]
        + [(dp, partner(tp, bit)) for bit in bits]
    )

    wholes = tuple(whole_outs[:4]) + tuple(held)
    slots = (wq_s, wk_s, wv_s, wg_s)
    pieces = [(a, 0, slots[a].shape[1]) for a in range(4)]
    groups = [(0, 1, 2, 3)]
    for pair in ((4,), (5, 6), (7,)):
        group = []
        for a in pair:
            size = shards[a].shape[0]
            parts = SPLIT if len(pair) == 1 else 1
            cuts = [size * j // parts // 16 * 16 for j in range(parts)] + [size]
            for low, high in zip(cuts, cuts[1:]):
                group.append(len(pieces))
                pieces.append((a, low, high - low))
        groups.append(tuple(group))
    ring_a, ring_b, ring_c, ring_d = groups

    def hop(i, p, side):
        a, low, size = pieces[p]
        span, lanes = pl.ds(low, size), pl.ds(side * LANE, LANE)
        if not (isinstance(i, int) and i == 0):
            source = wholes[a].at[i, span, lanes]
        elif a < 2:
            source = slots[a].at[0, span, lanes]
        else:
            source = shards[a].at[span, lanes]
        return pltpu.make_async_remote_copy(
            src_ref=source,
            dst_ref=wholes[a].at[i + 1, span, lanes],
            send_sem=ring_send.at[i, p, side],
            recv_sem=ring_recv.at[i, p, side],
            device_id=((cw, ccw)[side], tp),
            device_id_type=MESH,
        )

    def ring_start(group):
        for p in group:
            for side in range(2):
                hop(0, p, side).start()

    def ring_pass(s, p):
        for side in range(2):
            hop(s - 1, p, side).wait_recv()
            if isinstance(s, int):
                if s < n - 1:
                    hop(s, p, side).start()
            else:

                @pl.when(s < n - 1)
                def _():
                    hop(s, p, side).start()

    def ring_step(s, group, following=()):
        for p in group:
            ring_pass(s, p)
        if isinstance(s, int) and s == n - 2:
            ring_start(following)

    def store(source, target):
        copy = pltpu.make_async_copy(source, target, out_sem.at[len(stores)])
        copy.start()
        stores.append(copy)

    stores = []
    turned = [
        pltpu.make_async_copy(shards[a], (q_v, k_v)[a].at[pl.ds(0, BLOCK)], local_sem.at[2 + a])
        for a in range(2)
    ]
    for copy in turned:
        copy.start()
    ring_start(ring_a[2:])
    for a in range(2):
        turned[a].wait()
        natural_block = (q_v, k_v)[a][pl.ds(0, BLOCK), :]
        slots[a][0] = natural_block.astype(F32).T.astype(BF)
        ring_start(ring_a[a : a + 1])
    own_blocks = [
        pltpu.make_async_copy(shards[4 + i], held[i].at[0], local_sem.at[4 + i]) for i in range(4)
    ]

    def natural(i, side):
        at = ring_index((pos + (n - i if side == 0 else i)) % n, n) * BLOCK + side * LANE
        return pl.ds(pl.multiple_of(at, LANE), LANE)

    first = Share(dp, tp, n_tp, micro, rows, nall_v, first_send, first_recv)
    share = Share(dp, tp, n_tp, micro, rows, nall_v, share_send, share_recv)

    def cot_copy(bit, m, key):
        source = cot_v.at[pl.ds(m * rows, rows)]
        if key:
            source = call_out.at[pl.ds(m * window + key * rows, rows)]
        return pltpu.make_async_remote_copy(
            src_ref=source,
            dst_ref=call_out.at[pl.ds(m * window + (key ^ bit) * rows, rows)],
            send_sem=cot_send.at[m, key ^ bit],
            recv_sem=cot_recv.at[m, key ^ bit],
            device_id=(dp, partner(tp, bit)),
            device_id_type=MESH,
        )

    def cot_copies(bit, keys=None):
        for m in range(micro):
            for key in range(0, n_tp, 2 * bit):
                if keys is None or (key == 0) == keys:
                    yield cot_copy(bit, m, key)

    def project():
        cot_rel_v = own_v
        accs = (q_acc, k_acc, v_acc, g_v)

        def load(i, a):
            source = shards[a] if i == 0 else wholes[a].at[i]
            return pltpu.make_async_copy(
                source, slots[a].at[i % SLOTS], load_sem.at[i % SLOTS, a]
            )

        x_copy = pltpu.make_async_copy(x_ref, x_v, local_sem.at[0])
        x_copy.start()
        for a in range(2, 4):
            load(0, a).start()

        def gain_copy(k):
            return pltpu.make_async_remote_copy(
                src_ref=gains_ref,
                dst_ref=gain_v.at[k],
                send_sem=gain_send.at[k],
                recv_sem=gain_recv.at[k],
                device_id=(ring_index((pos + k) % n, n), tp),
                device_id_type=MESH,
            )

        own_gain = pltpu.make_async_copy(gains_ref, gain_v.at[0], local_sem.at[1])
        own_gain.start()
        for k in range(1, n):
            gain_copy(k).start()
        own_gain.wait()
        for k in range(1, n):
            gain_copy(k).wait()
        for i in range(n):
            gain_out[:, pl.ds(i * BLOCK, LANE)] = gain_v[i, :, pl.ds(0, LANE)]
            gain_out[:, pl.ds(i * BLOCK + LANE, LANE)] = gain_v[(n - i) % n, :, pl.ds(LANE, LANE)]
        x_copy.wait()

        def each_part(work):
            @pl.loop(0, mine // STEP)
            def _(r):
                at = pl.multiple_of(r * STEP, STEP)
                m, inner = at // rows, pl.multiple_of(at % rows, STEP)
                work(at, m, inner)

        def normalize_part(at, m, inner):
            chunk = x_v[m, pl.ds(inner, STEP), :]
            scale = lax.rsqrt(jnp.mean(chunk * chunk, axis=-1, keepdims=True) + EPS)
            there = pl.ds(pl.multiple_of(m * window + inner, STEP), STEP)
            for i in range(n):
                for side in range(2):
                    lanes = pl.ds(i * BLOCK + side * LANE, LANE)
                    part = x_v[m, pl.ds(inner, STEP), natural(i, side)]
                    row_v[pl.ds(at, STEP), lanes] = part
                    nall_v[there, lanes] = (part * scale * gain_out[0:1, lanes]).astype(BF)

        each_part(normalize_part)
        for m in range(micro):
            first.begin(m)
        store(row_v, xr_out)
        c_copy = pltpu.make_async_copy(cot_ref, x_v, local_sem.at[0])
        c_copy.start()
        cot_rel = pltpu.make_async_copy(cot_rel_v, cr_out, local_sem.at[1])

        def cot_part(at, m, inner):
            for i in range(n):
                for side in range(2):
                    lanes = pl.ds(i * BLOCK + side * LANE, LANE)
                    part = x_v[m, pl.ds(inner, STEP), natural(i, side)]
                    cot_rel_v[pl.ds(at, STEP), lanes] = part
                    cot_v[pl.ds(at, STEP), lanes] = part.astype(BF)

        def take_cot():
            c_copy.wait()
            each_part(cot_part)
            cot_rel.start()
            for m in range(micro):
                store(cot_v.at[pl.ds(m * rows, rows)], call_out.at[pl.ds(m * window, rows)])
            for copy in own_blocks:
                copy.start()

        def product(j, a, last):
            if j > 0 or a > 1:
                load(j, a).wait()
            if j == 0:
                pltpu.make_async_copy(
                    slots[a].at[0], wholes[a].at[0], load_sem.at[SLOTS, a]
                ).start()

            @pl.loop(0, total // tile)
            def _(r):
                at = pl.multiple_of(r * tile, tile)
                here = pl.ds(at, tile)
                part = nt(nall_v[here, pl.ds(j * BLOCK, BLOCK)], slots[a][j % SLOTS])
                if j > 0:
                    part = accs[a][here, :] + part
                if not last or a == 3:
                    accs[a][here, :] = part
                elif a == 2:
                    v_v[here, :] = part.astype(BF)
                else:
                    place = pl.ds(pl.multiple_of(at % window, tile), tile)
                    cosine, sine = cos_ref[place, :], sin_ref[place, :]
                    out = (q_v, k_v)[a]
                    for h in range(heads):
                        low = part[:, h * HK : h * HK + half]
                        high = part[:, h * HK + half : (h + 1) * HK]
                        out[here, pl.ds(h * HK, half)] = (low * cosine - high * sine).astype(BF)
                        out[here, pl.ds(h * HK + half, half)] = (
                            high * cosine + low * sine
                        ).astype(BF)

            if j == 0:
                pltpu.make_async_copy(
                    slots[a].at[0], wholes[a].at[0], load_sem.at[SLOTS, a]
                ).wait()

        start_at, done = 3, 0
        for i in range(n + 1):
            if i == 2:
                take_cot()
                fill_decay(decay_v, col_ref, row_ref, rate_ref)
            if i == start_at:
                for m in range(micro):
                    first.relay(m)
                store(nall_v, nall_out)
                for bit in bits[::-1]:
                    for copy in cot_copies(bit, True):
                        copy.start()
            if i == n - 1:
                for bit in bits[::-1]:
                    for copy in cot_copies(bit, False):
                        copy.start()
                    for copy in cot_copies(bit):
                        copy.wait_recv()
            todo = []
            if i >= start_at:
                goal = min(i - 1, done + 1) if i < n else n - 1
                todo = list(range(done, goal + 1))
                done = goal + 1
            for a in range(4):
                if 0 < i < n:
                    ring_pass(i, a)
                if i == n - 2 and a == 3:
                    ring_start(ring_b)
                for j in todo:
                    product(j, a, j == n - 1)
                if 0 < i < n:
                    if i == SLOTS and a < 2:
                        hop(0, a, 0).wait_send()
                        hop(0, a, 1).wait_send()
                    load(i, a).start()
                if i == n:
                    source, target = ((q_v, q_out), (k_v, k_out), (v_v, v_out), (g_v, g_out))[a]
                    store(source, target)
        cot_rel.wait()

    project()
    wo_v, wu_v, wl_v, wd_v = held
    units = shards[7].shape[0]

    def middle_part():
        for copy in own_blocks:
            copy.wait()

        def attend(m, h):
            keys = pl.ds(h * HK, HK)
            values = pl.ds(h * HV, HV)
            inside = pl.ds(m * window, window)

            @pl.loop(0, window // tile)
            def _(r):
                at = pl.multiple_of(r * tile, tile)
                here = pl.ds(pl.multiple_of(m * window + at, tile), tile)
                scores = nt(q_v[here, keys], k_v[inside, keys])
                weight = (scores * decay_v[h, pl.ds(at, tile), :]).astype(BF)
                kept = nn(weight, v_v[inside, values])
                group = lax.rsqrt(jnp.mean(kept * kept, axis=-1, keepdims=True) + GROUP_EPS)
                gate = g_v[here, values]
                gated_v[here, values] = (gate * jax.nn.sigmoid(gate) * (kept * group)).astype(BF)

        def times_blocks(left, weights, low, high):
            if low == high:
                return

            @pl.loop(low, high)
            def _(i):
                columns = pl.ds(pl.multiple_of(i * BLOCK, BLOCK), BLOCK)

                @pl.loop(0, total // tile)
                def _(r):
                    here = pl.ds(pl.multiple_of(r * tile, tile), tile)
                    back_v[here, columns] = nn(left[here, :], weights[i]).astype(BF)

        collect = Collect(dp, tp, n_tp, micro, rows, back_v, got_v, own_v, part_send, part_recv)
        jobs = [(m, h) for m in range(micro) for h in range(heads)]
        reached = 0
        while jobs:
            if reached < n - 1:
                reached += 1
                ring_step(reached, ring_b, ring_c)
            attend(*jobs.pop(0))
        store(gated_v, gated_out)
        ready = 0
        while ready < n:
            if reached < n - 1:
                reached += 1
                ring_step(reached, ring_b, ring_c)
            goal = min(n, reached + 1, ready + (2 if reached < n - 1 else n))
            times_blocks(gated_v, wo_v, ready, goal)
            ready = goal
        store(wo_v, whole_outs[4])
        first.finish()
        stores[0].wait()
        stores[micro + 1].wait()
        for m in range(micro):
            collect.start(bits[0], m)
        passed = [0]

        def pairs_to(goal):
            while passed[0] < min(goal, n - 1):
                passed[0] += 1
                ring_step(passed[0], ring_c, ring_d)

        for at, bit in enumerate(bits[:-1]):
            for m in range(micro):
                collect.add(bit, m)
                collect.start(bits[at + 1], m)
        pairs_to(1)
        for m in range(micro):
            pairs_to(2 + m)
            collect.add(bits[-1], m)

            @pl.loop(0, rows // STEP)
            def _(r):
                inner = pl.multiple_of(r * STEP, STEP)
                here = pl.ds(pl.multiple_of(m * rows + inner, STEP), STEP)
                there = pl.ds(pl.multiple_of(m * window + inner, STEP), STEP)
                middle = row_v[here, :] + own_v[here, :]
                row_v[here, :] = middle
                scale = lax.rsqrt(jnp.mean(middle * middle, axis=-1, keepdims=True) + EPS)
                nall_v[there, :] = (middle * scale * gain_out[1:2, :]).astype(BF)

            share.begin(m)
        store(row_v, middle_out)
        pairs_to(4)
        for m in range(micro):
            share.relay(m)
            pairs_to(5 + m)
        pairs_to(n - 1)
        store(nall_v, second_out)
        store(wu_v, whole_outs[5])
        store(wl_v, whole_outs[6])

        def rows_by(weights, here):
            result = None
            for i in range(n):
                term = nt(nall_v[here, pl.ds(i * BLOCK, BLOCK)], weights[i])
                result = term if result is None else result + term
            return result

        tiles = total // tile
        every = max(1, tiles // 2)
        inside_loop = min(tiles // every, n - 1)

        @pl.loop(0, tiles)
        def _(r):
            here = pl.ds(pl.multiple_of(r * tile, tile), tile)
            up_v[...] = rows_by(wu_v, here)
            gelu_val, gelu_slope = gelu_parts(rows_by(wl_v, here))
            up = up_v[...]
            hidden_v[here, :] = (gelu_val * up).astype(BF)
            value_v[here, :] = gelu_val.astype(BF)
            slope_v[here, :] = (up * gelu_slope).astype(BF)

            @pl.when((r % every == every - 1) & (r // every < inside_loop))
            def _():
                ring_step(r // every + 1, ring_d)

        store(hidden_v, hidden_out)
        store(value_v, value_out)
        store(slope_v, slope_out)
        collect.finish()
        ready = 0
        for s in range(inside_loop, n):
            if s > inside_loop:
                ring_step(s, ring_d)
            goal = min(n, s + 1, ready + (2 if s < n - 1 else n))
            times_blocks(hidden_v, wd_v, ready, goal)
            ready = goal
        store(wd_v, whole_outs[7])
        last = Collect(dp, tp, n_tp, micro, rows, back_v, got_v, own_v, last_send, last_recv)
        for at, bit in enumerate(bits[:-1]):
            for m in range(micro):
                last.start(bit, m)
            for m in range(micro):
                last.add(bit, m)
        store(own_v, near_out)
        for m in range(micro):
            store(
                back_v.at[pl.ds(m * window + bits[-1] * rows, rows)],
                far_out.at[pl.ds(m * rows, rows)],
            )
        last.finish(bits[:-1])
        for i in range(n - 1):
            for p in range(0 if i > 0 else 2, len(pieces)):
                hop(i, p, 0).wait_send()
                hop(i, p, 1).wait_send()
        share.finish()
        for bit in bits:
            for copy in cot_copies(bit):
                copy.wait_send()
        for at, copy in enumerate(stores):
            if at not in waited:
                copy.wait()

    waited = (0, micro + 1)
    middle_part()


def forward(n, n_tp, x, cot, gains, cosine, sine, tables, weights):
    micro, rows, width = x.shape
    window = n_tp * rows
    total, mine = micro * window, micro * rows
    sizes = [w.shape[1] for w in weights[:2]] + [w.shape[0] for w in weights[2:]]
    hv, units = sizes[2], sizes[7]
    shape = jax.ShapeDtypeStruct
    dma = pltpu.SemaphoreType.DMA
    count = 4 + SPLIT + 2 + SPLIT
    return pl.pallas_call(
        functools.partial(forward_kernel, n, n_tp),
        out_shape=(
            shape((total, sizes[0]), BF),
            shape((total, sizes[1]), BF),
            shape((total, hv), BF),
            shape((total, sizes[3]), F32),
            shape((mine, width), F32),
            shape((mine, width), F32),
            shape((2, width), F32),
            shape((total, width), BF),
            shape((total, width), BF),
        )
        + tuple(shape((n, s, BLOCK), BF) for s in sizes)
        + (
            shape((total, hv), BF),
            shape((mine, width), F32),
            shape((total, width), BF),
            shape((total, units), BF),
            shape((total, units), BF),
            shape((total, units), BF),
            shape((mine, width), F32),
            shape((mine, width), BF),
        ),
        in_specs=[anyspec()] * 3 + [vmem()] * 5 + [anyspec()] * 8,
        out_specs=(anyspec(),) * 6 + (vmem(),) + (anyspec(),) * 18,
        scratch_shapes=[
            pltpu.VMEM((total, width), BF),
            pltpu.VMEM((mine, width), F32),
            pltpu.VMEM((mine, width), BF),
            pltpu.VMEM((n, 2, BLOCK), F32),
            pltpu.VMEM((total, sizes[0]), BF),
            pltpu.VMEM((total, sizes[1]), BF),
            pltpu.VMEM((total, hv), BF),
            pltpu.VMEM((total, sizes[3]), F32),
            pltpu.VMEM((tables[2].shape[0], window, window), F32),
            pltpu.VMEM((n_tp - 1, mine, width), BF),
        ]
        + [pltpu.VMEM((n, s, BLOCK), BF) for s in sizes[4:]]
        + [pltpu.VMEM((micro, rows, width), F32)]
        + [pltpu.VMEM((total, s), F32) for s in sizes[:3]]
        + [pltpu.VMEM((SLOTS, s, BLOCK), BF) for s in sizes[:4]]
        + [
            pltpu.VMEM((total, width), BF),
            pltpu.VMEM((mine, width), F32),
            pltpu.VMEM((total, hv), BF),
            pltpu.VMEM((total, units), BF),
            pltpu.VMEM((total, units), BF),
            pltpu.VMEM((total, units), BF),
            pltpu.VMEM((256, units), F32),
        ]
        + [dma((n - 1, count, 2))] * 2
        + [dma((n,))] * 2
        + [dma((micro, n_tp))] * 6
        + [dma((n_tp - 1, micro))] * 4
        + [dma((SLOTS + 1, 4)), dma((8,)), dma((19 + micro,))],
        compiler_params=pltpu.CompilerParams(
            collective_id=1, has_side_effects=True, vmem_limit_bytes=66_500_000
        ),
        cost_estimate=pl.CostEstimate(
            flops=2 * total * width * sum(sizes), bytes_accessed=120_000_000, transcendentals=0
        ),
        name="forward_kernel",
    )(x, cot, gains, cosine, sine, *tables, *weights)


class LaneRing:
    def __init__(self, n, tp, cw, ccw, lanes, fresh, free, soon, done):
        self.n, self.tp, self.ways, self.lanes = n, tp, (cw, ccw), lanes
        self.fresh, self.free, self.soon, self.done = fresh, free, soon, done
        self.state = [dict(job=0, step=1, firsts=0, ready=False) for _ in lanes]
        self.allowed = [0 for _ in lanes]

    def hop(self, p, t):
        lane = self.lanes[p]
        size = lane["jobs"][t // (self.n - 1)][0]
        slots = lane["recv"].shape[0]
        copies = []
        for side in range(2):
            lanes = pl.ds(side * LANE, LANE)
            copies.append(
                pltpu.make_async_remote_copy(
                    src_ref=lane["send"].at[t % 2, pl.ds(0, size), lanes],
                    dst_ref=lane["recv"].at[t % slots, pl.ds(0, size), lanes],
                    send_sem=lane["send_sem"].at[t, side],
                    recv_sem=lane["recv_sem"].at[t, side],
                    device_id=(self.ways[side], self.tp),
                    device_id_type=MESH,
                )
            )
        return copies

    def fill(self, p, t, size, value_of):
        lane = self.lanes[p]
        if t >= 2:
            for copy in self.hop(p, t - 2):
                copy.wait_send()

        @pl.loop(0, size // STEP)
        def _(r):
            here = pl.ds(pl.multiple_of(r * STEP, STEP), STEP)
            lane["send"][t % 2, here, :] = value_of(here).astype(BF)

    def launch(self, p, t):
        slots = self.lanes[p]["recv"].shape[0]
        for side, copy in enumerate(self.hop(p, t)):
            if t >= slots:
                pl.semaphore_wait(self.free.at[p, side], 1)
            copy.start()

    def first(self, p):
        lane, state = self.lanes[p], self.state[p]
        job = state["firsts"]
        size, gradient, _ = lane["jobs"][job]
        state["firsts"] += 1
        gradient(1 % self.n, self.fresh.at[pl.ds(0, size)])
        self.fill(p, job * (self.n - 1), size, lambda here: self.fresh[here, :])
        self.launch(p, job * (self.n - 1))

    def prepare(self):
        for p, lane in enumerate(self.lanes):
            state = self.state[p]
            if state["job"] < state["firsts"] and not state["ready"]:
                size, gradient, _ = lane["jobs"][state["job"]]
                gradient((state["step"] + 1) % self.n, lane["part"].at[pl.ds(0, size)])
                state["ready"] = True

    def advance(self, only=(0, 1)):
        n = self.n
        self.prepare()
        for p in only:
            lane = self.lanes[p]
            state = self.state[p]
            job, step = state["job"], state["step"]
            count = len(lane["jobs"])
            if job >= state["firsts"]:
                if job < min(count, self.allowed[p]):
                    self.first(p)
                continue
            if step == n - 1 and state["firsts"] == job + 1 < min(count, self.allowed[p]):
                self.first(p)
            size, _, out = lane["jobs"][job]
            t = job * (n - 1) + step - 1
            slots = lane["recv"].shape[0]
            for copy in self.hop(p, t):
                copy.wait_recv()

            def value_of(here, lane=lane, slot=t % slots):
                return lane["part"][here, :] + lane["recv"][slot, here, :].astype(F32)

            state["ready"] = False
            if step == n - 1:
                self.done(p, job, size, value_of, out)
                state["job"], state["step"] = job + 1, 1
            else:
                self.fill(p, t + 1, size, value_of)
            if t + slots < count * (n - 1):
                for side in range(2):
                    pl.semaphore_signal(
                        self.free.at[p, side],
                        inc=1,
                        device_id=(self.ways[1 - side], self.tp),
                        device_id_type=MESH,
                    )
            if step < n - 1:
                self.launch(p, t + 1)
                state["step"] = step + 1
                if step == n - 2:
                    self.soon(p, out)

    def busy(self):
        return any(s["job"] < len(lane["jobs"]) for s, lane in zip(self.state, self.lanes))

    def finish(self):
        for p, lane in enumerate(self.lanes):
            last = len(lane["jobs"]) * (self.n - 1)
            for t in range(max(0, last - 2), last):
                for copy in self.hop(p, t):
                    copy.wait_send()


def backward_kernel(
    n,
    n_tp,
    gain_ref,
    own_gain_ref,
    col_ref,
    row_ref,
    rate_ref,
    cos_ref,
    sin_ref,
    *refs,
):
    hidden_ref, cot_ref, value_ref, slope_ref, second_ref, middle_ref, cotf_ref = refs[:7]
    q_ref, k_ref, v_ref, g_ref, gated_ref, nall_ref, x_ref = refs[7:14]
    wq_ref, wk_ref, wv_ref, wg_ref, wo_ref, wu_ref, wl_ref, wd_ref = refs[14:22]
    refs = refs[22:]
    dd_out, du_out, dl_out, do_out, ds_out, dv_out, dq_out, dk_out, sum_out, rows_out = refs[:10]
    cot_v, w_v, gu_v, gl_v, hidden_v, second_v, wu_s, wl_s, middle_v, cotf_v = refs[10:20]
    q_v, k_v, v_v, g_v, gs_v, gated_v, decay_v, gk_acc, gv_acc = refs[20:29]
    back_v, own_v, got_v, mall_v, rows_v, part0, part1, fresh_v = refs[29:37]
    send0, send1, recv0, recv1, done_v, own_w, sum_v = refs[37:44]
    ring_send0, ring_send1, ring_recv0, ring_recv1, ring_free = refs[44:49]
    part_send, part_recv, last_send, last_recv, share_send, share_recv = refs[49:55]
    sum_send, sum_recv, load_sem, done_sem, own_sem, local_sem = refs[55:]

    total, width = cot_v.shape
    mine = own_v.shape[0]
    window = col_ref.shape[0]
    micro = total // window
    rows = mine // micro
    heads = decay_v.shape[0]
    dp, tp, cw, ccw = neighbours(n)
    pos = ring_position(dp, n)
    bits = bits_of(n_tp)
    tile = 256
    half = HK // 2
    greet([(cw, tp), (ccw, tp)] + [(dp, partner(tp, bit)) for bit in bits])

    pairs = (
        (hidden_ref, hidden_v),
        (cot_ref, cot_v),
        (wd_ref, w_v),
        (value_ref, gu_v),
        (slope_ref, gl_v),
        (second_ref, second_v),
        (middle_ref, middle_v),
        (cotf_ref, cotf_v),
        (q_ref, q_v),
        (k_ref, k_v),
        (v_ref, v_v),
        (g_ref, g_v),
    )
    loads = [
        pltpu.make_async_copy(source, target, local_sem.at[at])
        for at, (source, target) in enumerate(pairs)
    ]
    for copy in loads[:2]:
        copy.start()

    def block_load(i, a):
        source, target = ((wu_ref, wu_s), (wl_ref, wl_s))[a]
        return pltpu.make_async_copy(
            source.at[i % n], target.at[i % 2], load_sem.at[i % 2, a]
        )

    def product(left, right):
        def gradient(i, target):
            @pl.loop(0, total // tile)
            def _(r):
                here = pl.ds(pl.multiple_of(r * tile, tile), tile)
                term = tn(left[here, :], right[here, pl.ds(i * BLOCK, BLOCK)])
                target[...] = jnp.where(r == 0, 0.0, target[...]) + term

        return gradient

    units, hv, hk = gu_v.shape[1], v_v.shape[1], q_v.shape[1]
    lanes = (
        dict(
            jobs=(
                (units, product(hidden_v, cot_v), (dd_out, None)),
                (units, product(gl_v, second_v), (dl_out, wl_ref)),
                (hv, product(gs_v, cot_v), (ds_out, wg_ref)),
                (hk, product(q_v, cot_v), (dq_out, wq_ref)),
            ),
            part=part0,
            send=send0,
            recv=recv0,
            send_sem=ring_send0,
            recv_sem=ring_recv0,
        ),
        dict(
            jobs=(
                (units, product(gu_v, second_v), (du_out, wu_ref)),
                (hv, product(hidden_v, mall_v), (do_out, None)),
                (hv, product(v_v, cot_v), (dv_out, wv_ref)),
                (hk, product(k_v, cot_v), (dk_out, wk_ref)),
            ),
            part=part1,
            send=send1,
            recv=recv1,
            send_sem=ring_send1,
            recv_sem=ring_recv1,
        ),
    )
    pending = {}

    def own_copy(p, weight):
        held = own_w.at[p, pl.ds(0, weight.shape[1])]
        return pltpu.make_async_copy(weight.at[0], held, own_sem.at[p])

    def soon(p, out):
        if out[1] is not None:
            own_copy(p, out[1]).start()

    def done(p, job, size, value_of, out):
        target, weight = out
        if p in pending:
            pending.pop(p).wait()

        @pl.loop(0, size // STEP)
        def _(r):
            here = pl.ds(pl.multiple_of(r * STEP, STEP), STEP)
            done_v[p, here, :] = value_of(here)

        pending[p] = pltpu.make_async_copy(
            done_v.at[p, pl.ds(0, size)], target, done_sem.at[p]
        )
        pending[p].start()
        if weight is not None:
            own_copy(p, weight).wait()
            line = jnp.sum(
                own_w[p, pl.ds(0, size), :].astype(F32) * done_v[p, pl.ds(0, size), :],
                axis=0,
                keepdims=True,
            )
            at = 1 if job < 2 else 0
            sum_v[0, at : at + 1, :] = sum_v[0, at : at + 1, :] + line

    sum_v[...] = jnp.zeros_like(sum_v)
    ring = LaneRing(n, tp, cw, ccw, lanes, fresh_v, ring_free, soon, done)
    loads[0].wait()
    loads[1].wait()
    for copy in loads[2:5]:
        copy.start()
    ring.allowed = [1, 0]
    ring.first(0)
    for copy in loads[2:5]:
        copy.wait()
    block_load(0, 0).start()
    block_load(0, 1).start()
    for copy in loads[5:]:
        copy.start()

    @pl.loop(0, total // tile)
    def _(r):
        here = pl.ds(pl.multiple_of(r * tile, tile), tile)
        grad = None
        for i in range(n):
            term = nt(cot_v[here, pl.ds(i * BLOCK, BLOCK)], w_v[i])
            grad = term if grad is None else grad + term
        gu_v[here, :] = (grad * gu_v[here, :].astype(F32)).astype(BF)
        gl_v[here, :] = (grad * gl_v[here, :].astype(F32)).astype(BF)

    wo_load = pltpu.make_async_copy(wo_ref, w_v, local_sem.at[2])
    wo_load.start()
    ring.advance((0,))
    loads[5].wait()
    ring.allowed = [2, 1]
    ring.first(1)
    ring.prepare()
    collect = Collect(dp, tp, n_tp, micro, rows, back_v, got_v, own_v, part_send, part_recv)
    share = Share(dp, tp, n_tp, micro, rows, mall_v, share_send, share_recv)
    for m in range(micro):

        @pl.loop(0, n)
        def _(i):
            at = m * n + i
            for a in range(2):
                block_load(at, a).wait()

                @pl.when(at + 1 < micro * n)
                def _():
                    block_load(at + 1, a).start()

            block = pl.ds(pl.multiple_of(i * BLOCK, BLOCK), BLOCK)

            @pl.loop(0, window // tile)
            def _(r):
                here = pl.ds(pl.multiple_of(m * window + r * tile, tile), tile)
                back_v[here, block] = (
                    nn(gu_v[here, :], wu_s[at % 2]) + nn(gl_v[here, :], wl_s[at % 2])
                ).astype(BF)

        collect.start(bits[0], m)
        ring.advance()
        ring.prepare()
    for at, bit in enumerate(bits[:-1]):
        for m in range(micro):
            collect.add(bit, m)
            collect.start(bits[at + 1], m)
    fill_decay(decay_v, col_ref, row_ref, rate_ref)
    loads[6].wait()
    loads[7].wait()
    for m in range(micro):
        ring.advance()
        ring.prepare()
        collect.add(bits[-1], m)

        @pl.loop(0, rows // STEP)
        def _(r):
            inner = pl.multiple_of(r * STEP, STEP)
            here = pl.ds(pl.multiple_of(m * rows + inner, STEP), STEP)
            there = pl.ds(pl.multiple_of(m * window + inner, STEP), STEP)
            middle = middle_v[here, :]
            scale = lax.rsqrt(jnp.mean(middle * middle, axis=-1, keepdims=True) + EPS)
            scaled = own_v[here, :] * gain_ref[1:2, :]
            inside = jnp.mean(scaled * middle, axis=-1, keepdims=True)
            grad = cotf_v[here, :] + scale * (scaled - middle * (scale * scale * inside))
            cotf_v[here, :] = grad
            mall_v[there, :] = grad.astype(BF)

        share.begin(m)
    x_load = pltpu.make_async_copy(x_ref, middle_v, local_sem.at[6])
    x_load.start()
    collect.finish()
    ring.advance()
    ring.prepare()
    for copy in loads[8:]:
        copy.wait()
    wo_load.wait()
    gated_load = None
    for m in range(micro):
        share.relay(m)
        if m == micro - 1 and gated_load is not None:
            gated_load.wait()
            ring.allowed = [2, 2]
        ring.advance()
        ring.prepare()
        for h in range(heads):
            keys = pl.ds(h * HK, HK)
            values = pl.ds(h * HV, HV)
            inside = pl.ds(m * window, window)
            gk_acc[...] = jnp.zeros_like(gk_acc)
            gv_acc[...] = jnp.zeros_like(gv_acc)

            @pl.loop(0, window // tile)
            def _(r):
                at = pl.multiple_of(r * tile, tile)
                here = pl.ds(pl.multiple_of(m * window + at, tile), tile)
                grad = None
                for i in range(n):
                    term = nt(mall_v[here, pl.ds(i * BLOCK, BLOCK)], w_v[i, values, :])
                    grad = term if grad is None else grad + term
                gated_v[pl.ds(at, tile), :] = grad

            @pl.loop(0, window // tile)
            def _(r):
                at = pl.multiple_of(r * tile, tile)
                local = pl.ds(at, tile)
                here = pl.ds(pl.multiple_of(m * window + at, tile), tile)
                decay = decay_v[h, local, :]
                query = q_v[here, keys]
                weight = (nt(query, k_v[inside, keys]) * decay).astype(BF)
                kept = nn(weight, v_v[inside, values])
                group = lax.rsqrt(jnp.mean(kept * kept, axis=-1, keepdims=True) + GROUP_EPS)
                gate = g_v[here, values]
                sigmoid = jax.nn.sigmoid(gate)
                grad = gated_v[local, :]
                gs_v[here, values] = (
                    grad * (kept * group) * (sigmoid * (1.0 + gate * (1.0 - sigmoid)))
                ).astype(BF)
                lifted = grad * (gate * sigmoid)
                mean = jnp.mean(lifted * kept, axis=-1, keepdims=True)
                grad_kept = (group * (lifted - kept * (group * group * mean))).astype(BF)
                gv_acc[...] += tn(weight, grad_kept)
                score = (nt(grad_kept, v_v[inside, values]) * decay).astype(BF)
                gk_acc[...] += tn(score, query)
                turned = nn(score, k_v[inside, keys])
                low, high = turned[:, :half], turned[:, half:]
                cosine, sine = cos_ref[local, :], sin_ref[local, :]
                q_v[here, pl.ds(h * HK, half)] = (low * cosine + high * sine).astype(BF)
                q_v[here, pl.ds(h * HK + half, half)] = (high * cosine - low * sine).astype(BF)

            low, high = gk_acc[:, :half], gk_acc[:, half:]
            cosine, sine = cos_ref[...], sin_ref[...]
            k_v[inside, pl.ds(h * HK, half)] = (low * cosine + high * sine).astype(BF)
            k_v[inside, pl.ds(h * HK + half, half)] = (high * cosine - low * sine).astype(BF)
            v_v[inside, values] = gv_acc[...].astype(BF)
            ring.advance()
            if ring.state[0]["job"] > 0 and gated_load is None:
                gated_load = pltpu.make_async_copy(gated_ref, hidden_v, local_sem.at[0])
                gated_load.start()
                nall_load = pltpu.make_async_copy(nall_ref, cot_v, local_sem.at[1])
                nall_load.start()
            ring.prepare()

    def settle():
        while ring.state[0]["job"] == 0:
            ring.advance()

    if gated_load is None:
        settle()
        gated_load = pltpu.make_async_copy(gated_ref, hidden_v, local_sem.at[0])
        gated_load.start()
        nall_load = pltpu.make_async_copy(nall_ref, cot_v, local_sem.at[1])
        nall_load.start()
    if ring.allowed[1] < 2:
        gated_load.wait()
    nall_load.wait()
    ring.allowed = [4, 4]

    wholes = (wq_ref, wk_ref, wv_ref, wg_ref)
    grads = (q_v, k_v, v_v, gs_v)
    sizes = (hk, hk, hv, hv)

    def weight_slot(i, a):
        return w_v.at[2 * a + i % 2, pl.ds(0, sizes[a])]

    def weight_load(i, a):
        return pltpu.make_async_copy(
            wholes[a].at[i], weight_slot(i, a), load_sem.at[2 + i % 2, a]
        )

    for a in range(4):
        weight_load(0, a).start()
    ring.advance()
    ring.prepare()
    for pair in range(n // 2):

        @pl.loop(2 * pair, 2 * pair + 2)
        def _(i):
            for a in range(4):
                weight_load(i, a).wait()

                @pl.when(i + 1 < n)
                def _():
                    weight_load(i + 1, a).start()

            columns = pl.ds(pl.multiple_of(i * BLOCK, BLOCK), BLOCK)

            @pl.loop(0, total // tile)
            def _(r):
                here = pl.ds(pl.multiple_of(r * tile, tile), tile)
                block = None
                for a in range(4):
                    term = nn(grads[a][here, :], weight_slot(i, a)[...])
                    block = term if block is None else block + term
                back_v[here, columns] = block.astype(BF)

        ring.advance()
        ring.prepare()
    last = Collect(dp, tp, n_tp, micro, rows, back_v, got_v, own_v, last_send, last_recv)
    for m in range(micro):
        last.start(bits[0], m)
    ring.advance()
    ring.prepare()
    for at, bit in enumerate(bits):
        for m in range(micro):
            last.add(bit, m)
            if at + 1 < len(bits):
                last.start(bits[at + 1], m)
        if at + 1 < len(bits):
            for _ in range(3):
                ring.advance()
                ring.prepare()
    x_load.wait()

    def natural(i, side):
        at = ring_index((pos + (n - i if side == 0 else i)) % n, n) * BLOCK + side * LANE
        return pl.ds(pl.multiple_of(at, LANE), LANE)

    @pl.loop(0, mine // STEP)
    def _(r):
        at = pl.multiple_of(r * STEP, STEP)
        m, inner = at // rows, pl.multiple_of(at % rows, STEP)
        here = pl.ds(at, STEP)
        x = middle_v[here, :]
        scale = lax.rsqrt(jnp.mean(x * x, axis=-1, keepdims=True) + EPS)
        inside = jnp.mean(own_v[here, :] * gain_ref[0:1, :] * x, axis=-1, keepdims=True)
        slope = scale * scale * inside
        for i in range(n):
            for side in range(2):
                lanes = pl.ds(i * BLOCK + side * LANE, LANE)
                scaled = own_v[here, lanes] * gain_ref[0:1, lanes]
                rows_v[m, pl.ds(inner, STEP), natural(i, side)] = cotf_v[
                    here, lanes
                ] + scale * (scaled - middle_v[here, lanes] * slope)

    rows_copy = pltpu.make_async_copy(rows_v, rows_out, local_sem.at[2])
    rows_copy.start()
    while ring.busy():
        ring.advance()
        ring.prepare()
    for at, bit in enumerate(bits):
        swap = pltpu.make_async_remote_copy(
            src_ref=sum_v.at[2 * at],
            dst_ref=sum_v.at[2 * at + 1],
            send_sem=sum_send.at[at],
            recv_sem=sum_recv.at[at],
            device_id=(dp, partner(tp, bit)),
            device_id_type=MESH,
        )
        swap.start()
        swap.wait()
        sum_v[2 * at + 2] = sum_v[2 * at] + sum_v[2 * at + 1]
    sum_out[...] = sum_v[2 * len(bits)] / own_gain_ref[...]
    ring.finish()
    share.finish()
    last.finish()
    rows_copy.wait()
    for copy in pending.values():
        copy.wait()


def backward(n, n_tp, rows, gain, own_gain, tables, cosine, sine, arrays, weights):
    total, width = arrays[1].shape
    mine = arrays[5].shape[0]
    units, hk, hv = arrays[0].shape[1], arrays[7].shape[1], arrays[9].shape[1]
    heads = tables[2].shape[0]
    window = tables[0].shape[0]
    micro = total // window
    tall = max(units, hv, hk)
    hops = 4 * (n - 1)
    count = len(bits_of(n_tp))
    shape = jax.ShapeDtypeStruct
    dma = pltpu.SemaphoreType.DMA
    sizes = (units, units, units, hv, hv, hv, hk, hk)
    return pl.pallas_call(
        functools.partial(backward_kernel, n, n_tp),
        out_shape=tuple(shape((s, BLOCK), F32) for s in sizes)
        + (shape((8, BLOCK), F32), shape((micro, rows, width), F32)),
        in_specs=[vmem()] * 7 + [anyspec()] * 22,
        out_specs=(anyspec(),) * 8 + (vmem(), anyspec()),
        scratch_shapes=[
            pltpu.VMEM((total, width), BF),
            pltpu.VMEM((n, tall, BLOCK), BF),
            pltpu.VMEM((total, units), BF),
            pltpu.VMEM((total, units), BF),
            pltpu.VMEM((total, units), BF),
            pltpu.VMEM((total, width), BF),
            pltpu.VMEM((2, units, BLOCK), BF),
            pltpu.VMEM((2, units, BLOCK), BF),
            pltpu.VMEM((mine, width), F32),
            pltpu.VMEM((mine, width), F32),
            pltpu.VMEM((total, hk), BF),
            pltpu.VMEM((total, hk), BF),
            pltpu.VMEM((total, hv), BF),
            pltpu.VMEM((total, hv), F32),
            pltpu.VMEM((total, hv), BF),
            pltpu.VMEM((window, HV), F32),
            pltpu.VMEM((heads, window, window), F32),
            pltpu.VMEM((window, HK), F32),
            pltpu.VMEM((window, HV), F32),
            pltpu.VMEM((total, width), BF),
            pltpu.VMEM((mine, width), F32),
            pltpu.VMEM((n_tp - 1, mine, width), BF),
            pltpu.VMEM((total, width), BF),
            pltpu.VMEM((micro, rows, width), F32),
            pltpu.VMEM((tall, BLOCK), F32),
            pltpu.VMEM((tall, BLOCK), F32),
            pltpu.VMEM((tall, BLOCK), F32),
            pltpu.VMEM((2, tall, BLOCK), BF),
            pltpu.VMEM((2, tall, BLOCK), BF),
            pltpu.VMEM((2, tall, BLOCK), BF),
            pltpu.VMEM((2, tall, BLOCK), BF),
            pltpu.VMEM((2, tall, BLOCK), F32),
            pltpu.VMEM((2, tall, BLOCK), BF),
            pltpu.VMEM((2 * count + 1, 8, BLOCK), F32),
        ]
        + [dma((hops, 2))] * 4
        + [pltpu.SemaphoreType.REGULAR((2, 2))]
        + [dma((n_tp - 1, micro))] * 4
        + [dma((micro, n_tp))] * 2
        + [dma((count,))] * 2
        + [dma((4, 4)), dma((2,)), dma((2,)), dma((12,))],
        compiler_params=pltpu.CompilerParams(
            collective_id=2, has_side_effects=True, vmem_limit_bytes=67_000_000
        ),
        cost_estimate=pl.CostEstimate(
            flops=4 * total * width * sum(sizes), bytes_accessed=120_000_000, transcendentals=0
        ),
        name="backward_kernel",
    )(gain, own_gain, *tables, cosine, sine, *arrays, *weights)


def finish_kernel(
    n,
    n_tp,
    passed,
    turned,
    *refs,
):
    sources = refs[: passed + turned]
    middle_ref, near_ref, far_ref = refs[passed + turned : passed + turned + 3]
    targets = refs[passed + turned + 3 : 2 * (passed + turned) + 3]
    block_out = refs[2 * (passed + turned) + 3]
    scratch = refs[2 * (passed + turned) + 4 :]
    held, (middle_v, near_v, far_v, block_v), (sem_in, sem_out) = (
        scratch[: passed + 2 * turned],
        scratch[passed + 2 * turned : passed + 2 * turned + 4],
        scratch[passed + 2 * turned + 4 :],
    )
    micro, rows, width = block_v.shape
    pos = ring_position(lax.axis_index("dp"), n)
    count = passed + turned
    ins = [
        pltpu.make_async_copy(sources[i], held[i], sem_in.at[i]) for i in range(count)
    ] + [
        pltpu.make_async_copy(source, target, sem_in.at[count + i])
        for i, (source, target) in enumerate(
            ((middle_ref, middle_v), (near_ref, near_v), (far_ref, far_v))
        )
    ]
    for copy in ins[count:] + ins[:count]:
        copy.start()
    results = list(held[:passed]) + list(held[count:])
    outs = [pltpu.make_async_copy(results[i], targets[i], sem_out.at[i]) for i in range(count)]
    outs.append(pltpu.make_async_copy(block_v, block_out, sem_out.at[count]))
    for copy in ins[count:]:
        copy.wait()

    @pl.loop(0, micro * rows // STEP)
    def _(r):
        at = pl.multiple_of(r * STEP, STEP)
        m, inner = at // rows, pl.multiple_of(at % rows, STEP)
        here = pl.ds(at, STEP)
        for i in range(n):
            for side in range(2):
                lanes = pl.ds(i * BLOCK + side * LANE, LANE)
                spot = ring_index((pos + (n - i if side == 0 else i)) % n, n)
                there = pl.ds(pl.multiple_of(spot * BLOCK + side * LANE, LANE), LANE)
                block_v[m, pl.ds(inner, STEP), there] = middle_v[here, lanes] + (
                    near_v[here, lanes] + far_v[here, lanes].astype(F32)
                )

    outs[count].start()
    for i in range(passed):
        ins[i].wait()
        outs[i].start()
    for i in range(turned):
        ins[passed + i].wait()
        held[count + i][...] = held[passed + i][...].T
        outs[passed + i].start()
    for copy in outs:
        copy.wait()


def finish(n, n_tp, passed, turned, middle, near, far, block_shape):
    shape = jax.ShapeDtypeStruct
    results = tuple(shape(a.shape, a.dtype) for a in passed) + tuple(
        shape(a.shape[::-1], a.dtype) for a in turned
    )
    count = len(passed) + len(turned)
    return pl.pallas_call(
        functools.partial(finish_kernel, n, n_tp, len(passed), len(turned)),
        out_shape=results + (shape(block_shape, F32),),
        in_specs=[anyspec()] * (count + 3),
        out_specs=(anyspec(),) * (count + 1),
        scratch_shapes=[pltpu.VMEM(a.shape, a.dtype) for a in passed]
        + [pltpu.VMEM(a.shape, a.dtype) for a in turned]
        + [pltpu.VMEM(a.shape[::-1], a.dtype) for a in turned]
        + [
            pltpu.VMEM(middle.shape, F32),
            pltpu.VMEM(near.shape, F32),
            pltpu.VMEM(far.shape, BF),
            pltpu.VMEM(block_shape, F32),
            pltpu.SemaphoreType.DMA((count + 3,)),
            pltpu.SemaphoreType.DMA((count + 1,)),
        ],
        compiler_params=pltpu.CompilerParams(vmem_limit_bytes=66_000_000),
        name="finish_kernel",
    )(*passed, *turned, middle, near, far)


def normalize(row_block, gain_vec):
    row_scale = lax.rsqrt(jnp.mean(row_block * row_block, axis=-1, keepdims=True) + EPS)
    return (row_block * row_scale * gain_vec.astype(jnp.float32), row_scale)


def norm_back(grad_rows, row_block, row_scale, gain_vec):
    scaled_grad = grad_rows * gain_vec.astype(jnp.float32)
    back_rows = row_scale * (
        scaled_grad
        - row_block
        * row_scale
        * row_scale
        * jnp.mean(scaled_grad * row_block, axis=-1, keepdims=True)
    )
    return (back_rows, jnp.sum(grad_rows * row_block * row_scale, axis=0))


def angles(length, feature_width):
    half_width = feature_width // 2
    frequency = jnp.exp(-math.log(10000.0) * jnp.arange(half_width, dtype=jnp.float32) / half_width)
    turns = jnp.arange(length, dtype=jnp.float32)[:, None] * frequency[None, :]
    return (jnp.cos(turns)[:, None, :], jnp.sin(turns)[:, None, :])


def decays(length, head_ids):
    places = jnp.arange(length, dtype=jnp.float32)
    spacing = places[:, None] - places[None, :]
    log_rate = jnp.log(1.0 - jnp.exp2(-5.0 - head_ids))
    return jnp.where(
        spacing[None] >= 0.0,
        jnp.exp(jnp.maximum(spacing, 0.0)[None] * log_rate[:, None, None]),
        0.0,
    )


def rotate(value_vectors, cosine_table, sine_table):
    half_width = value_vectors.shape[-1] // 2
    lower = value_vectors[..., :half_width]
    upper = value_vectors[..., half_width:]
    return jnp.concatenate(
        [lower * cosine_table - upper * sine_table, upper * cosine_table + lower * sine_table],
        axis=-1,
    )


def unrotate(value_vectors, cosine_table, sine_table):
    half_width = value_vectors.shape[-1] // 2
    lower = value_vectors[..., :half_width]
    upper = value_vectors[..., half_width:]
    return jnp.concatenate(
        [lower * cosine_table + upper * sine_table, upper * cosine_table - lower * sine_table],
        axis=-1,
    )


def plain_gelu_parts(pre_act):
    normal_cdf = 0.5 * (1.0 + lax.erf(pre_act * (1.0 / math.sqrt(2.0))))
    density = jnp.exp(-0.5 * pre_act * pre_act) * (1.0 / math.sqrt(2.0 * math.pi))
    return (pre_act * normal_cdf, normal_cdf + pre_act * density)


def inner_rows(left_rows, right_rows):
    return lax.dot_general(
        left_rows, right_rows, (((0,), (0,)), ((), ())), preferred_element_type=jnp.float32
    )


def times_t(left_rows, right_rows):
    return lax.dot_general(
        left_rows, right_rows, (((1,), (1,)), ((), ())), preferred_element_type=jnp.float32
    )


def forward_pass(rows_in, gathered, cosine_table, sine_table, decay_mask):
    (
        first_gain,
        second_gain,
        query_weight,
        key_weight,
        value_weight,
        swish_weight,
        output_weight,
        up_projection_matrix,
        gelu_weight,
        down_weight,
    ) = gathered
    local_heads = decay_mask.shape[0]
    scale_qk = 1.0 / math.sqrt(HK)
    normed, first_scale = normalize(rows_in, first_gain)
    normed_all = lax.all_gather(normed.astype(jnp.bfloat16), "tensor", axis=0, tiled=True)
    total_rows = normed_all.shape[0]
    sequences = total_rows // LEN
    query_turned_rows = rotate(
        jnp.dot(normed_all, query_weight, preferred_element_type=jnp.float32).reshape(
            sequences, LEN, local_heads, HK
        ),
        cosine_table,
        sine_table,
    ).astype(jnp.bfloat16)
    key_turned_rows = rotate(
        jnp.dot(normed_all, key_weight, preferred_element_type=jnp.float32).reshape(
            sequences, LEN, local_heads, HK
        ),
        cosine_table,
        sine_table,
    ).astype(jnp.bfloat16)
    value_rows = (
        jnp.dot(normed_all, value_weight, preferred_element_type=jnp.float32)
        .astype(jnp.bfloat16)
        .reshape(sequences, LEN, local_heads, HV)
    )
    gate_pre = jnp.dot(normed_all, swish_weight, preferred_element_type=jnp.float32)
    unscaled_logits = jnp.einsum(
        "snhd,smhd->shnm", query_turned_rows, key_turned_rows, preferred_element_type=jnp.float32
    )
    weight_bf = (unscaled_logits * (decay_mask * scale_qk)).astype(jnp.bfloat16)
    retained = jnp.einsum(
        "shnm,smhe->snhe", weight_bf, value_rows, preferred_element_type=jnp.float32
    )
    group_scale = lax.rsqrt(jnp.mean(retained * retained, axis=-1, keepdims=True) + GROUP_EPS)
    grouped = (retained * group_scale).reshape(total_rows, local_heads * HV)
    sigmoid_gate = jax.nn.sigmoid(gate_pre)
    swish_val = gate_pre * sigmoid_gate
    gated_rows = (swish_val * grouped).astype(jnp.bfloat16)
    attention = lax.psum_scatter(
        jnp.dot(gated_rows, output_weight, preferred_element_type=jnp.float32),
        "tensor",
        scatter_dimension=0,
        tiled=True,
    )
    middle = rows_in + attention
    second, second_scale = normalize(middle, second_gain)
    second_all = lax.all_gather(second.astype(jnp.bfloat16), "tensor", axis=0, tiled=True)
    up_pre = jnp.dot(second_all, up_projection_matrix, preferred_element_type=jnp.float32)
    gelu_pre = jnp.dot(second_all, gelu_weight, preferred_element_type=jnp.float32)
    gelu_val, gelu_slope = plain_gelu_parts(gelu_pre)
    hidden = (gelu_val * up_pre).astype(jnp.bfloat16)
    block_rows = middle + lax.psum_scatter(
        jnp.dot(hidden, down_weight, preferred_element_type=jnp.float32).astype(jnp.bfloat16),
        "tensor",
        scatter_dimension=0,
        tiled=True,
    ).astype(jnp.float32)
    kept_state = (
        rows_in,
        first_scale,
        normed_all,
        query_turned_rows,
        key_turned_rows,
        value_rows,
        gate_pre,
        weight_bf,
        retained,
        group_scale,
        grouped,
        gated_rows,
        middle,
        second_scale,
        second_all,
        up_pre,
        gelu_val,
        gelu_slope,
        hidden,
    )
    return (block_rows, kept_state)


def backward_pass(kept_state, cot_in, gathered, cosine_table, sine_table, decay_mask):
    (
        first_gain,
        second_gain,
        query_weight,
        key_weight,
        value_weight,
        swish_weight,
        output_weight,
        up_projection_matrix,
        gelu_weight,
        down_weight,
    ) = gathered
    (
        rows_in,
        first_scale,
        normed_all,
        query_turned_rows,
        key_turned_rows,
        value_rows,
        gate_pre,
        weight_bf,
        retained,
        group_scale,
        grouped,
        gated_rows,
        middle,
        second_scale,
        second_all,
        up_pre,
        gelu_val,
        gelu_slope,
        hidden,
    ) = kept_state
    local_heads = decay_mask.shape[0]
    total_rows = normed_all.shape[0]
    scale_qk = 1.0 / math.sqrt(HK)
    cot_all = lax.all_gather(cot_in.astype(jnp.bfloat16), "tensor", axis=0, tiled=True)
    grad_hidden = times_t(cot_all, down_weight)
    grad_down = inner_rows(hidden, cot_all)
    grad_uppre = (grad_hidden * gelu_val).astype(jnp.bfloat16)
    grad_gelupre = (grad_hidden * up_pre * gelu_slope).astype(jnp.bfloat16)
    grad_up = inner_rows(second_all, grad_uppre)
    grad_gelu = inner_rows(second_all, grad_gelupre)
    second_back = lax.psum_scatter(
        times_t(grad_uppre, up_projection_matrix) + times_t(grad_gelupre, gelu_weight),
        "tensor",
        scatter_dimension=0,
        tiled=True,
    )
    middle_back, grad_gain_two = norm_back(second_back, middle, second_scale, second_gain)
    grad_middle = cot_in + middle_back
    middle_all = lax.all_gather(grad_middle.astype(jnp.bfloat16), "tensor", axis=0, tiled=True)
    grad_gated = times_t(middle_all, output_weight)
    grad_out = inner_rows(gated_rows, middle_all)
    sigmoid_gate = jax.nn.sigmoid(gate_pre)
    swish_val = gate_pre * sigmoid_gate
    grad_swishpre = (
        grad_gated * grouped * (sigmoid_gate * (1.0 + gate_pre * (1.0 - sigmoid_gate)))
    ).astype(jnp.bfloat16)
    grad_grouped = (grad_gated * swish_val).reshape(retained.shape)
    grad_retained = (
        group_scale
        * (
            grad_grouped
            - retained
            * group_scale
            * group_scale
            * jnp.mean(grad_grouped * retained, axis=-1, keepdims=True)
        )
    ).astype(jnp.bfloat16)
    grad_valrows = jnp.einsum(
        "shnm,snhe->smhe", weight_bf, grad_retained, preferred_element_type=jnp.float32
    ).astype(jnp.bfloat16)
    grad_weight = jnp.einsum(
        "snhe,smhe->shnm", grad_retained, value_rows, preferred_element_type=jnp.float32
    )
    grad_retention_logits = (grad_weight * (decay_mask * scale_qk)).astype(jnp.bfloat16)
    grad_query_rotated_rows = jnp.einsum(
        "shnm,smhd->snhd",
        grad_retention_logits,
        key_turned_rows,
        preferred_element_type=jnp.float32,
    )
    grad_key_rotated_rows = jnp.einsum(
        "shnm,snhd->smhd",
        grad_retention_logits,
        query_turned_rows,
        preferred_element_type=jnp.float32,
    )
    grad_qpre = (
        unrotate(grad_query_rotated_rows, cosine_table, sine_table)
        .astype(jnp.bfloat16)
        .reshape(total_rows, local_heads * HK)
    )
    grad_kpre = (
        unrotate(grad_key_rotated_rows, cosine_table, sine_table)
        .astype(jnp.bfloat16)
        .reshape(total_rows, local_heads * HK)
    )
    grad_vflat = grad_valrows.reshape(total_rows, local_heads * HV)
    first_back = lax.psum_scatter(
        times_t(grad_qpre, query_weight)
        + times_t(grad_kpre, key_weight)
        + times_t(grad_vflat, value_weight)
        + times_t(grad_swishpre, swish_weight),
        "tensor",
        scatter_dimension=0,
        tiled=True,
    )
    grad_query = inner_rows(normed_all, grad_qpre)
    grad_key = inner_rows(normed_all, grad_kpre)
    grad_value = inner_rows(normed_all, grad_vflat)
    grad_swish = inner_rows(normed_all, grad_swishpre)
    input_back, grad_gain_one = norm_back(first_back, rows_in, first_scale, first_gain)
    grad_rows = grad_middle + input_back
    pieces = (
        grad_gain_one,
        grad_gain_two,
        grad_query,
        grad_key,
        grad_value,
        grad_swish,
        grad_out,
        grad_up,
        grad_gelu,
        grad_down,
    )
    return (grad_rows, pieces)


def plain_body(
    block_input,
    cotangent,
    first_gain,
    second_gain,
    query_weight,
    key_weight,
    value_weight,
    swish_weight,
    output_weight,
    up_projection_matrix,
    gelu_weight,
    down_weight,
):
    local_heads = query_weight.shape[1] // HK
    head_ids = (lax.axis_index("tensor") * local_heads + jnp.arange(local_heads)).astype(
        jnp.float32
    )
    cosine_table, sine_table = angles(LEN, HK)
    decay_mask = decays(LEN, head_ids)
    output_list = []
    grad_list = []
    totals = ()
    for micro_idx in range(block_input.shape[0]):
        forward_set = (
            lax.all_gather(first_gain, "dp", axis=0, tiled=True),
            lax.all_gather(second_gain, "dp", axis=0, tiled=True),
            lax.all_gather(query_weight, "dp", axis=0, tiled=True),
            lax.all_gather(key_weight, "dp", axis=0, tiled=True),
            lax.all_gather(value_weight, "dp", axis=0, tiled=True),
            lax.all_gather(swish_weight, "dp", axis=0, tiled=True),
            lax.all_gather(output_weight, "dp", axis=1, tiled=True),
            lax.all_gather(up_projection_matrix, "dp", axis=0, tiled=True),
            lax.all_gather(gelu_weight, "dp", axis=0, tiled=True),
            lax.all_gather(down_weight, "dp", axis=1, tiled=True),
        )
        block_rows, kept_state = forward_pass(
            block_input[micro_idx], forward_set, cosine_table, sine_table, decay_mask
        )
        held = lax.optimization_barrier(
            (
                (
                    first_gain,
                    second_gain,
                    query_weight,
                    key_weight,
                    value_weight,
                    swish_weight,
                    output_weight,
                    up_projection_matrix,
                    gelu_weight,
                    down_weight,
                ),
                block_rows,
            )
        )[0]
        backward_set = (
            lax.all_gather(held[0], "dp", axis=0, tiled=True),
            lax.all_gather(held[1], "dp", axis=0, tiled=True),
            lax.all_gather(held[2], "dp", axis=0, tiled=True),
            lax.all_gather(held[3], "dp", axis=0, tiled=True),
            lax.all_gather(held[4], "dp", axis=0, tiled=True),
            lax.all_gather(held[5], "dp", axis=0, tiled=True),
            lax.all_gather(held[6], "dp", axis=1, tiled=True),
            lax.all_gather(held[7], "dp", axis=0, tiled=True),
            lax.all_gather(held[8], "dp", axis=0, tiled=True),
            lax.all_gather(held[9], "dp", axis=1, tiled=True),
        )
        grad_rows, pieces = backward_pass(
            kept_state, cotangent[micro_idx], backward_set, cosine_table, sine_table, decay_mask
        )
        output_list.append(block_rows)
        grad_list.append(grad_rows)
        if micro_idx == 0:
            totals = tuple(pieces)
        else:
            totals = tuple((total + piece for total, piece in zip(totals, pieces)))
    totals = (
        lax.psum_scatter(totals[0], "dp", scatter_dimension=0, tiled=True),
        lax.psum_scatter(totals[1], "dp", scatter_dimension=0, tiled=True),
        lax.psum_scatter(totals[2], "dp", scatter_dimension=0, tiled=True),
        lax.psum_scatter(totals[3], "dp", scatter_dimension=0, tiled=True),
        lax.psum_scatter(totals[4], "dp", scatter_dimension=0, tiled=True),
        lax.psum_scatter(totals[5], "dp", scatter_dimension=0, tiled=True),
        lax.psum_scatter(totals[6], "dp", scatter_dimension=1, tiled=True),
        lax.psum_scatter(totals[7], "dp", scatter_dimension=0, tiled=True),
        lax.psum_scatter(totals[8], "dp", scatter_dimension=0, tiled=True),
        lax.psum_scatter(totals[9], "dp", scatter_dimension=1, tiled=True),
    )
    gain_first, gain_second = lax.psum((totals[0], totals[1]), "tensor")
    return (
        jnp.stack(output_list, axis=0),
        jnp.stack(grad_list, axis=0),
        gain_first,
        gain_second,
        totals[2],
        totals[3],
        totals[4],
        totals[5],
        totals[6],
        totals[7],
        totals[8],
        totals[9],
    )


def ring_body(
    n_dp,
    n_tp,
    block_input,
    cotangent,
    first_gain,
    second_gain,
    query_weight,
    key_weight,
    value_weight,
    swish_weight,
    output_weight,
    up_projection_matrix,
    gelu_weight,
    down_weight,
):
    micro, rows, width = block_input.shape
    local_heads = query_weight.shape[1] // HK
    window = n_tp * rows

    me = lax.axis_index("tensor")
    head_ids = (me * local_heads + jnp.arange(local_heads)).astype(F32)
    chunk_of = jnp.arange(n_tp) ^ me
    natural = (chunk_of[:, None] * rows + jnp.arange(rows)[None, :]).reshape(window)
    place = (natural % LEN).astype(F32)
    half_key = HK // 2
    frequency = jnp.exp(-math.log(10000.0) * jnp.arange(half_key, dtype=F32) / half_key)
    turns = place[:, None] * frequency[None, :]
    cosine, sine = jnp.cos(turns), jnp.sin(turns)
    log_rate = jnp.log(1.0 - jnp.exp2(-5.0 - head_ids))
    spots = natural.astype(F32)
    tables = (
        jnp.broadcast_to(spots[:, None], (window, LANE)),
        spots[None, :],
        jnp.broadcast_to(log_rate[:, None], (local_heads, window)),
    )

    gains_own = jnp.stack([first_gain, second_gain]).astype(F32)
    results = forward(
        n_dp,
        n_tp,
        block_input,
        cotangent,
        gains_own,
        cosine,
        sine,
        tables,
        (
            query_weight,
            key_weight,
            value_weight.T,
            swish_weight.T,
            output_weight,
            up_projection_matrix.T,
            gelu_weight.T,
            down_weight,
        ),
    )
    query, key, value, gate, x_rel, cot_rel, gains, normed, cot_all = results[:9]
    w_in, (w_o, w_u, w_l, w_d) = results[9:13], results[13:17]
    gated, middle, second, hidden, gelu_val, up_slope, near, far = results[17:]

    far = lax.ppermute(far, "tensor", [(i, i ^ (n_tp // 2)) for i in range(n_tp)])

    (
        grad_down,
        grad_up,
        grad_gelu,
        grad_out,
        grad_swish,
        grad_value,
        grad_query,
        grad_key,
        gain_grads,
        grad_rows,
    ) = backward(
        n_dp,
        n_tp,
        rows,
        gains,
        jnp.pad(gains_own, ((0, 6), (0, 0)), constant_values=1.0),
        tables,
        cosine,
        sine,
        (
            hidden,
            cot_all,
            gelu_val,
            up_slope,
            second,
            middle,
            cot_rel,
            query,
            key,
            value,
            gate,
            gated,
            normed,
            x_rel,
        ),
        (*w_in, w_o, w_u, w_l, w_d),
    )
    passed = (grad_value, grad_swish, grad_out, grad_up, grad_gelu, grad_down, grad_rows)
    *passed, grad_query, grad_key, block_rows = finish(
        n_dp, n_tp, passed, (grad_query, grad_key), middle, near, far, block_input.shape
    )
    grad_value, grad_swish, grad_out, grad_up, grad_gelu, grad_down, grad_rows = passed

    return (
        block_rows,
        grad_rows,
        gain_grads[0],
        gain_grads[1],
        grad_query,
        grad_key,
        grad_value.T,
        grad_swish.T,
        grad_out,
        grad_up.T,
        grad_gelu.T,
        grad_down,
    )


def solution(mesh):
    rows = P(None, ("dp", "tensor"), None)
    wide, tall, gain = P("dp", "tensor"), P("tensor", "dp"), P("dp")
    n_dp, n_tp = mesh.shape["dp"], mesh.shape["tensor"]

    def run(*arrays):
        blocks = arrays[2].shape[0] == BLOCK and n_dp % 2 == 0 and n_dp > 2
        pairs = n_tp > 1 and n_tp & (n_tp - 1) == 0
        aligned = (n_tp * arrays[0].shape[1]) % LEN == 0 and arrays[0].shape[1] % LANE == 0
        equal = arrays[6].shape[1] == arrays[9].shape[1] and arrays[6].shape[1] % STEP == 0
        if blocks and pairs and aligned and equal:
            return ring_body(n_dp, n_tp, *arrays)
        return plain_body(*arrays)

    return jax.shard_map(
        run,
        mesh=mesh,
        in_specs=(rows, rows, gain, gain) + (wide,) * 4 + (tall, wide, wide, tall),
        out_specs=(rows, rows, gain, gain) + (wide,) * 4 + (tall, wide, wide, tall),
        check_vma=False,
    )
```

```python
import functools
import math

import jax
import jax.numpy as jnp
from jax import lax
from jax.experimental import pallas as pl
from jax.experimental.pallas import tpu as pltpu
from jax.sharding import PartitionSpec as P

HK = 256
HV = 432
LEN = 512
EPS = 1e-05
GROUP_EPS = 1.0
BF = jnp.bfloat16
F32 = jnp.float32
MESH = pl.DeviceIdType.MESH
LANE = 128
BLOCK = 2 * LANE
SLOTS = 3
STEP = 32
SPLIT = 2


def ring_position(index, count):
    low = index // 2
    return low + (index % 2) * (count - 1 - 2 * low)


def ring_index(position, count):
    high = position // (count // 2)
    return (1 - high) * (2 * position) + high * (2 * (count - 1 - position) + 1)


def bits_of(count):
    return [1 << i for i in range(count.bit_length() - 1)]


def anyspec():
    return pl.BlockSpec(memory_space=pl.ANY)


def vmem():
    return pl.BlockSpec(memory_space=pltpu.VMEM)


def nt(left, right):
    return lax.dot_general(left, right, (((1,), (1,)), ((), ())), preferred_element_type=F32)


def nn(left, right):
    return lax.dot_general(left, right, (((1,), (0,)), ((), ())), preferred_element_type=F32)


def tn(left, right):
    return lax.dot_general(left, right, (((0,), (0,)), ((), ())), preferred_element_type=F32)


def partner(tp, bit):
    return tp + bit - 2 * bit * ((tp // bit) % 2)


def neighbours(n):
    dp, tp = lax.axis_index("dp"), lax.axis_index("tensor")
    pos = ring_position(dp, n)
    return dp, tp, ring_index((pos + 1) % n, n), ring_index((pos + n - 1) % n, n)


def greet(devices):
    barrier = pltpu.get_barrier_semaphore()
    for device in devices:
        pl.semaphore_signal(barrier, inc=1, device_id=device, device_id_type=MESH)
    pl.semaphore_wait(barrier, len(devices))


class Share:
    def __init__(self, dp, tp, n_tp, micro, rows, buf, send, recv):
        self.dp, self.tp, self.n_tp, self.micro, self.rows = dp, tp, n_tp, micro, rows
        self.buf, self.send, self.recv = buf, send, recv
        self.bits = bits_of(n_tp)[::-1]

    def copies(self, bit, m, keys=None):
        window = self.n_tp * self.rows
        for key in range(0, self.n_tp, 2 * bit):
            if keys is None or (key == 0) == keys:
                yield pltpu.make_async_remote_copy(
                    src_ref=self.buf.at[pl.ds(m * window + key * self.rows, self.rows)],
                    dst_ref=self.buf.at[pl.ds(m * window + (key ^ bit) * self.rows, self.rows)],
                    send_sem=self.send.at[m, key ^ bit],
                    recv_sem=self.recv.at[m, key ^ bit],
                    device_id=(self.dp, partner(self.tp, bit)),
                    device_id_type=MESH,
                )

    def begin(self, m):
        for bit in self.bits:
            for copy in self.copies(bit, m, True):
                copy.start()

    def relay(self, m):
        for bit in self.bits:
            for copy in self.copies(bit, m, False):
                copy.start()
            for copy in self.copies(bit, m):
                copy.wait_recv()

    def finish(self):
        for m in range(self.micro):
            for bit in self.bits:
                for copy in self.copies(bit, m):
                    copy.wait_send()


class Collect:
    def __init__(self, dp, tp, n_tp, micro, rows, back, got, own, send, recv, columns=None):
        self.columns = slice(None) if columns is None else pl.ds(*columns)
        self.dp, self.tp, self.n_tp, self.micro, self.rows = dp, tp, n_tp, micro, rows
        self.back, self.got, self.own, self.send, self.recv = back, got, own, send, recv
        self.bits = bits_of(n_tp)

    def keys(self, bit):
        return [key for key in range(0, self.n_tp, bit) if key & bit]

    def copies(self, bit, m):
        window = self.n_tp * self.rows
        for key in self.keys(bit):
            yield pltpu.make_async_remote_copy(
                src_ref=self.back.at[
                    pl.ds(m * window + key * self.rows, self.rows), self.columns
                ],
                dst_ref=self.got.at[key - 1, pl.ds(m * self.rows, self.rows), self.columns],
                send_sem=self.send.at[key - 1, m],
                recv_sem=self.recv.at[key - 1, m],
                device_id=(self.dp, partner(self.tp, bit)),
                device_id_type=MESH,
            )

    def start(self, bit, m):
        for copy in self.copies(bit, m):
            copy.start()

    def add(self, bit, m):
        window = self.n_tp * self.rows
        for copy in self.copies(bit, m):
            copy.wait_recv()
        for key in self.keys(bit):
            target = key ^ bit

            @pl.loop(0, self.rows // STEP)
            def _(r):
                inner = pl.multiple_of(r * STEP, STEP)
                here = pl.ds(pl.multiple_of(m * self.rows + inner, STEP), STEP)
                there = pl.ds(pl.multiple_of(m * window + target * self.rows + inner, STEP), STEP)
                cols = self.columns
                got = self.got[key - 1, here, cols].astype(F32)
                if target == 0:
                    held = self.back[there, cols].astype(F32) if bit == 1 else self.own[here, cols]
                    self.own[here, cols] = held + got
                else:
                    self.back[there, cols] = (self.back[there, cols].astype(F32) + got).astype(BF)

    def finish(self, bits=None):
        for m in range(self.micro):
            for bit in self.bits if bits is None else bits:
                for copy in self.copies(bit, m):
                    copy.wait_send()


def fill_decay(decay_v, col_ref, row_ref, rate_ref):
    heads, window, _ = decay_v.shape
    scale_qk = 1.0 / math.sqrt(HK)
    for h in range(heads):

        @pl.loop(0, window // LANE)
        def _(r):
            here = pl.ds(pl.multiple_of(r * LANE, LANE), LANE)
            col, row = col_ref[here, 0:1], row_ref[...]
            spacing = col - row
            same = jnp.floor(col * (1.0 / LEN)) == jnp.floor(row * (1.0 / LEN))
            kept = jnp.exp(jnp.maximum(spacing, 0.0) * rate_ref[h : h + 1, :]) * scale_qk
            decay_v[h, here, :] = jnp.where((spacing >= 0.0) & same, kept, 0.0)


def gelu_parts(pre_act):
    normal_cdf = 0.5 * (1.0 + lax.erf(pre_act * (1.0 / math.sqrt(2.0))))
    density = jnp.exp(-0.5 * pre_act * pre_act) * (1.0 / math.sqrt(2.0 * math.pi))
    return (pre_act * normal_cdf, normal_cdf + pre_act * density)


def forward_kernel(
    n,
    n_tp,
    x_ref,
    cot_ref,
    gains_ref,
    cos_ref,
    sin_ref,
    col_ref,
    row_ref,
    rate_ref,
    *refs,
):
    shards, refs = refs[:8], refs[8:]
    q_out, k_out, v_out, g_out, xr_out, cr_out, gain_out, nall_out, call_out = refs[:9]
    whole_outs, refs = refs[9:17], refs[17:]
    gated_out, middle_out, second_out, hidden_out, value_out, slope_out, near_out, far_out = refs[:8]
    nall_v, row_v, cot_v, gain_v, q_v, k_v, v_v, g_v, decay_v, got_v = refs[8:18]
    held, refs = refs[18:22], refs[22:]
    x_v, q_acc, k_acc, v_acc, wq_s, wk_s, wv_s, wg_s = refs[:8]
    back_v, own_v, gated_v, hidden_v, value_v, slope_v, up_v = refs[8:15]
    refs = refs[15:]
    ring_send, ring_recv, gain_send, gain_recv = refs[:4]
    first_send, first_recv, cot_send, cot_recv, share_send, share_recv = refs[4:10]
    part_send, part_recv, last_send, last_recv, end_send, end_recv = refs[10:16]
    load_sem, local_sem, out_sem = refs[16:]

    micro, rows, width = x_ref.shape
    window = n_tp * rows
    total, mine = micro * window, micro * rows
    dp, tp, cw, ccw = neighbours(n)
    pos = ring_position(dp, n)
    bits = bits_of(n_tp)
    heads = decay_v.shape[0]
    tile = 256
    half = HK // 2
    greet(
        [(ring_index((pos + k) % n, n), tp) for k in range(1, n)]
        + [(dp, partner(tp, bit)) for bit in bits]
    )

    wholes = tuple(whole_outs[:4]) + tuple(held)
    slots = (wq_s, wk_s, wv_s, wg_s)
    pieces = [(a, 0, slots[a].shape[1]) for a in range(4)]
    groups = [(0, 1, 2, 3)]
    for pair in ((4,), (5, 6), (7,)):
        group = []
        for a in pair:
            size = shards[a].shape[0]
            parts = SPLIT if len(pair) == 1 else 1
            cuts = [size * j // parts // 16 * 16 for j in range(parts)] + [size]
            for low, high in zip(cuts, cuts[1:]):
                group.append(len(pieces))
                pieces.append((a, low, high - low))
        groups.append(tuple(group))
    ring_a, ring_b, ring_c, ring_d = groups

    def hop(i, p, side):
        a, low, size = pieces[p]
        span, lanes = pl.ds(low, size), pl.ds(side * LANE, LANE)
        if not (isinstance(i, int) and i == 0):
            source = wholes[a].at[i, span, lanes]
        elif a < 2:
            source = slots[a].at[0, span, lanes]
        else:
            source = shards[a].at[span, lanes]
        return pltpu.make_async_remote_copy(
            src_ref=source,
            dst_ref=wholes[a].at[i + 1, span, lanes],
            send_sem=ring_send.at[i, p, side],
            recv_sem=ring_recv.at[i, p, side],
            device_id=((cw, ccw)[side], tp),
            device_id_type=MESH,
        )

    def ring_start(group):
        for p in group:
            for side in range(2):
                hop(0, p, side).start()

    def ring_pass(s, p):
        for side in range(2):
            hop(s - 1, p, side).wait_recv()
            if isinstance(s, int):
                if s < n - 1:
                    hop(s, p, side).start()
            else:

                @pl.when(s < n - 1)
                def _():
                    hop(s, p, side).start()

    def ring_step(s, group, following=()):
        for p in group:
            ring_pass(s, p)
        if isinstance(s, int) and s == n - 2:
            ring_start(following)

    def store(source, target):
        copy = pltpu.make_async_copy(source, target, out_sem.at[len(stores)])
        copy.start()
        stores.append(copy)

    stores = []
    turned = [
        pltpu.make_async_copy(shards[a], (q_v, k_v)[a].at[pl.ds(0, BLOCK)], local_sem.at[2 + a])
        for a in range(2)
    ]
    for copy in turned:
        copy.start()
    ring_start(ring_a[2:])
    for a in range(2):
        turned[a].wait()
        natural_block = (q_v, k_v)[a][pl.ds(0, BLOCK), :]
        slots[a][0] = natural_block.astype(F32).T.astype(BF)
        ring_start(ring_a[a : a + 1])
    own_blocks = [
        pltpu.make_async_copy(shards[4 + i], held[i].at[0], local_sem.at[4 + i]) for i in range(4)
    ]

    def natural(i, side):
        at = ring_index((pos + (n - i if side == 0 else i)) % n, n) * BLOCK + side * LANE
        return pl.ds(pl.multiple_of(at, LANE), LANE)

    first = Share(dp, tp, n_tp, micro, rows, nall_v, first_send, first_recv)
    share = Share(dp, tp, n_tp, micro, rows, nall_v, share_send, share_recv)

    def cot_copy(bit, m, key):
        source = cot_v.at[pl.ds(m * rows, rows)]
        if key:
            source = call_out.at[pl.ds(m * window + key * rows, rows)]
        return pltpu.make_async_remote_copy(
            src_ref=source,
            dst_ref=call_out.at[pl.ds(m * window + (key ^ bit) * rows, rows)],
            send_sem=cot_send.at[m, key ^ bit],
            recv_sem=cot_recv.at[m, key ^ bit],
            device_id=(dp, partner(tp, bit)),
            device_id_type=MESH,
        )

    def cot_copies(bit, keys=None):
        for m in range(micro):
            for key in range(0, n_tp, 2 * bit):
                if keys is None or (key == 0) == keys:
                    yield cot_copy(bit, m, key)

    def project():
        cot_rel_v = own_v
        accs = (q_acc, k_acc, v_acc, g_v)

        def load(i, a):
            source = shards[a] if i == 0 else wholes[a].at[i]
            return pltpu.make_async_copy(
                source, slots[a].at[i % SLOTS], load_sem.at[i % SLOTS, a]
            )

        x_copy = pltpu.make_async_copy(x_ref, x_v, local_sem.at[0])
        x_copy.start()
        for a in range(2, 4):
            load(0, a).start()

        def gain_copy(k):
            return pltpu.make_async_remote_copy(
                src_ref=gains_ref,
                dst_ref=gain_v.at[k],
                send_sem=gain_send.at[k],
                recv_sem=gain_recv.at[k],
                device_id=(ring_index((pos + k) % n, n), tp),
                device_id_type=MESH,
            )

        own_gain = pltpu.make_async_copy(gains_ref, gain_v.at[0], local_sem.at[1])
        own_gain.start()
        for k in range(1, n):
            gain_copy(k).start()
        own_gain.wait()
        for k in range(1, n):
            gain_copy(k).wait()
        for i in range(n):
            gain_out[:, pl.ds(i * BLOCK, LANE)] = gain_v[i, 0:2, pl.ds(0, LANE)]
            gain_out[:, pl.ds(i * BLOCK + LANE, LANE)] = gain_v[
                (n - i) % n, 0:2, pl.ds(LANE, LANE)
            ]
        x_copy.wait()

        def each_part(work):
            @pl.loop(0, mine // STEP)
            def _(r):
                at = pl.multiple_of(r * STEP, STEP)
                m, inner = at // rows, pl.multiple_of(at % rows, STEP)
                work(at, m, inner)

        def normalize_part(at, m, inner):
            chunk = x_v[m, pl.ds(inner, STEP), :]
            scale = lax.rsqrt(jnp.mean(chunk * chunk, axis=-1, keepdims=True) + EPS)
            there = pl.ds(pl.multiple_of(m * window + inner, STEP), STEP)
            for i in range(n):
                for side in range(2):
                    lanes = pl.ds(i * BLOCK + side * LANE, LANE)
                    part = x_v[m, pl.ds(inner, STEP), natural(i, side)]
                    row_v[pl.ds(at, STEP), lanes] = part
                    nall_v[there, lanes] = (part * scale * gain_out[0:1, lanes]).astype(BF)

        each_part(normalize_part)
        for m in range(micro):
            first.begin(m)
        store(row_v, xr_out)
        c_copy = pltpu.make_async_copy(cot_ref, x_v, local_sem.at[0])
        c_copy.start()
        cot_rel = pltpu.make_async_copy(cot_rel_v, cr_out, local_sem.at[1])

        def cot_part(at, m, inner):
            for i in range(n):
                for side in range(2):
                    lanes = pl.ds(i * BLOCK + side * LANE, LANE)
                    part = x_v[m, pl.ds(inner, STEP), natural(i, side)]
                    cot_rel_v[pl.ds(at, STEP), lanes] = part
                    cot_v[pl.ds(at, STEP), lanes] = part.astype(BF)

        def take_cot():
            c_copy.wait()
            each_part(cot_part)
            cot_rel.start()
            for m in range(micro):
                store(cot_v.at[pl.ds(m * rows, rows)], call_out.at[pl.ds(m * window, rows)])
            for copy in own_blocks:
                copy.start()

        def product(j, a, last):
            if j > 0 or a > 1:
                load(j, a).wait()
            if j == 0:
                pltpu.make_async_copy(
                    slots[a].at[0], wholes[a].at[0], load_sem.at[SLOTS, a]
                ).start()

            @pl.loop(0, total // tile)
            def _(r):
                at = pl.multiple_of(r * tile, tile)
                here = pl.ds(at, tile)
                part = nt(nall_v[here, pl.ds(j * BLOCK, BLOCK)], slots[a][j % SLOTS])
                if j > 0:
                    part = accs[a][here, :] + part
                if not last or a == 3:
                    accs[a][here, :] = part
                elif a == 2:
                    v_v[here, :] = part.astype(BF)
                else:
                    place = pl.ds(pl.multiple_of(at % window, tile), tile)
                    cosine, sine = cos_ref[place, :], sin_ref[place, :]
                    out = (q_v, k_v)[a]
                    for h in range(heads):
                        low = part[:, h * HK : h * HK + half]
                        high = part[:, h * HK + half : (h + 1) * HK]
                        out[here, pl.ds(h * HK, half)] = (low * cosine - high * sine).astype(BF)
                        out[here, pl.ds(h * HK + half, half)] = (
                            high * cosine + low * sine
                        ).astype(BF)

            if j == 0:
                pltpu.make_async_copy(
                    slots[a].at[0], wholes[a].at[0], load_sem.at[SLOTS, a]
                ).wait()

        start_at, done = 3, 0
        for i in range(n + 1):
            if i == 2:
                take_cot()
                fill_decay(decay_v, col_ref, row_ref, rate_ref)
            if i == start_at:
                for m in range(micro):
                    first.relay(m)
                store(nall_v, nall_out)
                for bit in bits[::-1]:
                    for copy in cot_copies(bit, True):
                        copy.start()
            if i == n - 1:
                for bit in bits[::-1]:
                    for copy in cot_copies(bit, False):
                        copy.start()
                    for copy in cot_copies(bit):
                        copy.wait_recv()
            todo = []
            if i >= start_at:
                goal = min(i - 1, done + 1) if i < n else n - 1
                todo = list(range(done, goal + 1))
                done = goal + 1
            for a in range(4):
                if 0 < i < n:
                    ring_pass(i, a)
                if i == n - 2 and a == 3:
                    ring_start(ring_b)
                for j in todo:
                    product(j, a, j == n - 1)
                if 0 < i < n:
                    if i == SLOTS and a < 2:
                        hop(0, a, 0).wait_send()
                        hop(0, a, 1).wait_send()
                    load(i, a).start()
                if i == n:
                    source, target = ((q_v, q_out), (k_v, k_out), (v_v, v_out), (g_v, g_out))[a]
                    store(source, target)
        cot_rel.wait()

    project()
    wo_v, wu_v, wl_v, wd_v = held
    units = shards[7].shape[0]

    def middle_part():
        for copy in own_blocks:
            copy.wait()

        def attend(m, h):
            keys = pl.ds(h * HK, HK)
            values = pl.ds(h * HV, HV)
            inside = pl.ds(m * window, window)

            @pl.loop(0, window // tile)
            def _(r):
                at = pl.multiple_of(r * tile, tile)
                here = pl.ds(pl.multiple_of(m * window + at, tile), tile)
                scores = nt(q_v[here, keys], k_v[inside, keys])
                weight = (scores * decay_v[h, pl.ds(at, tile), :]).astype(BF)
                kept = nn(weight, v_v[inside, values])
                group = lax.rsqrt(jnp.mean(kept * kept, axis=-1, keepdims=True) + GROUP_EPS)
                gate = g_v[here, values]
                gated_v[here, values] = (gate * jax.nn.sigmoid(gate) * (kept * group)).astype(BF)

        def times_block(left, weights, i):
            @pl.loop(0, total // tile)
            def _(r):
                here = pl.ds(pl.multiple_of(r * tile, tile), tile)
                back_v[here, pl.ds(i * BLOCK, BLOCK)] = nn(left[here, :], weights[i]).astype(BF)

        collect = Collect(dp, tp, n_tp, micro, rows, back_v, got_v, own_v, part_send, part_recv)
        jobs = [(m, h) for m in range(micro) for h in range(heads)]
        reached = 0
        while jobs:
            if reached < n - 1:
                reached += 1
                ring_step(reached, ring_b, ring_c)
            attend(*jobs.pop(0))
        store(gated_v, gated_out)
        ready = 0
        while ready < n:
            if reached < n - 1:
                reached += 1
                ring_step(reached, ring_b, ring_c)
            for _ in range(2 if reached < n - 1 else n):
                if ready < min(n, reached + 1):
                    times_block(gated_v, wo_v, ready)
                    ready += 1
        store(wo_v, whole_outs[4])
        first.finish()
        stores[0].wait()
        stores[micro + 1].wait()
        for m in range(micro):
            collect.start(bits[0], m)
        passed = [0]

        def pairs_to(goal):
            while passed[0] < min(goal, n - 1):
                passed[0] += 1
                ring_step(passed[0], ring_c, ring_d)

        for at, bit in enumerate(bits[:-1]):
            for m in range(micro):
                collect.add(bit, m)
                collect.start(bits[at + 1], m)
        pairs_to(1)
        for m in range(micro):
            pairs_to(2 + m)
            collect.add(bits[-1], m)

            @pl.loop(0, rows // STEP)
            def _(r):
                inner = pl.multiple_of(r * STEP, STEP)
                here = pl.ds(pl.multiple_of(m * rows + inner, STEP), STEP)
                there = pl.ds(pl.multiple_of(m * window + inner, STEP), STEP)
                middle = row_v[here, :] + own_v[here, :]
                row_v[here, :] = middle
                scale = lax.rsqrt(jnp.mean(middle * middle, axis=-1, keepdims=True) + EPS)
                nall_v[there, :] = (middle * scale * gain_out[1:2, :]).astype(BF)

            share.begin(m)
        store(row_v, middle_out)
        pairs_to(4)
        for m in range(micro):
            share.relay(m)
            pairs_to(5 + m)
        pairs_to(n - 1)
        store(nall_v, second_out)
        store(wu_v, whole_outs[5])
        store(wl_v, whole_outs[6])

        def rows_by(weights, here):
            result = None
            for i in range(n):
                term = nt(nall_v[here, pl.ds(i * BLOCK, BLOCK)], weights[i])
                result = term if result is None else result + term
            return result

        tiles = total // tile
        every = max(1, tiles // 2)
        inside_loop = min(tiles // every, n - 1)

        @pl.loop(0, tiles)
        def _(r):
            here = pl.ds(pl.multiple_of(r * tile, tile), tile)
            up_v[...] = rows_by(wu_v, here)
            gelu_val, gelu_slope = gelu_parts(rows_by(wl_v, here))
            up = up_v[...]
            hidden_v[here, :] = (gelu_val * up).astype(BF)
            value_v[here, :] = gelu_val.astype(BF)
            slope_v[here, :] = (up * gelu_slope).astype(BF)

            @pl.when((r % every == every - 1) & (r // every < inside_loop))
            def _():
                ring_step(r // every + 1, ring_d)

        store(hidden_v, hidden_out)
        store(value_v, value_out)
        store(slope_v, slope_out)
        collect.finish()
        ready = 0
        edge = n // 2 * BLOCK
        last = [
            Collect(dp, tp, n_tp, micro, rows, back_v, got_v, own_v, send, recv, columns)
            for send, recv, columns in (
                (last_send, last_recv, (0, edge)),
                (end_send, end_recv, (edge, width - edge)),
            )
        ]
        begun = False
        for s in range(inside_loop, n):
            if s > inside_loop:
                ring_step(s, ring_d)
            for _ in range(2 if s < n - 1 else n):
                if ready <= s and ready < n:
                    times_block(hidden_v, wd_v, ready)
                    ready += 1
            if ready >= n // 2 and not begun:
                begun = True
                for m in range(micro):
                    last[0].start(bits[0], m)
        store(wd_v, whole_outs[7])
        for m in range(micro):
            last[1].start(bits[0], m)
        for at, bit in enumerate(bits[:-1]):
            for part in last:
                for m in range(micro):
                    part.add(bit, m)
                    if at + 2 < len(bits):
                        part.start(bits[at + 1], m)
        store(own_v, near_out)
        for m in range(micro):
            store(
                back_v.at[pl.ds(m * window + bits[-1] * rows, rows)],
                far_out.at[pl.ds(m * rows, rows)],
            )
        for part in last:
            part.finish(bits[:-1])
        for i in range(n - 1):
            for p in range(0 if i > 0 else 2, len(pieces)):
                hop(i, p, 0).wait_send()
                hop(i, p, 1).wait_send()
        share.finish()
        for bit in bits:
            for copy in cot_copies(bit):
                copy.wait_send()
        for at, copy in enumerate(stores):
            if at not in waited:
                copy.wait()

    waited = (0, micro + 1)
    middle_part()


def forward(n, n_tp, x, cot, gains, cosine, sine, tables, weights):
    micro, rows, width = x.shape
    window = n_tp * rows
    total, mine = micro * window, micro * rows
    sizes = [w.shape[1] for w in weights[:2]] + [w.shape[0] for w in weights[2:]]
    hv, units = sizes[2], sizes[7]
    shape = jax.ShapeDtypeStruct
    dma = pltpu.SemaphoreType.DMA
    count = 4 + SPLIT + 2 + SPLIT
    return pl.pallas_call(
        functools.partial(forward_kernel, n, n_tp),
        out_shape=(
            shape((total, sizes[0]), BF),
            shape((total, sizes[1]), BF),
            shape((total, hv), BF),
            shape((total, sizes[3]), F32),
            shape((mine, width), F32),
            shape((mine, width), F32),
            shape((2, width), F32),
            shape((total, width), BF),
            shape((total, width), BF),
        )
        + tuple(shape((n, s, BLOCK), BF) for s in sizes)
        + (
            shape((total, hv), BF),
            shape((mine, width), F32),
            shape((total, width), BF),
            shape((total, units), BF),
            shape((total, units), BF),
            shape((total, units), BF),
            shape((mine, width), F32),
            shape((mine, width), BF),
        ),
        in_specs=[anyspec()] * 3 + [vmem()] * 5 + [anyspec()] * 8,
        out_specs=(anyspec(),) * 6 + (vmem(),) + (anyspec(),) * 18,
        scratch_shapes=[
            pltpu.VMEM((total, width), BF),
            pltpu.VMEM((mine, width), F32),
            pltpu.VMEM((mine, width), BF),
            pltpu.VMEM((n, 8, BLOCK), F32),
            pltpu.VMEM((total, sizes[0]), BF),
            pltpu.VMEM((total, sizes[1]), BF),
            pltpu.VMEM((total, hv), BF),
            pltpu.VMEM((total, sizes[3]), F32),
            pltpu.VMEM((tables[2].shape[0], window, window), F32),
            pltpu.VMEM((n_tp - 1, mine, width), BF),
        ]
        + [pltpu.VMEM((n, s, BLOCK), BF) for s in sizes[4:]]
        + [pltpu.VMEM((micro, rows, width), F32)]
        + [pltpu.VMEM((total, s), F32) for s in sizes[:3]]
        + [pltpu.VMEM((SLOTS, s, BLOCK), BF) for s in sizes[:4]]
        + [
            pltpu.VMEM((total, width), BF),
            pltpu.VMEM((mine, width), F32),
            pltpu.VMEM((total, hv), BF),
            pltpu.VMEM((total, units), BF),
            pltpu.VMEM((total, units), BF),
            pltpu.VMEM((total, units), BF),
            pltpu.VMEM((256, units), F32),
        ]
        + [dma((n - 1, count, 2))] * 2
        + [dma((n,))] * 2
        + [dma((micro, n_tp))] * 6
        + [dma((n_tp - 1, micro))] * 6
        + [dma((SLOTS + 1, 4)), dma((8,)), dma((19 + micro,))],
        compiler_params=pltpu.CompilerParams(
            collective_id=1, has_side_effects=True, vmem_limit_bytes=66_500_000
        ),
        cost_estimate=pl.CostEstimate(
            flops=2 * total * width * sum(sizes), bytes_accessed=120_000_000, transcendentals=0
        ),
        name="forward_kernel",
    )(x, cot, gains, cosine, sine, *tables, *weights)


class LaneRing:
    def __init__(self, n, tp, cw, ccw, lanes, fresh, free, soon, done):
        self.n, self.tp, self.ways, self.lanes = n, tp, (cw, ccw), lanes
        self.fresh, self.free, self.soon, self.done = fresh, free, soon, done
        self.state = [dict(job=0, step=1, firsts=0, ready=False) for _ in lanes]
        self.allowed = [0 for _ in lanes]

    def hop(self, p, t):
        lane = self.lanes[p]
        size = lane["jobs"][t // (self.n - 1)][0]
        slots = lane["recv"].shape[0]
        copies = []
        for side in range(2):
            lanes = pl.ds(side * LANE, LANE)
            copies.append(
                pltpu.make_async_remote_copy(
                    src_ref=lane["send"].at[t % 2, pl.ds(0, size), lanes],
                    dst_ref=lane["recv"].at[t % slots, pl.ds(0, size), lanes],
                    send_sem=lane["send_sem"].at[t, side],
                    recv_sem=lane["recv_sem"].at[t, side],
                    device_id=(self.ways[side], self.tp),
                    device_id_type=MESH,
                )
            )
        return copies

    def post(self, p, t, total):
        lane = self.lanes[p]
        slots = lane["recv"].shape[0]
        if t >= 2:
            for copy in self.hop(p, t - 2):
                copy.wait_send()
        lane["send"][t % 2, pl.ds(0, total.shape[0]), :] = total.astype(BF)
        for side, copy in enumerate(self.hop(p, t)):
            if t >= slots:
                pl.semaphore_wait(self.free.at[p, side], 1)
            copy.start()

    def first(self, p):
        lane, state = self.lanes[p], self.state[p]
        job = state["firsts"]
        size, gradient, _ = lane["jobs"][job]
        state["firsts"] += 1
        gradient(1 % self.n, self.fresh.at[pl.ds(0, size)])
        self.post(p, job * (self.n - 1), self.fresh[pl.ds(0, size), :])

    def prepare(self):
        for p, lane in enumerate(self.lanes):
            state = self.state[p]
            if state["job"] < state["firsts"] and not state["ready"]:
                size, gradient, _ = lane["jobs"][state["job"]]
                gradient((state["step"] + 1) % self.n, lane["part"].at[pl.ds(0, size)])
                state["ready"] = True

    def advance(self, only=(0, 1)):
        n = self.n
        self.prepare()
        for p in only:
            lane = self.lanes[p]
            state = self.state[p]
            job, step = state["job"], state["step"]
            count = len(lane["jobs"])
            if job >= state["firsts"]:
                if job < min(count, self.allowed[p]):
                    self.first(p)
                continue
            if step == n - 1 and state["firsts"] == job + 1 < min(count, self.allowed[p]):
                self.first(p)
            size, _, out = lane["jobs"][job]
            t = job * (n - 1) + step - 1
            slots = lane["recv"].shape[0]
            for copy in self.hop(p, t):
                copy.wait_recv()
            total = lane["part"][pl.ds(0, size), :] + lane["recv"][
                t % slots, pl.ds(0, size), :
            ].astype(F32)
            state["ready"] = False
            if step == n - 1:
                self.done(p, job, total, out)
                state["job"], state["step"] = job + 1, 1
            if t + slots < count * (n - 1):
                for side in range(2):
                    pl.semaphore_signal(
                        self.free.at[p, side],
                        inc=1,
                        device_id=(self.ways[1 - side], self.tp),
                        device_id_type=MESH,
                    )
            if step < n - 1:
                self.post(p, t + 1, total)
                state["step"] = step + 1
                if step == n - 2:
                    self.soon(p, out)

    def busy(self):
        return any(s["job"] < len(lane["jobs"]) for s, lane in zip(self.state, self.lanes))

    def finish(self):
        for p, lane in enumerate(self.lanes):
            last = len(lane["jobs"]) * (self.n - 1)
            for t in range(max(0, last - 2), last):
                for copy in self.hop(p, t):
                    copy.wait_send()


def backward_kernel(
    n,
    n_tp,
    gain_ref,
    own_gain_ref,
    col_ref,
    row_ref,
    rate_ref,
    cos_ref,
    sin_ref,
    *refs,
):
    hidden_ref, cot_ref, value_ref, slope_ref, second_ref, middle_ref, cotf_ref = refs[:7]
    q_ref, k_ref, v_ref, g_ref, gated_ref, nall_ref, x_ref = refs[7:14]
    wq_ref, wk_ref, wv_ref, wg_ref, wo_ref, wu_ref, wl_ref, wd_ref = refs[14:22]
    refs = refs[22:]
    dd_out, du_out, dl_out, do_out, ds_out, dv_out, dq_out, dk_out, sum_out, rows_out = refs[:10]
    cot_v, w_v, gu_v, gl_v, hidden_v, second_v, wu_s, wl_s, middle_v, cotf_v = refs[10:20]
    q_v, k_v, v_v, g_v, gs_v, gated_v, decay_v, gk_acc, gv_acc = refs[20:29]
    back_v, own_v, got_v, mall_v, rows_v, part0, part1, fresh_v = refs[29:37]
    send0, send1, recv0, recv1, done_v, own_w, sum_v = refs[37:44]
    ring_send0, ring_send1, ring_recv0, ring_recv1, ring_free = refs[44:49]
    part_send, part_recv, last_send, last_recv, share_send, share_recv = refs[49:55]
    sum_send, sum_recv, load_sem, done_sem, own_sem, local_sem = refs[55:]

    total, width = cot_v.shape
    mine = own_v.shape[0]
    window = col_ref.shape[0]
    micro = total // window
    rows = mine // micro
    heads = decay_v.shape[0]
    dp, tp, cw, ccw = neighbours(n)
    pos = ring_position(dp, n)
    bits = bits_of(n_tp)
    tile = 256
    half = HK // 2
    greet([(cw, tp), (ccw, tp)] + [(dp, partner(tp, bit)) for bit in bits])

    pairs = (
        (hidden_ref, hidden_v),
        (cot_ref, cot_v),
        (wd_ref, w_v),
        (value_ref, gu_v),
        (slope_ref, gl_v),
        (second_ref, second_v),
        (middle_ref, middle_v),
        (cotf_ref, cotf_v),
        (q_ref, q_v),
        (k_ref, k_v),
        (v_ref, v_v),
        (g_ref, g_v),
    )
    loads = [
        pltpu.make_async_copy(source, target, local_sem.at[at])
        for at, (source, target) in enumerate(pairs)
    ]
    for copy in loads[:2]:
        copy.start()

    def block_load(i, a):
        source, target = ((wu_ref, wu_s), (wl_ref, wl_s))[a]
        return pltpu.make_async_copy(
            source.at[i % n], target.at[i % 2], load_sem.at[i % 2, a]
        )

    def product(left, right):
        def gradient(i, target):
            target[...] = tn(left[...], right[:, pl.ds(i * BLOCK, BLOCK)])

        return gradient

    units, hv, hk = gu_v.shape[1], v_v.shape[1], q_v.shape[1]
    lanes = (
        dict(
            jobs=(
                (units, product(hidden_v, cot_v), (dd_out, None)),
                (units, product(gl_v, second_v), (dl_out, wl_ref)),
                (hv, product(gs_v, cot_v), (ds_out, wg_ref)),
                (hk, product(q_v, cot_v), (dq_out, wq_ref)),
            ),
            part=part0,
            send=send0,
            recv=recv0,
            send_sem=ring_send0,
            recv_sem=ring_recv0,
        ),
        dict(
            jobs=(
                (units, product(gu_v, second_v), (du_out, wu_ref)),
                (hv, product(hidden_v, mall_v), (do_out, None)),
                (hv, product(v_v, cot_v), (dv_out, wv_ref)),
                (hk, product(k_v, cot_v), (dk_out, wk_ref)),
            ),
            part=part1,
            send=send1,
            recv=recv1,
            send_sem=ring_send1,
            recv_sem=ring_recv1,
        ),
    )
    pending = {}

    def own_copy(p, weight):
        held = own_w.at[p, pl.ds(0, weight.shape[1])]
        return pltpu.make_async_copy(weight.at[0], held, own_sem.at[p])

    def soon(p, out):
        if out[1] is not None:
            own_copy(p, out[1]).start()

    def done(p, job, result, out):
        target, weight = out
        size = result.shape[0]
        if p in pending:
            pending.pop(p).wait()
        done_v[p, pl.ds(0, size), :] = result
        pending[p] = pltpu.make_async_copy(
            done_v.at[p, pl.ds(0, size)], target, done_sem.at[p]
        )
        pending[p].start()
        if weight is not None:
            own_copy(p, weight).wait()
            line = jnp.sum(
                own_w[p, pl.ds(0, size), :].astype(F32) * done_v[p, pl.ds(0, size), :],
                axis=0,
                keepdims=True,
            )
            at = 1 if job < 2 else 0
            sum_v[0, at : at + 1, :] = sum_v[0, at : at + 1, :] + line

    sum_v[...] = jnp.zeros_like(sum_v)
    ring = LaneRing(n, tp, cw, ccw, lanes, fresh_v, ring_free, soon, done)
    loads[0].wait()
    loads[1].wait()
    for copy in loads[2:5]:
        copy.start()
    ring.allowed = [1, 0]
    ring.first(0)
    for copy in loads[2:5]:
        copy.wait()
    block_load(0, 0).start()
    block_load(0, 1).start()
    for copy in loads[5:]:
        copy.start()

    @pl.loop(0, total // tile)
    def _(r):
        here = pl.ds(pl.multiple_of(r * tile, tile), tile)
        grad = None
        for i in range(n):
            term = nt(cot_v[here, pl.ds(i * BLOCK, BLOCK)], w_v[i])
            grad = term if grad is None else grad + term
        gu_v[here, :] = (grad * gu_v[here, :].astype(F32)).astype(BF)
        gl_v[here, :] = (grad * gl_v[here, :].astype(F32)).astype(BF)

    wo_load = pltpu.make_async_copy(wo_ref, w_v, local_sem.at[2])
    wo_load.start()
    ring.advance((0,))
    loads[5].wait()
    ring.allowed = [2, 1]
    ring.first(1)
    ring.prepare()
    collect = Collect(dp, tp, n_tp, micro, rows, back_v, got_v, own_v, part_send, part_recv)
    share = Share(dp, tp, n_tp, micro, rows, mall_v, share_send, share_recv)
    for m in range(micro):
        for i in range(n):
            at = m * n + i
            for a in range(2):
                block_load(at, a).wait()
                if at + 1 < micro * n:
                    block_load(at + 1, a).start()

            @pl.loop(0, window // tile)
            def _(r):
                here = pl.ds(pl.multiple_of(m * window + r * tile, tile), tile)
                back_v[here, pl.ds(i * BLOCK, BLOCK)] = (
                    nn(gu_v[here, :], wu_s[at % 2]) + nn(gl_v[here, :], wl_s[at % 2])
                ).astype(BF)

        collect.start(bits[0], m)
        ring.advance()
        ring.prepare()
    for at, bit in enumerate(bits[:-1]):
        for m in range(micro):
            collect.add(bit, m)
            collect.start(bits[at + 1], m)
    fill_decay(decay_v, col_ref, row_ref, rate_ref)
    loads[6].wait()
    loads[7].wait()
    for m in range(micro):
        ring.advance()
        ring.prepare()
        collect.add(bits[-1], m)

        @pl.loop(0, rows // STEP)
        def _(r):
            inner = pl.multiple_of(r * STEP, STEP)
            here = pl.ds(pl.multiple_of(m * rows + inner, STEP), STEP)
            there = pl.ds(pl.multiple_of(m * window + inner, STEP), STEP)
            middle = middle_v[here, :]
            scale = lax.rsqrt(jnp.mean(middle * middle, axis=-1, keepdims=True) + EPS)
            scaled = own_v[here, :] * gain_ref[1:2, :]
            inside = jnp.mean(scaled * middle, axis=-1, keepdims=True)
            grad = cotf_v[here, :] + scale * (scaled - middle * (scale * scale * inside))
            cotf_v[here, :] = grad
            mall_v[there, :] = grad.astype(BF)

        share.begin(m)
    x_load = pltpu.make_async_copy(x_ref, middle_v, local_sem.at[6])
    x_load.start()
    collect.finish()
    ring.advance()
    ring.prepare()
    for copy in loads[8:]:
        copy.wait()
    wo_load.wait()
    gated_load = None
    for m in range(micro):
        share.relay(m)
        if m == micro - 1 and gated_load is not None:
            gated_load.wait()
            ring.allowed = [2, 2]
        ring.advance()
        ring.prepare()
        for h in range(heads):
            keys = pl.ds(h * HK, HK)
            values = pl.ds(h * HV, HV)
            inside = pl.ds(m * window, window)
            gk_acc[...] = jnp.zeros_like(gk_acc)
            gv_acc[...] = jnp.zeros_like(gv_acc)

            @pl.loop(0, window // tile)
            def _(r):
                at = pl.multiple_of(r * tile, tile)
                here = pl.ds(pl.multiple_of(m * window + at, tile), tile)
                grad = None
                for i in range(n):
                    term = nt(mall_v[here, pl.ds(i * BLOCK, BLOCK)], w_v[i, values, :])
                    grad = term if grad is None else grad + term
                gated_v[pl.ds(at, tile), :] = grad

            @pl.loop(0, window // tile)
            def _(r):
                at = pl.multiple_of(r * tile, tile)
                local = pl.ds(at, tile)
                here = pl.ds(pl.multiple_of(m * window + at, tile), tile)
                decay = decay_v[h, local, :]
                query = q_v[here, keys]
                weight = (nt(query, k_v[inside, keys]) * decay).astype(BF)
                kept = nn(weight, v_v[inside, values])
                group = lax.rsqrt(jnp.mean(kept * kept, axis=-1, keepdims=True) + GROUP_EPS)
                gate = g_v[here, values]
                sigmoid = jax.nn.sigmoid(gate)
                grad = gated_v[local, :]
                gs_v[here, values] = (
                    grad * (kept * group) * (sigmoid * (1.0 + gate * (1.0 - sigmoid)))
                ).astype(BF)
                lifted = grad * (gate * sigmoid)
                mean = jnp.mean(lifted * kept, axis=-1, keepdims=True)
                grad_kept = (group * (lifted - kept * (group * group * mean))).astype(BF)
                gv_acc[...] += tn(weight, grad_kept)
                score = (nt(grad_kept, v_v[inside, values]) * decay).astype(BF)
                gk_acc[...] += tn(score, query)
                turned = nn(score, k_v[inside, keys])
                low, high = turned[:, :half], turned[:, half:]
                cosine, sine = cos_ref[local, :], sin_ref[local, :]
                q_v[here, pl.ds(h * HK, half)] = (low * cosine + high * sine).astype(BF)
                q_v[here, pl.ds(h * HK + half, half)] = (high * cosine - low * sine).astype(BF)

            low, high = gk_acc[:, :half], gk_acc[:, half:]
            cosine, sine = cos_ref[...], sin_ref[...]
            k_v[inside, pl.ds(h * HK, half)] = (low * cosine + high * sine).astype(BF)
            k_v[inside, pl.ds(h * HK + half, half)] = (high * cosine - low * sine).astype(BF)
            v_v[inside, values] = gv_acc[...].astype(BF)
            ring.advance()
            if ring.state[0]["job"] > 0 and gated_load is None:
                gated_load = pltpu.make_async_copy(gated_ref, hidden_v, local_sem.at[0])
                gated_load.start()
                nall_load = pltpu.make_async_copy(nall_ref, cot_v, local_sem.at[1])
                nall_load.start()
            ring.prepare()

    def settle():
        while ring.state[0]["job"] == 0:
            ring.advance()

    if gated_load is None:
        settle()
        gated_load = pltpu.make_async_copy(gated_ref, hidden_v, local_sem.at[0])
        gated_load.start()
        nall_load = pltpu.make_async_copy(nall_ref, cot_v, local_sem.at[1])
        nall_load.start()
    if ring.allowed[1] < 2:
        gated_load.wait()
    nall_load.wait()
    ring.allowed = [4, 4]

    wholes = (wq_ref, wk_ref, wv_ref, wg_ref)
    grads = (q_v, k_v, v_v, gs_v)
    sizes = (hk, hk, hv, hv)

    def weight_slot(i, a):
        return w_v.at[2 * a + i % 2, pl.ds(0, sizes[a])]

    def weight_load(i, a):
        return pltpu.make_async_copy(
            wholes[a].at[i], weight_slot(i, a), load_sem.at[2 + i % 2, a]
        )

    for a in range(4):
        weight_load(0, a).start()
    ring.advance()
    ring.prepare()
    for i in range(n):
        for a in range(4):
            weight_load(i, a).wait()
            if i + 1 < n:
                weight_load(i + 1, a).start()

        @pl.loop(0, total // tile)
        def _(r):
            here = pl.ds(pl.multiple_of(r * tile, tile), tile)
            block = None
            for a in range(4):
                term = nn(grads[a][here, :], weight_slot(i, a)[...])
                block = term if block is None else block + term
            back_v[here, pl.ds(i * BLOCK, BLOCK)] = block.astype(BF)

        if i % 2 == 1:
            ring.advance()
            ring.prepare()
    last = Collect(dp, tp, n_tp, micro, rows, back_v, got_v, own_v, last_send, last_recv)
    for m in range(micro):
        last.start(bits[0], m)
    ring.advance()
    ring.prepare()
    for at, bit in enumerate(bits):
        for m in range(micro):
            last.add(bit, m)
            if at + 1 < len(bits):
                last.start(bits[at + 1], m)
        if at + 1 < len(bits):
            for _ in range(3):
                ring.advance()
                ring.prepare()
    x_load.wait()

    def natural(i, side):
        at = ring_index((pos + (n - i if side == 0 else i)) % n, n) * BLOCK + side * LANE
        return pl.ds(pl.multiple_of(at, LANE), LANE)

    @pl.loop(0, mine // STEP)
    def _(r):
        at = pl.multiple_of(r * STEP, STEP)
        m, inner = at // rows, pl.multiple_of(at % rows, STEP)
        here = pl.ds(at, STEP)
        x = middle_v[here, :]
        scale = lax.rsqrt(jnp.mean(x * x, axis=-1, keepdims=True) + EPS)
        inside = jnp.mean(own_v[here, :] * gain_ref[0:1, :] * x, axis=-1, keepdims=True)
        slope = scale * scale * inside
        for i in range(n):
            for side in range(2):
                lanes = pl.ds(i * BLOCK + side * LANE, LANE)
                scaled = own_v[here, lanes] * gain_ref[0:1, lanes]
                rows_v[m, pl.ds(inner, STEP), natural(i, side)] = cotf_v[
                    here, lanes
                ] + scale * (scaled - middle_v[here, lanes] * slope)

    rows_copy = pltpu.make_async_copy(rows_v, rows_out, local_sem.at[2])
    rows_copy.start()
    while ring.busy():
        ring.advance()
        ring.prepare()
    for at, bit in enumerate(bits):
        swap = pltpu.make_async_remote_copy(
            src_ref=sum_v.at[2 * at],
            dst_ref=sum_v.at[2 * at + 1],
            send_sem=sum_send.at[at],
            recv_sem=sum_recv.at[at],
            device_id=(dp, partner(tp, bit)),
            device_id_type=MESH,
        )
        swap.start()
        swap.wait()
        sum_v[2 * at + 2] = sum_v[2 * at] + sum_v[2 * at + 1]
    sum_out[...] = sum_v[2 * len(bits)] / own_gain_ref[...]
    ring.finish()
    share.finish()
    last.finish()
    rows_copy.wait()
    for copy in pending.values():
        copy.wait()


def backward(n, n_tp, rows, gain, own_gain, tables, cosine, sine, arrays, weights):
    total, width = arrays[1].shape
    mine = arrays[5].shape[0]
    units, hk, hv = arrays[0].shape[1], arrays[7].shape[1], arrays[9].shape[1]
    heads = tables[2].shape[0]
    window = tables[0].shape[0]
    micro = total // window
    tall = max(units, hv, hk)
    hops = 4 * (n - 1)
    count = len(bits_of(n_tp))
    shape = jax.ShapeDtypeStruct
    dma = pltpu.SemaphoreType.DMA
    sizes = (units, units, units, hv, hv, hv, hk, hk)
    return pl.pallas_call(
        functools.partial(backward_kernel, n, n_tp),
        out_shape=tuple(shape((s, BLOCK), F32) for s in sizes)
        + (shape((8, BLOCK), F32), shape((micro, rows, width), F32)),
        in_specs=[vmem()] * 7 + [anyspec()] * 22,
        out_specs=(anyspec(),) * 8 + (vmem(), anyspec()),
        scratch_shapes=[
            pltpu.VMEM((total, width), BF),
            pltpu.VMEM((n, tall, BLOCK), BF),
            pltpu.VMEM((total, units), BF),
            pltpu.VMEM((total, units), BF),
            pltpu.VMEM((total, units), BF),
            pltpu.VMEM((total, width), BF),
            pltpu.VMEM((2, units, BLOCK), BF),
            pltpu.VMEM((2, units, BLOCK), BF),
            pltpu.VMEM((mine, width), F32),
            pltpu.VMEM((mine, width), F32),
            pltpu.VMEM((total, hk), BF),
            pltpu.VMEM((total, hk), BF),
            pltpu.VMEM((total, hv), BF),
            pltpu.VMEM((total, hv), F32),
            pltpu.VMEM((total, hv), BF),
            pltpu.VMEM((window, HV), F32),
            pltpu.VMEM((heads, window, window), F32),
            pltpu.VMEM((window, HK), F32),
            pltpu.VMEM((window, HV), F32),
            pltpu.VMEM((total, width), BF),
            pltpu.VMEM((mine, width), F32),
            pltpu.VMEM((n_tp - 1, mine, width), BF),
            pltpu.VMEM((total, width), BF),
            pltpu.VMEM((micro, rows, width), F32),
            pltpu.VMEM((tall, BLOCK), F32),
            pltpu.VMEM((tall, BLOCK), F32),
            pltpu.VMEM((tall, BLOCK), F32),
            pltpu.VMEM((2, tall, BLOCK), BF),
            pltpu.VMEM((2, tall, BLOCK), BF),
            pltpu.VMEM((2, tall, BLOCK), BF),
            pltpu.VMEM((2, tall, BLOCK), BF),
            pltpu.VMEM((2, tall, BLOCK), F32),
            pltpu.VMEM((2, tall, BLOCK), BF),
            pltpu.VMEM((2 * count + 1, 8, BLOCK), F32),
        ]
        + [dma((hops, 2))] * 4
        + [pltpu.SemaphoreType.REGULAR((2, 2))]
        + [dma((n_tp - 1, micro))] * 4
        + [dma((micro, n_tp))] * 2
        + [dma((count,))] * 2
        + [dma((4, 4)), dma((2,)), dma((2,)), dma((12,))],
        compiler_params=pltpu.CompilerParams(
            collective_id=2, has_side_effects=True, vmem_limit_bytes=67_000_000
        ),
        cost_estimate=pl.CostEstimate(
            flops=4 * total * width * sum(sizes), bytes_accessed=120_000_000, transcendentals=0
        ),
        name="backward_kernel",
    )(gain, own_gain, *tables, cosine, sine, *arrays, *weights)


def finish_kernel(
    n,
    n_tp,
    passed,
    turned,
    *refs,
):
    sources = refs[: passed + turned]
    middle_ref, near_ref, far_ref = refs[passed + turned : passed + turned + 3]
    targets = refs[passed + turned + 3 : 2 * (passed + turned) + 3]
    block_out = refs[2 * (passed + turned) + 3]
    scratch = refs[2 * (passed + turned) + 4 :]
    held, (middle_v, near_v, far_v, block_v), (sem_in, sem_out) = (
        scratch[: passed + 2 * turned],
        scratch[passed + 2 * turned : passed + 2 * turned + 4],
        scratch[passed + 2 * turned + 4 :],
    )
    micro, rows, width = block_v.shape
    pos = ring_position(lax.axis_index("dp"), n)
    count = passed + turned
    ins = [
        pltpu.make_async_copy(sources[i], held[i], sem_in.at[i]) for i in range(count)
    ] + [
        pltpu.make_async_copy(source, target, sem_in.at[count + i])
        for i, (source, target) in enumerate(
            ((middle_ref, middle_v), (near_ref, near_v), (far_ref, far_v))
        )
    ]
    for copy in ins[count:] + ins[:count]:
        copy.start()
    results = list(held[:passed]) + list(held[count:])
    outs = [pltpu.make_async_copy(results[i], targets[i], sem_out.at[i]) for i in range(count)]
    outs.append(pltpu.make_async_copy(block_v, block_out, sem_out.at[count]))
    for copy in ins[count:]:
        copy.wait()

    @pl.loop(0, micro * rows // STEP)
    def _(r):
        at = pl.multiple_of(r * STEP, STEP)
        m, inner = at // rows, pl.multiple_of(at % rows, STEP)
        here = pl.ds(at, STEP)
        for i in range(n):
            for side in range(2):
                lanes = pl.ds(i * BLOCK + side * LANE, LANE)
                spot = ring_index((pos + (n - i if side == 0 else i)) % n, n)
                there = pl.ds(pl.multiple_of(spot * BLOCK + side * LANE, LANE), LANE)
                block_v[m, pl.ds(inner, STEP), there] = middle_v[here, lanes] + (
                    near_v[here, lanes] + far_v[here, lanes].astype(F32)
                )

    outs[count].start()
    for i in range(passed):
        ins[i].wait()
        outs[i].start()
    for i in range(turned):
        ins[passed + i].wait()
        held[count + i][...] = held[passed + i][...].T
        outs[passed + i].start()
    for copy in outs:
        copy.wait()


def finish(n, n_tp, passed, turned, middle, near, far, block_shape):
    shape = jax.ShapeDtypeStruct
    results = tuple(shape(a.shape, a.dtype) for a in passed) + tuple(
        shape(a.shape[::-1], a.dtype) for a in turned
    )
    count = len(passed) + len(turned)
    return pl.pallas_call(
        functools.partial(finish_kernel, n, n_tp, len(passed), len(turned)),
        out_shape=results + (shape(block_shape, F32),),
        in_specs=[anyspec()] * (count + 3),
        out_specs=(anyspec(),) * (count + 1),
        scratch_shapes=[pltpu.VMEM(a.shape, a.dtype) for a in passed]
        + [pltpu.VMEM(a.shape, a.dtype) for a in turned]
        + [pltpu.VMEM(a.shape[::-1], a.dtype) for a in turned]
        + [
            pltpu.VMEM(middle.shape, F32),
            pltpu.VMEM(near.shape, F32),
            pltpu.VMEM(far.shape, BF),
            pltpu.VMEM(block_shape, F32),
            pltpu.SemaphoreType.DMA((count + 3,)),
            pltpu.SemaphoreType.DMA((count + 1,)),
        ],
        compiler_params=pltpu.CompilerParams(vmem_limit_bytes=66_000_000),
        name="finish_kernel",
    )(*passed, *turned, middle, near, far)


def normalize(row_block, gain_vec):
    row_scale = lax.rsqrt(jnp.mean(row_block * row_block, axis=-1, keepdims=True) + EPS)
    return (row_block * row_scale * gain_vec.astype(jnp.float32), row_scale)


def norm_back(grad_rows, row_block, row_scale, gain_vec):
    scaled_grad = grad_rows * gain_vec.astype(jnp.float32)
    back_rows = row_scale * (
        scaled_grad
        - row_block
        * row_scale
        * row_scale
        * jnp.mean(scaled_grad * row_block, axis=-1, keepdims=True)
    )
    return (back_rows, jnp.sum(grad_rows * row_block * row_scale, axis=0))


def angles(length, feature_width):
    half_width = feature_width // 2
    frequency = jnp.exp(-math.log(10000.0) * jnp.arange(half_width, dtype=jnp.float32) / half_width)
    turns = jnp.arange(length, dtype=jnp.float32)[:, None] * frequency[None, :]
    return (jnp.cos(turns)[:, None, :], jnp.sin(turns)[:, None, :])


def decays(length, head_ids):
    places = jnp.arange(length, dtype=jnp.float32)
    spacing = places[:, None] - places[None, :]
    log_rate = jnp.log(1.0 - jnp.exp2(-5.0 - head_ids))
    return jnp.where(
        spacing[None] >= 0.0,
        jnp.exp(jnp.maximum(spacing, 0.0)[None] * log_rate[:, None, None]),
        0.0,
    )


def rotate(value_vectors, cosine_table, sine_table):
    half_width = value_vectors.shape[-1] // 2
    lower = value_vectors[..., :half_width]
    upper = value_vectors[..., half_width:]
    return jnp.concatenate(
        [lower * cosine_table - upper * sine_table, upper * cosine_table + lower * sine_table],
        axis=-1,
    )


def unrotate(value_vectors, cosine_table, sine_table):
    half_width = value_vectors.shape[-1] // 2
    lower = value_vectors[..., :half_width]
    upper = value_vectors[..., half_width:]
    return jnp.concatenate(
        [lower * cosine_table + upper * sine_table, upper * cosine_table - lower * sine_table],
        axis=-1,
    )


def plain_gelu_parts(pre_act):
    normal_cdf = 0.5 * (1.0 + lax.erf(pre_act * (1.0 / math.sqrt(2.0))))
    density = jnp.exp(-0.5 * pre_act * pre_act) * (1.0 / math.sqrt(2.0 * math.pi))
    return (pre_act * normal_cdf, normal_cdf + pre_act * density)


def inner_rows(left_rows, right_rows):
    return lax.dot_general(
        left_rows, right_rows, (((0,), (0,)), ((), ())), preferred_element_type=jnp.float32
    )


def times_t(left_rows, right_rows):
    return lax.dot_general(
        left_rows, right_rows, (((1,), (1,)), ((), ())), preferred_element_type=jnp.float32
    )


def forward_pass(rows_in, gathered, cosine_table, sine_table, decay_mask):
    (
        first_gain,
        second_gain,
        query_weight,
        key_weight,
        value_weight,
        swish_weight,
        output_weight,
        up_projection_matrix,
        gelu_weight,
        down_weight,
    ) = gathered
    local_heads = decay_mask.shape[0]
    scale_qk = 1.0 / math.sqrt(HK)
    normed, first_scale = normalize(rows_in, first_gain)
    normed_all = lax.all_gather(normed.astype(jnp.bfloat16), "tensor", axis=0, tiled=True)
    total_rows = normed_all.shape[0]
    sequences = total_rows // LEN
    query_turned_rows = rotate(
        jnp.dot(normed_all, query_weight, preferred_element_type=jnp.float32).reshape(
            sequences, LEN, local_heads, HK
        ),
        cosine_table,
        sine_table,
    ).astype(jnp.bfloat16)
    key_turned_rows = rotate(
        jnp.dot(normed_all, key_weight, preferred_element_type=jnp.float32).reshape(
            sequences, LEN, local_heads, HK
        ),
        cosine_table,
        sine_table,
    ).astype(jnp.bfloat16)
    value_rows = (
        jnp.dot(normed_all, value_weight, preferred_element_type=jnp.float32)
        .astype(jnp.bfloat16)
        .reshape(sequences, LEN, local_heads, HV)
    )
    gate_pre = jnp.dot(normed_all, swish_weight, preferred_element_type=jnp.float32)
    unscaled_logits = jnp.einsum(
        "snhd,smhd->shnm", query_turned_rows, key_turned_rows, preferred_element_type=jnp.float32
    )
    weight_bf = (unscaled_logits * (decay_mask * scale_qk)).astype(jnp.bfloat16)
    retained = jnp.einsum(
        "shnm,smhe->snhe", weight_bf, value_rows, preferred_element_type=jnp.float32
    )
    group_scale = lax.rsqrt(jnp.mean(retained * retained, axis=-1, keepdims=True) + GROUP_EPS)
    grouped = (retained * group_scale).reshape(total_rows, local_heads * HV)
    sigmoid_gate = jax.nn.sigmoid(gate_pre)
    swish_val = gate_pre * sigmoid_gate
    gated_rows = (swish_val * grouped).astype(jnp.bfloat16)
    attention = lax.psum_scatter(
        jnp.dot(gated_rows, output_weight, preferred_element_type=jnp.float32),
        "tensor",
        scatter_dimension=0,
        tiled=True,
    )
    middle = rows_in + attention
    second, second_scale = normalize(middle, second_gain)
    second_all = lax.all_gather(second.astype(jnp.bfloat16), "tensor", axis=0, tiled=True)
    up_pre = jnp.dot(second_all, up_projection_matrix, preferred_element_type=jnp.float32)
    gelu_pre = jnp.dot(second_all, gelu_weight, preferred_element_type=jnp.float32)
    gelu_val, gelu_slope = plain_gelu_parts(gelu_pre)
    hidden = (gelu_val * up_pre).astype(jnp.bfloat16)
    block_rows = middle + lax.psum_scatter(
        jnp.dot(hidden, down_weight, preferred_element_type=jnp.float32).astype(jnp.bfloat16),
        "tensor",
        scatter_dimension=0,
        tiled=True,
    ).astype(jnp.float32)
    kept_state = (
        rows_in,
        first_scale,
        normed_all,
        query_turned_rows,
        key_turned_rows,
        value_rows,
        gate_pre,
        weight_bf,
        retained,
        group_scale,
        grouped,
        gated_rows,
        middle,
        second_scale,
        second_all,
        up_pre,
        gelu_val,
        gelu_slope,
        hidden,
    )
    return (block_rows, kept_state)


def backward_pass(kept_state, cot_in, gathered, cosine_table, sine_table, decay_mask):
    (
        first_gain,
        second_gain,
        query_weight,
        key_weight,
        value_weight,
        swish_weight,
        output_weight,
        up_projection_matrix,
        gelu_weight,
        down_weight,
    ) = gathered
    (
        rows_in,
        first_scale,
        normed_all,
        query_turned_rows,
        key_turned_rows,
        value_rows,
        gate_pre,
        weight_bf,
        retained,
        group_scale,
        grouped,
        gated_rows,
        middle,
        second_scale,
        second_all,
        up_pre,
        gelu_val,
        gelu_slope,
        hidden,
    ) = kept_state
    local_heads = decay_mask.shape[0]
    total_rows = normed_all.shape[0]
    scale_qk = 1.0 / math.sqrt(HK)
    cot_all = lax.all_gather(cot_in.astype(jnp.bfloat16), "tensor", axis=0, tiled=True)
    grad_hidden = times_t(cot_all, down_weight)
    grad_down = inner_rows(hidden, cot_all)
    grad_uppre = (grad_hidden * gelu_val).astype(jnp.bfloat16)
    grad_gelupre = (grad_hidden * up_pre * gelu_slope).astype(jnp.bfloat16)
    grad_up = inner_rows(second_all, grad_uppre)
    grad_gelu = inner_rows(second_all, grad_gelupre)
    second_back = lax.psum_scatter(
        times_t(grad_uppre, up_projection_matrix) + times_t(grad_gelupre, gelu_weight),
        "tensor",
        scatter_dimension=0,
        tiled=True,
    )
    middle_back, grad_gain_two = norm_back(second_back, middle, second_scale, second_gain)
    grad_middle = cot_in + middle_back
    middle_all = lax.all_gather(grad_middle.astype(jnp.bfloat16), "tensor", axis=0, tiled=True)
    grad_gated = times_t(middle_all, output_weight)
    grad_out = inner_rows(gated_rows, middle_all)
    sigmoid_gate = jax.nn.sigmoid(gate_pre)
    swish_val = gate_pre * sigmoid_gate
    grad_swishpre = (
        grad_gated * grouped * (sigmoid_gate * (1.0 + gate_pre * (1.0 - sigmoid_gate)))
    ).astype(jnp.bfloat16)
    grad_grouped = (grad_gated * swish_val).reshape(retained.shape)
    grad_retained = (
        group_scale
        * (
            grad_grouped
            - retained
            * group_scale
            * group_scale
            * jnp.mean(grad_grouped * retained, axis=-1, keepdims=True)
        )
    ).astype(jnp.bfloat16)
    grad_valrows = jnp.einsum(
        "shnm,snhe->smhe", weight_bf, grad_retained, preferred_element_type=jnp.float32
    ).astype(jnp.bfloat16)
    grad_weight = jnp.einsum(
        "snhe,smhe->shnm", grad_retained, value_rows, preferred_element_type=jnp.float32
    )
    grad_retention_logits = (grad_weight * (decay_mask * scale_qk)).astype(jnp.bfloat16)
    grad_query_rotated_rows = jnp.einsum(
        "shnm,smhd->snhd",
        grad_retention_logits,
        key_turned_rows,
        preferred_element_type=jnp.float32,
    )
    grad_key_rotated_rows = jnp.einsum(
        "shnm,snhd->smhd",
        grad_retention_logits,
        query_turned_rows,
        preferred_element_type=jnp.float32,
    )
    grad_qpre = (
        unrotate(grad_query_rotated_rows, cosine_table, sine_table)
        .astype(jnp.bfloat16)
        .reshape(total_rows, local_heads * HK)
    )
    grad_kpre = (
        unrotate(grad_key_rotated_rows, cosine_table, sine_table)
        .astype(jnp.bfloat16)
        .reshape(total_rows, local_heads * HK)
    )
    grad_vflat = grad_valrows.reshape(total_rows, local_heads * HV)
    first_back = lax.psum_scatter(
        times_t(grad_qpre, query_weight)
        + times_t(grad_kpre, key_weight)
        + times_t(grad_vflat, value_weight)
        + times_t(grad_swishpre, swish_weight),
        "tensor",
        scatter_dimension=0,
        tiled=True,
    )
    grad_query = inner_rows(normed_all, grad_qpre)
    grad_key = inner_rows(normed_all, grad_kpre)
    grad_value = inner_rows(normed_all, grad_vflat)
    grad_swish = inner_rows(normed_all, grad_swishpre)
    input_back, grad_gain_one = norm_back(first_back, rows_in, first_scale, first_gain)
    grad_rows = grad_middle + input_back
    pieces = (
        grad_gain_one,
        grad_gain_two,
        grad_query,
        grad_key,
        grad_value,
        grad_swish,
        grad_out,
        grad_up,
        grad_gelu,
        grad_down,
    )
    return (grad_rows, pieces)


def plain_body(
    block_input,
    cotangent,
    first_gain,
    second_gain,
    query_weight,
    key_weight,
    value_weight,
    swish_weight,
    output_weight,
    up_projection_matrix,
    gelu_weight,
    down_weight,
):
    local_heads = query_weight.shape[1] // HK
    head_ids = (lax.axis_index("tensor") * local_heads + jnp.arange(local_heads)).astype(
        jnp.float32
    )
    cosine_table, sine_table = angles(LEN, HK)
    decay_mask = decays(LEN, head_ids)
    output_list = []
    grad_list = []
    totals = ()
    for micro_idx in range(block_input.shape[0]):
        forward_set = (
            lax.all_gather(first_gain, "dp", axis=0, tiled=True),
            lax.all_gather(second_gain, "dp", axis=0, tiled=True),
            lax.all_gather(query_weight, "dp", axis=0, tiled=True),
            lax.all_gather(key_weight, "dp", axis=0, tiled=True),
            lax.all_gather(value_weight, "dp", axis=0, tiled=True),
            lax.all_gather(swish_weight, "dp", axis=0, tiled=True),
            lax.all_gather(output_weight, "dp", axis=1, tiled=True),
            lax.all_gather(up_projection_matrix, "dp", axis=0, tiled=True),
            lax.all_gather(gelu_weight, "dp", axis=0, tiled=True),
            lax.all_gather(down_weight, "dp", axis=1, tiled=True),
        )
        block_rows, kept_state = forward_pass(
            block_input[micro_idx], forward_set, cosine_table, sine_table, decay_mask
        )
        held = lax.optimization_barrier(
            (
                (
                    first_gain,
                    second_gain,
                    query_weight,
                    key_weight,
                    value_weight,
                    swish_weight,
                    output_weight,
                    up_projection_matrix,
                    gelu_weight,
                    down_weight,
                ),
                block_rows,
            )
        )[0]
        backward_set = (
            lax.all_gather(held[0], "dp", axis=0, tiled=True),
            lax.all_gather(held[1], "dp", axis=0, tiled=True),
            lax.all_gather(held[2], "dp", axis=0, tiled=True),
            lax.all_gather(held[3], "dp", axis=0, tiled=True),
            lax.all_gather(held[4], "dp", axis=0, tiled=True),
            lax.all_gather(held[5], "dp", axis=0, tiled=True),
            lax.all_gather(held[6], "dp", axis=1, tiled=True),
            lax.all_gather(held[7], "dp", axis=0, tiled=True),
            lax.all_gather(held[8], "dp", axis=0, tiled=True),
            lax.all_gather(held[9], "dp", axis=1, tiled=True),
        )
        grad_rows, pieces = backward_pass(
            kept_state, cotangent[micro_idx], backward_set, cosine_table, sine_table, decay_mask
        )
        output_list.append(block_rows)
        grad_list.append(grad_rows)
        if micro_idx == 0:
            totals = tuple(pieces)
        else:
            totals = tuple((total + piece for total, piece in zip(totals, pieces)))
    totals = (
        lax.psum_scatter(totals[0], "dp", scatter_dimension=0, tiled=True),
        lax.psum_scatter(totals[1], "dp", scatter_dimension=0, tiled=True),
        lax.psum_scatter(totals[2], "dp", scatter_dimension=0, tiled=True),
        lax.psum_scatter(totals[3], "dp", scatter_dimension=0, tiled=True),
        lax.psum_scatter(totals[4], "dp", scatter_dimension=0, tiled=True),
        lax.psum_scatter(totals[5], "dp", scatter_dimension=0, tiled=True),
        lax.psum_scatter(totals[6], "dp", scatter_dimension=1, tiled=True),
        lax.psum_scatter(totals[7], "dp", scatter_dimension=0, tiled=True),
        lax.psum_scatter(totals[8], "dp", scatter_dimension=0, tiled=True),
        lax.psum_scatter(totals[9], "dp", scatter_dimension=1, tiled=True),
    )
    gain_first, gain_second = lax.psum((totals[0], totals[1]), "tensor")
    return (
        jnp.stack(output_list, axis=0),
        jnp.stack(grad_list, axis=0),
        gain_first,
        gain_second,
        totals[2],
        totals[3],
        totals[4],
        totals[5],
        totals[6],
        totals[7],
        totals[8],
        totals[9],
    )


def ring_body(
    n_dp,
    n_tp,
    block_input,
    cotangent,
    first_gain,
    second_gain,
    query_weight,
    key_weight,
    value_weight,
    swish_weight,
    output_weight,
    up_projection_matrix,
    gelu_weight,
    down_weight,
):
    micro, rows, width = block_input.shape
    local_heads = query_weight.shape[1] // HK
    window = n_tp * rows

    me = lax.axis_index("tensor")
    head_ids = (me * local_heads + jnp.arange(local_heads)).astype(F32)
    chunk_of = jnp.arange(n_tp) ^ me
    natural = (chunk_of[:, None] * rows + jnp.arange(rows)[None, :]).reshape(window)
    place = (natural % LEN).astype(F32)
    half_key = HK // 2
    frequency = jnp.exp(-math.log(10000.0) * jnp.arange(half_key, dtype=F32) / half_key)
    turns = place[:, None] * frequency[None, :]
    cosine, sine = jnp.cos(turns), jnp.sin(turns)
    log_rate = jnp.log(1.0 - jnp.exp2(-5.0 - head_ids))
    spots = natural.astype(F32)
    tables = (
        jnp.broadcast_to(spots[:, None], (window, LANE)),
        spots[None, :],
        jnp.broadcast_to(log_rate[:, None], (local_heads, window)),
    )

    gains_own = jnp.stack([first_gain] + [second_gain] * 7).astype(F32)
    results = forward(
        n_dp,
        n_tp,
        block_input,
        cotangent,
        gains_own,
        cosine,
        sine,
        tables,
        (
            query_weight,
            key_weight,
            value_weight.T,
            swish_weight.T,
            output_weight,
            up_projection_matrix.T,
            gelu_weight.T,
            down_weight,
        ),
    )
    query, key, value, gate, x_rel, cot_rel, gains, normed, cot_all = results[:9]
    w_in, (w_o, w_u, w_l, w_d) = results[9:13], results[13:17]
    gated, middle, second, hidden, gelu_val, up_slope, near, far = results[17:]

    far = lax.ppermute(far, "tensor", [(i, i ^ (n_tp // 2)) for i in range(n_tp)])

    (
        grad_down,
        grad_up,
        grad_gelu,
        grad_out,
        grad_swish,
        grad_value,
        grad_query,
        grad_key,
        gain_grads,
        grad_rows,
    ) = backward(
        n_dp,
        n_tp,
        rows,
        gains,
        gains_own,
        tables,
        cosine,
        sine,
        (
            hidden,
            cot_all,
            gelu_val,
            up_slope,
            second,
            middle,
            cot_rel,
            query,
            key,
            value,
            gate,
            gated,
            normed,
            x_rel,
        ),
        (*w_in, w_o, w_u, w_l, w_d),
    )
    passed = (grad_value, grad_swish, grad_out, grad_up, grad_gelu, grad_down, grad_rows)
    *passed, grad_query, grad_key, block_rows = finish(
        n_dp, n_tp, passed, (grad_query, grad_key), middle, near, far, block_input.shape
    )
    grad_value, grad_swish, grad_out, grad_up, grad_gelu, grad_down, grad_rows = passed

    return (
        block_rows,
        grad_rows,
        gain_grads[0],
        gain_grads[1],
        grad_query,
        grad_key,
        grad_value.T,
        grad_swish.T,
        grad_out,
        grad_up.T,
        grad_gelu.T,
        grad_down,
    )


def solution(mesh):
    rows = P(None, ("dp", "tensor"), None)
    wide, tall, gain = P("dp", "tensor"), P("tensor", "dp"), P("dp")
    n_dp, n_tp = mesh.shape["dp"], mesh.shape["tensor"]

    def run(*arrays):
        blocks = arrays[2].shape[0] == BLOCK and n_dp % 2 == 0 and n_dp > 2
        pairs = n_tp > 1 and n_tp & (n_tp - 1) == 0
        aligned = (n_tp * arrays[0].shape[1]) % LEN == 0 and arrays[0].shape[1] % LANE == 0
        equal = arrays[6].shape[1] == arrays[9].shape[1] and arrays[6].shape[1] % STEP == 0
        if blocks and pairs and aligned and equal:
            return ring_body(n_dp, n_tp, *arrays)
        return plain_body(*arrays)

    return jax.shard_map(
        run,
        mesh=mesh,
        in_specs=(rows, rows, gain, gain) + (wide,) * 4 + (tall, wide, wide, tall),
        out_specs=(rows, rows, gain, gain) + (wide,) * 4 + (tall, wide, wide, tall),
        check_vma=False,
    )
```
